32 devices in a mesh: section: 2 (over core), dp: 16 (over z, y, x).
Axes of the slice: x: 2, y: 2, z: 4, core: 2. Of those that a mesh axis runs over, the one named last changes fastest.
Arguments:
- tokens: bfloat16 [2, 2048, 1536], P(None, 'dp'), may hold values from -6 to 6
- cotangent: bfloat16 [2, 2048, 1536], P(None, 'dp'), may hold values from -6 to 6
- lengths: int32 [2, 16, 4], P(None, 'dp'), may hold values from 1 to 64, 128 in all within a row
- routes: int32 [2, 2, 2048, 8], P('section', None, 'dp'), may hold values from 0 to 15, all different within a row; in each aligned block of 128 rows (0 to 127, 128 to 255, ..., all dimensions but the last counted through in order) at most 80 rows name the same one
- combined_weight: bfloat16 [2, 1536, 2560], P('section', 'dp'), may hold values from -0.15625 to 0.15625
- output_weight: bfloat16 [2, 1536, 1536], P('section', 'dp'), may hold values from -0.625 to 0.625
- router_weight: bfloat16 [2, 1536, 16], P('section', 'dp'), may hold values from -0.078125 to 0.078125
- attention_gain: bfloat16 [2, 1536], P('section', 'dp'), may hold values from 0.5 to 1.5
- mixture_gain: bfloat16 [2, 1536], P('section', 'dp'), may hold values from 0.5 to 1.5
- expert_gate_up: bfloat16 [2, 16, 1536, 1024], P('section', 'dp'), may hold values from -0.3125 to 0.3125
- expert_down: bfloat16 [2, 16, 512, 1536], P('section', 'dp'), may hold values from -0.5 to 0.5
Outputs:
- boundary: bfloat16 [2, 2, 2048, 1536], P('section', None, 'dp')
- joint_grad: float32 [2, 1536, 2560], P('section', 'dp')
- output_grad: float32 [2, 1536, 1536], P('section', 'dp')
- router_grad: float32 [2, 1536, 16], P('section', 'dp')
- attention_gain_grad: float32 [2, 1536], P('section', 'dp')
- mixture_gain_grad: float32 [2, 1536], P('section', 'dp')
- expert_gate_up_grad: float32 [2, 16, 1536, 1024], P('section', 'dp')
- expert_down_grad: float32 [2, 16, 512, 1536], P('section', 'dp')
The draws below stay inside these ranges and needn't reach their ends.
Inputs may be any that keep to these rules, and one draw needn't show every extreme that they name: Each row of 4 lengths fills the 128 rows of one device's micro-batch, and its longest sequence has 64 rows. `routes`: each token names 8 different experts; among the rows of one device in one micro-batch and layer no expert is named more than 80 times, a bound that some block reaches.
All inputs are finite; a program needn't handle non-finite values.
Results may differ from the reference program's by a relative error of at most 0.023.
Values may be sent and summed in bfloat16 or wider, within the bound.
A program may use at most 256 MiB of HBM per device.

```python
import math
import jax
import jax.numpy as jnp
import numpy as np
from jax import lax

MODEL_WIDTH = 1536
QUERY_HEADS = 24
KEY_VALUE_HEADS = 8
HEAD_SIZE = 64
FFE = 512
TOPK = 8
DEVICE_ROWS = 128
MB = 2
NSEQ = 4
SECTION_LAYERS = 2
EXPERTS = 16
TOKENS = 2048
SEQ_MAX = 64
CAP = 80
N_DP = 16


def steps_of(key, extent, cuts, low, largest):
    def one(position, parts):
        heights = jax.random.uniform(jax.random.fold_in(jax.random.fold_in(key, 6), position), (parts,), jnp.float32, low / len(cuts), largest / len(cuts))
        return jnp.repeat(jnp.exp(heights), extent[position] // parts).reshape((-1,) + (1,) * (len(extent) - position - 1))

    level = one(*cuts[0])
    for cut in cuts[1:]:
        level = level * one(*cut)
    return level


def profile(count, total, reach, skew):
    loads = [(1 << 20) // math.isqrt(standing ** skew) + 1 for standing in range(2, count + 1)]
    rest, given = total - reach - (count - 1), [1] * (count - 1)
    while rest > 0:
        movable = [i for i in range(count - 1) if given[i] < reach]
        mass, remaining = sum([loads[i] for i in movable]), rest
        for i in movable:
            extra = min(reach - given[i], max(1, remaining * loads[i] // mass), rest)
            given[i] = given[i] + extra
            rest = rest - extra
    return np.array([reach] + given)


def uneven(stream_key, count, total, bound, skew):
    if count == 2:
        one = jax.random.randint(stream_key, (), max(1, total - bound), min(bound, total - 1) + 1)
        return jnp.stack([one, total - one])
    tallies = jnp.asarray(profile(count, total, bound, skew), jnp.int32)
    couples = (count - 1) // 2
    giver, taker = tallies[1:1 + 2 * couples:2], tallies[2:2 + 2 * couples:2]
    room = jnp.minimum(giver - 1, bound - taker)
    shifted = jax.random.randint(jax.random.fold_in(stream_key, 1), (couples,), 0, 1 << 20) % (room + 1)
    tallies = tallies.at[1:1 + 2 * couples:2].set(giver - shifted).at[2:2 + 2 * couples:2].set(taker + shifted)
    return tallies[jax.random.permutation(jax.random.fold_in(stream_key, 2), count)]


def routed_block(own_key, own, number, rows, amount, top, bound, slope):
    order = jax.random.permutation(own_key, amount)
    heavy_load, ordinary = load_shares(amount, rows * top, bound, slope, True), load_shares(amount, rows * top, bound, slope, False)
    places = jnp.arange(amount)

    def named(sizes, rotation):
        used = int((sizes > 0).sum())
        fixed = max(1, used // 4)
        moved = fixed + (places - fixed + rotation * (used - fixed)) % max(1, amount - fixed)
        return jnp.zeros((amount,), jnp.int32).at[order[jnp.where(places < fixed, places, moved)]].set(jnp.asarray(sizes, jnp.int32))

    sizes = jnp.where(number % 4 == 0, named(heavy_load, number // 4), named(ordinary, number - number // 4 - 1))
    mixed = jax.random.permutation(jax.random.fold_in(own, 3), amount)
    donor, sink = mixed[0:amount // 2 * 2:2], mixed[1:amount // 2 * 2:2]
    margin = jnp.minimum(sizes[donor] - 1, bound - sizes[sink]) // 2
    margin = jnp.where((donor == order[0]) | (sink == order[0]) | (sizes[sink] == 0), 0, jnp.maximum(margin, 0))
    moved = jax.random.randint(jax.random.fold_in(own, 4), (amount // 2,), 0, 1 << 20) % (margin + 1)
    sizes = sizes.at[donor].add(-moved).at[sink].add(moved)
    labels = jnp.searchsorted(jnp.cumsum(sizes), jnp.arange(rows * top), side="right").astype(jnp.int32)
    grid = labels.reshape(top, rows).T
    grid = grid[jax.random.permutation(jax.random.fold_in(own, 1), rows)]
    rotation = jax.random.randint(jax.random.fold_in(own, 2), (rows, 1), 0, top)
    return jnp.take_along_axis(grid, (jnp.arange(top)[None, :] + rotation) % top, axis=1)


def load_shares(amount, total, limit, skew, full):
    loads = [(1 << 20) // math.isqrt(grade ** skew) + 1 for grade in range(1, amount + 1)]
    largest = limit if full else min(limit, max(-(-total // amount), total * loads[0] // sum(loads)))
    least = 1 if total - largest >= amount - 1 else 0
    given, spare = [largest] + [least] * (amount - 1), total - largest - least * (amount - 1)
    while spare > 0:
        free = [i for i in range(1, amount) if given[i] < largest] or [i for i in range(1, amount) if given[i] < limit]
        pool, left = sum([loads[i] for i in free]), spare
        for i in free:
            addition = min(limit - given[i], max(1, left * loads[i] // pool), spare)
            given[i] = given[i] + addition
            spare = spare - addition
    return np.array(given)


def gaussian(own_key, extent, scale, reach, cuts=(), kind=jnp.bfloat16):
    level = steps_of(own_key, extent, cuts, -0.22, 0.18) if cuts else 1.0
    values = jax.random.normal(own_key, extent, jnp.float32) * scale * level
    return jnp.minimum(jnp.maximum(values, -reach), reach).astype(kind)


def setup_inputs(seed: int = 0) -> dict:
    seeds = jax.random.split(jax.random.key(seed), 12)
    tokens = gaussian(seeds[0], (MB, TOKENS, MODEL_WIDTH), 1.0, 6.0, ((1, 16),))
    cotangent = gaussian(seeds[1], (MB, TOKENS, MODEL_WIDTH), 1.0, 6.0, ((1, 16),))
    lengths = jax.vmap(lambda own: uneven(own, NSEQ, DEVICE_ROWS, SEQ_MAX, 2))(jax.random.split(seeds[2], MB * N_DP)).reshape((MB, N_DP, NSEQ)).astype(jnp.int32)
    routes_keys = jax.random.split(jax.random.fold_in(seeds[3], 1), SECTION_LAYERS * MB * TOKENS // DEVICE_ROWS)
    routes_turns = jax.random.permutation(jax.random.fold_in(seeds[3], 3), SECTION_LAYERS * MB * TOKENS // DEVICE_ROWS)
    routes = jax.vmap(lambda own, number: routed_block(jax.random.fold_in(seeds[3], 2), own, number, DEVICE_ROWS, EXPERTS, TOPK, CAP, 2))(routes_keys, routes_turns).reshape((SECTION_LAYERS, MB, TOKENS, TOPK))
    combined_weight = gaussian(seeds[4], (SECTION_LAYERS, MODEL_WIDTH, (QUERY_HEADS + 2 * KEY_VALUE_HEADS) * HEAD_SIZE), MODEL_WIDTH ** -0.5, 0.15625, ((0, 2), (1, 16)))
    output_weight = gaussian(seeds[5], (SECTION_LAYERS, QUERY_HEADS * HEAD_SIZE, MODEL_WIDTH), (QUERY_HEADS * HEAD_SIZE // 16) ** -0.5, 0.625, ((0, 2), (1, 16)))
    router_weight = gaussian(seeds[6], (SECTION_LAYERS, MODEL_WIDTH, EXPERTS), (4 * MODEL_WIDTH) ** -0.5, 0.078125, ((0, 2), (1, 16)))
    attention_gain = jnp.clip(1.0 + 0.1 * jax.random.normal(seeds[7], (SECTION_LAYERS, MODEL_WIDTH), jnp.float32), 0.5, 1.5).astype(jnp.bfloat16)
    mixture_gain = jnp.clip(1.0 + 0.1 * jax.random.normal(seeds[8], (SECTION_LAYERS, MODEL_WIDTH), jnp.float32), 0.5, 1.5).astype(jnp.bfloat16)
    expert_gate_up = gaussian(seeds[9], (SECTION_LAYERS, EXPERTS, MODEL_WIDTH, 2 * FFE), (MODEL_WIDTH // 4) ** -0.5, 0.3125, ((0, 2), (1, 16)))
    expert_down = gaussian(seeds[10], (SECTION_LAYERS, EXPERTS, FFE, MODEL_WIDTH), (max(1, 64 * FFE // (EXPERTS * EXPERTS))) ** -0.5, 0.5, ((0, 2), (1, 16)))
    return {"tokens": tokens, "cotangent": cotangent, "lengths": lengths, "routes": routes, "combined_weight": combined_weight, "output_weight": output_weight, "router_weight": router_weight, "attention_gain": attention_gain, "mixture_gain": mixture_gain, "expert_gate_up": expert_gate_up, "expert_down": expert_down}


@jax.custom_vjp
def lower_half(v):
    return lax.optimization_barrier(v.astype(jnp.bfloat16)).astype(jnp.float32)

@jax.custom_vjp
def low_back(v):
    return v

def low_keep(v):
    return (lower_half(v), None)

def low_pass(kept, grad):
    return (grad,)

def back_keep(v):
    return (v, None)

def back_low(kept, grad):
    return (lower_half(grad),)
lower_half.defvjp(low_keep, low_pass)
low_back.defvjp(back_keep, back_low)
highest = lax.Precision.HIGHEST
norm_epsilon = 1e-06

def layout(length_rows):
    seq_ends = jnp.cumsum(length_rows, axis=-1).astype(jnp.int32)
    seq_starts = seq_ends - length_rows
    row_ids = jnp.arange(DEVICE_ROWS, dtype=jnp.int32)
    segment = lax.optimization_barrier(jnp.sum((row_ids[None, :, None] >= seq_ends[:, None, :]).astype(jnp.int32), axis=-1))
    member = (segment[:, :, None] == jnp.arange(NSEQ, dtype=jnp.int32)[None, None, :]).astype(jnp.int32)
    token_position = row_ids[None, :] - lax.optimization_barrier(jnp.sum(member * seq_starts[:, None, :], axis=-1))
    return (segment, token_position)

def rotary_embedding(values, token_position, direction):
    half_width = HEAD_SIZE // 2
    frequency = 10000.0 ** (-2.0 * jnp.arange(half_width, dtype=jnp.float32) / HEAD_SIZE)
    angles = direction * token_position.astype(jnp.float32)[..., None] * frequency
    cosine = jnp.cos(angles)[..., None, :]
    sine_part = jnp.sin(angles)[..., None, :]
    former = values[..., :half_width]
    latter = values[..., half_width:]
    return jnp.concatenate([former * cosine - latter * sine_part, latter * cosine + former * sine_part], axis=-1)

def normalize(values, gain):
    return values * lax.rsqrt(lax.optimization_barrier(jnp.mean(values * values, axis=-1, keepdims=True)) + norm_epsilon) * gain

def attend_block(pieces):
    query_matrix, key_matrix, value_matrix, segment = pieces
    grouped_heads = query_matrix.reshape(DEVICE_ROWS, KEY_VALUE_HEADS, QUERY_HEADS // KEY_VALUE_HEADS, HEAD_SIZE)
    scores = low_back(jnp.einsum('qhgd,khd->hgqk', grouped_heads, key_matrix, precision=highest) * HEAD_SIZE ** (-0.5))
    row_ids = jnp.arange(DEVICE_ROWS, dtype=jnp.int32)
    allowed = (row_ids[:, None] >= row_ids[None, :]) & (segment[:, None] == segment[None, :])
    exponent = jnp.where(allowed, jnp.exp(scores), 0.0)
    attention = lower_half(exponent / lax.optimization_barrier(jnp.sum(exponent, axis=-1, keepdims=True)))
    context = jnp.einsum('hgqk,khd->qhgd', attention, value_matrix, precision=highest)
    return context.reshape(DEVICE_ROWS, QUERY_HEADS * HEAD_SIZE)

def slot_tables(route):
    chosen = route.reshape(N_DP, DEVICE_ROWS * TOPK)
    member = (chosen[..., None] == jnp.arange(EXPERTS, dtype=jnp.int32)).astype(jnp.int32)
    ranking = lax.optimization_barrier(jnp.sum((jnp.cumsum(member, axis=1) - member) * member, axis=-1))
    device = jnp.arange(N_DP, dtype=jnp.int32)[:, None]
    target = ((chosen * N_DP + device) * CAP + ranking).reshape(-1).astype(jnp.int32)
    anchor = (device * DEVICE_ROWS + jnp.arange(DEVICE_ROWS * TOPK, dtype=jnp.int32)[None, :] // TOPK).reshape(-1).astype(jnp.int32)
    source = jnp.full((EXPERTS * N_DP * CAP,), N_DP * DEVICE_ROWS, jnp.int32).at[target].set(anchor)
    return (target, source)

def layer_forward(hidden, params, segment, token_position, route, target, source):
    joint, result_output, router, gain_attention, gain_mixture, gate_up, down = params
    query_total_width = QUERY_HEADS * HEAD_SIZE
    rotary_pair_width = KEY_VALUE_HEADS * HEAD_SIZE
    normed = lower_half(normalize(hidden, gain_attention))
    projected_rows = low_back(jnp.dot(normed, joint, precision=highest))
    query_matrix = lower_half(rotary_embedding(projected_rows[:, :query_total_width].reshape(N_DP, DEVICE_ROWS, QUERY_HEADS, HEAD_SIZE), token_position, 1.0))
    key_matrix = lower_half(rotary_embedding(projected_rows[:, query_total_width:query_total_width + rotary_pair_width].reshape(N_DP, DEVICE_ROWS, KEY_VALUE_HEADS, HEAD_SIZE), token_position, 1.0))
    value_matrix = lower_half(projected_rows[:, query_total_width + rotary_pair_width:].reshape(N_DP, DEVICE_ROWS, KEY_VALUE_HEADS, HEAD_SIZE))
    context = lax.map(jax.checkpoint(attend_block), (query_matrix, key_matrix, value_matrix, segment))
    context = lower_half(low_back(context.reshape(N_DP * DEVICE_ROWS, query_total_width)))
    middle = hidden + low_back(jnp.dot(context, result_output, precision=highest))
    normed_two = lower_half(normalize(middle, gain_mixture))
    logits = low_back(jnp.dot(normed_two, router, precision=highest))
    exponent = jnp.exp(logits)
    probability = exponent / lax.optimization_barrier(jnp.sum(exponent, axis=-1, keepdims=True))
    weight = jnp.take_along_axis(probability, route, axis=1)
    padded = jnp.concatenate([normed_two, jnp.zeros((1, MODEL_WIDTH), jnp.float32)], axis=0)
    buffer = low_back(padded[source]).reshape(EXPERTS, N_DP * CAP, MODEL_WIDTH)
    gate_values = low_back(jnp.einsum('esd,edf->esf', buffer, gate_up, precision=highest))
    activated = lower_half(jax.nn.silu(gate_values[..., :FFE]) * gate_values[..., FFE:])
    produced = lower_half(low_back(jnp.einsum('esf,efd->esd', activated, down, precision=highest)))
    picked = produced.reshape(-1, MODEL_WIDTH)[target].reshape(N_DP * DEVICE_ROWS, TOPK, MODEL_WIDTH)
    return middle + jnp.einsum('tk,tkd->td', weight, picked, precision=highest)

def reference(tokens, cotangent, lengths, routes, combined_weight, output_weight, router_weight, attention_gain, mixture_gain, expert_gate_up, expert_down):
    layouts = [layout(lengths[micro_id]) for micro_id in range(MB)]
    tables = [[slot_tables(routes[layer_id, micro_id]) for micro_id in range(MB)] for layer_id in range(SECTION_LAYERS)]
    params = tuple((argument.astype(jnp.float32) for argument in (combined_weight, output_weight, router_weight, attention_gain, mixture_gain, expert_gate_up, expert_down)))

    def forward(inputs, weights):
        results = []
        for micro_id in range(MB):
            hidden = inputs[micro_id]
            segment, token_position = layouts[micro_id]
            for layer_id in range(SECTION_LAYERS):
                layer_params = tuple((argument[layer_id] for argument in weights))
                target, source = tables[layer_id][micro_id]
                hidden = layer_forward(hidden, layer_params, segment, token_position, routes[layer_id, micro_id], target, source)
                if layer_id + 1 < SECTION_LAYERS:
                    hidden = lower_half(low_back(hidden))
            results.append(hidden)
        return jnp.stack(results)
    last_out, pullback = jax.vjp(forward, tokens.astype(jnp.float32), params)
    input_grad, weight_grads = pullback(cotangent.astype(jnp.float32))
    boundary = jnp.stack([input_grad, last_out]).astype(jnp.bfloat16)
    return (boundary, weight_grads[0], weight_grads[1], weight_grads[2], weight_grads[3], weight_grads[4], weight_grads[5], weight_grads[6])
```

```python
import functools
import jax
import jax.numpy as jnp
from jax import lax
from jax.experimental import pallas as pl
from jax.experimental.pallas import tpu as pltpu
from jax.sharding import PartitionSpec as P

MODEL_WIDTH = 1536
QUERY_HEADS = 24
KEY_VALUE_HEADS = 8
GROUP = QUERY_HEADS // KEY_VALUE_HEADS
HEAD_SIZE = 64
FFE = 512
TOPK = 8
DEVICE_ROWS = 128
NSEQ = 4
QUERY_WIDTH = QUERY_HEADS * HEAD_SIZE
KEY_WIDTH = KEY_VALUE_HEADS * HEAD_SIZE
SCORE_SCALE = HEAD_SIZE ** (-0.5)
norm_epsilon = 1e-06
CHUNK_ROWS = 2048

VMEM_BYTES = 66_000_000


def torus_axes(count):
    side = 1
    while (side + 1) ** 3 <= count:
        side += 1
    assert count % (side * side) == 0
    return [(side * side, count // (side * side)), (1, side), (side, side)]


def offsets(sizes):
    return [(k, j, i) for k in range(sizes[0]) for j in range(sizes[1]) for i in range(sizes[2])]


class Place:
    def __init__(self, axes, order):
        self.me = lax.axis_index("dp")
        self.sec = lax.axis_index("section")
        long, first, second = axes
        if order is None:
            flip = self.sec
            stride_one = first[0] + (second[0] - first[0]) * flip
            stride_two = second[0] + (first[0] - second[0]) * flip
            assert first[1] == second[1]
            self.axes = [long, (stride_one, first[1]), (stride_two, second[1])]
        elif order == 0:
            self.axes = [long, first, second]
        else:
            self.axes = [long, second, first]
        self.sizes = [size for _, size in self.axes]

    def moved(self, steps):
        out = self.me
        for (stride, size), step in zip(self.axes, steps):
            if step % size:
                digit = lax.rem(lax.div(self.me, stride), size)
                out = out + (lax.rem(digit + (step % size), size) - digit) * stride
        return out

    def source(self, offs):
        return self.moved([-o for o in offs])

    def target(self, offs):
        return self.moved(list(offs))

    def flat(self, offs):
        return (offs[0] * self.sizes[1] + offs[1]) * self.sizes[2] + offs[2]


def last_hop(offs):
    for axis in (2, 1, 0):
        if offs[axis]:
            hop = [0, 0, 0]
            hop[axis] = offs[axis]
            base = list(offs)
            base[axis] = 0
            return tuple(hop), tuple(base)
    return None


def greet(axes, pair):
    place = Place(axes, 0)
    barrier = pltpu.get_barrier_semaphore()
    count = 0
    for axis in range(3):
        for step in range(1, place.sizes[axis]):
            hop = [0, 0, 0]
            hop[axis] = step
            pl.semaphore_signal(barrier, inc=1, device_id={"dp": place.target(hop)}, device_id_type=pl.DeviceIdType.MESH)
            count += 1
    if pair:
        pl.semaphore_signal(barrier, inc=1, device_id={"section": 1 - place.sec}, device_id_type=pl.DeviceIdType.MESH)
        count += 1
    pl.semaphore_wait(barrier, count)


def gather_kernel(axes, pair, count, *refs):
    ins, outs = refs[:count], refs[count : 2 * count]
    send, recv, local = refs[2 * count : 2 * count + 3]
    psend, precv = refs[2 * count + 3 :] if pair else (None, None)
    streams = []
    for a in range(count):
        if pair:
            place = Place(axes, None)
            half = ins[a].shape[1]
            cols = pl.ds(pl.multiple_of(place.sec * half, 128), half)
            streams.append((place, ins[a], lambda b, o=outs[a], c=cols: o.at[b, :, c]))
        else:
            half = ins[a].shape[0] // 2
            for h in range(2):
                rows = pl.ds(h * half, half)
                streams.append((Place(axes, h), ins[a].at[rows], lambda b, o=outs[a], r=rows: o.at[b, r]))

    def copy(s, offs):
        place, own, out = streams[s]
        hop, base = last_hop(offs)
        block = place.source(base)
        src = out(block) if any(base) else own
        f = place.flat(offs)
        return pltpu.make_async_remote_copy(
            src_ref=src, dst_ref=out(block), send_sem=send.at[s, f], recv_sem=recv.at[s, f],
            device_id={"dp": place.target(hop)}, device_id_type=pl.DeviceIdType.MESH)

    def share(s, offs):
        place, own, out = streams[s]
        block = place.source(offs)
        src = out(block) if any(offs) else own
        f = place.flat(offs)
        return pltpu.make_async_remote_copy(
            src_ref=src, dst_ref=out(block), send_sem=psend.at[s, f], recv_sem=precv.at[s, f],
            device_id={"section": 1 - place.sec}, device_id_type=pl.DeviceIdType.MESH)

    greet(axes, pair)
    ids = range(len(streams))
    n0, n1, n2 = streams[0][0].sizes
    keep = []
    for s in ids:
        place, own, out = streams[s]
        c = pltpu.make_async_copy(own, out(place.me), local.at[s])
        c.start()
        keep.append(c)
    for k in range(1, n0):
        for s in ids:
            copy(s, (k, 0, 0)).start()

    def first(k):
        for s in ids:
            if k:
                copy(s, (k, 0, 0)).wait_recv()
            for j in range(1, n1):
                copy(s, (k, j, 0)).start()
            for i in range(1, n2):
                copy(s, (k, 0, i)).start()
            if pair:
                share(s, (k, 0, 0)).start()

    def second(k):
        for j in range(1, n1):
            for s in ids:
                copy(s, (k, j, 0)).wait_recv()
                for i in range(1, n2):
                    copy(s, (k, j, i)).start()
                if pair:
                    share(s, (k, j, 0)).start()

    def third(k):
        for j in range(n1):
            for i in range(1, n2):
                for s in ids:
                    copy(s, (k, j, i)).wait_recv()
                    if pair:
                        share(s, (k, j, i)).start()

    for k in range(n0 + 2):
        if k < n0:
            first(k)
        if 0 <= k - 1 < n0:
            second(k - 1)
        if 0 <= k - 2 < n0:
            third(k - 2)
    for s in ids:
        for offs in offsets((n0, n1, n2)):
            if any(offs):
                copy(s, offs).wait_send()
            if pair:
                share(s, offs).wait()
    for c in keep:
        c.wait()


def gather_all(arrays, count, cid, pair=False):
    axes = torus_axes(count)
    streams = len(arrays) * (1 if pair else 2)
    sem = pltpu.SemaphoreType.DMA((streams, count))
    out_shape = [jax.ShapeDtypeStruct((count, a.shape[0], a.shape[1] * (2 if pair else 1)), a.dtype) for a in arrays]
    scratch = [sem, sem, pltpu.SemaphoreType.DMA((streams,))]
    if pair:
        scratch += [sem, sem]
    sent = sum(a.size * a.dtype.itemsize for a in arrays) * (count - 1)
    return pl.pallas_call(
        functools.partial(gather_kernel, axes, pair, len(arrays)),
        out_shape=out_shape,
        in_specs=[pl.BlockSpec(memory_space=pltpu.VMEM)] * len(arrays),
        out_specs=[pl.BlockSpec(memory_space=pl.ANY)] * len(arrays),
        scratch_shapes=scratch,
        compiler_params=pltpu.CompilerParams(collective_id=cid, has_side_effects=True),
        cost_estimate=pl.CostEstimate(flops=0, bytes_accessed=2 * sent, transcendentals=0),
        name="spread" if not pair else "spread_pair",
    )(*arrays)


def reduce_kernel(axes, pair, count, *refs):
    ins, outs = refs[:count], refs[count : 2 * count]
    rest = list(refs[2 * count :])
    send, recv = rest[:2]
    rest = rest[2:]
    if pair:
        psend, precv = rest[:2]
        rest = rest[2:]
    streams = []
    for a in range(count):
        if pair:
            got, held, pgot, psum = rest[:4]
            rest = rest[4:]
            place = Place(axes, None)
            half = outs[a].shape[1]
            mine = pl.ds(pl.multiple_of(place.sec * half, 128), half)
            other = pl.ds(pl.multiple_of((1 - place.sec) * half, 128), half)
            streams.append(dict(place=place, got=got, held=held, pgot=pgot, psum=psum, raw=ins[a], mine=mine, other=other,
                                out=outs[a], rows=outs[a].shape[0]))
        else:
            got, held = rest[:2]
            rest = rest[2:]
            half = outs[a].shape[0] // 2
            for h in range(2):
                rows = pl.ds(h * half, half)
                streams.append(dict(place=Place(axes, h), got=got.at[h], held=held.at[h], raw=ins[a], span=rows,
                                    out=outs[a].at[rows], rows=half))
    step = 8 if streams[0]["rows"] % 16 else 16

    def own_ref(t, offs):
        if pair:
            return t["psum"].at[t["place"].flat(offs)]
        return t["raw"].at[t["place"].target(offs), t["span"]]

    def summed(t, sources, dest):
        def one(r, _):
            rows = pl.ds(pl.multiple_of(r * step, step), step)
            total = sources[0][rows].astype(jnp.float32)
            for source in sources[1:]:
                total = total + source[rows].astype(jnp.float32)
            dest[rows] = total.astype(dest.dtype)
            return 0

        lax.fori_loop(0, t["rows"] // step, one, 0)

    def copy(s, offs):
        t = streams[s]
        place = t["place"]
        hop, base = last_hop(offs)
        f = place.flat(offs)
        src = own_ref(t, offs) if hop[2] else t["held"].at[f // place.sizes[2]]
        return pltpu.make_async_remote_copy(
            src_ref=src, dst_ref=t["got"].at[f], send_sem=send.at[s, f], recv_sem=recv.at[s, f],
            device_id={"dp": place.target(hop)}, device_id_type=pl.DeviceIdType.MESH)

    def share(s, offs):
        t = streams[s]
        place = t["place"]
        f = place.flat(offs)
        return pltpu.make_async_remote_copy(
            src_ref=t["raw"].at[place.target((offs[0], offs[2], offs[1])), :, t["other"]], dst_ref=t["pgot"].at[f],
            send_sem=psend.at[s, f], recv_sem=precv.at[s, f],
            device_id={"section": 1 - place.sec}, device_id_type=pl.DeviceIdType.MESH)

    ids = range(len(streams))
    n0, n1, n2 = streams[0]["place"].sizes
    greet(axes, pair)

    def phase_pair(k):
        for j in reversed(range(n1)):
            for i in reversed(range(n2)):
                for s in ids:
                    share(s, (k, j, i)).start()

    def phase_first(k):
        for j in reversed(range(n1)):
            for i in reversed(range(n2)):
                for s in ids:
                    t = streams[s]
                    if pair:
                        share(s, (k, j, i)).wait_recv()
                        f = t["place"].flat((k, j, i))
                        summed(t, [t["raw"].at[t["place"].target((k, j, i)), :, t["mine"]], t["pgot"].at[f]], t["psum"].at[f])
                    if i:
                        copy(s, (k, j, i)).start()

    def phase_second(k):
        for j in range(1, n1):
            for s in ids:
                t = streams[s]
                for i in range(1, n2):
                    copy(s, (k, j, i)).wait_recv()
                parts = [own_ref(t, (k, j, 0))] + [t["got"].at[t["place"].flat((k, j, i))] for i in range(1, n2)]
                summed(t, parts, t["held"].at[t["place"].flat((k, j, 0)) // n2])
                copy(s, (k, j, 0)).start()

    def gathered_parts(s, k):
        t = streams[s]
        offs = [(k, 0, i) for i in range(1, n2)] + [(k, j, 0) for j in range(1, n1)]
        for o in offs:
            copy(s, o).wait_recv()
        return [own_ref(t, (k, 0, 0))] + [t["got"].at[t["place"].flat(o)] for o in offs]

    def phase_third(k):
        for s in ids:
            t = streams[s]
            parts = gathered_parts(s, k)
            if k:
                summed(t, parts, t["held"].at[t["place"].flat((k, 0, 0)) // n2])
                copy(s, (k, 0, 0)).start()
            else:
                for q in range(1, n0):
                    copy(s, (q, 0, 0)).wait_recv()
                    parts.append(t["got"].at[t["place"].flat((q, 0, 0))])
                summed(t, parts, t["out"])

    chunks = list(range(1, n0)) + [0]
    if pair:
        phase_pair(chunks[0])
    for c in range(n0 + 3):
        if pair and c + 1 < n0:
            phase_pair(chunks[c + 1])
        if c < n0:
            phase_first(chunks[c])
        if 0 <= c - 1 < n0:
            phase_second(chunks[c - 1])
        if 0 <= c - 2 < n0:
            phase_third(chunks[c - 2])
    for s in ids:
        for offs in offsets((n0, n1, n2)):
            if any(offs):
                copy(s, offs).wait_send()
            if pair:
                share(s, offs).wait_send()


def reduce_all(arrays, count, cid, pair=False):
    axes = torus_axes(count)
    streams = len(arrays) * (1 if pair else 2)
    sem = pltpu.SemaphoreType.DMA((streams, count))
    scratch = [sem, sem]
    if pair:
        scratch += [sem, sem]
    groups = count // axes[2][1]
    out_shape = []
    for a in arrays:
        rows, cols = a.shape[1:]
        if pair:
            cols = cols // 2
            scratch += [pltpu.VMEM((count, rows, cols), a.dtype), pltpu.VMEM((groups, rows, cols), a.dtype),
                        pltpu.VMEM((count, rows, cols), a.dtype), pltpu.VMEM((count, rows, cols), a.dtype)]
        else:
            scratch += [pltpu.VMEM((2, count, rows // 2, cols), a.dtype), pltpu.VMEM((2, groups, rows // 2, cols), a.dtype)]
        out_shape.append(jax.ShapeDtypeStruct((rows, cols), jnp.float32))
    sent = sum(a.size * a.dtype.itemsize for a in arrays)
    return pl.pallas_call(
        functools.partial(reduce_kernel, axes, pair, len(arrays)),
        out_shape=out_shape,
        in_specs=[pl.BlockSpec(memory_space=pltpu.VMEM)] * len(arrays),
        out_specs=[pl.BlockSpec(memory_space=pltpu.VMEM)] * len(arrays),
        scratch_shapes=scratch,
        compiler_params=pltpu.CompilerParams(collective_id=cid, has_side_effects=True, vmem_limit_bytes=VMEM_BYTES),
        cost_estimate=pl.CostEstimate(flops=0, bytes_accessed=2 * sent, transcendentals=0),
        name="fold" if not pair else "fold_pair",
    )(*arrays)

def swapped(value):
    return lax.ppermute(value, "section", [(0, 1), (1, 0)])


def layout(length_row):
    seq_ends = jnp.cumsum(length_row)
    seq_starts = seq_ends - length_row
    row_ids = jnp.arange(DEVICE_ROWS, dtype=jnp.int32)
    segment = jnp.sum((row_ids[:, None] >= seq_ends[None, :]).astype(jnp.int32), axis=-1)
    member = (segment[:, None] == jnp.arange(NSEQ, dtype=jnp.int32)[None, :]).astype(jnp.int32)
    token_position = row_ids - jnp.sum(member * seq_starts[None, :], axis=-1)
    return segment, token_position


def rotation(token_position):
    half_width = HEAD_SIZE // 2
    frequency = 10000.0 ** (-2.0 * jnp.arange(half_width, dtype=jnp.float32) / HEAD_SIZE)
    angles = token_position.astype(jnp.float32)[:, None] * frequency
    return jnp.cos(angles)[:, None, :], jnp.sin(angles)[:, None, :]


def rotary_embedding(values, cosine, sine):
    half_width = HEAD_SIZE // 2
    former, latter = values[..., :half_width], values[..., half_width:]
    return jnp.concatenate([former * cosine - latter * sine, latter * cosine + former * sine], axis=-1)


def dot(left, right):
    return jnp.dot(left, right, preferred_element_type=jnp.float32)


def dot_rows(left, right):
    return lax.dot_general(left, right, (((0,), (0,)), ((), ())), preferred_element_type=jnp.float32)


def dot_columns(left, right):
    return lax.dot_general(left, right, (((1,), (1,)), ((), ())), preferred_element_type=jnp.float32)


def router_chances(normed_two, router):
    chance = jnp.exp(dot(normed_two, router))
    return chance / jnp.sum(chance, axis=-1, keepdims=True)


def front(hidden, place, weights):
    joint, result_output, router, gain_attention, gain_mixture = weights
    allowed, cosine, sine = place
    rows = hidden.shape[0]
    inverse_one = lax.rsqrt(jnp.mean(hidden * hidden, axis=-1, keepdims=True) + norm_epsilon)
    scaled_one = hidden * inverse_one
    normed = (scaled_one * gain_attention).astype(jnp.bfloat16)
    projected = dot(normed, joint)
    query = rotary_embedding(projected[:, :QUERY_WIDTH].reshape(rows, QUERY_HEADS, HEAD_SIZE), cosine, sine)
    query = query.astype(jnp.bfloat16).reshape(rows, KEY_VALUE_HEADS, GROUP, HEAD_SIZE)
    key = rotary_embedding(projected[:, QUERY_WIDTH : QUERY_WIDTH + KEY_WIDTH].reshape(rows, KEY_VALUE_HEADS, HEAD_SIZE), cosine, sine)
    key = key.astype(jnp.bfloat16)
    value = projected[:, QUERY_WIDTH + KEY_WIDTH :].reshape(rows, KEY_VALUE_HEADS, HEAD_SIZE).astype(jnp.bfloat16)
    scores = jnp.einsum("qhgd,khd->hgqk", query, key, preferred_element_type=jnp.float32) * SCORE_SCALE
    exponent = jnp.where(allowed, jnp.exp(scores), 0.0)
    attention = exponent / jnp.sum(exponent, axis=-1, keepdims=True)
    context = jnp.einsum("hgqk,khd->qhgd", attention.astype(jnp.bfloat16), value, preferred_element_type=jnp.float32)
    context = context.reshape(rows, QUERY_WIDTH).astype(jnp.bfloat16)
    middle = hidden + dot(context, result_output)
    inverse_two = lax.rsqrt(jnp.mean(middle * middle, axis=-1, keepdims=True) + norm_epsilon)
    scaled_two = middle * inverse_two
    normed_two = (scaled_two * gain_mixture).astype(jnp.bfloat16)
    kept = (inverse_one, scaled_one, normed, query, key, value, attention, context, inverse_two, scaled_two, normed_two)
    return middle, normed_two, kept


def gates(everyone, up_weight):
    both = dot(everyone, up_weight)
    return both[:, :FFE], both[:, FFE:]


def expert_forward(everyone, mask, router, expert, count, me):
    up_weight, down_weight = expert
    chance = router_chances(everyone, router)
    own = jnp.arange(count, dtype=jnp.int32) == me
    weight = jnp.sum(jnp.where(own[None, :] & mask, chance, 0.0), axis=-1)
    gate, up = gates(everyone, up_weight)
    activated = (jax.nn.silu(gate) * up).astype(jnp.bfloat16)
    share = (dot(activated, down_weight) * weight[:, None]).astype(jnp.bfloat16)
    return share, weight, (gate, up)


def expert_backward(grads, everyone, weight, mask, held, expert):
    up_weight, down_weight = expert
    gate, up = held if held is not None else gates(everyone, up_weight)
    sigmoid = jax.nn.sigmoid(gate)
    silu = gate * sigmoid
    activated = silu * up
    grad_plain = dot_columns(grads, down_weight)
    grad_weight = jnp.where(mask[:, 0], jnp.sum(activated * grad_plain, axis=-1), 0.0)
    grad_act = grad_plain * weight[:, None]
    grad_gate = grad_act * up * sigmoid * (1.0 + gate * (1.0 - sigmoid))
    grad_gate_up = jnp.concatenate([grad_gate, grad_act * silu], axis=-1).astype(jnp.bfloat16)
    grad_down = dot_rows((activated * weight[:, None]).astype(jnp.bfloat16), grads)
    grad_up_weight = dot_rows(everyone, grad_gate_up)
    share = dot_columns(grad_gate_up, up_weight).astype(jnp.bfloat16)
    return share, grad_weight, grad_up_weight, grad_down


def pieces(value):
    return value.reshape(-1, CHUNK_ROWS, *value.shape[1:])


def mixture_forward(normed_two, router, mask, expert, count, me):
    (spread,) = gather_all([normed_two], count, 0)
    everyone = spread.reshape(-1, MODEL_WIDTH)
    if everyone.shape[0] <= CHUNK_ROWS:
        share, weight, held = expert_forward(everyone, mask, router, expert, count, me)
    else:
        share, weight = lax.map(
            lambda part: expert_forward(part[0], part[1], router, expert, count, me)[:2], (pieces(everyone), pieces(mask)))
        held = None
    (mixed,) = reduce_all([share.reshape(spread.shape)], count, 1)
    return mixed, (everyone, weight.reshape(-1), held)


def mixture_backward(grad_out, mask, kept, expert, count):
    everyone, weight, held = kept
    (spread,) = gather_all([grad_out], count, 0)
    grads = spread.reshape(-1, MODEL_WIDTH)
    if grads.shape[0] <= CHUNK_ROWS:
        share, grad_weight, grad_up, grad_down = expert_backward(grads, everyone, weight, mask, held, expert)
    else:
        def step(sums, part):
            share, grad_weight, grad_up, grad_down = expert_backward(*part, None, expert)
            return (sums[0] + grad_up, sums[1] + grad_down), (share, grad_weight)

        zero = tuple(jnp.zeros(w.shape, jnp.float32) for w in expert)
        (grad_up, grad_down), (share, grad_weight) = lax.scan(
            step, zero, (pieces(grads), pieces(everyone), pieces(weight), pieces(mask)))
    grad_chance = lax.all_to_all(grad_weight.reshape(count, DEVICE_ROWS), "dp", split_axis=0, concat_axis=0, tiled=True)
    (mixed,) = reduce_all([share.reshape(spread.shape)], count, 1)
    return mixed, grad_chance.T, grad_up, grad_down


def front_backward(grad_out, grad_mixed, grad_chance, kept, place, weights):
    joint, result_output, router, gain_attention, gain_mixture = weights
    allowed, cosine, sine = place
    inverse_one, scaled_one, normed, query, key, value, attention, context, inverse_two, scaled_two, normed_two = kept
    rows = normed.shape[0]
    chance = router_chances(normed_two, router)
    grad_logit = (chance * (grad_chance - jnp.sum(grad_chance * chance, axis=-1, keepdims=True))).astype(jnp.bfloat16)
    grad_router = dot_rows(normed_two, grad_logit)
    grad_normed_two = grad_mixed + dot_columns(grad_logit, router)
    grad_gain_two = jnp.sum(grad_normed_two * scaled_two, axis=0)
    scaled_grad_two = grad_normed_two * gain_mixture
    grad_middle = grad_out + inverse_two * (scaled_grad_two - scaled_two * jnp.mean(scaled_grad_two * scaled_two, axis=-1, keepdims=True))
    branch = grad_middle.astype(jnp.bfloat16)
    grad_output = dot_rows(context, branch)
    grad_context = dot_columns(branch, result_output).astype(jnp.bfloat16).reshape(rows, KEY_VALUE_HEADS, GROUP, HEAD_SIZE)
    grad_attention = jnp.einsum("qhgd,khd->hgqk", grad_context, value, preferred_element_type=jnp.float32)
    grad_value = jnp.einsum("hgqk,qhgd->khd", attention.astype(jnp.bfloat16), grad_context, preferred_element_type=jnp.float32)
    grad_scores = (attention * (grad_attention - jnp.sum(grad_attention * attention, axis=-1, keepdims=True))).astype(jnp.bfloat16)
    grad_query = jnp.einsum("hgqk,khd->qhgd", grad_scores, key, preferred_element_type=jnp.float32).reshape(rows, QUERY_HEADS, HEAD_SIZE)
    grad_key = jnp.einsum("hgqk,qhgd->khd", grad_scores, query, preferred_element_type=jnp.float32)
    grad_query = rotary_embedding(grad_query * SCORE_SCALE, cosine, -sine)
    grad_key = rotary_embedding(grad_key * SCORE_SCALE, cosine, -sine)
    grad_projected = jnp.concatenate(
        [grad_query.reshape(rows, -1), grad_key.reshape(rows, -1), grad_value.reshape(rows, -1)], axis=-1).astype(jnp.bfloat16)
    grad_joint = dot_rows(normed, grad_projected)
    grad_normed = dot_columns(grad_projected, joint)
    grad_gain_one = jnp.sum(grad_normed * scaled_one, axis=0)
    scaled_grad_one = grad_normed * gain_attention
    grad_hidden = grad_middle + inverse_one * (scaled_grad_one - scaled_one * jnp.mean(scaled_grad_one * scaled_one, axis=-1, keepdims=True))
    return grad_hidden, (grad_joint, grad_output, grad_router, grad_gain_one, grad_gain_two)


def small_halves(rows, router, gains, codes):
    second = jnp.concatenate([gains, codes], axis=1)
    width = -(-max(router.shape[1], second.shape[1]) // 128) * 128
    pad = lambda v: jnp.pad(v, ((0, 0), (0, width - v.shape[1])))
    return pad(router), pad(second)


def body(tokens, cotangent, lengths, routes, combined_weight, output_weight, router_weight, attention_gain, mixture_gain,
         expert_gate_up, expert_down):
    count = lax.axis_size("dp")
    me, sec = lax.axis_index("dp"), lax.axis_index("section")
    layers = lax.axis_size("section")
    leading = sec == 0
    shard = combined_weight.shape[1]
    micro = lambda a, axis: lax.dynamic_index_in_dim(a, sec, axis, keepdims=False)

    gains = jnp.stack([attention_gain[0], mixture_gain[0]], axis=1)
    codes = routes[0].astype(jnp.bfloat16).reshape(-1)
    code_count = codes.shape[0]
    codes = jnp.pad(codes, (0, -code_count % shard)).reshape(shard, -1)
    small = small_halves(shard, router_weight[0], gains, codes)
    small_width = small[0].shape[1]
    halves = [
        (combined_weight[0, :, : combined_weight.shape[2] // 2], combined_weight[0, :, combined_weight.shape[2] // 2 :]),
        (output_weight[0, :, : output_weight.shape[2] // 2], output_weight[0, :, output_weight.shape[2] // 2 :]),
        small,
    ]
    widths = [h[0].shape[1] for h in halves]
    mine = jnp.concatenate([jnp.where(leading, a, b) for a, b in halves], axis=1)
    given = swapped(jnp.concatenate([jnp.where(leading, b, a) for a, b in halves], axis=1))
    packs = [jnp.where(leading, mine, given), jnp.where(leading, given, mine)]
    partner_expert = tuple(swapped(w[0, 0]) for w in (expert_gate_up, expert_down))
    experts = []
    for layer in range(layers):
        keep = sec == layer
        experts.append((jnp.where(keep, expert_gate_up[0, 0], partner_expert[0]), jnp.where(keep, expert_down[0, 0], partner_expert[1])))

    def layer_weights(layer):
        at, parts = 0, []
        for w in widths:
            parts.append(packs[layer][:, at : at + w])
            at += w
        joint, output, tail = gather_all(parts, count, 2, pair=True)
        joint = joint.reshape(MODEL_WIDTH, -1)
        output = output.reshape(MODEL_WIDTH, -1)
        tail = tail.reshape(MODEL_WIDTH, -1)
        second = tail[:, small_width:]
        weights = (joint, output, tail[:, : router_weight.shape[2]], second[:, 0].astype(jnp.float32), second[:, 1].astype(jnp.float32))
        code = second[:, 2 : 2 + codes.shape[1]].reshape(count, -1)[:, :code_count].reshape(count, -1, DEVICE_ROWS, TOPK)
        named = lax.dynamic_index_in_dim(code, sec, 1, keepdims=False).reshape(count * DEVICE_ROWS, TOPK)
        mask = jnp.any(named == me.astype(jnp.bfloat16), axis=-1, keepdims=True)
        return weights, mask

    segment, token_position = layout(micro(lengths[:, 0], 0))
    row_ids = jnp.arange(DEVICE_ROWS, dtype=jnp.int32)
    allowed = (row_ids[:, None] >= row_ids[None, :]) & (segment[:, None] == segment[None, :])
    place = (allowed,) + rotation(token_position)

    weights, masks, stores = [], [], []
    hidden = micro(tokens, 0)
    for layer in range(layers):
        got, mask = layer_weights(layer)
        weights.append(got)
        masks.append(mask)
        middle, normed_two, kept = front(hidden.astype(jnp.float32), place, got)
        mixed, kept_mixture = mixture_forward(normed_two, got[2], mask, experts[layer], count, me)
        hidden = (middle + mixed).astype(jnp.bfloat16)
        stores.append((kept, kept_mixture))
    last = hidden
    grad = micro(cotangent, 0)
    shares, expert_grads = [None] * layers, [None] * layers
    for layer in reversed(range(layers)):
        kept, kept_mixture = stores[layer]
        mixed, grad_chance, grad_up, grad_down = mixture_backward(grad, masks[layer], kept_mixture, experts[layer], count)
        expert_grads[layer] = (grad_up, grad_down)
        grad_hidden, parts = front_backward(grad.astype(jnp.float32), mixed, grad_chance, kept, place, weights[layer])
        grad = grad_hidden.astype(jnp.bfloat16)
        tail = small_halves(MODEL_WIDTH, parts[2], jnp.stack([parts[3], parts[4]], axis=1), parts[2][:, :0])
        packed = [parts[0], parts[1], jnp.concatenate(tail, axis=1)]
        packed = [a.astype(jnp.bfloat16).reshape(count, shard, -1) for a in packed]
        shares[layer] = reduce_all(packed, count, 3, pair=True)
    outs = []
    for a in range(3):
        kept_half = jnp.where(leading, shares[0][a], shares[1][a])
        got_half = swapped(jnp.where(leading, shares[1][a], shares[0][a]))
        outs.append(jnp.concatenate([jnp.where(leading, kept_half, got_half), jnp.where(leading, got_half, kept_half)], axis=1))
    expert_outs = []
    for a in range(2):
        kept_sum = jnp.where(leading, expert_grads[0][a], expert_grads[1][a])
        got_sum = swapped(jnp.where(leading, expert_grads[1][a], expert_grads[0][a]))
        expert_outs.append((kept_sum + got_sum)[None, None])
    partner = swapped(jnp.where(leading, last, grad))
    boundary = jnp.where(leading, jnp.stack([grad, partner]), jnp.stack([partner, last]))[None]
    half = outs[2].shape[1] // 2
    return (
        boundary,
        outs[0][None],
        outs[1][None],
        outs[2][None, :, : router_weight.shape[2]],
        outs[2][None, :, half],
        outs[2][None, :, half + 1],
        expert_outs[0],
        expert_outs[1],
    )


def solution(mesh):
    return jax.shard_map(
        body,
        mesh=mesh,
        in_specs=(
            P(None, "dp", None),
            P(None, "dp", None),
            P(None, "dp", None),
            P("section", None, "dp", None),
            P("section", "dp", None),
            P("section", "dp", None),
            P("section", "dp", None),
            P("section", "dp"),
            P("section", "dp"),
            P("section", "dp", None, None),
            P("section", "dp", None, None),
        ),
        out_specs=(
            P("section", None, "dp", None),
            P("section", "dp", None),
            P("section", "dp", None),
            P("section", "dp", None),
            P("section", "dp"),
            P("section", "dp"),
            P("section", "dp", None, None),
            P("section", "dp", None, None),
        ),
        check_vma=False,
    )
```

```python
import functools
import jax
import jax.numpy as jnp
from jax import lax
from jax.experimental import pallas as pl
from jax.experimental.pallas import tpu as pltpu
from jax.sharding import PartitionSpec as P

MODEL_WIDTH = 1536
QUERY_HEADS = 24
KEY_VALUE_HEADS = 8
GROUP = QUERY_HEADS // KEY_VALUE_HEADS
HEAD_SIZE = 64
FFE = 512
TOPK = 8
DEVICE_ROWS = 128
NSEQ = 4
QUERY_WIDTH = QUERY_HEADS * HEAD_SIZE
KEY_WIDTH = KEY_VALUE_HEADS * HEAD_SIZE
SCORE_SCALE = HEAD_SIZE ** (-0.5)
norm_epsilon = 1e-06
CHUNK_ROWS = 2048

VMEM_BYTES = 66_000_000


def torus_axes(count):
    side = 1
    while (side + 1) ** 3 <= count:
        side += 1
    assert count % (side * side) == 0
    return [(side * side, count // (side * side)), (1, side), (side, side)]


def offsets(sizes):
    return [(k, j, i) for k in range(sizes[0]) for j in range(sizes[1]) for i in range(sizes[2])]


class Place:
    def __init__(self, axes, order):
        self.me = lax.axis_index("dp")
        self.sec = lax.axis_index("section")
        long, first, second = axes
        if order is None:
            flip = self.sec
            stride_one = first[0] + (second[0] - first[0]) * flip
            stride_two = second[0] + (first[0] - second[0]) * flip
            assert first[1] == second[1]
            self.axes = [long, (stride_one, first[1]), (stride_two, second[1])]
        elif order == 0:
            self.axes = [long, first, second]
        else:
            self.axes = [long, second, first]
        self.sizes = [size for _, size in self.axes]

    def moved(self, steps):
        out = self.me
        for (stride, size), step in zip(self.axes, steps):
            if step % size:
                digit = lax.rem(lax.div(self.me, stride), size)
                out = out + (lax.rem(digit + (step % size), size) - digit) * stride
        return out

    def source(self, offs):
        return self.moved([-o for o in offs])

    def target(self, offs):
        return self.moved(list(offs))

    def flat(self, offs):
        return (offs[0] * self.sizes[1] + offs[1]) * self.sizes[2] + offs[2]


def last_hop(offs):
    for axis in (2, 1, 0):
        if offs[axis]:
            hop = [0, 0, 0]
            hop[axis] = offs[axis]
            base = list(offs)
            base[axis] = 0
            return tuple(hop), tuple(base)
    return None


def greet(axes, pair):
    place = Place(axes, 0)
    barrier = pltpu.get_barrier_semaphore()
    count = 0
    for axis in range(3):
        for step in range(1, place.sizes[axis]):
            hop = [0, 0, 0]
            hop[axis] = step
            pl.semaphore_signal(barrier, inc=1, device_id={"dp": place.target(hop)}, device_id_type=pl.DeviceIdType.MESH)
            count += 1
    if pair:
        pl.semaphore_signal(barrier, inc=1, device_id={"section": 1 - place.sec}, device_id_type=pl.DeviceIdType.MESH)
        count += 1
    pl.semaphore_wait(barrier, count)


def gather_kernel(axes, pair, count, *refs):
    ins, outs = refs[:count], refs[count : 2 * count]
    send, recv, local = refs[2 * count : 2 * count + 3]
    psend, precv = refs[2 * count + 3 :] if pair else (None, None)
    streams = []
    for a in range(count):
        if pair:
            place = Place(axes, None)
            half = ins[a].shape[1]
            cols = pl.ds(pl.multiple_of(place.sec * half, 128), half)
            streams.append((place, ins[a], lambda b, o=outs[a], c=cols: o.at[b, :, c]))
        else:
            half = ins[a].shape[0] // 2
            for h in range(2):
                rows = pl.ds(h * half, half)
                streams.append((Place(axes, h), ins[a].at[rows], lambda b, o=outs[a], r=rows: o.at[b, r]))

    def copy(s, offs):
        place, own, out = streams[s]
        hop, base = last_hop(offs)
        block = place.source(base)
        src = out(block) if any(base) else own
        f = place.flat(offs)
        return pltpu.make_async_remote_copy(
            src_ref=src, dst_ref=out(block), send_sem=send.at[s, f], recv_sem=recv.at[s, f],
            device_id={"dp": place.target(hop)}, device_id_type=pl.DeviceIdType.MESH)

    def share(s, offs):
        place, own, out = streams[s]
        block = place.source(offs)
        src = out(block) if any(offs) else own
        f = place.flat(offs)
        return pltpu.make_async_remote_copy(
            src_ref=src, dst_ref=out(block), send_sem=psend.at[s, f], recv_sem=precv.at[s, f],
            device_id={"section": 1 - place.sec}, device_id_type=pl.DeviceIdType.MESH)

    greet(axes, pair)
    ids = range(len(streams))
    n0, n1, n2 = streams[0][0].sizes
    keep = []
    for s in ids:
        place, own, out = streams[s]
        c = pltpu.make_async_copy(own, out(place.me), local.at[s])
        c.start()
        keep.append(c)
    for k in range(1, n0):
        for s in ids:
            copy(s, (k, 0, 0)).start()

    def first(k):
        for s in ids:
            if k:
                copy(s, (k, 0, 0)).wait_recv()
            for j in range(1, n1):
                copy(s, (k, j, 0)).start()
            for i in range(1, n2):
                copy(s, (k, 0, i)).start()
            if pair:
                share(s, (k, 0, 0)).start()

    def second(k):
        for j in range(1, n1):
            for s in ids:
                copy(s, (k, j, 0)).wait_recv()
                for i in range(1, n2):
                    copy(s, (k, j, i)).start()
                if pair:
                    share(s, (k, j, 0)).start()

    def third(k):
        for j in range(n1):
            for i in range(1, n2):
                for s in ids:
                    copy(s, (k, j, i)).wait_recv()
                    if pair:
                        share(s, (k, j, i)).start()

    for k in range(n0 + 2):
        if k < n0:
            first(k)
        if 0 <= k - 1 < n0:
            second(k - 1)
        if 0 <= k - 2 < n0:
            third(k - 2)
    for s in ids:
        for offs in offsets((n0, n1, n2)):
            if any(offs):
                copy(s, offs).wait_send()
            if pair:
                share(s, offs).wait()
    for c in keep:
        c.wait()


def gather_all(arrays, count, cid, pair=False):
    axes = torus_axes(count)
    streams = len(arrays) * (1 if pair else 2)
    sem = pltpu.SemaphoreType.DMA((streams, count))
    out_shape = [jax.ShapeDtypeStruct((count, a.shape[0], a.shape[1] * (2 if pair else 1)), a.dtype) for a in arrays]
    scratch = [sem, sem, pltpu.SemaphoreType.DMA((streams,))]
    if pair:
        scratch += [sem, sem]
    sent = sum(a.size * a.dtype.itemsize for a in arrays) * (count - 1)
    return pl.pallas_call(
        functools.partial(gather_kernel, axes, pair, len(arrays)),
        out_shape=out_shape,
        in_specs=[pl.BlockSpec(memory_space=pltpu.VMEM)] * len(arrays),
        out_specs=[pl.BlockSpec(memory_space=pl.ANY)] * len(arrays),
        scratch_shapes=scratch,
        compiler_params=pltpu.CompilerParams(collective_id=cid, has_side_effects=True),
        cost_estimate=pl.CostEstimate(flops=0, bytes_accessed=2 * sent, transcendentals=0),
        name="spread" if not pair else "spread_pair",
    )(*arrays)


def reduce_kernel(axes, pair, count, *refs):
    ins, outs = refs[:count], refs[count : 2 * count]
    rest = list(refs[2 * count :])
    send, recv = rest[:2]
    rest = rest[2:]
    if pair:
        psend, precv = rest[:2]
        rest = rest[2:]
    streams = []
    for a in range(count):
        if pair:
            got, held, pgot, psum = rest[:4]
            rest = rest[4:]
            place = Place(axes, None)
            half = outs[a].shape[1]
            mine = pl.ds(pl.multiple_of(place.sec * half, 128), half)
            other = pl.ds(pl.multiple_of((1 - place.sec) * half, 128), half)
            streams.append(dict(place=place, got=got, held=held, pgot=pgot, psum=psum, raw=ins[a], mine=mine, other=other,
                                out=outs[a], rows=outs[a].shape[0]))
        else:
            got, held = rest[:2]
            rest = rest[2:]
            half = outs[a].shape[0] // 2
            for h in range(2):
                rows = pl.ds(h * half, half)
                streams.append(dict(place=Place(axes, h), got=got.at[h], held=held.at[h], raw=ins[a], span=rows,
                                    out=outs[a].at[rows], rows=half))
    step = 8 if streams[0]["rows"] % 16 else 16

    def own_ref(t, offs):
        if pair:
            return t["psum"].at[t["place"].flat(offs)]
        return t["raw"].at[t["place"].target(offs), t["span"]]

    def summed(t, sources, dest):
        def one(r, _):
            rows = pl.ds(pl.multiple_of(r * step, step), step)
            total = sources[0][rows].astype(jnp.float32)
            for source in sources[1:]:
                total = total + source[rows].astype(jnp.float32)
            dest[rows] = total.astype(dest.dtype)
            return 0

        lax.fori_loop(0, t["rows"] // step, one, 0)

    def copy(s, offs):
        t = streams[s]
        place = t["place"]
        hop, base = last_hop(offs)
        f = place.flat(offs)
        src = own_ref(t, offs) if hop[2] else t["held"].at[f // place.sizes[2]]
        return pltpu.make_async_remote_copy(
            src_ref=src, dst_ref=t["got"].at[f], send_sem=send.at[s, f], recv_sem=recv.at[s, f],
            device_id={"dp": place.target(hop)}, device_id_type=pl.DeviceIdType.MESH)

    def share(s, offs):
        t = streams[s]
        place = t["place"]
        f = place.flat(offs)
        return pltpu.make_async_remote_copy(
            src_ref=t["raw"].at[place.target((offs[0], offs[2], offs[1])), :, t["other"]], dst_ref=t["pgot"].at[f],
            send_sem=psend.at[s, f], recv_sem=precv.at[s, f],
            device_id={"section": 1 - place.sec}, device_id_type=pl.DeviceIdType.MESH)

    ids = range(len(streams))
    n0, n1, n2 = streams[0]["place"].sizes
    greet(axes, pair)

    def phase_pair(k):
        for j in reversed(range(n1)):
            for i in reversed(range(n2)):
                for s in ids:
                    share(s, (k, j, i)).start()

    def phase_first(k):
        for j in reversed(range(n1)):
            for i in reversed(range(n2)):
                for s in ids:
                    t = streams[s]
                    if pair:
                        share(s, (k, j, i)).wait_recv()
                        f = t["place"].flat((k, j, i))
                        summed(t, [t["raw"].at[t["place"].target((k, j, i)), :, t["mine"]], t["pgot"].at[f]], t["psum"].at[f])
                    if i:
                        copy(s, (k, j, i)).start()

    def phase_second(k):
        for j in range(1, n1):
            for s in ids:
                t = streams[s]
                for i in range(1, n2):
                    copy(s, (k, j, i)).wait_recv()
                parts = [own_ref(t, (k, j, 0))] + [t["got"].at[t["place"].flat((k, j, i))] for i in range(1, n2)]
                summed(t, parts, t["held"].at[t["place"].flat((k, j, 0)) // n2])
                copy(s, (k, j, 0)).start()

    def gathered_parts(s, k):
        t = streams[s]
        offs = [(k, 0, i) for i in range(1, n2)] + [(k, j, 0) for j in range(1, n1)]
        for o in offs:
            copy(s, o).wait_recv()
        return [own_ref(t, (k, 0, 0))] + [t["got"].at[t["place"].flat(o)] for o in offs]

    def phase_third(k):
        for s in ids:
            t = streams[s]
            parts = gathered_parts(s, k)
            if k:
                summed(t, parts, t["held"].at[t["place"].flat((k, 0, 0)) // n2])
                copy(s, (k, 0, 0)).start()
            else:
                for q in range(1, n0):
                    copy(s, (q, 0, 0)).wait_recv()
                    parts.append(t["got"].at[t["place"].flat((q, 0, 0))])
                summed(t, parts, t["out"])

    chunks = list(range(1, n0)) + [0]
    if pair:
        phase_pair(chunks[0])
    for c in range(n0 + 3):
        if pair and c + 1 < n0:
            phase_pair(chunks[c + 1])
        if c < n0:
            phase_first(chunks[c])
        if 0 <= c - 1 < n0:
            phase_second(chunks[c - 1])
        if 0 <= c - 2 < n0:
            phase_third(chunks[c - 2])
    for s in ids:
        for offs in offsets((n0, n1, n2)):
            if any(offs):
                copy(s, offs).wait_send()
            if pair:
                share(s, offs).wait_send()


def reduce_all(arrays, count, cid, pair=False):
    axes = torus_axes(count)
    streams = len(arrays) * (1 if pair else 2)
    sem = pltpu.SemaphoreType.DMA((streams, count))
    scratch = [sem, sem]
    if pair:
        scratch += [sem, sem]
    groups = count // axes[2][1]
    out_shape = []
    for a in arrays:
        rows, cols = a.shape[1:]
        if pair:
            cols = cols // 2
            scratch += [pltpu.VMEM((count, rows, cols), a.dtype), pltpu.VMEM((groups, rows, cols), a.dtype),
                        pltpu.VMEM((count, rows, cols), a.dtype), pltpu.VMEM((count, rows, cols), a.dtype)]
        else:
            scratch += [pltpu.VMEM((2, count, rows // 2, cols), a.dtype), pltpu.VMEM((2, groups, rows // 2, cols), a.dtype)]
        out_shape.append(jax.ShapeDtypeStruct((rows, cols), jnp.float32))
    sent = sum(a.size * a.dtype.itemsize for a in arrays)
    return pl.pallas_call(
        functools.partial(reduce_kernel, axes, pair, len(arrays)),
        out_shape=out_shape,
        in_specs=[pl.BlockSpec(memory_space=pltpu.VMEM)] * len(arrays),
        out_specs=[pl.BlockSpec(memory_space=pltpu.VMEM)] * len(arrays),
        scratch_shapes=scratch,
        compiler_params=pltpu.CompilerParams(collective_id=cid, has_side_effects=True, vmem_limit_bytes=VMEM_BYTES),
        cost_estimate=pl.CostEstimate(flops=0, bytes_accessed=2 * sent, transcendentals=0),
        name="fold" if not pair else "fold_pair",
    )(*arrays)


ROWS = 128
TILE = 256
STRIP = 32


class Spread:
    def __init__(self, axes, pairs, send, recv):
        self.send, self.recv = send, recv
        self.streams = []
        for own, full in pairs:
            for h in range(2):
                rows = pl.ds(h * (ROWS // 2), ROWS // 2)
                self.streams.append((Place(axes, h), own.at[rows], lambda b, f=full, r=rows: f.at[b, r]))
        self.ids = range(len(self.streams))
        self.sizes = self.streams[0][0].sizes

    def copy(self, s, offs):
        place, own, out = self.streams[s]
        hop, base = last_hop(offs)
        block = place.source(base)
        f = place.flat(offs)
        return pltpu.make_async_remote_copy(
            src_ref=out(block) if any(base) else own, dst_ref=out(block), send_sem=self.send.at[s, f], recv_sem=self.recv.at[s, f],
            device_id={"dp": place.target(hop)}, device_id_type=pl.DeviceIdType.MESH)

    def begin(self):
        for k in range(1, self.sizes[0]):
            for s in self.ids:
                self.copy(s, (k, 0, 0)).start()

    def first(self, k):
        for s in self.ids:
            if k:
                self.copy(s, (k, 0, 0)).wait_recv()
            for j in range(1, self.sizes[1]):
                self.copy(s, (k, j, 0)).start()
            for i in range(1, self.sizes[2]):
                self.copy(s, (k, 0, i)).start()

    def second(self, k):
        for j in range(1, self.sizes[1]):
            for s in self.ids:
                self.copy(s, (k, j, 0)).wait_recv()
                for i in range(1, self.sizes[2]):
                    self.copy(s, (k, j, i)).start()

    def third(self, k):
        for j in range(self.sizes[1]):
            for i in range(1, self.sizes[2]):
                for s in self.ids:
                    self.copy(s, (k, j, i)).wait_recv()

    def end(self):
        for s in self.ids:
            for offs in offsets(self.sizes):
                if any(offs):
                    self.copy(s, offs).wait_send()


def add_rows(sources, dest, rows, step=16):
    def one(r, _):
        at = pl.ds(pl.multiple_of(r * step, step), step)
        total = sources[0][at].astype(jnp.float32)
        for source in sources[1:]:
            total = total + source[at].astype(jnp.float32)
        dest[at] = total.astype(dest.dtype)
        return 0

    lax.fori_loop(0, rows // step, one, 0)


class Fold:
    def __init__(self, axes, triples, send, recv):
        self.send, self.recv = send, recv
        self.streams = []
        for share, got, out in triples:
            for h in range(2):
                rows = pl.ds(h * (ROWS // 2), ROWS // 2)
                self.streams.append((Place(axes, h), lambda b, a=share, r=rows: a.at[b, r], got.at[h], out.at[rows]))
        self.ids = range(len(self.streams))
        self.sizes = self.streams[0][0].sizes

    def copy(self, s, offs):
        place, share, got, _ = self.streams[s]
        hop, _ = last_hop(offs)
        f = place.flat(offs)
        return pltpu.make_async_remote_copy(
            src_ref=share(place.target(offs)), dst_ref=got.at[f], send_sem=self.send.at[s, f], recv_sem=self.recv.at[s, f],
            device_id={"dp": place.target(hop)}, device_id_type=pl.DeviceIdType.MESH)

    def first(self, k):
        for j in reversed(range(self.sizes[1])):
            for i in range(1, self.sizes[2]):
                for s in self.ids:
                    self.copy(s, (k, j, i)).start()

    def second(self, k):
        for j in range(1, self.sizes[1]):
            for s in self.ids:
                self.settle(s, (k, j, 0), [(k, j, i) for i in range(1, self.sizes[2])])
                self.copy(s, (k, j, 0)).start()

    def third(self, k):
        for s in self.ids:
            arrived = [(k, 0, i) for i in range(1, self.sizes[2])] + [(k, j, 0) for j in range(1, self.sizes[1])]
            if k:
                self.settle(s, (k, 0, 0), arrived)
                self.copy(s, (k, 0, 0)).start()
            else:
                self.settle(s, (0, 0, 0), arrived + [(q, 0, 0) for q in range(1, self.sizes[0])], last=True)

    def settle(self, s, offs, arrived, last=False):
        place, share, got, out = self.streams[s]
        for o in arrived:
            self.copy(s, o).wait_recv()
        own = share(place.target(offs))
        add_rows([own] + [got.at[place.flat(o)] for o in arrived], out if last else own, ROWS // 2)

    def end(self):
        for s in self.ids:
            for offs in offsets(self.sizes):
                if any(offs):
                    self.copy(s, offs).wait_send()


def greet_all(axes):
    place = Place(axes, 0)
    barrier = pltpu.get_barrier_semaphore()
    peers = [offs for offs in offsets(place.sizes) if any(offs)]
    for offs in peers:
        pl.semaphore_signal(barrier, inc=1, device_id={"dp": place.target(offs)}, device_id_type=pl.DeviceIdType.MESH)
    pl.semaphore_wait(barrier, len(peers))


def contract(left, right, dims):
    return lax.dot_general(left, right, ((dims[:1], dims[1:]), ((), ())), preferred_element_type=jnp.float32)


def mixture_kernel(mode, axes, count, layer, *refs):
    fore, back = "f" in mode, "b" in mode
    refs = list(refs)
    take = lambda n: [refs.pop(0) for _ in range(n)]
    mask_ref, router_ref, up_own, up_other, down_own, down_other = take(6)
    x_in = take(1)[0]
    g_in = take(1)[0] if back else None
    mixed_out = take(1)[0] if fore else None
    saved_out = take(1)[0] if mode == "f" else None
    if back:
        grad_out, chance_out, up_grad_out, down_grad_out = take(4)
    up, down, xg, gates_at, weight_at, local = take(6)
    ag_send, ag_recv, rs_send, rs_recv = take(4)
    spread_pairs, fold_triples = [], []
    if fore:
        share_f, got_f, act_at = take(3)
        spread_pairs.append((x_in, xg))
        fold_triples.append((share_f, got_f, mixed_out))
    if back:
        gg, share_b, got_b, plain_at, ggu_at, actw_at, high_at, low_at, up_sum, down_sum, chance_row, chance_got, c_send, c_recv = take(14)
        spread_pairs.append((g_in, gg))
        fold_triples.append((share_b, got_b, grad_out))
    me, sec = lax.axis_index("dp"), lax.axis_index("section")
    n0, n1, n2 = [size for _, size in axes]
    plane = n1 * n2
    if back:
        greet_all(axes)
    else:
        greet(axes, False)
    spread = Spread(axes, spread_pairs, ag_send, ag_recv)
    fold = Fold(axes, fold_triples, rs_send, rs_recv)
    spread.begin()
    spread.first(0)
    loads = []

    @pl.when(sec == layer)
    def _():
        pltpu.make_async_copy(up_own, up, local.at[0]).start()
        pltpu.make_async_copy(down_own, down, local.at[1]).start()

    @pl.when(sec != layer)
    def _():
        pltpu.make_async_copy(up_other, up, local.at[0]).start()
        pltpu.make_async_copy(down_other, down, local.at[1]).start()

    if not fore:
        bring = pltpu.make_async_copy(x_in, xg, local.at[2])
        bring.start()
    else:
        xg[me] = x_in[...]
    if back:
        gg[me] = g_in[...]

        def clear(r, _):
            up_sum[pl.ds(pl.multiple_of(r * 8, 8), 8)] = jnp.zeros((8, up_sum.shape[1]), jnp.float32)
            return 0

        lax.fori_loop(0, up_sum.shape[0] // 8, clear, 0)

        def clear_down(r, _):
            down_sum[pl.ds(pl.multiple_of(r * 8, 8), 8)] = jnp.zeros((8, down_sum.shape[1]), jnp.float32)
            return 0

        lax.fori_loop(0, down_sum.shape[0] // 8, clear_down, 0)
    pltpu.make_async_copy(up_own, up, local.at[0]).wait()
    pltpu.make_async_copy(down_own, down, local.at[1]).wait()
    if not fore:
        bring.wait()

    def span(n, size=TILE):
        return pl.ds(pl.multiple_of(n * size, size), size)

    def tile(b0):
        blocks = pl.ds(b0, TILE // ROWS)
        x = xg[blocks].reshape(TILE, MODEL_WIDTH)
        lane = lax.broadcasted_iota(jnp.int32, (TILE, router_ref.shape[1]), 1)
        chance = jnp.where(lane < count, jnp.exp(dot(x, router_ref[...])), 0.0)
        total = jnp.sum(chance, axis=1, keepdims=True)
        named = mask_ref[blocks].reshape(TILE, 1)
        weight = jnp.sum(jnp.where(lane == me, chance, 0.0), axis=1, keepdims=True) / total * named
        weight_at[...] = jnp.where(lane[:, :128] == 0, weight, named)

        def gate_step(n, _):
            gates_at[:, span(n)] = dot(xg[blocks].reshape(TILE, MODEL_WIDTH), up[:, span(n)])
            return 0

        lax.fori_loop(0, 2 * FFE // TILE, gate_step, 0)
        if back:
            def plain_step(n, _):
                plain_at[:, span(n)] = contract(gg[blocks].reshape(TILE, MODEL_WIDTH), down[span(n), :], (1, 1))
                return 0

            lax.fori_loop(0, FFE // TILE, plain_step, 0)

        def strip(r, _):
            at = pl.ds(pl.multiple_of(r * STRIP, STRIP), STRIP)
            gate, raise_ = gates_at[at, :FFE], gates_at[at, FFE:]
            sigmoid = 1.0 / (1.0 + jnp.exp(-gate))
            silu = gate * sigmoid
            activated = silu * raise_
            if fore:
                act_at[at] = activated.astype(jnp.bfloat16)
            if back:
                w, m = weight_at[at, 0:1], weight_at[at, 1:2]
                plain = plain_at[at]
                grad_act = plain * w
                ggu_at[at, :FFE] = (grad_act * raise_ * sigmoid * (1.0 + gate * (1.0 - sigmoid))).astype(jnp.bfloat16)
                ggu_at[at, FFE:] = (grad_act * silu).astype(jnp.bfloat16)
                actw_at[at] = (activated * w).astype(jnp.bfloat16)
                product = activated * plain * m
                high = product.astype(jnp.bfloat16)
                high_at[at] = high
                low_at[at] = (product - high.astype(jnp.float32)).astype(jnp.bfloat16)
            return 0

        lax.fori_loop(0, TILE // STRIP, strip, 0)
        if fore:
            def share_step(n, _):
                part = dot(act_at[...], down[:, span(n)]) * weight_at[:, 0:1]
                share_f[blocks, :, span(n)] = part.astype(jnp.bfloat16).reshape(TILE // ROWS, ROWS, TILE)
                return 0

            lax.fori_loop(0, MODEL_WIDTH // TILE, share_step, 0)
        if back:
            ones = jnp.ones((8, FFE), jnp.bfloat16)
            row = contract(ones, high_at[...], (1, 1)) + contract(ones, low_at[...], (1, 1))
            for b in range(TILE // ROWS):
                chance_row[b0 + b] = row[:, b * ROWS : (b + 1) * ROWS]

            def back_step(n, _):
                part = contract(ggu_at[...], up[span(n), :], (1, 1))
                share_b[blocks, :, span(n)] = part.astype(jnp.bfloat16).reshape(TILE // ROWS, ROWS, TILE)
                return 0

            lax.fori_loop(0, MODEL_WIDTH // TILE, back_step, 0)

            def up_step(n, _):
                left = xg[blocks, :, span(n)].reshape(TILE, TILE)
                up_sum[span(n), :] += contract(left, ggu_at[...], (0, 0))
                return 0

            lax.fori_loop(0, MODEL_WIDTH // TILE, up_step, 0)

            def down_step(n, _):
                down_sum[span(n), :] += contract(actw_at[:, span(n)], gg[blocks].reshape(TILE, MODEL_WIDTH), (0, 0))
                return 0

            lax.fori_loop(0, FFE // TILE, down_step, 0)

    long_stride = axes[0][0]
    digit = lax.div(me, long_stride)

    def chunk(c, _):
        k = lax.rem(c + 1, n0)

        @pl.when(c == 0)
        def _():
            spread.first(1)
            spread.second(0)
            for t in range(2, n0):
                spread.first(t)
                spread.second(t - 1)
                spread.third(t - 2)

        @pl.when(c == 1)
        def _():
            spread.second(n0 - 1)
            spread.third(n0 - 2)

        @pl.when(c == 2)
        def _():
            spread.third(n0 - 1)

        source = lax.rem(digit - k + n0, n0)

        def step(q, _):
            tile(source * plane + q * (TILE // ROWS))
            return 0

        lax.fori_loop(0, plane * ROWS // TILE, step, 0)
        order = [(n0 - (v + 1)) % n0 for v in range(n0)]
        for v in range(n0):
            @pl.when(c == v)
            def _(v=v):
                fold.first(order[v])
                if v >= 1:
                    fold.second(order[v - 1])
                if v >= 2:
                    fold.third(order[v - 2])
        return 0

    assert n0 == 4
    lax.fori_loop(0, n0, chunk, 0)
    order = [(n0 - (v + 1)) % n0 for v in range(n0)]
    if back:
        place = Place(axes, 0)

        def chance_copy(offs):
            f = place.flat(offs)
            return pltpu.make_async_remote_copy(
                src_ref=chance_row.at[place.target(offs)], dst_ref=chance_got.at[me], send_sem=c_send.at[f], recv_sem=c_recv.at[f],
                device_id={"dp": place.target(offs)}, device_id_type=pl.DeviceIdType.MESH)

        others = [offs for offs in offsets((n0, n1, n2)) if any(offs)]
        for offs in others:
            chance_copy(offs).start()
        chance_got[me] = chance_row[me]
        outs = [pltpu.make_async_copy(up_sum, up_grad_out, local.at[0]), pltpu.make_async_copy(down_sum, down_grad_out, local.at[1])]
        for c in outs:
            c.start()
    if saved_out is not None:
        save = pltpu.make_async_copy(xg, saved_out, local.at[2])
        save.start()
    fold.second(order[n0 - 1])
    fold.third(order[n0 - 2])
    fold.third(order[n0 - 1])
    spread.end()
    fold.end()
    if back:
        for offs in others:
            chance_copy(offs).wait()
        chance_out[...] = chance_got[...]
        for c in outs:
            c.wait()
    if saved_out is not None:
        save.wait()


def mixture_call(mode, count, layer, cid, mask, router, expert, partner, x, g=None):
    axes = torus_axes(count)
    fore, back = "f" in mode, "b" in mode
    vmem, anywhere = pl.BlockSpec(memory_space=pltpu.VMEM), pl.BlockSpec(memory_space=pl.ANY)
    args = [mask, router, expert[0], partner[0], expert[1], partner[1], x]
    in_specs = [vmem, vmem] + [anywhere] * 4 + [vmem if fore else anywhere]
    if back:
        args.append(g)
        in_specs.append(vmem)
    whole = (count, ROWS, MODEL_WIDTH)
    out_shape, out_specs = [], []
    block = jax.ShapeDtypeStruct((ROWS, MODEL_WIDTH), jnp.float32)
    if fore:
        out_shape.append(block)
        out_specs.append(vmem)
    if mode == "f":
        out_shape.append(jax.ShapeDtypeStruct(whole, jnp.bfloat16))
        out_specs.append(anywhere)
    if back:
        out_shape += [block, jax.ShapeDtypeStruct((count, 8, ROWS), jnp.float32)]
        out_shape += [jax.ShapeDtypeStruct(w.shape, jnp.float32) for w in expert]
        out_specs += [vmem, vmem, anywhere, anywhere]
    streams = 2 * (fore + back)
    dma = pltpu.SemaphoreType.DMA
    scratch = [pltpu.VMEM(expert[0].shape, jnp.bfloat16), pltpu.VMEM(expert[1].shape, jnp.bfloat16), pltpu.VMEM(whole, jnp.bfloat16),
               pltpu.VMEM((TILE, 2 * FFE), jnp.float32), pltpu.VMEM((TILE, 128), jnp.float32), dma((3,))]
    ag = streams if mode != "b" else 2
    scratch += [dma((ag, count)), dma((ag, count)), dma((streams, count)), dma((streams, count))]
    half = pltpu.VMEM((2, count, ROWS // 2, MODEL_WIDTH), jnp.bfloat16)
    low = lambda width: pltpu.VMEM((TILE, width), jnp.bfloat16)
    if fore:
        scratch += [pltpu.VMEM(whole, jnp.bfloat16), half, low(FFE)]
    if back:
        scratch += [pltpu.VMEM(whole, jnp.bfloat16), pltpu.VMEM(whole, jnp.bfloat16), half, pltpu.VMEM((TILE, FFE), jnp.float32),
                    low(2 * FFE), low(FFE), low(FFE), low(FFE), pltpu.VMEM(expert[0].shape, jnp.float32),
                    pltpu.VMEM(expert[1].shape, jnp.float32), pltpu.VMEM((count, 8, ROWS), jnp.float32),
                    pltpu.VMEM((count, 8, ROWS), jnp.float32), dma((count,)), dma((count,))]
    rows = count * ROWS
    flops = rows * 6 * MODEL_WIDTH * FFE * (fore + 2 * back + (mode == "b"))
    return pl.pallas_call(
        functools.partial(mixture_kernel, mode, axes, count, layer),
        out_shape=out_shape,
        in_specs=in_specs,
        out_specs=out_specs,
        scratch_shapes=scratch,
        compiler_params=pltpu.CompilerParams(collective_id=cid, has_side_effects=True, vmem_limit_bytes=VMEM_BYTES),
        cost_estimate=pl.CostEstimate(flops=flops, bytes_accessed=4 * rows * MODEL_WIDTH, transcendentals=rows * FFE),
        name="mixture_" + mode,
    )(*args)

def swapped(value):
    return lax.ppermute(value, "section", [(0, 1), (1, 0)])


def layout(length_row):
    seq_ends = jnp.cumsum(length_row)
    seq_starts = seq_ends - length_row
    row_ids = jnp.arange(DEVICE_ROWS, dtype=jnp.int32)
    segment = jnp.sum((row_ids[:, None] >= seq_ends[None, :]).astype(jnp.int32), axis=-1)
    member = (segment[:, None] == jnp.arange(NSEQ, dtype=jnp.int32)[None, :]).astype(jnp.int32)
    token_position = row_ids - jnp.sum(member * seq_starts[None, :], axis=-1)
    return segment, token_position


def rotation(token_position):
    half_width = HEAD_SIZE // 2
    frequency = 10000.0 ** (-2.0 * jnp.arange(half_width, dtype=jnp.float32) / HEAD_SIZE)
    angles = token_position.astype(jnp.float32)[:, None] * frequency
    return jnp.cos(angles)[:, None, :], jnp.sin(angles)[:, None, :]


def rotary_embedding(values, cosine, sine):
    half_width = HEAD_SIZE // 2
    former, latter = values[..., :half_width], values[..., half_width:]
    return jnp.concatenate([former * cosine - latter * sine, latter * cosine + former * sine], axis=-1)


def dot(left, right):
    return jnp.dot(left, right, preferred_element_type=jnp.float32)


def dot_rows(left, right):
    return lax.dot_general(left, right, (((0,), (0,)), ((), ())), preferred_element_type=jnp.float32)


def dot_columns(left, right):
    return lax.dot_general(left, right, (((1,), (1,)), ((), ())), preferred_element_type=jnp.float32)


def router_chances(normed_two, router):
    chance = jnp.exp(dot(normed_two, router))
    return chance / jnp.sum(chance, axis=-1, keepdims=True)


def front(hidden, place, weights):
    joint, result_output, router, gain_attention, gain_mixture = weights
    allowed, cosine, sine = place
    rows = hidden.shape[0]
    inverse_one = lax.rsqrt(jnp.mean(hidden * hidden, axis=-1, keepdims=True) + norm_epsilon)
    scaled_one = hidden * inverse_one
    normed = (scaled_one * gain_attention).astype(jnp.bfloat16)
    projected = dot(normed, joint)
    query = rotary_embedding(projected[:, :QUERY_WIDTH].reshape(rows, QUERY_HEADS, HEAD_SIZE), cosine, sine)
    query = query.astype(jnp.bfloat16).reshape(rows, KEY_VALUE_HEADS, GROUP, HEAD_SIZE)
    key = rotary_embedding(projected[:, QUERY_WIDTH : QUERY_WIDTH + KEY_WIDTH].reshape(rows, KEY_VALUE_HEADS, HEAD_SIZE), cosine, sine)
    key = key.astype(jnp.bfloat16)
    value = projected[:, QUERY_WIDTH + KEY_WIDTH :].reshape(rows, KEY_VALUE_HEADS, HEAD_SIZE).astype(jnp.bfloat16)
    scores = jnp.einsum("qhgd,khd->hgqk", query, key, preferred_element_type=jnp.float32) * SCORE_SCALE
    exponent = jnp.where(allowed, jnp.exp(scores), 0.0)
    attention = exponent / jnp.sum(exponent, axis=-1, keepdims=True)
    context = jnp.einsum("hgqk,khd->qhgd", attention.astype(jnp.bfloat16), value, preferred_element_type=jnp.float32)
    context = context.reshape(rows, QUERY_WIDTH).astype(jnp.bfloat16)
    middle = hidden + dot(context, result_output)
    inverse_two = lax.rsqrt(jnp.mean(middle * middle, axis=-1, keepdims=True) + norm_epsilon)
    scaled_two = middle * inverse_two
    normed_two = (scaled_two * gain_mixture).astype(jnp.bfloat16)
    kept = (inverse_one, scaled_one, normed, query, key, value, attention, context, inverse_two, scaled_two, normed_two)
    return middle, normed_two, kept


def gates(everyone, up_weight):
    both = dot(everyone, up_weight)
    return both[:, :FFE], both[:, FFE:]


def expert_forward(everyone, mask, router, expert, count, me):
    up_weight, down_weight = expert
    chance = router_chances(everyone, router)
    own = jnp.arange(count, dtype=jnp.int32) == me
    weight = jnp.sum(jnp.where(own[None, :] & mask, chance, 0.0), axis=-1)
    gate, up = gates(everyone, up_weight)
    activated = (jax.nn.silu(gate) * up).astype(jnp.bfloat16)
    share = (dot(activated, down_weight) * weight[:, None]).astype(jnp.bfloat16)
    return share, weight, (gate, up)


def expert_backward(grads, everyone, weight, mask, held, expert):
    up_weight, down_weight = expert
    gate, up = held if held is not None else gates(everyone, up_weight)
    sigmoid = jax.nn.sigmoid(gate)
    silu = gate * sigmoid
    activated = silu * up
    grad_plain = dot_columns(grads, down_weight)
    grad_weight = jnp.where(mask[:, 0], jnp.sum(activated * grad_plain, axis=-1), 0.0)
    grad_act = grad_plain * weight[:, None]
    grad_gate = grad_act * up * sigmoid * (1.0 + gate * (1.0 - sigmoid))
    grad_gate_up = jnp.concatenate([grad_gate, grad_act * silu], axis=-1).astype(jnp.bfloat16)
    grad_down = dot_rows((activated * weight[:, None]).astype(jnp.bfloat16), grads)
    grad_up_weight = dot_rows(everyone, grad_gate_up)
    share = dot_columns(grad_gate_up, up_weight).astype(jnp.bfloat16)
    return share, grad_weight, grad_up_weight, grad_down


def pieces(value):
    return value.reshape(-1, CHUNK_ROWS, *value.shape[1:])


def mixture_forward(normed_two, router, mask, expert, count, me):
    (spread,) = gather_all([normed_two], count, 0)
    everyone = spread.reshape(-1, MODEL_WIDTH)
    if everyone.shape[0] <= CHUNK_ROWS:
        share, weight, held = expert_forward(everyone, mask, router, expert, count, me)
    else:
        share, weight = lax.map(
            lambda part: expert_forward(part[0], part[1], router, expert, count, me)[:2], (pieces(everyone), pieces(mask)))
        held = None
    (mixed,) = reduce_all([share.reshape(spread.shape)], count, 1)
    return mixed, (everyone, weight.reshape(-1), held)


def mixture_backward(grad_out, mask, kept, expert, count):
    everyone, weight, held = kept
    (spread,) = gather_all([grad_out], count, 0)
    grads = spread.reshape(-1, MODEL_WIDTH)
    if grads.shape[0] <= CHUNK_ROWS:
        share, grad_weight, grad_up, grad_down = expert_backward(grads, everyone, weight, mask, held, expert)
    else:
        def step(sums, part):
            share, grad_weight, grad_up, grad_down = expert_backward(*part, None, expert)
            return (sums[0] + grad_up, sums[1] + grad_down), (share, grad_weight)

        zero = tuple(jnp.zeros(w.shape, jnp.float32) for w in expert)
        (grad_up, grad_down), (share, grad_weight) = lax.scan(
            step, zero, (pieces(grads), pieces(everyone), pieces(weight), pieces(mask)))
    grad_chance = lax.all_to_all(grad_weight.reshape(count, DEVICE_ROWS), "dp", split_axis=0, concat_axis=0, tiled=True)
    (mixed,) = reduce_all([share.reshape(spread.shape)], count, 1)
    return mixed, grad_chance.T, grad_up, grad_down


def front_backward(grad_out, grad_mixed, grad_chance, kept, place, weights):
    joint, result_output, router, gain_attention, gain_mixture = weights
    allowed, cosine, sine = place
    inverse_one, scaled_one, normed, query, key, value, attention, context, inverse_two, scaled_two, normed_two = kept
    rows = normed.shape[0]
    chance = router_chances(normed_two, router)
    grad_logit = (chance * (grad_chance - jnp.sum(grad_chance * chance, axis=-1, keepdims=True))).astype(jnp.bfloat16)
    grad_router = dot_rows(normed_two, grad_logit)
    grad_normed_two = grad_mixed + dot_columns(grad_logit, router)
    grad_gain_two = jnp.sum(grad_normed_two * scaled_two, axis=0)
    scaled_grad_two = grad_normed_two * gain_mixture
    grad_middle = grad_out + inverse_two * (scaled_grad_two - scaled_two * jnp.mean(scaled_grad_two * scaled_two, axis=-1, keepdims=True))
    branch = grad_middle.astype(jnp.bfloat16)
    grad_output = dot_rows(context, branch)
    grad_context = dot_columns(branch, result_output).astype(jnp.bfloat16).reshape(rows, KEY_VALUE_HEADS, GROUP, HEAD_SIZE)
    grad_attention = jnp.einsum("qhgd,khd->hgqk", grad_context, value, preferred_element_type=jnp.float32)
    grad_value = jnp.einsum("hgqk,qhgd->khd", attention.astype(jnp.bfloat16), grad_context, preferred_element_type=jnp.float32)
    grad_scores = (attention * (grad_attention - jnp.sum(grad_attention * attention, axis=-1, keepdims=True))).astype(jnp.bfloat16)
    grad_query = jnp.einsum("hgqk,khd->qhgd", grad_scores, key, preferred_element_type=jnp.float32).reshape(rows, QUERY_HEADS, HEAD_SIZE)
    grad_key = jnp.einsum("hgqk,qhgd->khd", grad_scores, query, preferred_element_type=jnp.float32)
    grad_query = rotary_embedding(grad_query * SCORE_SCALE, cosine, -sine)
    grad_key = rotary_embedding(grad_key * SCORE_SCALE, cosine, -sine)
    grad_projected = jnp.concatenate(
        [grad_query.reshape(rows, -1), grad_key.reshape(rows, -1), grad_value.reshape(rows, -1)], axis=-1).astype(jnp.bfloat16)
    grad_joint = dot_rows(normed, grad_projected)
    grad_normed = dot_columns(grad_projected, joint)
    grad_gain_one = jnp.sum(grad_normed * scaled_one, axis=0)
    scaled_grad_one = grad_normed * gain_attention
    grad_hidden = grad_middle + inverse_one * (scaled_grad_one - scaled_one * jnp.mean(scaled_grad_one * scaled_one, axis=-1, keepdims=True))
    return grad_hidden, (grad_joint, grad_output, grad_router, grad_gain_one, grad_gain_two)


def small_halves(rows, router, gains, codes):
    second = jnp.concatenate([gains, codes], axis=1)
    width = -(-max(router.shape[1], second.shape[1]) // 128) * 128
    pad = lambda v: jnp.pad(v, ((0, 0), (0, width - v.shape[1])))
    return pad(router), pad(second)


def body(tokens, cotangent, lengths, routes, combined_weight, output_weight, router_weight, attention_gain, mixture_gain,
         expert_gate_up, expert_down):
    count = lax.axis_size("dp")
    me, sec = lax.axis_index("dp"), lax.axis_index("section")
    layers = lax.axis_size("section")
    leading = sec == 0
    shard = combined_weight.shape[1]
    micro = lambda a, axis: lax.dynamic_index_in_dim(a, sec, axis, keepdims=False)

    gains = jnp.stack([attention_gain[0], mixture_gain[0]], axis=1)
    codes = routes[0].astype(jnp.bfloat16).reshape(-1)
    code_count = codes.shape[0]
    codes = jnp.pad(codes, (0, -code_count % shard)).reshape(shard, -1)
    small = small_halves(shard, router_weight[0], gains, codes)
    small_width = small[0].shape[1]
    halves = [
        (combined_weight[0, :, : combined_weight.shape[2] // 2], combined_weight[0, :, combined_weight.shape[2] // 2 :]),
        (output_weight[0, :, : output_weight.shape[2] // 2], output_weight[0, :, output_weight.shape[2] // 2 :]),
        small,
    ]
    widths = [h[0].shape[1] for h in halves]
    mine = jnp.concatenate([jnp.where(leading, a, b) for a, b in halves], axis=1)
    given = swapped(jnp.concatenate([jnp.where(leading, b, a) for a, b in halves], axis=1))
    packs = [jnp.where(leading, mine, given), jnp.where(leading, given, mine)]
    partner_expert = tuple(swapped(w[0, 0]) for w in (expert_gate_up, expert_down))
    own_expert = (expert_gate_up[0, 0], expert_down[0, 0])
    fused = count * DEVICE_ROWS <= CHUNK_ROWS
    experts, routers = [], []
    for layer in range(0 if fused else layers):
        keep = sec == layer
        experts.append((jnp.where(keep, expert_gate_up[0, 0], partner_expert[0]), jnp.where(keep, expert_down[0, 0], partner_expert[1])))

    def layer_weights(layer):
        at, parts = 0, []
        for w in widths:
            parts.append(packs[layer][:, at : at + w])
            at += w
        joint, output, tail = gather_all(parts, count, 2, pair=True)
        joint = joint.reshape(MODEL_WIDTH, -1)
        output = output.reshape(MODEL_WIDTH, -1)
        tail = tail.reshape(MODEL_WIDTH, -1)
        second = tail[:, small_width:]
        weights = (joint, output, tail[:, : router_weight.shape[2]], second[:, 0].astype(jnp.float32), second[:, 1].astype(jnp.float32))
        routers.append(tail[:, :small_width])
        code = second[:, 2 : 2 + codes.shape[1]].reshape(count, -1)[:, :code_count].reshape(count, -1, DEVICE_ROWS, TOPK)
        named = lax.dynamic_index_in_dim(code, sec, 1, keepdims=False).reshape(count * DEVICE_ROWS, TOPK)
        mask = jnp.any(named == me.astype(jnp.bfloat16), axis=-1, keepdims=True)
        return weights, mask

    segment, token_position = layout(micro(lengths[:, 0], 0))
    row_ids = jnp.arange(DEVICE_ROWS, dtype=jnp.int32)
    allowed = (row_ids[:, None] >= row_ids[None, :]) & (segment[:, None] == segment[None, :])
    place = (allowed,) + rotation(token_position)

    weights, masks, stores = [], [], []
    hidden = micro(tokens, 0)
    for layer in range(layers):
        got, mask = layer_weights(layer)
        weights.append(got)
        masks.append(mask)
        middle, normed_two, kept = front(hidden.astype(jnp.float32), place, got)
        if not fused:
            mixed, kept_mixture = mixture_forward(normed_two, got[2], mask, experts[layer], count, me)
        else:
            named = mask.astype(jnp.float32).reshape(count, DEVICE_ROWS, 1)
            call = lambda mode, cid, *data: mixture_call(mode, count, layer, cid, named, routers[layer], own_expert, partner_expert, *data)
            if layer < layers - 1:
                mixed, everyone = call("f", 4, normed_two)
                kept_mixture = (named, everyone)
            else:
                mixed, *kept_mixture = call("fb", 5, normed_two, micro(cotangent, 0))
        hidden = (middle + mixed).astype(jnp.bfloat16)
        stores.append((kept, kept_mixture))
    last = hidden
    grad = micro(cotangent, 0)
    shares, expert_grads = [None] * layers, [None] * layers
    for layer in reversed(range(layers)):
        kept, kept_mixture = stores[layer]
        if not fused:
            mixed, grad_chance, grad_up, grad_down = mixture_backward(grad, masks[layer], kept_mixture, experts[layer], count)
        else:
            if layer < layers - 1:
                named, everyone = kept_mixture
                kept_mixture = mixture_call("b", count, layer, 6, named, routers[layer], own_expert, partner_expert, everyone, grad)
            mixed, rows, grad_up, grad_down = kept_mixture
            grad_chance = rows[:, 0].T
        expert_grads[layer] = (grad_up, grad_down)
        grad_hidden, parts = front_backward(grad.astype(jnp.float32), mixed, grad_chance, kept, place, weights[layer])
        grad = grad_hidden.astype(jnp.bfloat16)
        tail = small_halves(MODEL_WIDTH, parts[2], jnp.stack([parts[3], parts[4]], axis=1), parts[2][:, :0])
        packed = [parts[0], parts[1], jnp.concatenate(tail, axis=1)]
        packed = [a.astype(jnp.bfloat16).reshape(count, shard, -1) for a in packed]
        shares[layer] = reduce_all(packed, count, 3, pair=True)
    outs = []
    for a in range(3):
        kept_half = jnp.where(leading, shares[0][a], shares[1][a])
        got_half = swapped(jnp.where(leading, shares[1][a], shares[0][a]))
        outs.append(jnp.concatenate([jnp.where(leading, kept_half, got_half), jnp.where(leading, got_half, kept_half)], axis=1))
    expert_outs = []
    for a in range(2):
        kept_sum = jnp.where(leading, expert_grads[0][a], expert_grads[1][a])
        got_sum = swapped(jnp.where(leading, expert_grads[1][a], expert_grads[0][a]))
        expert_outs.append((kept_sum + got_sum)[None, None])
    partner = swapped(jnp.where(leading, last, grad))
    boundary = jnp.where(leading, jnp.stack([grad, partner]), jnp.stack([partner, last]))[None]
    half = outs[2].shape[1] // 2
    return (
        boundary,
        outs[0][None],
        outs[1][None],
        outs[2][None, :, : router_weight.shape[2]],
        outs[2][None, :, half],
        outs[2][None, :, half + 1],
        expert_outs[0],
        expert_outs[1],
    )


def solution(mesh):
    return jax.shard_map(
        body,
        mesh=mesh,
        in_specs=(
            P(None, "dp", None),
            P(None, "dp", None),
            P(None, "dp", None),
            P("section", None, "dp", None),
            P("section", "dp", None),
            P("section", "dp", None),
            P("section", "dp", None),
            P("section", "dp"),
            P("section", "dp"),
            P("section", "dp", None, None),
            P("section", "dp", None, None),
        ),
        out_specs=(
            P("section", None, "dp", None),
            P("section", "dp", None),
            P("section", "dp", None),
            P("section", "dp", None),
            P("section", "dp"),
            P("section", "dp"),
            P("section", "dp", None, None),
            P("section", "dp", None, None),
        ),
        check_vma=False,
    )
```

```python
import functools
import jax
import jax.numpy as jnp
from jax import lax
from jax.experimental import pallas as pl
from jax.experimental.pallas import tpu as pltpu
from jax.sharding import PartitionSpec as P

MODEL_WIDTH = 1536
QUERY_HEADS = 24
KEY_VALUE_HEADS = 8
GROUP = QUERY_HEADS // KEY_VALUE_HEADS
HEAD_SIZE = 64
FFE = 512
TOPK = 8
DEVICE_ROWS = 128
NSEQ = 4
QUERY_WIDTH = QUERY_HEADS * HEAD_SIZE
KEY_WIDTH = KEY_VALUE_HEADS * HEAD_SIZE
SCORE_SCALE = HEAD_SIZE ** (-0.5)
norm_epsilon = 1e-06
CHUNK_ROWS = 2048

VMEM_BYTES = 66_000_000


def torus_axes(count):
    side = 1
    while (side + 1) ** 3 <= count:
        side += 1
    assert count % (side * side) == 0
    return [(side * side, count // (side * side)), (1, side), (side, side)]


def offsets(sizes):
    return [(k, j, i) for k in range(sizes[0]) for j in range(sizes[1]) for i in range(sizes[2])]


class Place:
    def __init__(self, axes, order):
        self.me = lax.axis_index("dp")
        self.sec = lax.axis_index("section")
        long, first, second = axes
        if order is None:
            flip = self.sec
            stride_one = first[0] + (second[0] - first[0]) * flip
            stride_two = second[0] + (first[0] - second[0]) * flip
            assert first[1] == second[1]
            self.axes = [long, (stride_one, first[1]), (stride_two, second[1])]
        elif order == 0:
            self.axes = [long, first, second]
        else:
            self.axes = [long, second, first]
        self.sizes = [size for _, size in self.axes]

    def moved(self, steps):
        out = self.me
        for (stride, size), step in zip(self.axes, steps):
            if step % size:
                digit = lax.rem(lax.div(self.me, stride), size)
                out = out + (lax.rem(digit + (step % size), size) - digit) * stride
        return out

    def source(self, offs):
        return self.moved([-o for o in offs])

    def target(self, offs):
        return self.moved(list(offs))

    def flat(self, offs):
        return (offs[0] * self.sizes[1] + offs[1]) * self.sizes[2] + offs[2]


def last_hop(offs):
    for axis in (2, 1, 0):
        if offs[axis]:
            hop = [0, 0, 0]
            hop[axis] = offs[axis]
            base = list(offs)
            base[axis] = 0
            return tuple(hop), tuple(base)
    return None


def greet(axes, pair):
    place = Place(axes, 0)
    barrier = pltpu.get_barrier_semaphore()
    count = 0
    for axis in range(3):
        for step in range(1, place.sizes[axis]):
            hop = [0, 0, 0]
            hop[axis] = step
            pl.semaphore_signal(barrier, inc=1, device_id={"dp": place.target(hop)}, device_id_type=pl.DeviceIdType.MESH)
            count += 1
    if pair:
        pl.semaphore_signal(barrier, inc=1, device_id={"section": 1 - place.sec}, device_id_type=pl.DeviceIdType.MESH)
        count += 1
    pl.semaphore_wait(barrier, count)


def gather_kernel(axes, pair, count, *refs):
    ins, outs = refs[:count], refs[count : 2 * count]
    send, recv, local = refs[2 * count : 2 * count + 3]
    psend, precv = refs[2 * count + 3 :] if pair else (None, None)
    streams = []
    for a in range(count):
        if pair:
            place = Place(axes, None)
            half = ins[a].shape[1]
            cols = pl.ds(pl.multiple_of(place.sec * half, 128), half)
            streams.append((place, ins[a], lambda b, o=outs[a], c=cols: o.at[b, :, c]))
        else:
            half = ins[a].shape[0] // 2
            for h in range(2):
                rows = pl.ds(h * half, half)
                streams.append((Place(axes, h), ins[a].at[rows], lambda b, o=outs[a], r=rows: o.at[b, r]))

    def copy(s, offs):
        place, own, out = streams[s]
        hop, base = last_hop(offs)
        block = place.source(base)
        src = out(block) if any(base) else own
        f = place.flat(offs)
        return pltpu.make_async_remote_copy(
            src_ref=src, dst_ref=out(block), send_sem=send.at[s, f], recv_sem=recv.at[s, f],
            device_id={"dp": place.target(hop)}, device_id_type=pl.DeviceIdType.MESH)

    def share(s, offs):
        place, own, out = streams[s]
        block = place.source(offs)
        src = out(block) if any(offs) else own
        f = place.flat(offs)
        return pltpu.make_async_remote_copy(
            src_ref=src, dst_ref=out(block), send_sem=psend.at[s, f], recv_sem=precv.at[s, f],
            device_id={"section": 1 - place.sec}, device_id_type=pl.DeviceIdType.MESH)

    greet(axes, pair)
    ids = range(len(streams))
    n0, n1, n2 = streams[0][0].sizes
    keep = []
    for s in ids:
        place, own, out = streams[s]
        c = pltpu.make_async_copy(own, out(place.me), local.at[s])
        c.start()
        keep.append(c)
    for k in range(1, n0):
        for s in ids:
            copy(s, (k, 0, 0)).start()

    def first(k):
        for s in ids:
            if k:
                copy(s, (k, 0, 0)).wait_recv()
            for j in range(1, n1):
                copy(s, (k, j, 0)).start()
            for i in range(1, n2):
                copy(s, (k, 0, i)).start()
            if pair:
                share(s, (k, 0, 0)).start()

    def second(k):
        for j in range(1, n1):
            for s in ids:
                copy(s, (k, j, 0)).wait_recv()
                for i in range(1, n2):
                    copy(s, (k, j, i)).start()
                if pair:
                    share(s, (k, j, 0)).start()

    def third(k):
        for j in range(n1):
            for i in range(1, n2):
                for s in ids:
                    copy(s, (k, j, i)).wait_recv()
                    if pair:
                        share(s, (k, j, i)).start()

    for k in range(n0 + 2):
        if k < n0:
            first(k)
        if 0 <= k - 1 < n0:
            second(k - 1)
        if 0 <= k - 2 < n0:
            third(k - 2)
    for s in ids:
        for offs in offsets((n0, n1, n2)):
            if any(offs):
                copy(s, offs).wait_send()
            if pair:
                share(s, offs).wait()
    for c in keep:
        c.wait()


def gather_all(arrays, count, cid, pair=False):
    axes = torus_axes(count)
    streams = len(arrays) * (1 if pair else 2)
    sem = pltpu.SemaphoreType.DMA((streams, count))
    out_shape = [jax.ShapeDtypeStruct((count, a.shape[0], a.shape[1] * (2 if pair else 1)), a.dtype) for a in arrays]
    scratch = [sem, sem, pltpu.SemaphoreType.DMA((streams,))]
    if pair:
        scratch += [sem, sem]
    sent = sum(a.size * a.dtype.itemsize for a in arrays) * (count - 1)
    return pl.pallas_call(
        functools.partial(gather_kernel, axes, pair, len(arrays)),
        out_shape=out_shape,
        in_specs=[pl.BlockSpec(memory_space=pltpu.VMEM)] * len(arrays),
        out_specs=[pl.BlockSpec(memory_space=pl.ANY)] * len(arrays),
        scratch_shapes=scratch,
        compiler_params=pltpu.CompilerParams(collective_id=cid, has_side_effects=True),
        cost_estimate=pl.CostEstimate(flops=0, bytes_accessed=2 * sent, transcendentals=0),
        name="spread" if not pair else "spread_pair",
    )(*arrays)


def reduce_kernel(axes, pair, count, *refs):
    ins, outs = refs[:count], refs[count : 2 * count]
    rest = list(refs[2 * count :])
    send, recv = rest[:2]
    rest = rest[2:]
    if pair:
        psend, precv = rest[:2]
        rest = rest[2:]
    streams = []
    for a in range(count):
        if pair:
            got, held, pgot, psum = rest[:4]
            rest = rest[4:]
            place = Place(axes, None)
            half = outs[a].shape[1]
            mine = pl.ds(pl.multiple_of(place.sec * half, 128), half)
            other = pl.ds(pl.multiple_of((1 - place.sec) * half, 128), half)
            streams.append(dict(place=place, got=got, held=held, pgot=pgot, psum=psum, raw=ins[a], mine=mine, other=other,
                                out=outs[a], rows=outs[a].shape[0]))
        else:
            got, held = rest[:2]
            rest = rest[2:]
            half = outs[a].shape[0] // 2
            for h in range(2):
                rows = pl.ds(h * half, half)
                streams.append(dict(place=Place(axes, h), got=got.at[h], held=held.at[h], raw=ins[a], span=rows,
                                    out=outs[a].at[rows], rows=half))
    step = 8 if streams[0]["rows"] % 16 else 16

    def own_ref(t, offs):
        if pair:
            return t["psum"].at[t["place"].flat(offs)]
        return t["raw"].at[t["place"].target(offs), t["span"]]

    def summed(t, sources, dest):
        def one(r, _):
            rows = pl.ds(pl.multiple_of(r * step, step), step)
            total = sources[0][rows].astype(jnp.float32)
            for source in sources[1:]:
                total = total + source[rows].astype(jnp.float32)
            dest[rows] = total.astype(dest.dtype)
            return 0

        lax.fori_loop(0, t["rows"] // step, one, 0)

    def copy(s, offs):
        t = streams[s]
        place = t["place"]
        hop, base = last_hop(offs)
        f = place.flat(offs)
        src = own_ref(t, offs) if hop[2] else t["held"].at[f // place.sizes[2]]
        return pltpu.make_async_remote_copy(
            src_ref=src, dst_ref=t["got"].at[f], send_sem=send.at[s, f], recv_sem=recv.at[s, f],
            device_id={"dp": place.target(hop)}, device_id_type=pl.DeviceIdType.MESH)

    def share(s, offs):
        t = streams[s]
        place = t["place"]
        f = place.flat(offs)
        return pltpu.make_async_remote_copy(
            src_ref=t["raw"].at[place.target((offs[0], offs[2], offs[1])), :, t["other"]], dst_ref=t["pgot"].at[f],
            send_sem=psend.at[s, f], recv_sem=precv.at[s, f],
            device_id={"section": 1 - place.sec}, device_id_type=pl.DeviceIdType.MESH)

    ids = range(len(streams))
    n0, n1, n2 = streams[0]["place"].sizes
    greet(axes, pair)

    def phase_pair(k):
        for j in reversed(range(n1)):
            for i in reversed(range(n2)):
                for s in ids:
                    share(s, (k, j, i)).start()

    def phase_first(k):
        for j in reversed(range(n1)):
            for i in reversed(range(n2)):
                for s in ids:
                    t = streams[s]
                    if pair:
                        share(s, (k, j, i)).wait_recv()
                        f = t["place"].flat((k, j, i))
                        summed(t, [t["raw"].at[t["place"].target((k, j, i)), :, t["mine"]], t["pgot"].at[f]], t["psum"].at[f])
                    if i:
                        copy(s, (k, j, i)).start()

    def phase_second(k):
        for j in range(1, n1):
            for s in ids:
                t = streams[s]
                for i in range(1, n2):
                    copy(s, (k, j, i)).wait_recv()
                parts = [own_ref(t, (k, j, 0))] + [t["got"].at[t["place"].flat((k, j, i))] for i in range(1, n2)]
                summed(t, parts, t["held"].at[t["place"].flat((k, j, 0)) // n2])
                copy(s, (k, j, 0)).start()

    def gathered_parts(s, k):
        t = streams[s]
        offs = [(k, 0, i) for i in range(1, n2)] + [(k, j, 0) for j in range(1, n1)]
        for o in offs:
            copy(s, o).wait_recv()
        return [own_ref(t, (k, 0, 0))] + [t["got"].at[t["place"].flat(o)] for o in offs]

    def phase_third(k):
        for s in ids:
            t = streams[s]
            parts = gathered_parts(s, k)
            if k:
                summed(t, parts, t["held"].at[t["place"].flat((k, 0, 0)) // n2])
                copy(s, (k, 0, 0)).start()
            else:
                for q in range(1, n0):
                    copy(s, (q, 0, 0)).wait_recv()
                    parts.append(t["got"].at[t["place"].flat((q, 0, 0))])
                summed(t, parts, t["out"])

    chunks = list(range(1, n0)) + [0]
    if pair:
        phase_pair(chunks[0])
    for c in range(n0 + 3):
        if pair and c + 1 < n0:
            phase_pair(chunks[c + 1])
        if c < n0:
            phase_first(chunks[c])
        if 0 <= c - 1 < n0:
            phase_second(chunks[c - 1])
        if 0 <= c - 2 < n0:
            phase_third(chunks[c - 2])
    for s in ids:
        for offs in offsets((n0, n1, n2)):
            if any(offs):
                copy(s, offs).wait_send()
            if pair:
                share(s, offs).wait_send()


def reduce_all(arrays, count, cid, pair=False):
    axes = torus_axes(count)
    streams = len(arrays) * (1 if pair else 2)
    sem = pltpu.SemaphoreType.DMA((streams, count))
    scratch = [sem, sem]
    if pair:
        scratch += [sem, sem]
    groups = count // axes[2][1]
    out_shape = []
    for a in arrays:
        rows, cols = a.shape[1:]
        if pair:
            cols = cols // 2
            scratch += [pltpu.VMEM((count, rows, cols), a.dtype), pltpu.VMEM((groups, rows, cols), a.dtype),
                        pltpu.VMEM((count, rows, cols), a.dtype), pltpu.VMEM((count, rows, cols), a.dtype)]
        else:
            scratch += [pltpu.VMEM((2, count, rows // 2, cols), a.dtype), pltpu.VMEM((2, groups, rows // 2, cols), a.dtype)]
        out_shape.append(jax.ShapeDtypeStruct((rows, cols), jnp.float32))
    sent = sum(a.size * a.dtype.itemsize for a in arrays)
    return pl.pallas_call(
        functools.partial(reduce_kernel, axes, pair, len(arrays)),
        out_shape=out_shape,
        in_specs=[pl.BlockSpec(memory_space=pltpu.VMEM)] * len(arrays),
        out_specs=[pl.BlockSpec(memory_space=pltpu.VMEM)] * len(arrays),
        scratch_shapes=scratch,
        compiler_params=pltpu.CompilerParams(collective_id=cid, has_side_effects=True, vmem_limit_bytes=VMEM_BYTES),
        cost_estimate=pl.CostEstimate(flops=0, bytes_accessed=2 * sent, transcendentals=0),
        name="fold" if not pair else "fold_pair",
    )(*arrays)


ROWS = 128
TILE = 512
STRIP = 16
SPAN = 512
SKIP = set()
PIECE = 256
MESH = pl.DeviceIdType.MESH
TOKEN_PARTS = (((0, 1, 2), 0, 64), ((0, 2, 1), 64, 64))


class Route:
    def __init__(self, axes, order):
        self.axes, self.order = axes, order
        self.sizes = [size for _, size in axes]
        self.me = lax.axis_index("dp")
        self.all = offsets(self.sizes)
        self.others = [o for o in self.all if any(o)]

    def moved(self, steps):
        out = self.me
        for (stride, size), step in zip(self.axes, steps):
            if step % size:
                digit = lax.rem(lax.div(self.me, stride), size)
                out = out + (lax.rem(digit + (step % size), size) - digit) * stride
        return out

    def source(self, offs):
        return self.moved([-o for o in offs])

    def target(self, offs):
        return self.moved(list(offs))

    def flat(self, offs):
        return (offs[0] * self.sizes[1] + offs[1]) * self.sizes[2] + offs[2]

    def last_axis(self, offs):
        for axis in reversed(self.order):
            if offs[axis]:
                return axis

    def base(self, offs):
        out = list(offs)
        out[self.last_axis(offs)] = 0
        return tuple(out)

    def hop(self, offs):
        axis = self.last_axis(offs)
        out = [0, 0, 0]
        out[axis] = offs[axis]
        return tuple(out)

    def children(self, offs):
        return [o for o in self.others if self.base(o) == offs]


class Spread:
    def __init__(self, streams, send, recv, psend=None, precv=None):
        self.streams, self.send, self.recv, self.psend, self.precv = streams, send, recv, psend, precv
        self.ids = range(len(streams))

    def copy(self, s, offs):
        route, own, out = self.streams[s]
        base = route.base(offs)
        block, f = route.source(base), route.flat(offs)
        return pltpu.make_async_remote_copy(
            src_ref=out(block) if any(base) else own, dst_ref=out(block), send_sem=self.send.at[s, f], recv_sem=self.recv.at[s, f],
            device_id={"dp": route.target(route.hop(offs))}, device_id_type=MESH)

    def share(self, s, offs):
        route, own, out = self.streams[s]
        block, f = route.source(offs), route.flat(offs)
        return pltpu.make_async_remote_copy(
            src_ref=out(block) if any(offs) else own, dst_ref=out(block), send_sem=self.psend.at[s, f], recv_sem=self.precv.at[s, f],
            device_id={"section": 1 - lax.axis_index("section")}, device_id_type=MESH)

    def step(self, t):
        if "comm" in SKIP:
            return
        work = [(offs, s) for s in self.ids for offs in self.streams[s][0].all if offs[0] + (offs[1] > 0) + (offs[2] > 0) == t]
        kids = {(offs, s): self.streams[s][0].children(offs) for offs, s in work}
        if t == 0:
            for child, s in sorted([(child, s) for offs, s in work for child in kids[offs, s]], key=lambda e: (e[0][0], e[0], e[1])):
                self.copy(s, child).start()
            kids = {e: [] for e in work}
        for offs, s in sorted(work, key=lambda e: (not kids[e], -e[0][0], e[0], e[1])):
            if any(offs):
                self.copy(s, offs).wait_recv()
            for child in kids[offs, s]:
                self.copy(s, child).start()
            if self.psend is not None:
                self.share(s, offs).start()

    def end(self):
        if "comm" in SKIP:
            return
        for s in self.ids:
            route = self.streams[s][0]
            for offs in route.all:
                if any(offs):
                    self.copy(s, offs).wait_send()
                if self.psend is not None:
                    self.share(s, offs).wait()


def add_rows(sources, dest, rows, step=16):
    def one(r, _):
        at = pl.ds(pl.multiple_of(r * step, step), step)
        total = sources[0][at].astype(jnp.float32)
        for source in sources[1:]:
            total = total + source[at].astype(jnp.float32)
        dest[at] = total.astype(dest.dtype)
        return 0

    lax.fori_loop(0, rows // step, one, 0)


class Fold:
    def __init__(self, streams, send, recv, chunks):
        self.streams, self.send, self.recv = streams, send, recv
        self.ids = range(len(streams))
        self.turn = {k: c for c, k in enumerate(chunks)}

    def when(self, route, offs):
        return max([self.turn[offs[0]]] + [self.when(route, o) + 1 for o in route.children(offs)])

    def copy(self, s, offs):
        route, share, got, _, _ = self.streams[s]
        f = route.flat(offs)
        return pltpu.make_async_remote_copy(
            src_ref=share(offs), dst_ref=got(f), send_sem=self.send.at[s, f], recv_sem=self.recv.at[s, f],
            device_id={"dp": route.target(route.hop(offs))}, device_id_type=MESH)

    def step(self, t):
        if "comm" in SKIP:
            return
        work = [(offs, s) for s in self.ids for offs in self.streams[s][0].all if self.when(self.streams[s][0], offs) == t]
        kids = {(offs, s): self.streams[s][0].children(offs) for offs, s in work}
        for offs, s in sorted(work, key=lambda e: (bool(kids[e]), not (e[0][1] or e[0][2]), [-o for o in e[0]], e[1])):
            route, share, got, out, rows = self.streams[s]
            for o in kids[offs, s]:
                self.copy(s, o).wait_recv()
            if kids[offs, s]:
                own = share(offs)
                add_rows([own] + [got(route.flat(o)) for o in kids[offs, s]], own if any(offs) else out, rows)
            if any(offs):
                self.copy(s, offs).start()

    def steps(self):
        return 1 + max(self.when(self.streams[s][0], (0, 0, 0)) for s in self.ids)

    def end(self):
        if "comm" in SKIP:
            return
        for s in self.ids:
            for offs in self.streams[s][0].others:
                self.copy(s, offs).wait_send()


def meet(axes, everyone, pair):
    route = Route(axes, (0, 1, 2))
    barrier = pltpu.get_barrier_semaphore()
    peers = [o for o in route.others if everyone or sum(1 for v in o if v) == 1]
    for offs in peers:
        pl.semaphore_signal(barrier, inc=1, device_id={"dp": route.target(offs)}, device_id_type=MESH)
    if pair:
        pl.semaphore_signal(barrier, inc=1, device_id={"section": 1 - lax.axis_index("section")}, device_id_type=MESH)
    pl.semaphore_wait(barrier, len(peers) + (1 if pair else 0))


def contract(left, right, dims):
    return lax.dot_general(left, right, ((dims[:1], dims[1:]), ((), ())), preferred_element_type=jnp.float32)


def weight_parts(rows):
    half = rows // 2
    return (((0, 1, 2), 0, half), ((0, 2, 1), half, half))


def weight_columns(half):
    sec = lax.axis_index("section")
    return pl.ds(pl.multiple_of(sec * half, 128), half), pl.ds(pl.multiple_of((1 - sec) * half, 128), half)


def weight_streams(axes, ins, outs):
    streams = []
    for own, full in zip(ins, outs):
        rows, half = own.shape
        cols, _ = weight_columns(half)
        for order, at, size in weight_parts(rows):
            span = pl.ds(at, size)
            streams.append((Route(axes, order), own.at[span], lambda b, o=full, r=span, c=cols: o.at[b, r, c]))
    return streams


def weight_stream_count(arrays):
    return sum(len(weight_parts(a.shape[0])) for a in arrays)


class WeightFold:
    def __init__(self, axes, raws, sums, gots, loads, outs, sems, chunks):
        self.send, self.recv, self.psend, self.precv, self.local = sems
        self.arrays = list(zip(raws, sums, loads, outs))
        self.chunks = chunks
        streams = []
        for raw, total, load, got, out in zip(raws, sums, loads, gots, outs):
            for order, at, size in weight_parts(out.shape[0]):
                rows, route = pl.ds(at, size), Route(axes, order)
                streams.append((route, lambda o, t=total, r=rows, w=route: t.at[w.flat(o), r], lambda f, g=got, r=rows: g.at[f, r],
                                out.at[rows], size))
        self.route = Route(axes, (0, 1, 2))
        self.fold = Fold(streams, self.send, self.recv, chunks)

    def block(self, c):
        return [o for o in self.route.all if o[0] == self.chunks[c]]

    def give(self, a, offs):
        raw, total, _, out = self.arrays[a]
        f = self.route.flat(offs)
        return pltpu.make_async_remote_copy(
            src_ref=raw.at[self.route.target(offs), :, weight_columns(out.shape[1])[1]], dst_ref=total.at[f],
            send_sem=self.psend.at[a, f], recv_sem=self.precv.at[a, f], device_id={"section": 1 - lax.axis_index("section")},
            device_id_type=MESH)

    def load(self, a, offs):
        raw, _, load, out = self.arrays[a]
        slot = offs[1] * self.route.sizes[2] + offs[2]
        return pltpu.make_async_copy(raw.at[self.route.target(offs), :, weight_columns(out.shape[1])[0]], load.at[slot],
                                     self.local.at[a, self.route.flat(offs)])

    def begin(self):
        for c in range(len(self.chunks)):
            for offs in self.block(c):
                for a in range(len(self.arrays)):
                    self.give(a, offs).start()
                    if c == 0:
                        self.load(a, offs).start()

    def step(self, t):
        if t < len(self.chunks):
            for a, (_, total, load, out) in enumerate(self.arrays):
                for offs in self.block(t):
                    self.load(a, offs).wait()
                    self.give(a, offs).wait_recv()
                    here = total.at[self.route.flat(offs)]
                    add_rows([load.at[offs[1] * self.route.sizes[2] + offs[2]], here], here, out.shape[0])
            if t + 1 < len(self.chunks):
                for offs in self.block(t + 1):
                    for a in range(len(self.arrays)):
                        self.load(a, offs).start()
        self.fold.step(t)

    def steps(self):
        return self.fold.steps()

    def end(self):
        self.fold.end()
        for a in range(len(self.arrays)):
            for offs in self.route.all:
                self.give(a, offs).wait_send()


def fold_scratch(arrays, axes):
    count, dma = arrays[0].shape[0], pltpu.SemaphoreType.DMA
    half = [(a.shape[1], a.shape[2] // 2) for a in arrays]
    full = [pltpu.VMEM((count, *h), jnp.bfloat16) for h in half]
    loads = [pltpu.VMEM((axes[1][1] * axes[2][1], *h), jnp.bfloat16) for h in half]
    streams = sum(len(weight_parts(rows)) for rows, _ in half)
    return full + full + loads + [dma((streams, count))] * 2 + [dma((len(arrays), count))] * 3


def closing_kernel(axes, count, *refs):
    refs = list(refs)
    take = lambda n: [refs.pop(0) for _ in range(n)]
    raws, others = take(count), take(count)
    first_up, first_down, last_up, last_down, grad_in, last_in = take(6)
    outs = take(count)
    up_out, down_out, edge_out = take(3)
    sums, gots, loads = take(count), take(count), take(count)
    sems = take(5)
    results, given, taken = take(count), take(count), take(count)
    own_up, own_down, got_up, got_down, edge_give, edge_got, x_send, x_recv, x_local, h_send, h_recv = take(11)
    sec = lax.axis_index("section")
    partner = {"section": 1 - sec}
    chunks = [axes[0][1] - 1 - c for c in range(axes[0][1])]
    meet(axes, False, True)
    fold = WeightFold(axes, raws, sums, gots, loads, results, sems, chunks)
    fold.begin()
    leading = sec == 0

    def remote(src, dst, n):
        return pltpu.make_async_remote_copy(src_ref=src, dst_ref=dst, send_sem=x_send.at[n], recv_sem=x_recv.at[n], device_id=partner,
                                            device_id_type=MESH)

    edge_give[...] = jnp.where(leading, last_in[...], grad_in[...])
    edge = remote(edge_give, edge_got, 2)
    edge.start()
    edge_out[sec] = jnp.where(leading, grad_in[...], last_in[...])

    @pl.when(leading)
    def _():
        remote(last_up, got_up, 0).start()
        remote(last_down, got_down, 1).start()
        pltpu.make_async_copy(first_up, own_up, x_local.at[0]).start()
        pltpu.make_async_copy(first_down, own_down, x_local.at[1]).start()

    @pl.when(jnp.logical_not(leading))
    def _():
        remote(first_up, got_up, 0).start()
        remote(first_down, got_down, 1).start()
        pltpu.make_async_copy(last_up, own_up, x_local.at[0]).start()
        pltpu.make_async_copy(last_down, own_down, x_local.at[1]).start()

    steps = fold.steps()
    for t in range(steps - 1):
        fold.step(t)
        if t == 3:
            for n, (own, got, out, src) in enumerate(((own_up, got_up, up_out, first_up), (own_down, got_down, down_out, first_down))):
                pltpu.make_async_copy(src, own, x_local.at[n]).wait()
                remote(src, got, n).wait_recv()
                add_rows([own, got], own, own.shape[0], 8)
                pltpu.make_async_copy(own, out, x_local.at[n]).start()
            edge.wait_recv()
            edge_out[1 - sec] = edge_got[...]
    fold.step(steps - 1)
    hands = []
    for a in range(count):
        half = results[a].shape[1]
        mine, theirs = weight_columns(half)
        given[a][...] = jnp.where(leading, others[a][...], results[a][...])
        c = pltpu.make_async_remote_copy(src_ref=given[a], dst_ref=taken[a], send_sem=h_send.at[a], recv_sem=h_recv.at[a],
                                         device_id=partner, device_id_type=MESH)
        c.start()
        hands.append(c)
        outs[a][:, mine] = jnp.where(leading, results[a][...], others[a][...])
    fold.end()
    edge.wait_send()
    for n, (own, got, out, src) in enumerate(((own_up, got_up, up_out, first_up), (own_down, got_down, down_out, first_down))):
        remote(src, got, n).wait_send()
        pltpu.make_async_copy(own, out, x_local.at[n]).wait()
    for a in range(count):
        hands[a].wait()
        outs[a][:, weight_columns(results[a].shape[1])[1]] = taken[a][...]


def closing(raws, others, first, last, grad, final, count, cid):
    axes, n = torus_axes(count), len(raws)
    vmem, anywhere = pl.BlockSpec(memory_space=pltpu.VMEM), pl.BlockSpec(memory_space=pl.ANY)
    dma, f32 = pltpu.SemaphoreType.DMA, jnp.float32
    halves = [pltpu.VMEM((a.shape[1], a.shape[2] // 2), f32) for a in raws]
    experts = [pltpu.VMEM(w.shape, f32) for w in first]
    block = pltpu.VMEM(grad.shape, grad.dtype)
    return pl.pallas_call(
        functools.partial(closing_kernel, axes, n),
        out_shape=[jax.ShapeDtypeStruct(a.shape[1:], f32) for a in raws] + [jax.ShapeDtypeStruct(w.shape, f32) for w in first]
        + [jax.ShapeDtypeStruct((2, *grad.shape), grad.dtype)],
        in_specs=[anywhere] * n + [vmem] * n + [anywhere] * 4 + [vmem] * 2,
        out_specs=[vmem] * n + [anywhere] * 2 + [vmem],
        scratch_shapes=fold_scratch(raws, axes) + halves * 3 + experts * 2 + [block, block, dma((3,)), dma((3,)), dma((2,)), dma((n,)), dma((n,))],
        compiler_params=pltpu.CompilerParams(collective_id=cid, has_side_effects=True, vmem_limit_bytes=VMEM_BYTES),
        cost_estimate=pl.CostEstimate(flops=0, bytes_accessed=100_000_000, transcendentals=0),
        name="closing",
    )(*raws, *others, *first, *last, grad, final)


def weight_spread_kernel(axes, count, *refs):
    ins, outs = refs[:count], refs[count : 2 * count]
    send, recv, psend, precv, local = refs[2 * count :]
    meet(axes, False, True)
    spread = Spread(weight_streams(axes, ins, outs), send, recv, psend, precv)
    spread.step(0)
    keep = own_copies(ins, outs, local)
    for t in range(1, axes[0][1] + 2):
        spread.step(t)
    spread.end()
    for c in keep:
        c.wait()


def own_copies(ins, outs, local):
    keep = []
    me, sec = lax.axis_index("dp"), lax.axis_index("section")
    for a, (own, full) in enumerate(zip(ins, outs)):
        half = own.shape[1]
        c = pltpu.make_async_copy(own, full.at[me, :, pl.ds(pl.multiple_of(sec * half, 128), half)], local.at[a])
        c.start()
        keep.append(c)
    return keep


def weight_shapes(arrays, count):
    return [jax.ShapeDtypeStruct((count, a.shape[0], 2 * a.shape[1]), a.dtype) for a in arrays]


def weight_sems(arrays, count):
    sem = pltpu.SemaphoreType.DMA((weight_stream_count(arrays), count))
    return [sem] * 4 + [pltpu.SemaphoreType.DMA((len(arrays),))]


def weight_spread(arrays, count, cid):
    return pl.pallas_call(
        functools.partial(weight_spread_kernel, torus_axes(count), len(arrays)),
        out_shape=weight_shapes(arrays, count),
        in_specs=[pl.BlockSpec(memory_space=pltpu.VMEM)] * len(arrays),
        out_specs=[pl.BlockSpec(memory_space=pl.ANY)] * len(arrays),
        scratch_shapes=weight_sems(arrays, count),
        compiler_params=pltpu.CompilerParams(collective_id=cid, has_side_effects=True),
        name="weight_spread",
    )(*arrays)


def mixture_kernel(mode, axes, count, layer, extra, folded, *refs):
    fore, back = "f" in mode, "b" in mode
    refs = list(refs)
    take = lambda n: [refs.pop(0) for _ in range(n)]
    mask_ref, router_ref, up_own, up_other, down_own, down_other, x_in = take(7)
    g_in = take(1)[0] if back else None
    next_in = take(extra)
    raws = take(folded)
    mixed_out = take(1)[0] if fore else None
    saved_out = take(1)[0] if mode == "f" else None
    if back:
        grad_out, chance_out, up_grad_out, down_grad_out = take(4)
    next_out = take(extra)
    raw_outs = take(folded)
    up, down, xg, gates_at, weight_at, local = take(6)
    ag_send, ag_recv, rs_send, rs_recv = take(4)
    gathers, folds = [], []
    if fore:
        share_f, got_f, act_at = take(3)
        gathers.append((x_in, xg))
        folds.append((share_f, got_f, mixed_out))
    if back:
        (gg, share_b, got_b, plain_at, ggu_at, actw_at, high_at, low_at, up_sum, down_sum, chance_row, chance_got, c_send, c_recv,
         out_sem) = take(15)
        gathers.append((g_in, gg))
        folds.append((share_b, got_b, grad_out))
    me, sec = lax.axis_index("dp"), lax.axis_index("section")
    n0, n1, n2 = [size for _, size in axes]
    plane = n1 * n2
    assert n0 == 4
    meet(axes, back, bool(extra or folded))
    spread_streams, fold_streams = [], []
    for own, full in gathers:
        for order, at, size in TOKEN_PARTS:
            rows = pl.ds(at, size)
            spread_streams.append((Route(axes, order), own.at[rows], lambda b, f=full, r=rows: f.at[b, r]))
    for share, got, out in folds:
        for order, at, size in TOKEN_PARTS:
            rows, route = pl.ds(at, size), Route(axes, order)
            fold_streams.append((route, lambda o, a=share, r=rows, w=route: a.at[w.target(o), r], lambda f, g=got, r=rows: g.at[f, r],
                                 out.at[rows], size))
    spread = Spread(spread_streams, ag_send, ag_recv)
    fold = Fold(fold_streams, rs_send, rs_recv, [3, 2, 1, 0])
    spread.step(0)
    if extra:
        w_send, w_recv, w_psend, w_precv, w_local = take(5)
        other = Spread(weight_streams(axes, next_in, next_out), w_send, w_recv, w_psend, w_precv)
    if folded:
        aside = WeightFold(axes, raws, take(folded), take(folded), take(folded), raw_outs, take(5), [3, 2, 1, 0])
        aside.begin()

    @pl.when(sec == layer)
    def _():
        pltpu.make_async_copy(up_own, up, local.at[0]).start()
        pltpu.make_async_copy(down_own, down, local.at[1]).start()

    @pl.when(sec != layer)
    def _():
        pltpu.make_async_copy(up_other, up, local.at[0]).start()
        pltpu.make_async_copy(down_other, down, local.at[1]).start()

    if not fore:
        bring = pltpu.make_async_copy(x_in, xg, local.at[2])
        bring.start()
    else:
        xg[me] = x_in[...]
    if back:
        gg[me] = g_in[...]
    pltpu.make_async_copy(up_own, up, local.at[0]).wait()
    pltpu.make_async_copy(down_own, down, local.at[1]).wait()
    if not fore:
        bring.wait()

    def span(n, size=SPAN):
        return pl.ds(pl.multiple_of(n * size, size), size)

    def tile(b0):
        blocks = pl.ds(b0, TILE // ROWS)
        here = pl.ds(pl.multiple_of(b0 * ROWS, TILE), TILE)
        x = xg[blocks].reshape(TILE, MODEL_WIDTH)
        lane = lax.broadcasted_iota(jnp.int32, (TILE, router_ref.shape[1]), 1)
        chance = jnp.where(lane < count, jnp.exp(dot(x, router_ref[...])), 0.0)
        total = jnp.sum(chance, axis=1, keepdims=True)
        named = mask_ref[blocks].reshape(TILE, 1)
        weight = jnp.sum(jnp.where(lane == me, chance, 0.0), axis=1, keepdims=True) / total * named
        weight_at[...] = jnp.where(lane[:, :128] == 0, weight, named)

        def gate_step(n, _):
            gates_at[:, span(n)] = dot(xg[blocks].reshape(TILE, MODEL_WIDTH), up[:, span(n)])
            return 0

        lax.fori_loop(0, 2 * FFE // SPAN, gate_step, 0)
        if back:
            def plain_step(n, _):
                plain_at[:, span(n)] = contract(gg[blocks].reshape(TILE, MODEL_WIDTH), down[span(n), :], (1, 1))
                return 0

            lax.fori_loop(0, FFE // SPAN, plain_step, 0)

        def strip(r, _):
            at = pl.ds(pl.multiple_of(r * STRIP, STRIP), STRIP)
            gate, raise_ = gates_at[at, :FFE], gates_at[at, FFE:]
            sigmoid = 1.0 / (1.0 + jnp.exp(-gate))
            silu = gate * sigmoid
            activated = silu * raise_
            if fore:
                act_at[at] = activated.astype(jnp.bfloat16)
            if back:
                row = pl.ds(pl.multiple_of(b0 * ROWS + r * STRIP, STRIP), STRIP)
                w, m = weight_at[at, 0:1], weight_at[at, 1:2]
                plain = plain_at[at]
                grad_act = plain * w
                ggu_at[row, :FFE] = (grad_act * raise_ * sigmoid * (1.0 + gate * (1.0 - sigmoid))).astype(jnp.bfloat16)
                ggu_at[row, FFE:] = (grad_act * silu).astype(jnp.bfloat16)
                actw_at[row] = (activated * w).astype(jnp.bfloat16)
                product = activated * plain * m
                high = product.astype(jnp.bfloat16)
                high_at[at] = high
                low_at[at] = (product - high.astype(jnp.float32)).astype(jnp.bfloat16)
            return 0

        lax.fori_loop(0, TILE // STRIP, strip, 0)
        if back:
            def back_step(n, _):
                part = contract(ggu_at[here], up[span(n), :], (1, 1))
                share_b[blocks, :, span(n)] = part.astype(jnp.bfloat16).reshape(TILE // ROWS, ROWS, SPAN)
                return 0

            lax.fori_loop(0, MODEL_WIDTH // SPAN, back_step, 0)
        if fore:
            def share_step(n, _):
                part = dot(act_at[...], down[:, span(n)]) * weight_at[:, 0:1]
                share_f[blocks, :, span(n)] = part.astype(jnp.bfloat16).reshape(TILE // ROWS, ROWS, SPAN)
                return 0

            lax.fori_loop(0, MODEL_WIDTH // SPAN, share_step, 0)
        if back:
            ones = jnp.ones((8, FFE), jnp.bfloat16)
            row = contract(ones, high_at[...], (1, 1)) + contract(ones, low_at[...], (1, 1))
            for b in range(TILE // ROWS):
                chance_row[b0 + b] = row[:, b * ROWS : (b + 1) * ROWS]

    digit = lax.div(me, axes[0][0])

    def chunk(c, _):
        k = lax.rem(c + 1, n0)

        @pl.when(c == 0)
        def _():
            for t in range(1, 4):
                spread.step(t)
                if folded and t < 3:
                    aside.step(t - 1)

        @pl.when(c == 1)
        def _():
            spread.step(4)
            if extra:
                other.step(0)
            if folded:
                aside.step(2)

        @pl.when(c == 2)
        def _():
            spread.step(5)
            if folded:
                aside.step(3)

        source = lax.rem(digit - k + n0, n0)

        def step(q, _):
            if "tile" not in SKIP:
                tile(source * plane + q * (TILE // ROWS))
            return 0

        lax.fori_loop(0, plane * ROWS // TILE, step, 0)
        for v in range(n0):
            @pl.when(c == v)
            def _(v=v):
                fold.step(v)
                if extra and v >= 2:
                    other.step(v - 1)
        return 0

    lax.fori_loop(0, n0, chunk, 0)
    if back:
        route = Route(axes, (0, 1, 2))

        def chance_copy(offs):
            f = route.flat(offs)
            return pltpu.make_async_remote_copy(
                src_ref=chance_row.at[route.target(offs)], dst_ref=chance_got.at[me], send_sem=c_send.at[f], recv_sem=c_recv.at[f],
                device_id={"dp": route.target(offs)}, device_id_type=MESH)

        for offs in route.others:
            chance_copy(offs).start()
        chance_got[me] = chance_row[me]

        def up_piece(n):
            return pltpu.make_async_copy(up_sum.at[n % 2], up_grad_out.at[pl.ds(n * PIECE, PIECE)], out_sem.at[0, n % 2])

        def down_piece(n):
            return pltpu.make_async_copy(down_sum.at[0], down_grad_out.at[pl.ds(n * PIECE, PIECE)], out_sem.at[1, 0])

        ups, downs = MODEL_WIDTH // PIECE, FFE // PIECE

        def gradient(n):
            if n < ups:
                if n >= 2:
                    up_piece(n - 2).wait()
                left = xg[:, :, n * PIECE : (n + 1) * PIECE].reshape(count * ROWS, PIECE)
                up_sum[n % 2] = contract(left, ggu_at[...], (0, 0))
                up_piece(n).start()
            else:
                n -= ups
                if n:
                    down_piece(n - 1).wait()
                down_sum[0] = contract(actw_at[:, n * PIECE : (n + 1) * PIECE], gg[...].reshape(count * ROWS, MODEL_WIDTH), (0, 0))
                down_piece(n).start()

        work = list(range(ups + downs))
    else:
        work = []
    if saved_out is not None:
        save = pltpu.make_async_copy(xg, saved_out, local.at[2])
        save.start()
    keep = own_copies(next_in, next_out, w_local) if extra else []
    last = fold.steps()
    for t in range(n0, last):
        share = -(-len(work) // (last - t))
        for _ in range(share):
            n = work.pop(0)
            if "grad" not in SKIP:
                gradient(n)
        fold.step(t)
        if extra:
            other.step(t - 1)
        if folded:
            aside.step(t)
    if folded:
        assert aside.steps() == last
        aside.end()
    if extra:
        for t in range(last - 1, n0 + 2):
            other.step(t)
        other.end()
        for c in keep:
            c.wait()
    spread.end()
    fold.end()
    if back:
        for n in range(max(0, ups - 2), ups) if "grad" not in SKIP else ():
            up_piece(n).wait()
        for n in range(downs - 1, downs) if "grad" not in SKIP else ():
            down_piece(n).wait()
        for offs in route.others:
            chance_copy(offs).wait()
        chance_out[...] = chance_got[...]
    if saved_out is not None:
        save.wait()


def mixture_call(mode, count, layer, cid, mask, router, expert, partner, x, g=None, following=(), summed=()):
    axes = torus_axes(count)
    fore, back = "f" in mode, "b" in mode
    vmem, anywhere = pl.BlockSpec(memory_space=pltpu.VMEM), pl.BlockSpec(memory_space=pl.ANY)
    args = [mask, router, expert[0], partner[0], expert[1], partner[1], x]
    in_specs = [vmem, vmem] + [anywhere] * 4 + [vmem if fore else anywhere]
    if back:
        args.append(g)
        in_specs.append(vmem)
    args += list(following) + list(summed)
    in_specs += [vmem] * len(following) + [anywhere] * len(summed)
    whole = (count, ROWS, MODEL_WIDTH)
    out_shape, out_specs = [], []
    block = jax.ShapeDtypeStruct((ROWS, MODEL_WIDTH), jnp.float32)
    if fore:
        out_shape.append(block)
        out_specs.append(vmem)
    if mode == "f":
        out_shape.append(jax.ShapeDtypeStruct(whole, jnp.bfloat16))
        out_specs.append(anywhere)
    if back:
        out_shape += [block, jax.ShapeDtypeStruct((count, 8, ROWS), jnp.float32)]
        out_shape += [jax.ShapeDtypeStruct(w.shape, jnp.float32) for w in expert]
        out_specs += [vmem, vmem, anywhere, anywhere]
    out_shape += weight_shapes(following, count)
    out_specs += [anywhere] * len(following) + [vmem] * len(summed)
    out_shape += [jax.ShapeDtypeStruct((a.shape[1], a.shape[2] // 2), jnp.float32) for a in summed]
    dma = pltpu.SemaphoreType.DMA
    scratch = [pltpu.VMEM(expert[0].shape, jnp.bfloat16), pltpu.VMEM(expert[1].shape, jnp.bfloat16), pltpu.VMEM(whole, jnp.bfloat16),
               pltpu.VMEM((TILE, 2 * FFE), jnp.float32), pltpu.VMEM((TILE, 128), jnp.float32), dma((3,))]
    parts = len(TOKEN_PARTS)
    ag, rs = parts * (1 if mode == "b" else fore + back), parts * (fore + back)
    scratch += [dma((ag, count)), dma((ag, count)), dma((rs, count)), dma((rs, count))]
    blocks = pltpu.VMEM(whole, jnp.bfloat16)
    low = lambda rows, width: pltpu.VMEM((rows, width), jnp.bfloat16)
    if fore:
        scratch += [blocks, blocks, low(TILE, FFE)]
    if back:
        scratch += [blocks, blocks, blocks, pltpu.VMEM((TILE, FFE), jnp.float32),
                    low(count * ROWS, 2 * FFE), low(count * ROWS, FFE), low(TILE, FFE), low(TILE, FFE),
                    pltpu.VMEM((2, PIECE, 2 * FFE), jnp.float32), pltpu.VMEM((1, PIECE, MODEL_WIDTH), jnp.float32),
                    pltpu.VMEM((count, 8, ROWS), jnp.float32), pltpu.VMEM((count, 8, ROWS), jnp.float32), dma((count,)), dma((count,)),
                    dma((2, 2))]
    if following:
        scratch += weight_sems(following, count)
    if summed:
        scratch += fold_scratch(summed, axes)
    rows = count * ROWS
    flops = rows * 6 * MODEL_WIDTH * FFE * (fore + 2 * back + (mode == "b"))
    return pl.pallas_call(
        functools.partial(mixture_kernel, mode, axes, count, layer, len(following), len(summed)),
        out_shape=out_shape,
        in_specs=in_specs,
        out_specs=out_specs,
        scratch_shapes=scratch,
        compiler_params=pltpu.CompilerParams(collective_id=cid, has_side_effects=True, vmem_limit_bytes=VMEM_BYTES),
        cost_estimate=pl.CostEstimate(flops=flops, bytes_accessed=4 * rows * MODEL_WIDTH, transcendentals=rows * FFE),
        name="mixture_" + mode,
    )(*args)

def swapped(value):
    return lax.ppermute(value, "section", [(0, 1), (1, 0)])


def layout(length_row):
    seq_ends = jnp.cumsum(length_row)
    seq_starts = seq_ends - length_row
    row_ids = jnp.arange(DEVICE_ROWS, dtype=jnp.int32)
    segment = jnp.sum((row_ids[:, None] >= seq_ends[None, :]).astype(jnp.int32), axis=-1)
    member = (segment[:, None] == jnp.arange(NSEQ, dtype=jnp.int32)[None, :]).astype(jnp.int32)
    token_position = row_ids - jnp.sum(member * seq_starts[None, :], axis=-1)
    return segment, token_position


def rotation(token_position):
    half_width = HEAD_SIZE // 2
    frequency = 10000.0 ** (-2.0 * jnp.arange(half_width, dtype=jnp.float32) / HEAD_SIZE)
    angles = token_position.astype(jnp.float32)[:, None] * frequency
    return jnp.cos(angles)[:, None, :], jnp.sin(angles)[:, None, :]


def rotary_embedding(values, cosine, sine):
    half_width = HEAD_SIZE // 2
    former, latter = values[..., :half_width], values[..., half_width:]
    return jnp.concatenate([former * cosine - latter * sine, latter * cosine + former * sine], axis=-1)


def dot(left, right):
    return jnp.dot(left, right, preferred_element_type=jnp.float32)


def dot_rows(left, right):
    return lax.dot_general(left, right, (((0,), (0,)), ((), ())), preferred_element_type=jnp.float32)


def dot_columns(left, right):
    return lax.dot_general(left, right, (((1,), (1,)), ((), ())), preferred_element_type=jnp.float32)


def router_chances(normed_two, router):
    chance = jnp.exp(dot(normed_two, router))
    return chance / jnp.sum(chance, axis=-1, keepdims=True)


def front(hidden, place, weights):
    joint, result_output, router, gain_attention, gain_mixture = weights
    allowed, cosine, sine = place
    rows = hidden.shape[0]
    inverse_one = lax.rsqrt(jnp.mean(hidden * hidden, axis=-1, keepdims=True) + norm_epsilon)
    scaled_one = hidden * inverse_one
    normed = (scaled_one * gain_attention).astype(jnp.bfloat16)
    projected = dot(normed, joint)
    query = rotary_embedding(projected[:, :QUERY_WIDTH].reshape(rows, QUERY_HEADS, HEAD_SIZE), cosine, sine)
    query = query.astype(jnp.bfloat16).reshape(rows, KEY_VALUE_HEADS, GROUP, HEAD_SIZE)
    key = rotary_embedding(projected[:, QUERY_WIDTH : QUERY_WIDTH + KEY_WIDTH].reshape(rows, KEY_VALUE_HEADS, HEAD_SIZE), cosine, sine)
    key = key.astype(jnp.bfloat16)
    value = projected[:, QUERY_WIDTH + KEY_WIDTH :].reshape(rows, KEY_VALUE_HEADS, HEAD_SIZE).astype(jnp.bfloat16)
    scores = jnp.einsum("qhgd,khd->hgqk", query, key, preferred_element_type=jnp.float32) * SCORE_SCALE
    exponent = jnp.where(allowed, jnp.exp(scores), 0.0)
    attention = exponent / jnp.sum(exponent, axis=-1, keepdims=True)
    context = jnp.einsum("hgqk,khd->qhgd", attention.astype(jnp.bfloat16), value, preferred_element_type=jnp.float32)
    context = context.reshape(rows, QUERY_WIDTH).astype(jnp.bfloat16)
    middle = hidden + dot(context, result_output)
    inverse_two = lax.rsqrt(jnp.mean(middle * middle, axis=-1, keepdims=True) + norm_epsilon)
    scaled_two = middle * inverse_two
    normed_two = (scaled_two * gain_mixture).astype(jnp.bfloat16)
    kept = (inverse_one, scaled_one, normed, query, key, value, attention, context, inverse_two, scaled_two, normed_two)
    return middle, normed_two, kept


def gates(everyone, up_weight):
    both = dot(everyone, up_weight)
    return both[:, :FFE], both[:, FFE:]


def expert_forward(everyone, mask, router, expert, count, me):
    up_weight, down_weight = expert
    chance = router_chances(everyone, router)
    own = jnp.arange(count, dtype=jnp.int32) == me
    weight = jnp.sum(jnp.where(own[None, :] & mask, chance, 0.0), axis=-1)
    gate, up = gates(everyone, up_weight)
    activated = (jax.nn.silu(gate) * up).astype(jnp.bfloat16)
    share = (dot(activated, down_weight) * weight[:, None]).astype(jnp.bfloat16)
    return share, weight, (gate, up)


def expert_backward(grads, everyone, weight, mask, held, expert):
    up_weight, down_weight = expert
    gate, up = held if held is not None else gates(everyone, up_weight)
    sigmoid = jax.nn.sigmoid(gate)
    silu = gate * sigmoid
    activated = silu * up
    grad_plain = dot_columns(grads, down_weight)
    grad_weight = jnp.where(mask[:, 0], jnp.sum(activated * grad_plain, axis=-1), 0.0)
    grad_act = grad_plain * weight[:, None]
    grad_gate = grad_act * up * sigmoid * (1.0 + gate * (1.0 - sigmoid))
    grad_gate_up = jnp.concatenate([grad_gate, grad_act * silu], axis=-1).astype(jnp.bfloat16)
    grad_down = dot_rows((activated * weight[:, None]).astype(jnp.bfloat16), grads)
    grad_up_weight = dot_rows(everyone, grad_gate_up)
    share = dot_columns(grad_gate_up, up_weight).astype(jnp.bfloat16)
    return share, grad_weight, grad_up_weight, grad_down


def pieces(value):
    return value.reshape(-1, CHUNK_ROWS, *value.shape[1:])


def mixture_forward(normed_two, router, mask, expert, count, me):
    (spread,) = gather_all([normed_two], count, 0)
    everyone = spread.reshape(-1, MODEL_WIDTH)
    if everyone.shape[0] <= CHUNK_ROWS:
        share, weight, held = expert_forward(everyone, mask, router, expert, count, me)
    else:
        share, weight = lax.map(
            lambda part: expert_forward(part[0], part[1], router, expert, count, me)[:2], (pieces(everyone), pieces(mask)))
        held = None
    (mixed,) = reduce_all([share.reshape(spread.shape)], count, 1)
    return mixed, (everyone, weight.reshape(-1), held)


def mixture_backward(grad_out, mask, kept, expert, count):
    everyone, weight, held = kept
    (spread,) = gather_all([grad_out], count, 0)
    grads = spread.reshape(-1, MODEL_WIDTH)
    if grads.shape[0] <= CHUNK_ROWS:
        share, grad_weight, grad_up, grad_down = expert_backward(grads, everyone, weight, mask, held, expert)
    else:
        def step(sums, part):
            share, grad_weight, grad_up, grad_down = expert_backward(*part, None, expert)
            return (sums[0] + grad_up, sums[1] + grad_down), (share, grad_weight)

        zero = tuple(jnp.zeros(w.shape, jnp.float32) for w in expert)
        (grad_up, grad_down), (share, grad_weight) = lax.scan(
            step, zero, (pieces(grads), pieces(everyone), pieces(weight), pieces(mask)))
    grad_chance = lax.all_to_all(grad_weight.reshape(count, DEVICE_ROWS), "dp", split_axis=0, concat_axis=0, tiled=True)
    (mixed,) = reduce_all([share.reshape(spread.shape)], count, 1)
    return mixed, grad_chance.T, grad_up, grad_down


def front_backward(grad_out, grad_mixed, grad_chance, kept, place, weights):
    joint, result_output, router, gain_attention, gain_mixture = weights
    allowed, cosine, sine = place
    inverse_one, scaled_one, normed, query, key, value, attention, context, inverse_two, scaled_two, normed_two = kept
    rows = normed.shape[0]
    chance = router_chances(normed_two, router)
    grad_logit = (chance * (grad_chance - jnp.sum(grad_chance * chance, axis=-1, keepdims=True))).astype(jnp.bfloat16)
    grad_router = dot_rows(normed_two, grad_logit)
    grad_normed_two = grad_mixed + dot_columns(grad_logit, router)
    grad_gain_two = jnp.sum(grad_normed_two * scaled_two, axis=0)
    scaled_grad_two = grad_normed_two * gain_mixture
    grad_middle = grad_out + inverse_two * (scaled_grad_two - scaled_two * jnp.mean(scaled_grad_two * scaled_two, axis=-1, keepdims=True))
    branch = grad_middle.astype(jnp.bfloat16)
    grad_output = dot_rows(context, branch)
    grad_context = dot_columns(branch, result_output).astype(jnp.bfloat16).reshape(rows, KEY_VALUE_HEADS, GROUP, HEAD_SIZE)
    grad_attention = jnp.einsum("qhgd,khd->hgqk", grad_context, value, preferred_element_type=jnp.float32)
    grad_value = jnp.einsum("hgqk,qhgd->khd", attention.astype(jnp.bfloat16), grad_context, preferred_element_type=jnp.float32)
    grad_scores = (attention * (grad_attention - jnp.sum(grad_attention * attention, axis=-1, keepdims=True))).astype(jnp.bfloat16)
    grad_query = jnp.einsum("hgqk,khd->qhgd", grad_scores, key, preferred_element_type=jnp.float32).reshape(rows, QUERY_HEADS, HEAD_SIZE)
    grad_key = jnp.einsum("hgqk,qhgd->khd", grad_scores, query, preferred_element_type=jnp.float32)
    grad_query = rotary_embedding(grad_query * SCORE_SCALE, cosine, -sine)
    grad_key = rotary_embedding(grad_key * SCORE_SCALE, cosine, -sine)
    grad_projected = jnp.concatenate(
        [grad_query.reshape(rows, -1), grad_key.reshape(rows, -1), grad_value.reshape(rows, -1)], axis=-1).astype(jnp.bfloat16)
    grad_joint = dot_rows(normed, grad_projected)
    grad_normed = dot_columns(grad_projected, joint)
    grad_gain_one = jnp.sum(grad_normed * scaled_one, axis=0)
    scaled_grad_one = grad_normed * gain_attention
    grad_hidden = grad_middle + inverse_one * (scaled_grad_one - scaled_one * jnp.mean(scaled_grad_one * scaled_one, axis=-1, keepdims=True))
    return grad_hidden, (grad_joint, grad_output, grad_router, grad_gain_one, grad_gain_two)


def small_halves(rows, router, gains, codes):
    second = jnp.concatenate([gains, codes], axis=1)
    width = -(-max(router.shape[1], second.shape[1]) // 128) * 128
    pad = lambda v: jnp.pad(v, ((0, 0), (0, width - v.shape[1])))
    return pad(router), pad(second)


def body(tokens, cotangent, lengths, routes, combined_weight, output_weight, router_weight, attention_gain, mixture_gain,
         expert_gate_up, expert_down):
    count = lax.axis_size("dp")
    me, sec = lax.axis_index("dp"), lax.axis_index("section")
    layers = lax.axis_size("section")
    leading = sec == 0
    shard = combined_weight.shape[1]
    micro = lambda a, axis: lax.dynamic_index_in_dim(a, sec, axis, keepdims=False)

    gains = jnp.stack([attention_gain[0], mixture_gain[0]], axis=1)
    codes = routes[0].astype(jnp.bfloat16).reshape(-1)
    code_count = codes.shape[0]
    codes = jnp.pad(codes, (0, -code_count % shard)).reshape(shard, -1)
    small = small_halves(shard, router_weight[0], gains, codes)
    small_width = small[0].shape[1]
    halves = [
        (combined_weight[0, :, : combined_weight.shape[2] // 2], combined_weight[0, :, combined_weight.shape[2] // 2 :]),
        (output_weight[0, :, : output_weight.shape[2] // 2], output_weight[0, :, output_weight.shape[2] // 2 :]),
        small,
    ]
    widths = [h[0].shape[1] for h in halves]
    mine = jnp.concatenate([jnp.where(leading, a, b) for a, b in halves], axis=1)
    given = swapped(jnp.concatenate([jnp.where(leading, b, a) for a, b in halves], axis=1))
    packs = [jnp.where(leading, mine, given), jnp.where(leading, given, mine)]
    partner_expert = tuple(swapped(w[0, 0]) for w in (expert_gate_up, expert_down))
    own_expert = (expert_gate_up[0, 0], expert_down[0, 0])
    fused = count * DEVICE_ROWS <= CHUNK_ROWS
    experts, routers = [], []
    for layer in range(0 if fused else layers):
        keep = sec == layer
        experts.append((jnp.where(keep, expert_gate_up[0, 0], partner_expert[0]), jnp.where(keep, expert_down[0, 0], partner_expert[1])))

    def layer_parts(layer):
        at, parts = 0, []
        for w in widths:
            parts.append(packs[layer][:, at : at + w])
            at += w
        return parts

    def layer_weights(arrays):
        joint, output, tail = [a.reshape(MODEL_WIDTH, -1) for a in arrays]
        second = tail[:, small_width:]
        weights = (joint, output, tail[:, : router_weight.shape[2]], second[:, 0].astype(jnp.float32), second[:, 1].astype(jnp.float32))
        routers.append(tail[:, :small_width])
        code = second[:, 2 : 2 + codes.shape[1]].reshape(count, -1)[:, :code_count].reshape(count, -1, DEVICE_ROWS, TOPK)
        named = lax.dynamic_index_in_dim(code, sec, 1, keepdims=False).reshape(count * DEVICE_ROWS, TOPK)
        mask = jnp.any(named == me.astype(jnp.bfloat16), axis=-1, keepdims=True)
        return weights, mask

    segment, token_position = layout(micro(lengths[:, 0], 0))
    row_ids = jnp.arange(DEVICE_ROWS, dtype=jnp.int32)
    allowed = (row_ids[:, None] >= row_ids[None, :]) & (segment[:, None] == segment[None, :])
    place = (allowed,) + rotation(token_position)

    weights, masks, stores = [], [], []
    hidden = micro(tokens, 0)
    for layer in range(layers):
        if not fused:
            arrays = gather_all(layer_parts(layer), count, 2, pair=True)
        elif layer == 0:
            arrays = weight_spread(layer_parts(layer), count, 2)
        got, mask = layer_weights(arrays)
        weights.append(got)
        masks.append(mask)
        middle, normed_two, kept = front(hidden.astype(jnp.float32), place, got)
        if not fused:
            mixed, kept_mixture = mixture_forward(normed_two, got[2], mask, experts[layer], count, me)
        else:
            named = mask.astype(jnp.float32).reshape(count, DEVICE_ROWS, 1)
            call = lambda mode, cid, *data, **more: mixture_call(
                mode, count, layer, cid, named, routers[layer], own_expert, partner_expert, *data, **more)
            if layer < layers - 1:
                mixed, everyone, *arrays = call("f", 4, normed_two, following=layer_parts(layer + 1))
                kept_mixture = (named, everyone)
            else:
                mixed, *kept_mixture = call("fb", 5, normed_two, micro(cotangent, 0))
        hidden = (middle + mixed).astype(jnp.bfloat16)
        stores.append((kept, kept_mixture))
    last = hidden
    grad = micro(cotangent, 0)
    shares, expert_grads = [None] * layers, [None] * layers
    for layer in reversed(range(layers)):
        kept, kept_mixture = stores[layer]
        if not fused:
            mixed, grad_chance, grad_up, grad_down = mixture_backward(grad, masks[layer], kept_mixture, experts[layer], count)
        else:
            if layer < layers - 1:
                named, everyone = kept_mixture
                kept_mixture = mixture_call("b", count, layer, 6, named, routers[layer], own_expert, partner_expert, everyone, grad,
                                            summed=packs[layer + 1])
            mixed, rows, grad_up, grad_down, *more = kept_mixture
            if layer < layers - 1:
                shares[layer + 1] = more
            grad_chance = rows[:, 0].T
        expert_grads[layer] = (grad_up, grad_down)
        grad_hidden, parts = front_backward(grad.astype(jnp.float32), mixed, grad_chance, kept, place, weights[layer])
        grad = grad_hidden.astype(jnp.bfloat16)
        tail = small_halves(MODEL_WIDTH, parts[2], jnp.stack([parts[3], parts[4]], axis=1), parts[2][:, :0])
        packed = [parts[0], parts[1], jnp.concatenate(tail, axis=1)]
        packs[layer] = [a.astype(jnp.bfloat16).reshape(count, shard, -1) for a in packed]
        if not fused:
            shares[layer] = reduce_all(packs[layer], count, 3, pair=True)
    if fused:
        *outs, grad_up, grad_down, boundary = closing(packs[0], shares[1], expert_grads[0], expert_grads[1], grad, last, count, 3)
        half = outs[2].shape[1] // 2
        return (
            boundary[None],
            outs[0][None],
            outs[1][None],
            outs[2][None, :, : router_weight.shape[2]],
            outs[2][None, :, half],
            outs[2][None, :, half + 1],
            grad_up[None, None],
            grad_down[None, None],
        )
    outs = []
    for a in range(3):
        kept_half = jnp.where(leading, shares[0][a], shares[1][a])
        got_half = swapped(jnp.where(leading, shares[1][a], shares[0][a]))
        outs.append(jnp.concatenate([jnp.where(leading, kept_half, got_half), jnp.where(leading, got_half, kept_half)], axis=1))
    expert_outs = []
    for a in range(2):
        kept_sum = jnp.where(leading, expert_grads[0][a], expert_grads[1][a])
        got_sum = swapped(jnp.where(leading, expert_grads[1][a], expert_grads[0][a]))
        expert_outs.append((kept_sum + got_sum)[None, None])
    partner = swapped(jnp.where(leading, last, grad))
    boundary = jnp.where(leading, jnp.stack([grad, partner]), jnp.stack([partner, last]))[None]
    half = outs[2].shape[1] // 2
    return (
        boundary,
        outs[0][None],
        outs[1][None],
        outs[2][None, :, : router_weight.shape[2]],
        outs[2][None, :, half],
        outs[2][None, :, half + 1],
        expert_outs[0],
        expert_outs[1],
    )


def solution(mesh):
    return jax.shard_map(
        body,
        mesh=mesh,
        in_specs=(
            P(None, "dp", None),
            P(None, "dp", None),
            P(None, "dp", None),
            P("section", None, "dp", None),
            P("section", "dp", None),
            P("section", "dp", None),
            P("section", "dp", None),
            P("section", "dp"),
            P("section", "dp"),
            P("section", "dp", None, None),
            P("section", "dp", None, None),
        ),
        out_specs=(
            P("section", None, "dp", None),
            P("section", "dp", None),
            P("section", "dp", None),
            P("section", "dp", None),
            P("section", "dp"),
            P("section", "dp"),
            P("section", "dp", None, None),
            P("section", "dp", None, None),
        ),
        check_vma=False,
    )
```

```python
import functools
import jax
import jax.numpy as jnp
from jax import lax
from jax.experimental import pallas as pl
from jax.experimental.pallas import tpu as pltpu
from jax.sharding import PartitionSpec as P

MODEL_WIDTH = 1536
QUERY_HEADS = 24
KEY_VALUE_HEADS = 8
GROUP = QUERY_HEADS // KEY_VALUE_HEADS
HEAD_SIZE = 64
FFE = 512
TOPK = 8
DEVICE_ROWS = 128
NSEQ = 4
QUERY_WIDTH = QUERY_HEADS * HEAD_SIZE
KEY_WIDTH = KEY_VALUE_HEADS * HEAD_SIZE
SCORE_SCALE = HEAD_SIZE ** (-0.5)
norm_epsilon = 1e-06
CHUNK_ROWS = 2048

VMEM_BYTES = 67_000_000


def torus_axes(count):
    side = 1
    while (side + 1) ** 3 <= count:
        side += 1
    assert count % (side * side) == 0
    return [(side * side, count // (side * side)), (1, side), (side, side)]


def offsets(sizes):
    return [(k, j, i) for k in range(sizes[0]) for j in range(sizes[1]) for i in range(sizes[2])]


class Place:
    def __init__(self, axes, order):
        self.me = lax.axis_index("dp")
        self.sec = lax.axis_index("section")
        long, first, second = axes
        if order is None:
            flip = self.sec
            stride_one = first[0] + (second[0] - first[0]) * flip
            stride_two = second[0] + (first[0] - second[0]) * flip
            assert first[1] == second[1]
            self.axes = [long, (stride_one, first[1]), (stride_two, second[1])]
        elif order == 0:
            self.axes = [long, first, second]
        else:
            self.axes = [long, second, first]
        self.sizes = [size for _, size in self.axes]

    def moved(self, steps):
        out = self.me
        for (stride, size), step in zip(self.axes, steps):
            if step % size:
                digit = lax.rem(lax.div(self.me, stride), size)
                out = out + (lax.rem(digit + (step % size), size) - digit) * stride
        return out

    def source(self, offs):
        return self.moved([-o for o in offs])

    def target(self, offs):
        return self.moved(list(offs))

    def flat(self, offs):
        return (offs[0] * self.sizes[1] + offs[1]) * self.sizes[2] + offs[2]


def last_hop(offs):
    for axis in (2, 1, 0):
        if offs[axis]:
            hop = [0, 0, 0]
            hop[axis] = offs[axis]
            base = list(offs)
            base[axis] = 0
            return tuple(hop), tuple(base)
    return None


def greet(axes, pair):
    place = Place(axes, 0)
    barrier = pltpu.get_barrier_semaphore()
    count = 0
    for axis in range(3):
        for step in range(1, place.sizes[axis]):
            hop = [0, 0, 0]
            hop[axis] = step
            pl.semaphore_signal(barrier, inc=1, device_id={"dp": place.target(hop)}, device_id_type=pl.DeviceIdType.MESH)
            count += 1
    if pair:
        pl.semaphore_signal(barrier, inc=1, device_id={"section": 1 - place.sec}, device_id_type=pl.DeviceIdType.MESH)
        count += 1
    pl.semaphore_wait(barrier, count)


def gather_kernel(axes, pair, count, *refs):
    ins, outs = refs[:count], refs[count : 2 * count]
    send, recv, local = refs[2 * count : 2 * count + 3]
    psend, precv = refs[2 * count + 3 :] if pair else (None, None)
    streams = []
    for a in range(count):
        if pair:
            place = Place(axes, None)
            half = ins[a].shape[1]
            cols = pl.ds(pl.multiple_of(place.sec * half, 128), half)
            streams.append((place, ins[a], lambda b, o=outs[a], c=cols: o.at[b, :, c]))
        else:
            half = ins[a].shape[0] // 2
            for h in range(2):
                rows = pl.ds(h * half, half)
                streams.append((Place(axes, h), ins[a].at[rows], lambda b, o=outs[a], r=rows: o.at[b, r]))

    def copy(s, offs):
        place, own, out = streams[s]
        hop, base = last_hop(offs)
        block = place.source(base)
        src = out(block) if any(base) else own
        f = place.flat(offs)
        return pltpu.make_async_remote_copy(
            src_ref=src, dst_ref=out(block), send_sem=send.at[s, f], recv_sem=recv.at[s, f],
            device_id={"dp": place.target(hop)}, device_id_type=pl.DeviceIdType.MESH)

    def share(s, offs):
        place, own, out = streams[s]
        block = place.source(offs)
        src = out(block) if any(offs) else own
        f = place.flat(offs)
        return pltpu.make_async_remote_copy(
            src_ref=src, dst_ref=out(block), send_sem=psend.at[s, f], recv_sem=precv.at[s, f],
            device_id={"section": 1 - place.sec}, device_id_type=pl.DeviceIdType.MESH)

    greet(axes, pair)
    ids = range(len(streams))
    n0, n1, n2 = streams[0][0].sizes
    keep = []
    for s in ids:
        place, own, out = streams[s]
        c = pltpu.make_async_copy(own, out(place.me), local.at[s])
        c.start()
        keep.append(c)
    for k in range(1, n0):
        for s in ids:
            copy(s, (k, 0, 0)).start()

    def first(k):
        for s in ids:
            if k:
                copy(s, (k, 0, 0)).wait_recv()
            for j in range(1, n1):
                copy(s, (k, j, 0)).start()
            for i in range(1, n2):
                copy(s, (k, 0, i)).start()
            if pair:
                share(s, (k, 0, 0)).start()

    def second(k):
        for j in range(1, n1):
            for s in ids:
                copy(s, (k, j, 0)).wait_recv()
                for i in range(1, n2):
                    copy(s, (k, j, i)).start()
                if pair:
                    share(s, (k, j, 0)).start()

    def third(k):
        for j in range(n1):
            for i in range(1, n2):
                for s in ids:
                    copy(s, (k, j, i)).wait_recv()
                    if pair:
                        share(s, (k, j, i)).start()

    for k in range(n0 + 2):
        if k < n0:
            first(k)
        if 0 <= k - 1 < n0:
            second(k - 1)
        if 0 <= k - 2 < n0:
            third(k - 2)
    for s in ids:
        for offs in offsets((n0, n1, n2)):
            if any(offs):
                copy(s, offs).wait_send()
            if pair:
                share(s, offs).wait()
    for c in keep:
        c.wait()


def gather_all(arrays, count, cid, pair=False):
    axes = torus_axes(count)
    streams = len(arrays) * (1 if pair else 2)
    sem = pltpu.SemaphoreType.DMA((streams, count))
    out_shape = [jax.ShapeDtypeStruct((count, a.shape[0], a.shape[1] * (2 if pair else 1)), a.dtype) for a in arrays]
    scratch = [sem, sem, pltpu.SemaphoreType.DMA((streams,))]
    if pair:
        scratch += [sem, sem]
    sent = sum(a.size * a.dtype.itemsize for a in arrays) * (count - 1)
    return pl.pallas_call(
        functools.partial(gather_kernel, axes, pair, len(arrays)),
        out_shape=out_shape,
        in_specs=[pl.BlockSpec(memory_space=pltpu.VMEM)] * len(arrays),
        out_specs=[pl.BlockSpec(memory_space=pl.ANY)] * len(arrays),
        scratch_shapes=scratch,
        compiler_params=pltpu.CompilerParams(collective_id=cid, has_side_effects=True),
        cost_estimate=pl.CostEstimate(flops=0, bytes_accessed=2 * sent, transcendentals=0),
        name="spread" if not pair else "spread_pair",
    )(*arrays)


def reduce_kernel(axes, pair, count, *refs):
    ins, outs = refs[:count], refs[count : 2 * count]
    rest = list(refs[2 * count :])
    send, recv = rest[:2]
    rest = rest[2:]
    if pair:
        psend, precv = rest[:2]
        rest = rest[2:]
    streams = []
    for a in range(count):
        if pair:
            got, held, pgot, psum = rest[:4]
            rest = rest[4:]
            place = Place(axes, None)
            half = outs[a].shape[1]
            mine = pl.ds(pl.multiple_of(place.sec * half, 128), half)
            other = pl.ds(pl.multiple_of((1 - place.sec) * half, 128), half)
            streams.append(dict(place=place, got=got, held=held, pgot=pgot, psum=psum, raw=ins[a], mine=mine, other=other,
                                out=outs[a], rows=outs[a].shape[0]))
        else:
            got, held = rest[:2]
            rest = rest[2:]
            half = outs[a].shape[0] // 2
            for h in range(2):
                rows = pl.ds(h * half, half)
                streams.append(dict(place=Place(axes, h), got=got.at[h], held=held.at[h], raw=ins[a], span=rows,
                                    out=outs[a].at[rows], rows=half))
    step = 8 if streams[0]["rows"] % 16 else 16

    def own_ref(t, offs):
        if pair:
            return t["psum"].at[t["place"].flat(offs)]
        return t["raw"].at[t["place"].target(offs), t["span"]]

    def summed(t, sources, dest):
        def one(r, _):
            rows = pl.ds(pl.multiple_of(r * step, step), step)
            total = sources[0][rows].astype(jnp.float32)
            for source in sources[1:]:
                total = total + source[rows].astype(jnp.float32)
            dest[rows] = total.astype(dest.dtype)
            return 0

        lax.fori_loop(0, t["rows"] // step, one, 0)

    def copy(s, offs):
        t = streams[s]
        place = t["place"]
        hop, base = last_hop(offs)
        f = place.flat(offs)
        src = own_ref(t, offs) if hop[2] else t["held"].at[f // place.sizes[2]]
        return pltpu.make_async_remote_copy(
            src_ref=src, dst_ref=t["got"].at[f], send_sem=send.at[s, f], recv_sem=recv.at[s, f],
            device_id={"dp": place.target(hop)}, device_id_type=pl.DeviceIdType.MESH)

    def share(s, offs):
        t = streams[s]
        place = t["place"]
        f = place.flat(offs)
        return pltpu.make_async_remote_copy(
            src_ref=t["raw"].at[place.target((offs[0], offs[2], offs[1])), :, t["other"]], dst_ref=t["pgot"].at[f],
            send_sem=psend.at[s, f], recv_sem=precv.at[s, f],
            device_id={"section": 1 - place.sec}, device_id_type=pl.DeviceIdType.MESH)

    ids = range(len(streams))
    n0, n1, n2 = streams[0]["place"].sizes
    greet(axes, pair)

    def phase_pair(k):
        for j in reversed(range(n1)):
            for i in reversed(range(n2)):
                for s in ids:
                    share(s, (k, j, i)).start()

    def phase_first(k):
        for j in reversed(range(n1)):
            for i in reversed(range(n2)):
                for s in ids:
                    t = streams[s]
                    if pair:
                        share(s, (k, j, i)).wait_recv()
                        f = t["place"].flat((k, j, i))
                        summed(t, [t["raw"].at[t["place"].target((k, j, i)), :, t["mine"]], t["pgot"].at[f]], t["psum"].at[f])
                    if i:
                        copy(s, (k, j, i)).start()

    def phase_second(k):
        for j in range(1, n1):
            for s in ids:
                t = streams[s]
                for i in range(1, n2):
                    copy(s, (k, j, i)).wait_recv()
                parts = [own_ref(t, (k, j, 0))] + [t["got"].at[t["place"].flat((k, j, i))] for i in range(1, n2)]
                summed(t, parts, t["held"].at[t["place"].flat((k, j, 0)) // n2])
                copy(s, (k, j, 0)).start()

    def gathered_parts(s, k):
        t = streams[s]
        offs = [(k, 0, i) for i in range(1, n2)] + [(k, j, 0) for j in range(1, n1)]
        for o in offs:
            copy(s, o).wait_recv()
        return [own_ref(t, (k, 0, 0))] + [t["got"].at[t["place"].flat(o)] for o in offs]

    def phase_third(k):
        for s in ids:
            t = streams[s]
            parts = gathered_parts(s, k)
            if k:
                summed(t, parts, t["held"].at[t["place"].flat((k, 0, 0)) // n2])
                copy(s, (k, 0, 0)).start()
            else:
                for q in range(1, n0):
                    copy(s, (q, 0, 0)).wait_recv()
                    parts.append(t["got"].at[t["place"].flat((q, 0, 0))])
                summed(t, parts, t["out"])

    chunks = list(range(1, n0)) + [0]
    if pair:
        phase_pair(chunks[0])
    for c in range(n0 + 3):
        if pair and c + 1 < n0:
            phase_pair(chunks[c + 1])
        if c < n0:
            phase_first(chunks[c])
        if 0 <= c - 1 < n0:
            phase_second(chunks[c - 1])
        if 0 <= c - 2 < n0:
            phase_third(chunks[c - 2])
    for s in ids:
        for offs in offsets((n0, n1, n2)):
            if any(offs):
                copy(s, offs).wait_send()
            if pair:
                share(s, offs).wait_send()


def reduce_all(arrays, count, cid, pair=False):
    axes = torus_axes(count)
    streams = len(arrays) * (1 if pair else 2)
    sem = pltpu.SemaphoreType.DMA((streams, count))
    scratch = [sem, sem]
    if pair:
        scratch += [sem, sem]
    groups = count // axes[2][1]
    out_shape = []
    for a in arrays:
        rows, cols = a.shape[1:]
        if pair:
            cols = cols // 2
            scratch += [pltpu.VMEM((count, rows, cols), a.dtype), pltpu.VMEM((groups, rows, cols), a.dtype),
                        pltpu.VMEM((count, rows, cols), a.dtype), pltpu.VMEM((count, rows, cols), a.dtype)]
        else:
            scratch += [pltpu.VMEM((2, count, rows // 2, cols), a.dtype), pltpu.VMEM((2, groups, rows // 2, cols), a.dtype)]
        out_shape.append(jax.ShapeDtypeStruct((rows, cols), jnp.float32))
    sent = sum(a.size * a.dtype.itemsize for a in arrays)
    return pl.pallas_call(
        functools.partial(reduce_kernel, axes, pair, len(arrays)),
        out_shape=out_shape,
        in_specs=[pl.BlockSpec(memory_space=pltpu.VMEM)] * len(arrays),
        out_specs=[pl.BlockSpec(memory_space=pltpu.VMEM)] * len(arrays),
        scratch_shapes=scratch,
        compiler_params=pltpu.CompilerParams(collective_id=cid, has_side_effects=True, vmem_limit_bytes=VMEM_BYTES),
        cost_estimate=pl.CostEstimate(flops=0, bytes_accessed=2 * sent, transcendentals=0),
        name="fold" if not pair else "fold_pair",
    )(*arrays)


ROWS = 128
TILE = 512
STRIP = 16
SPAN = 512
SKIP = set()
PIECE = 256
MESH = pl.DeviceIdType.MESH
ORDERS = ((0, 1, 2), (0, 2, 1), (1, 0, 2), (2, 0, 1))
TOKEN_PARTS = tuple((order, 32 * n, 32) for n, order in enumerate(ORDERS))


class Route:
    def __init__(self, axes, order):
        self.axes, self.order = axes, order
        self.sizes = [size for _, size in axes]
        assert self.sizes == [4, 2, 2]
        self.me = lax.axis_index("dp")
        self.all = offsets(self.sizes)
        self.others = [o for o in self.all if any(o)]
        self.z = lax.div(self.me, axes[0][0])
        self.inner = jnp.logical_and(self.z >= 1, self.z <= 2)
        later = order[order.index(0) + 1 :]
        self.lines = [(j, i) for j in range(2) for i in range(2) if all((0, j, i)[a] == 0 for a in later)]

    def digit(self, axis):
        stride, size = self.axes[axis]
        return lax.rem(lax.div(self.me, stride), size)

    def plane(self, rank):
        z = self.z
        if rank == 1:
            return z + 1 - 2 * lax.rem(z, 2)
        if rank == 2:
            return 2 - lax.div(z, 2)
        if rank == 3:
            return 3 - 3 * lax.div(z, 2)
        return z

    def block(self, offs):
        out = self.me + (self.plane(offs[0]) - self.z) * self.axes[0][0]
        for axis in (1, 2):
            if offs[axis]:
                out = out + (1 - 2 * self.digit(axis)) * self.axes[axis][0]
        return out

    def flat(self, offs):
        return (offs[0] * 2 + offs[1]) * 2 + offs[2]

    def extra(self, line, n):
        return 16 + 2 * self.lines.index(line) + n

    def last_axis(self, offs):
        for axis in reversed(self.order):
            if offs[axis]:
                return axis

    def base(self, offs):
        out = list(offs)
        out[self.last_axis(offs)] = 0
        return tuple(out)

    def across(self, offs):
        return [o for o in self.others if self.last_axis(o) and self.base(o) == offs]


def remote(src, dst, send, recv, peer):
    return pltpu.make_async_remote_copy(src_ref=src, dst_ref=dst, send_sem=send, recv_sem=recv, device_id=peer, device_id_type=MESH)


class Spread:
    def __init__(self, streams, send, recv):
        self.streams, self.send, self.recv = streams, send, recv
        self.ids = range(len(streams))

    def copy(self, s, offs, target, key, slot):
        route, own, out = self.streams[s]
        block = route.block(offs)
        return remote(out(block) if any(offs) else own, out(block), self.send.at[s, slot], self.recv.at[s, route.flat(key)], {"dp": target})

    def arrival(self, s, offs):
        route, own, out = self.streams[s]
        f = route.flat(offs)
        return remote(own, out(route.block(offs)), self.send.at[s, f], self.recv.at[s, f], {"dp": route.block(offs)})

    def onward(self, s, offs):
        route = self.streams[s][0]
        k, line = offs[0], offs[1:]
        out = [(o, False, self.copy(s, offs, route.block((0, *[int(o[a] != offs[a]) for a in (1, 2)])), o, route.flat(o)))
               for o in route.across(offs)]
        if line in route.lines:
            near, facing = route.block((1, 0, 0)), route.block((2, 0, 0))
            if k == 0:
                out.append(((1, *line), False, self.copy(s, offs, near, (1, *line), route.flat((1, *line)))))
                out.append(((2, *line), True, self.copy(s, offs, facing, (2, *line), route.extra(line, 0))))
            elif k == 1:
                out.append(((3, *line), True, self.copy(s, offs, facing, (3, *line), route.extra(line, 1))))
            else:
                out.append((offs, True, self.copy(s, offs, near, offs, route.flat(offs))))
        return out

    def launch(self, items):
        for s, (_, inner, copy) in items:
            if inner:
                pl.when(self.streams[s][0].inner)(copy.start)
            else:
                copy.start()

    def step(self, t):
        if "comm" in SKIP or "ag" in SKIP:
            return
        work = [(offs, s) for s in self.ids for offs in self.streams[s][0].all if offs[0] + offs[1] + offs[2] == t]
        if t == 0:
            first = [(s, item) for offs, s in work for item in self.onward(s, offs)]
            self.launch(sorted(first, key=lambda e: (e[1][0][0], e[1][0], e[0])))
            return
        ends = lambda e: not self.streams[e[1]][0].across(e[0]) and e[0][1:] not in self.streams[e[1]][0].lines
        for offs, s in sorted(work, key=lambda e: (ends(e), -e[0][0], e[0], e[1])):
            self.arrival(s, offs).wait_recv()
            self.launch([(s, item) for item in sorted(self.onward(s, offs), key=lambda e: (e[1], e[0]))])

    def end(self):
        if "comm" in SKIP or "ag" in SKIP:
            return
        for s in self.ids:
            for offs in self.streams[s][0].all:
                for _, inner, copy in self.onward(s, offs):
                    if inner:
                        pl.when(self.streams[s][0].inner)(copy.wait_send)
                    else:
                        copy.wait_send()


SPREAD_STEPS = 6


def add_rows(sources, dest, rows, step=16):
    cols = dest.shape[-1]
    width = next(w for w in (640, 512, 384, 128) if cols % w == 0)

    def one(r, _):
        at = pl.ds(pl.multiple_of(r * step, step), step)

        def part(c, _):
            span = pl.ds(pl.multiple_of(c * width, width), width)
            total = sources[0][at, span].astype(jnp.float32)
            for source in sources[1:]:
                total = total + source[at, span].astype(jnp.float32)
            dest[at, span] = total.astype(dest.dtype)
            return 0

        return lax.fori_loop(0, cols // width, part, 0)

    lax.fori_loop(0, rows // step, one, 0)


class Fold:
    def __init__(self, streams, send, recv, ranks):
        self.streams, self.send, self.recv = streams, send, recv
        self.ids = range(len(streams))
        self.turn = {k: c for c, k in enumerate(ranks)}
        self.plan = []
        for s in self.ids:
            route = self.streams[s][0]
            for offs in route.all:
                if offs[0] and offs[1:] in route.lines:
                    self.plan.append((self.ready(route, offs), 1, -offs[0], s, offs, self.outer))
                    self.plan.append((self.passed(route, offs), 2, -offs[0], s, offs, self.middle))
                else:
                    when = self.done(route, offs)
                    rank = 3 if not any(offs) else 1 if self.near(route, offs) or not offs[0] and offs[1:] in route.lines else 0
                    self.plan.append((when, rank, -offs[0], s, offs, self.plain))
        self.plan.sort(key=lambda e: e[:5])

    def near(self, route, offs):
        return [o for o in route.across(offs) if o[0] == offs[0]]

    def ready(self, route, offs):
        return max([self.turn[offs[0]]] + [self.done(route, o) + 1 for o in self.near(route, offs)])

    def passed(self, route, offs):
        line = offs[1:]
        return self.ready(route, offs) + 1 if offs[0] > 1 else max(self.ready(route, offs), self.ready(route, (3, *line)) + 2)

    def done(self, route, offs):
        when = self.ready(route, offs)
        if not offs[0] and offs[1:] in route.lines:
            when = max(when, self.passed(route, (1, *offs[1:])) + 1, self.passed(route, (2, *offs[1:])) + 1)
        return when

    def arrival(self, s, slot):
        route, share, got, _, _ = self.streams[s]
        return remote(share((0, 0, 0)), got(slot), self.send.at[s, slot], self.recv.at[s, slot], {"dp": route.block((1, 0, 0))})

    def copy(self, s, offs):
        route, share, got, _, _ = self.streams[s]
        f = route.flat(offs)
        if route.last_axis(offs):
            hop = [0, 0, 0]
            hop[route.last_axis(offs)] = 1
            return remote(share(offs), got(f), self.send.at[s, f], self.recv.at[s, f], {"dp": route.block(hop)})
        near, facing = route.block((1, 0, 0)), route.block((2, 0, 0))
        if offs[0] == 1:
            return remote(share(offs), got(f), self.send.at[s, f], self.recv.at[s, f], {"dp": near})
        slot = f + (route.extra(offs[1:], offs[0] - 2) - f) * route.inner.astype(jnp.int32)
        return remote(share(offs), got(slot), self.send.at[s, f], self.recv.at[s, slot], {"dp": jnp.where(route.inner, facing, near)})

    def settle(self, s, offs, slots, out=None):
        route, share, got, _, rows = self.streams[s]
        if slots:
            for f in slots:
                self.arrival(s, f).wait_recv()
            own = share(offs)
            add_rows([own] + [got(f) for f in slots], own if out is None else out, rows)

    def outer(self, s, offs):
        route = self.streams[s][0]
        self.settle(s, offs, [route.flat(o) for o in self.near(route, offs)])
        pl.when(jnp.logical_not(route.inner))(self.copy(s, offs).start)

    def middle(self, s, offs):
        route = self.streams[s][0]

        @pl.when(route.inner)
        def _():
            self.settle(s, offs, [route.flat(offs) if offs[0] > 1 else route.extra(offs[1:], 1)])
            self.copy(s, offs).start()

    def plain(self, s, offs):
        route, share, got, out, rows = self.streams[s]
        slots = [route.flat(o) for o in self.near(route, offs)]
        if not offs[0] and offs[1:] in route.lines:
            slots.append(route.flat((1, *offs[1:])))
            facing = route.extra(offs[1:], 0)

            @pl.when(route.inner)
            def _():
                self.settle(s, offs, [facing])

        self.settle(s, offs, slots, None if any(offs) else out)
        if any(offs):
            self.copy(s, offs).start()

    def step(self, t):
        if "comm" in SKIP or "rs" in SKIP:
            return
        for when, _, _, s, offs, action in self.plan:
            if when == t:
                action(s, offs)

    def steps(self):
        return 1 + max(e[0] for e in self.plan)

    def end(self):
        if "comm" in SKIP or "rs" in SKIP:
            return
        for s in self.ids:
            for offs in self.streams[s][0].others:
                self.copy(s, offs).wait_send()


def meet(axes, everyone, pair):
    route = Route(axes, ORDERS[0])
    barrier = pltpu.get_barrier_semaphore()
    if everyone:
        for offs in route.others:
            pl.semaphore_signal(barrier, inc=1, device_id={"dp": route.block(offs)}, device_id_type=MESH)
    else:
        for offs in ((0, 0, 1), (0, 1, 0), (1, 0, 0)):
            pl.semaphore_signal(barrier, inc=1, device_id={"dp": route.block(offs)}, device_id_type=MESH)

        @pl.when(route.inner)
        def _():
            pl.semaphore_signal(barrier, inc=1, device_id={"dp": route.block((2, 0, 0))}, device_id_type=MESH)

    if pair:
        pl.semaphore_signal(barrier, inc=1, device_id={"section": 1 - lax.axis_index("section")}, device_id_type=MESH)
    pl.semaphore_wait(barrier, (len(route.others) if everyone else 3 + route.inner.astype(jnp.int32)) + (1 if pair else 0))


def contract(left, right, dims):
    return lax.dot_general(left, right, ((dims[:1], dims[1:]), ((), ())), preferred_element_type=jnp.float32)


def weight_parts(rows):
    third = rows // 3
    sizes = (third, third, third // 2, third // 2)
    return tuple((order, sum(sizes[:n]), sizes[n]) for n, order in enumerate(ORDERS))


def weight_columns(half):
    sec = lax.axis_index("section")
    return pl.ds(pl.multiple_of(sec * half, 128), half), pl.ds(pl.multiple_of((1 - sec) * half, 128), half)


def packed_columns(widths):
    return [pl.ds(sum(widths[:n]), w) for n, w in enumerate(widths)]


class WeightSpread:
    def __init__(self, axes, own, full, outs, sems):
        send, recv, self.psend, self.precv, self.local = sems
        self.own, self.full, self.outs = own, full, outs
        self.route = Route(axes, ORDERS[0])
        streams = []
        for order, at, size in weight_parts(own.shape[0]):
            rows = pl.ds(at, size)
            streams.append((Route(axes, order), own.at[rows], lambda b, r=rows: full.at[b, r]))
        self.spread = Spread(streams, send, recv)
        self.widths = [out.shape[2] // 2 for out in outs]

    def deliveries(self, offs):
        block, f = self.route.block(offs), self.route.flat(offs)
        for a, cols in enumerate(packed_columns(self.widths)):
            src = self.full.at[block, :, cols] if any(offs) else self.own.at[:, cols]
            dst = self.outs[a].at[block, :, weight_columns(self.widths[a])[0]]
            yield pltpu.make_async_copy(src, dst, self.local.at[a, f])
            yield remote(src, dst, self.psend.at[a, f], self.precv.at[a, f], {"section": 1 - lax.axis_index("section")})

    def step(self, t):
        self.spread.step(t)
        for offs in self.route.all:
            if sum(offs) == t:
                for copy in self.deliveries(offs):
                    copy.start()

    def end(self):
        self.spread.end()
        for offs in self.route.all:
            for copy in self.deliveries(offs):
                copy.wait()


def weight_shapes(pack, widths, count):
    return [jax.ShapeDtypeStruct((count, pack.shape[0], 2 * w), pack.dtype) for w in widths]


def weight_scratch(pack, widths, count):
    dma = pltpu.SemaphoreType.DMA
    return [pltpu.VMEM((count, *pack.shape), pack.dtype)] + [dma((len(ORDERS), count + 4))] * 2 + [dma((len(widths), count))] * 3


def weight_spread_kernel(axes, arrays, *refs):
    own, outs, full, sems = refs[0], refs[1 : 1 + arrays], refs[1 + arrays], refs[2 + arrays :]
    meet(axes, False, True)
    spread = WeightSpread(axes, own, full, outs, sems)
    for t in range(SPREAD_STEPS):
        spread.step(t)
    spread.end()


def weight_spread(pack, widths, count, cid):
    return pl.pallas_call(
        functools.partial(weight_spread_kernel, torus_axes(count), len(widths)),
        out_shape=weight_shapes(pack, widths, count),
        in_specs=[pl.BlockSpec(memory_space=pltpu.VMEM)],
        out_specs=[pl.BlockSpec(memory_space=pl.ANY)] * len(widths),
        scratch_shapes=weight_scratch(pack, widths, count),
        compiler_params=pltpu.CompilerParams(collective_id=cid, has_side_effects=True),
        name="weight_spread",
    )(pack)


class WeightFold:
    def __init__(self, axes, raws, total, got, load, out, sems, ranks):
        send, recv, self.psend, self.precv, self.local = sems
        self.raws, self.total, self.held, self.rows = raws, total, load, out.shape[0]
        self.widths = [raw.shape[2] // 2 for raw in raws]
        self.ranks = ranks
        streams = []
        for order, at, size in weight_parts(self.rows):
            rows, route = pl.ds(at, size), Route(axes, order)
            streams.append((route, lambda o, r=rows, w=route: total.at[w.flat(o), r], lambda f, r=rows: got.at[f, r], out.at[rows], size))
        self.route = Route(axes, ORDERS[0])
        self.fold = Fold(streams, send, recv, ranks)

    def pieces(self, c):
        cols = packed_columns(self.widths)
        return [(o, a, cols[a]) for o in self.route.all if o[0] == self.ranks[c] for a in range(len(self.raws))]

    def give(self, offs, a, cols):
        f = self.route.flat(offs)
        src = self.raws[a].at[self.route.block(offs), :, weight_columns(self.widths[a])[1]]
        return remote(src, self.total.at[f, :, cols], self.psend.at[a, f], self.precv.at[a, f], {"section": 1 - lax.axis_index("section")})

    def load(self, offs, a, cols):
        src = self.raws[a].at[self.route.block(offs), :, weight_columns(self.widths[a])[0]]
        return pltpu.make_async_copy(src, self.held.at[offs[1] * 2 + offs[2], :, cols], self.local.at[a, self.route.flat(offs)])

    def begin(self):
        for c in range(len(self.ranks)):
            for piece in self.pieces(c):
                self.give(*piece).start()
                if c == 0:
                    self.load(*piece).start()

    def step(self, t):
        if t < len(self.ranks):
            for piece in self.pieces(t):
                self.load(*piece).wait()
                self.give(*piece).wait_recv()
            for offs in self.route.all:
                if offs[0] == self.ranks[t]:
                    here = self.total.at[self.route.flat(offs)]
                    add_rows([self.held.at[offs[1] * 2 + offs[2]], here], here, self.rows)
            if t + 1 < len(self.ranks):
                for piece in self.pieces(t + 1):
                    self.load(*piece).start()
        self.fold.step(t)

    def steps(self):
        return self.fold.steps()

    def end(self):
        self.fold.end()
        for c in range(len(self.ranks)):
            for piece in self.pieces(c):
                self.give(*piece).wait_send()


def fold_shape(arrays):
    return jax.ShapeDtypeStruct((arrays[0].shape[1], sum(a.shape[2] // 2 for a in arrays)), jnp.float32)


def fold_scratch(arrays, axes):
    count, dma, block = arrays[0].shape[0], pltpu.SemaphoreType.DMA, fold_shape(arrays).shape
    blocks = [pltpu.VMEM((n, *block), jnp.bfloat16) for n in (count, count + 4, axes[1][1] * axes[2][1])]
    return blocks + [dma((len(ORDERS), count + 4))] * 2 + [dma((len(arrays), count))] * 3


def closing_kernel(axes, count, *refs):
    refs = list(refs)
    take = lambda n: [refs.pop(0) for _ in range(n)]
    raws = take(count)
    other = take(1)[0]
    first_up, first_down, last_up, last_down, grad_in, last_in = take(6)
    outs = take(count)
    up_out, down_out, edge_out = take(3)
    blocks, sems = take(3), take(5)
    result, given, taken = take(3)
    own_up, own_down, got_up, got_down, edge_give, edge_got, x_send, x_recv, x_local, h_send, h_recv = take(11)
    sec = lax.axis_index("section")
    partner = {"section": 1 - sec}
    chunks = [axes[0][1] - 1 - c for c in range(axes[0][1])]
    meet(axes, False, True)
    fold = WeightFold(axes, raws, *blocks, result, sems, chunks)
    fold.begin()
    leading = sec == 0

    def cross(src, dst, n):
        return remote(src, dst, x_send.at[n], x_recv.at[n], partner)

    edge_give[...] = jnp.where(leading, last_in[...], grad_in[...])
    edge = cross(edge_give, edge_got, 2)
    edge.start()
    edge_out[sec] = jnp.where(leading, grad_in[...], last_in[...])

    @pl.when(leading)
    def _():
        cross(last_up, got_up, 0).start()
        cross(last_down, got_down, 1).start()
        pltpu.make_async_copy(first_up, own_up, x_local.at[0]).start()
        pltpu.make_async_copy(first_down, own_down, x_local.at[1]).start()

    @pl.when(jnp.logical_not(leading))
    def _():
        cross(first_up, got_up, 0).start()
        cross(first_down, got_down, 1).start()
        pltpu.make_async_copy(last_up, own_up, x_local.at[0]).start()
        pltpu.make_async_copy(last_down, own_down, x_local.at[1]).start()

    steps = fold.steps()
    for t in range(steps - 1):
        fold.step(t)
        for n, (own, got, out, src) in enumerate(((own_up, got_up, up_out, first_up), (own_down, got_down, down_out, first_down))):
            if t == 2:
                pltpu.make_async_copy(src, own, x_local.at[n]).wait()
                cross(src, got, n).wait_recv()
            if t in (2, 3):
                size = own.shape[0] // 2
                rows = pl.ds((t - 2) * size, size)
                add_rows([own.at[rows], got.at[rows]], own.at[rows], size, 8)
            if t == 3:
                pltpu.make_async_copy(own, out, x_local.at[n]).start()
        if t == 2:
            edge.wait_recv()
            edge_out[1 - sec] = edge_got[...]
    assert steps > 4
    fold.step(steps - 1)
    given[...] = jnp.where(leading, other[...], result[...])
    hand = remote(given, taken, h_send.at[0], h_recv.at[0], partner)
    hand.start()
    packed = packed_columns(fold.widths)
    for a in range(count):
        outs[a][:, weight_columns(fold.widths[a])[0]] = jnp.where(leading, result[:, packed[a]], other[:, packed[a]])
    fold.end()
    edge.wait_send()
    for n, (own, got, out, src) in enumerate(((own_up, got_up, up_out, first_up), (own_down, got_down, down_out, first_down))):
        cross(src, got, n).wait_send()
        pltpu.make_async_copy(own, out, x_local.at[n]).wait()
    hand.wait()
    for a in range(count):
        outs[a][:, weight_columns(fold.widths[a])[1]] = taken[:, packed[a]]


def closing(raws, other, first, last, grad, final, count, cid):
    axes, n = torus_axes(count), len(raws)
    vmem, anywhere = pl.BlockSpec(memory_space=pltpu.VMEM), pl.BlockSpec(memory_space=pl.ANY)
    dma, f32 = pltpu.SemaphoreType.DMA, jnp.float32
    half = pltpu.VMEM(fold_shape(raws).shape, f32)
    experts = [pltpu.VMEM(w.shape, f32) for w in first]
    block = pltpu.VMEM(grad.shape, grad.dtype)
    return pl.pallas_call(
        functools.partial(closing_kernel, axes, n),
        out_shape=[jax.ShapeDtypeStruct(a.shape[1:], f32) for a in raws] + [jax.ShapeDtypeStruct(w.shape, f32) for w in first]
        + [jax.ShapeDtypeStruct((2, *grad.shape), grad.dtype)],
        in_specs=[anywhere] * n + [vmem] + [anywhere] * 4 + [vmem] * 2,
        out_specs=[vmem] * n + [anywhere] * 2 + [vmem],
        scratch_shapes=fold_scratch(raws, axes) + [half] * 3 + experts * 2 + [block, block, dma((3,)), dma((3,)), dma((2,)), dma((1,)), dma((1,))],
        compiler_params=pltpu.CompilerParams(collective_id=cid, has_side_effects=True, vmem_limit_bytes=VMEM_BYTES),
        cost_estimate=pl.CostEstimate(flops=0, bytes_accessed=100_000_000, transcendentals=0),
        name="closing",
    )(*raws, other, *first, *last, grad, final)


def mixture_kernel(mode, axes, count, layer, extra, folded, *refs):
    fore, back = "f" in mode, "b" in mode
    refs = list(refs)
    take = lambda n: [refs.pop(0) for _ in range(n)]
    mask_ref, router_ref, up_own, up_other, down_own, down_other, x_in = take(7)
    g_in = take(1)[0] if back else None
    next_in = take(1)[0] if extra else None
    raws = take(folded)
    mixed_out = take(1)[0] if fore else None
    saved_out = take(1)[0] if mode == "f" else None
    if back:
        grad_out, chance_out, up_grad_out, down_grad_out = take(4)
    next_out = take(extra)
    raw_out = take(1)[0] if folded else None
    up, down, xg, gates_at, weight_at, local = take(6)
    ag_send, ag_recv, rs_send, rs_recv = take(4)
    gathers, folds = [], []
    if fore:
        share_f, got_f, act_at = take(3)
        gathers.append((x_in, xg))
        folds.append((share_f, got_f, mixed_out))
    if back:
        (gg, share_b, got_b, plain_at, ggu_at, actw_at, high_at, low_at, up_sum, down_sum, chance_row, chance_got, c_send, c_recv,
         out_sem) = take(15)
        gathers.append((g_in, gg))
        folds.append((share_b, got_b, grad_out))
    me, sec = lax.axis_index("dp"), lax.axis_index("section")
    n0, n1, n2 = [size for _, size in axes]
    plane = n1 * n2
    assert n0 == 4
    meet(axes, back, bool(extra or folded))
    spread_streams, fold_streams = [], []
    for own, full in gathers:
        for order, at, size in TOKEN_PARTS:
            rows = pl.ds(at, size)
            spread_streams.append((Route(axes, order), own.at[rows], lambda b, f=full, r=rows: f.at[b, r]))
    for share, got, out in folds:
        for order, at, size in TOKEN_PARTS:
            rows, route = pl.ds(at, size), Route(axes, order)
            fold_streams.append((route, lambda o, a=share, r=rows, w=route: a.at[w.block(o), r], lambda f, g=got, r=rows: g.at[f, r],
                                 out.at[rows], size))
    spread = Spread(spread_streams, ag_send, ag_recv)
    ranks = [3, 2, 1, 0]
    fold = Fold(fold_streams, rs_send, rs_recv, ranks)
    spread.step(0)
    if extra:
        other = WeightSpread(axes, next_in, take(1)[0], next_out, take(5))
    if folded:
        aside = WeightFold(axes, raws, *take(3), raw_out, take(5), ranks)
        aside.begin()

    @pl.when(sec == layer)
    def _():
        pltpu.make_async_copy(up_own, up, local.at[0]).start()
        pltpu.make_async_copy(down_own, down, local.at[1]).start()

    @pl.when(sec != layer)
    def _():
        pltpu.make_async_copy(up_other, up, local.at[0]).start()
        pltpu.make_async_copy(down_other, down, local.at[1]).start()

    if not fore:
        bring = pltpu.make_async_copy(x_in, xg, local.at[2])
        bring.start()
    else:
        xg[me] = x_in[...]
    if back:
        gg[me] = g_in[...]
    pltpu.make_async_copy(up_own, up, local.at[0]).wait()
    pltpu.make_async_copy(down_own, down, local.at[1]).wait()
    if not fore:
        bring.wait()

    def span(n, size=SPAN):
        return pl.ds(pl.multiple_of(n * size, size), size)

    def tile(b0):
        blocks = pl.ds(b0, TILE // ROWS)
        here = pl.ds(pl.multiple_of(b0 * ROWS, TILE), TILE)
        x = xg[blocks].reshape(TILE, MODEL_WIDTH)
        lane = lax.broadcasted_iota(jnp.int32, (TILE, router_ref.shape[1]), 1)
        chance = jnp.where(lane < count, jnp.exp(dot(x, router_ref[...])), 0.0)
        total = jnp.sum(chance, axis=1, keepdims=True)
        named = mask_ref[blocks].reshape(TILE, 1).astype(jnp.float32)
        weight = jnp.sum(jnp.where(lane == me, chance, 0.0), axis=1, keepdims=True) / total * named
        weight_at[...] = jnp.where(lane[:, :128] == 0, weight, named)

        def gate_step(n, _):
            gates_at[:, span(n)] = dot(xg[blocks].reshape(TILE, MODEL_WIDTH), up[:, span(n)])
            return 0

        lax.fori_loop(0, 2 * FFE // SPAN, gate_step, 0)
        if back:
            def plain_step(n, _):
                plain_at[:, span(n)] = contract(gg[blocks].reshape(TILE, MODEL_WIDTH), down[span(n), :], (1, 1))
                return 0

            lax.fori_loop(0, FFE // SPAN, plain_step, 0)

        def strip(r, _):
            at = pl.ds(pl.multiple_of(r * STRIP, STRIP), STRIP)
            gate, raise_ = gates_at[at, :FFE], gates_at[at, FFE:]
            sigmoid = 1.0 / (1.0 + jnp.exp(-gate))
            silu = gate * sigmoid
            activated = silu * raise_
            if fore:
                act_at[at] = activated.astype(jnp.bfloat16)
            if back:
                row = pl.ds(pl.multiple_of(b0 * ROWS + r * STRIP, STRIP), STRIP)
                w, m = weight_at[at, 0:1], weight_at[at, 1:2]
                plain = plain_at[at]
                grad_act = plain * w
                ggu_at[row, :FFE] = (grad_act * raise_ * sigmoid * (1.0 + gate * (1.0 - sigmoid))).astype(jnp.bfloat16)
                ggu_at[row, FFE:] = (grad_act * silu).astype(jnp.bfloat16)
                actw_at[row] = (activated * w).astype(jnp.bfloat16)
                product = activated * plain * m
                high = product.astype(jnp.bfloat16)
                high_at[at] = high
                low_at[at] = (product - high.astype(jnp.float32)).astype(jnp.bfloat16)
            return 0

        lax.fori_loop(0, TILE // STRIP, strip, 0)
        if back:
            def back_step(n, _):
                part = contract(ggu_at[here], up[span(n), :], (1, 1))
                share_b[blocks, :, span(n)] = part.astype(jnp.bfloat16).reshape(TILE // ROWS, ROWS, SPAN)
                return 0

            lax.fori_loop(0, MODEL_WIDTH // SPAN, back_step, 0)
        if fore:
            def share_step(n, _):
                part = dot(act_at[...], down[:, span(n)]) * weight_at[:, 0:1]
                share_f[blocks, :, span(n)] = part.astype(jnp.bfloat16).reshape(TILE // ROWS, ROWS, SPAN)
                return 0

            lax.fori_loop(0, MODEL_WIDTH // SPAN, share_step, 0)
        if back:
            ones = jnp.ones((8, FFE), jnp.bfloat16)
            row = contract(ones, high_at[...], (1, 1)) + contract(ones, low_at[...], (1, 1))
            for b in range(TILE // ROWS):
                chance_row[b0 + b] = row[:, b * ROWS : (b + 1) * ROWS]

    for t in range(1, SPREAD_STEPS):
        spread.step(t)
        if folded:
            aside.step(t - 1)
    if extra:
        other.step(0)
    route = Route(axes, ORDERS[0])
    sources = [route.plane(k) for k in ranks]

    def chunk(c, _):
        source = sources[0]
        for v in range(1, n0):
            source = jnp.where(c == v, sources[v], source)

        def step(q, _):
            if "tile" not in SKIP:
                tile(source * plane + q * (TILE // ROWS))
            return 0

        lax.fori_loop(0, plane * ROWS // TILE, step, 0)
        for v in range(n0):
            @pl.when(c == v)
            def _(v=v):
                fold.step(v)
                if extra and v:
                    other.step(v)
                if folded:
                    aside.step(SPREAD_STEPS - 1 + v)
        return 0

    lax.fori_loop(0, n0, chunk, 0)
    if back:

        def chance_copy(offs, sender):
            block = route.block(offs)
            return remote(chance_row.at[block], chance_got.at[sender], c_send.at[route.flat(offs)], c_recv.at[sender], {"dp": block})

        for offs in route.others:
            chance_copy(offs, me).start()
        chance_got[me] = chance_row[me]

        def up_piece(n):
            return pltpu.make_async_copy(up_sum.at[0], up_grad_out.at[pl.ds(n * PIECE, PIECE)], out_sem.at[0, 0])

        def down_piece(n):
            return pltpu.make_async_copy(down_sum.at[0], down_grad_out.at[pl.ds(n * PIECE, PIECE)], out_sem.at[1, 0])

        ups, downs = MODEL_WIDTH // PIECE, FFE // PIECE

        def gradient(n):
            if n < ups:
                if n:
                    up_piece(n - 1).wait()
                left = xg[:, :, n * PIECE : (n + 1) * PIECE].reshape(count * ROWS, PIECE)
                up_sum[0] = contract(left, ggu_at[...], (0, 0))
                up_piece(n).start()
            else:
                n -= ups
                if n:
                    down_piece(n - 1).wait()
                down_sum[0] = contract(actw_at[:, n * PIECE : (n + 1) * PIECE], gg[...].reshape(count * ROWS, MODEL_WIDTH), (0, 0))
                down_piece(n).start()

        work = list(range(ups + downs))
    else:
        work = []
    if saved_out is not None:
        save = pltpu.make_async_copy(xg, saved_out, local.at[2])
        save.start()
    last = fold.steps()
    for t in range(n0, last):
        share = -(-len(work) // (last - t))
        for _ in range(share):
            n = work.pop(0)
            if "grad" not in SKIP:
                gradient(n)
        fold.step(t)
        if extra:
            other.step(t)
        if folded:
            aside.step(SPREAD_STEPS - 1 + t)
    if folded:
        assert aside.steps() <= SPREAD_STEPS - 1 + last
        aside.end()
    if extra:
        assert last >= SPREAD_STEPS
        other.end()
    spread.end()
    fold.end()
    if back:
        for n in range(ups - 1, ups) if "grad" not in SKIP else ():
            up_piece(n).wait()
        for n in range(downs - 1, downs) if "grad" not in SKIP else ():
            down_piece(n).wait()
        for offs in route.others:
            chance_copy(offs, route.block(offs)).wait()
        chance_out[...] = chance_got[...]
    if saved_out is not None:
        save.wait()


def mixture_call(mode, count, layer, cid, mask, router, expert, partner, x, g=None, following=None, widths=(), summed=()):
    axes = torus_axes(count)
    fore, back = "f" in mode, "b" in mode
    vmem, anywhere = pl.BlockSpec(memory_space=pltpu.VMEM), pl.BlockSpec(memory_space=pl.ANY)
    args = [mask, router, expert[0], partner[0], expert[1], partner[1], x]
    in_specs = [vmem, vmem] + [anywhere] * 4 + [vmem if fore else anywhere]
    if back:
        args.append(g)
        in_specs.append(vmem)
    args += ([following] if widths else []) + list(summed)
    in_specs += ([vmem] if widths else []) + [anywhere] * len(summed)
    whole = (count, ROWS, MODEL_WIDTH)
    out_shape, out_specs = [], []
    block = jax.ShapeDtypeStruct((ROWS, MODEL_WIDTH), jnp.float32)
    if fore:
        out_shape.append(block)
        out_specs.append(vmem)
    if mode == "f":
        out_shape.append(jax.ShapeDtypeStruct(whole, jnp.bfloat16))
        out_specs.append(anywhere)
    if back:
        out_shape += [block, jax.ShapeDtypeStruct((count, 8, ROWS), jnp.float32)]
        out_shape += [jax.ShapeDtypeStruct(w.shape, jnp.float32) for w in expert]
        out_specs += [vmem, vmem, anywhere, anywhere]
    if widths:
        out_shape += weight_shapes(following, widths, count)
        out_specs += [anywhere] * len(widths)
    if summed:
        out_shape.append(fold_shape(summed))
        out_specs.append(vmem)
    dma = pltpu.SemaphoreType.DMA
    scratch = [pltpu.VMEM(expert[0].shape, jnp.bfloat16), pltpu.VMEM(expert[1].shape, jnp.bfloat16), pltpu.VMEM(whole, jnp.bfloat16),
               pltpu.VMEM((TILE, 2 * FFE), jnp.float32), pltpu.VMEM((TILE, 128), jnp.float32), dma((3,))]
    parts = len(TOKEN_PARTS)
    ag, rs = parts * (1 if mode == "b" else fore + back), parts * (fore + back)
    scratch += [dma((ag, count + 4)), dma((ag, count + 4)), dma((rs, count + 4)), dma((rs, count + 4))]
    blocks = pltpu.VMEM(whole, jnp.bfloat16)
    arrivals = pltpu.VMEM((count + 4, *whole[1:]), jnp.bfloat16)
    low = lambda rows, width: pltpu.VMEM((rows, width), jnp.bfloat16)
    if fore:
        scratch += [blocks, arrivals, low(TILE, FFE)]
    if back:
        scratch += [blocks, blocks, arrivals, pltpu.VMEM((TILE, FFE), jnp.float32),
                    low(count * ROWS, 2 * FFE), low(count * ROWS, FFE), low(TILE, FFE), low(TILE, FFE),
                    pltpu.VMEM((1, PIECE, 2 * FFE), jnp.float32), pltpu.VMEM((1, PIECE, MODEL_WIDTH), jnp.float32),
                    pltpu.VMEM((count, 8, ROWS), jnp.float32), pltpu.VMEM((count, 8, ROWS), jnp.float32), dma((count,)), dma((count,)),
                    dma((2, 2))]
    if widths:
        scratch += weight_scratch(following, widths, count)
    if summed:
        scratch += fold_scratch(summed, axes)
    rows = count * ROWS
    flops = rows * 6 * MODEL_WIDTH * FFE * (fore + 2 * back + (mode == "b"))
    return pl.pallas_call(
        functools.partial(mixture_kernel, mode, axes, count, layer, len(widths), len(summed)),
        out_shape=out_shape,
        in_specs=in_specs,
        out_specs=out_specs,
        scratch_shapes=scratch,
        compiler_params=pltpu.CompilerParams(collective_id=cid, has_side_effects=True, vmem_limit_bytes=VMEM_BYTES),
        cost_estimate=pl.CostEstimate(flops=flops, bytes_accessed=4 * rows * MODEL_WIDTH, transcendentals=rows * FFE),
        name="mixture_" + mode,
    )(*args)

def swapped(value):
    return lax.ppermute(value, "section", [(0, 1), (1, 0)])


def layout(length_row):
    seq_ends = jnp.cumsum(length_row)
    seq_starts = seq_ends - length_row
    row_ids = jnp.arange(DEVICE_ROWS, dtype=jnp.int32)
    segment = jnp.sum((row_ids[:, None] >= seq_ends[None, :]).astype(jnp.int32), axis=-1)
    member = (segment[:, None] == jnp.arange(NSEQ, dtype=jnp.int32)[None, :]).astype(jnp.int32)
    token_position = row_ids - jnp.sum(member * seq_starts[None, :], axis=-1)
    return segment, token_position


def rotation(token_position):
    half_width = HEAD_SIZE // 2
    frequency = 10000.0 ** (-2.0 * jnp.arange(half_width, dtype=jnp.float32) / HEAD_SIZE)
    angles = token_position.astype(jnp.float32)[:, None] * frequency
    return jnp.cos(angles)[:, None, :], jnp.sin(angles)[:, None, :]


def rotary_embedding(values, cosine, sine):
    half_width = HEAD_SIZE // 2
    former, latter = values[..., :half_width], values[..., half_width:]
    return jnp.concatenate([former * cosine - latter * sine, latter * cosine + former * sine], axis=-1)


def dot(left, right):
    return jnp.dot(left, right, preferred_element_type=jnp.float32)


def dot_rows(left, right):
    return lax.dot_general(left, right, (((0,), (0,)), ((), ())), preferred_element_type=jnp.float32)


def dot_columns(left, right):
    return lax.dot_general(left, right, (((1,), (1,)), ((), ())), preferred_element_type=jnp.float32)


def router_chances(normed_two, router):
    chance = jnp.exp(dot(normed_two, router))
    return chance / jnp.sum(chance, axis=-1, keepdims=True)


def front(hidden, place, weights):
    joint, result_output, router, gain_attention, gain_mixture = weights
    allowed, cosine, sine = place
    rows = hidden.shape[0]
    inverse_one = lax.rsqrt(jnp.mean(hidden * hidden, axis=-1, keepdims=True) + norm_epsilon)
    scaled_one = hidden * inverse_one
    normed = (scaled_one * gain_attention).astype(jnp.bfloat16)
    projected = dot(normed, joint)
    query = rotary_embedding(projected[:, :QUERY_WIDTH].reshape(rows, QUERY_HEADS, HEAD_SIZE), cosine, sine)
    query = query.astype(jnp.bfloat16).reshape(rows, KEY_VALUE_HEADS, GROUP, HEAD_SIZE)
    key = rotary_embedding(projected[:, QUERY_WIDTH : QUERY_WIDTH + KEY_WIDTH].reshape(rows, KEY_VALUE_HEADS, HEAD_SIZE), cosine, sine)
    key = key.astype(jnp.bfloat16)
    value = projected[:, QUERY_WIDTH + KEY_WIDTH :].reshape(rows, KEY_VALUE_HEADS, HEAD_SIZE).astype(jnp.bfloat16)
    scores = jnp.einsum("qhgd,khd->hgqk", query, key, preferred_element_type=jnp.float32) * SCORE_SCALE
    exponent = jnp.where(allowed, jnp.exp(scores), 0.0)
    attention = exponent / jnp.sum(exponent, axis=-1, keepdims=True)
    context = jnp.einsum("hgqk,khd->qhgd", attention.astype(jnp.bfloat16), value, preferred_element_type=jnp.float32)
    context = context.reshape(rows, QUERY_WIDTH).astype(jnp.bfloat16)
    middle = hidden + dot(context, result_output)
    inverse_two = lax.rsqrt(jnp.mean(middle * middle, axis=-1, keepdims=True) + norm_epsilon)
    scaled_two = middle * inverse_two
    normed_two = (scaled_two * gain_mixture).astype(jnp.bfloat16)
    kept = (inverse_one, scaled_one, normed, query, key, value, attention, context, inverse_two, scaled_two, normed_two)
    return middle, normed_two, kept


def gates(everyone, up_weight):
    both = dot(everyone, up_weight)
    return both[:, :FFE], both[:, FFE:]


def expert_forward(everyone, mask, router, expert, count, me):
    up_weight, down_weight = expert
    chance = router_chances(everyone, router)
    own = jnp.arange(count, dtype=jnp.int32) == me
    weight = jnp.sum(jnp.where(own[None, :] & mask, chance, 0.0), axis=-1)
    gate, up = gates(everyone, up_weight)
    activated = (jax.nn.silu(gate) * up).astype(jnp.bfloat16)
    share = (dot(activated, down_weight) * weight[:, None]).astype(jnp.bfloat16)
    return share, weight, (gate, up)


def expert_backward(grads, everyone, weight, mask, held, expert):
    up_weight, down_weight = expert
    gate, up = held if held is not None else gates(everyone, up_weight)
    sigmoid = jax.nn.sigmoid(gate)
    silu = gate * sigmoid
    activated = silu * up
    grad_plain = dot_columns(grads, down_weight)
    grad_weight = jnp.where(mask[:, 0], jnp.sum(activated * grad_plain, axis=-1), 0.0)
    grad_act = grad_plain * weight[:, None]
    grad_gate = grad_act * up * sigmoid * (1.0 + gate * (1.0 - sigmoid))
    grad_gate_up = jnp.concatenate([grad_gate, grad_act * silu], axis=-1).astype(jnp.bfloat16)
    grad_down = dot_rows((activated * weight[:, None]).astype(jnp.bfloat16), grads)
    grad_up_weight = dot_rows(everyone, grad_gate_up)
    share = dot_columns(grad_gate_up, up_weight).astype(jnp.bfloat16)
    return share, grad_weight, grad_up_weight, grad_down


def pieces(value):
    return value.reshape(-1, CHUNK_ROWS, *value.shape[1:])


def mixture_forward(normed_two, router, mask, expert, count, me):
    (spread,) = gather_all([normed_two], count, 0)
    everyone = spread.reshape(-1, MODEL_WIDTH)
    if everyone.shape[0] <= CHUNK_ROWS:
        share, weight, held = expert_forward(everyone, mask, router, expert, count, me)
    else:
        share, weight = lax.map(
            lambda part: expert_forward(part[0], part[1], router, expert, count, me)[:2], (pieces(everyone), pieces(mask)))
        held = None
    (mixed,) = reduce_all([share.reshape(spread.shape)], count, 1)
    return mixed, (everyone, weight.reshape(-1), held)


def mixture_backward(grad_out, mask, kept, expert, count):
    everyone, weight, held = kept
    (spread,) = gather_all([grad_out], count, 0)
    grads = spread.reshape(-1, MODEL_WIDTH)
    if grads.shape[0] <= CHUNK_ROWS:
        share, grad_weight, grad_up, grad_down = expert_backward(grads, everyone, weight, mask, held, expert)
    else:
        def step(sums, part):
            share, grad_weight, grad_up, grad_down = expert_backward(*part, None, expert)
            return (sums[0] + grad_up, sums[1] + grad_down), (share, grad_weight)

        zero = tuple(jnp.zeros(w.shape, jnp.float32) for w in expert)
        (grad_up, grad_down), (share, grad_weight) = lax.scan(
            step, zero, (pieces(grads), pieces(everyone), pieces(weight), pieces(mask)))
    grad_chance = lax.all_to_all(grad_weight.reshape(count, DEVICE_ROWS), "dp", split_axis=0, concat_axis=0, tiled=True)
    (mixed,) = reduce_all([share.reshape(spread.shape)], count, 1)
    return mixed, grad_chance.T, grad_up, grad_down


def front_backward(grad_out, grad_mixed, grad_chance, kept, place, weights):
    joint, result_output, router, gain_attention, gain_mixture = weights
    allowed, cosine, sine = place
    inverse_one, scaled_one, normed, query, key, value, attention, context, inverse_two, scaled_two, normed_two = kept
    rows = normed.shape[0]
    chance = router_chances(normed_two, router)
    grad_logit = (chance * (grad_chance - jnp.sum(grad_chance * chance, axis=-1, keepdims=True))).astype(jnp.bfloat16)
    grad_router = dot_rows(normed_two, grad_logit)
    grad_normed_two = grad_mixed + dot_columns(grad_logit, router)
    grad_gain_two = jnp.sum(grad_normed_two * scaled_two, axis=0)
    scaled_grad_two = grad_normed_two * gain_mixture
    grad_middle = grad_out + inverse_two * (scaled_grad_two - scaled_two * jnp.mean(scaled_grad_two * scaled_two, axis=-1, keepdims=True))
    branch = grad_middle.astype(jnp.bfloat16)
    grad_output = dot_rows(context, branch)
    grad_context = dot_columns(branch, result_output).astype(jnp.bfloat16).reshape(rows, KEY_VALUE_HEADS, GROUP, HEAD_SIZE)
    grad_attention = jnp.einsum("qhgd,khd->hgqk", grad_context, value, preferred_element_type=jnp.float32)
    grad_value = jnp.einsum("hgqk,qhgd->khd", attention.astype(jnp.bfloat16), grad_context, preferred_element_type=jnp.float32)
    grad_scores = (attention * (grad_attention - jnp.sum(grad_attention * attention, axis=-1, keepdims=True))).astype(jnp.bfloat16)
    grad_query = jnp.einsum("hgqk,khd->qhgd", grad_scores, key, preferred_element_type=jnp.float32).reshape(rows, QUERY_HEADS, HEAD_SIZE)
    grad_key = jnp.einsum("hgqk,qhgd->khd", grad_scores, query, preferred_element_type=jnp.float32)
    grad_query = rotary_embedding(grad_query * SCORE_SCALE, cosine, -sine)
    grad_key = rotary_embedding(grad_key * SCORE_SCALE, cosine, -sine)
    grad_projected = jnp.concatenate(
        [grad_query.reshape(rows, -1), grad_key.reshape(rows, -1), grad_value.reshape(rows, -1)], axis=-1).astype(jnp.bfloat16)
    grad_joint = dot_rows(normed, grad_projected)
    grad_normed = dot_columns(grad_projected, joint)
    grad_gain_one = jnp.sum(grad_normed * scaled_one, axis=0)
    scaled_grad_one = grad_normed * gain_attention
    grad_hidden = grad_middle + inverse_one * (scaled_grad_one - scaled_one * jnp.mean(scaled_grad_one * scaled_one, axis=-1, keepdims=True))
    return grad_hidden, (grad_joint, grad_output, grad_router, grad_gain_one, grad_gain_two)


def small_halves(rows, router, gains, codes):
    second = jnp.concatenate([gains, codes], axis=1)
    width = -(-max(router.shape[1], second.shape[1]) // 128) * 128
    pad = lambda v: jnp.pad(v, ((0, 0), (0, width - v.shape[1])))
    return pad(router), pad(second)


def body(tokens, cotangent, lengths, routes, combined_weight, output_weight, router_weight, attention_gain, mixture_gain,
         expert_gate_up, expert_down):
    count = lax.axis_size("dp")
    me, sec = lax.axis_index("dp"), lax.axis_index("section")
    layers = lax.axis_size("section")
    leading = sec == 0
    shard = combined_weight.shape[1]
    micro = lambda a, axis: lax.dynamic_index_in_dim(a, sec, axis, keepdims=False)

    gains = jnp.stack([attention_gain[0], mixture_gain[0]], axis=1)
    codes = routes[0].astype(jnp.bfloat16).reshape(-1)
    code_count = codes.shape[0]
    codes = jnp.pad(codes, (0, -code_count % shard)).reshape(shard, -1)
    small = small_halves(shard, router_weight[0], gains, codes)
    small_width = small[0].shape[1]
    halves = [
        (combined_weight[0, :, : combined_weight.shape[2] // 2], combined_weight[0, :, combined_weight.shape[2] // 2 :]),
        (output_weight[0, :, : output_weight.shape[2] // 2], output_weight[0, :, output_weight.shape[2] // 2 :]),
        small,
    ]
    widths = [h[0].shape[1] for h in halves]
    mine = jnp.concatenate([jnp.where(leading, a, b) for a, b in halves], axis=1)
    given = swapped(jnp.concatenate([jnp.where(leading, b, a) for a, b in halves], axis=1))
    packs = [jnp.where(leading, mine, given), jnp.where(leading, given, mine)]
    partner_expert = tuple(swapped(w[0, 0]) for w in (expert_gate_up, expert_down))
    own_expert = (expert_gate_up[0, 0], expert_down[0, 0])
    fused = count * DEVICE_ROWS <= CHUNK_ROWS
    experts, routers = [], []
    for layer in range(0 if fused else layers):
        keep = sec == layer
        experts.append((jnp.where(keep, expert_gate_up[0, 0], partner_expert[0]), jnp.where(keep, expert_down[0, 0], partner_expert[1])))

    def layer_parts(layer):
        at, parts = 0, []
        for w in widths:
            parts.append(packs[layer][:, at : at + w])
            at += w
        return parts

    def layer_weights(arrays):
        joint, output, tail = [a.reshape(MODEL_WIDTH, -1) for a in arrays]
        second = tail[:, small_width:]
        weights = (joint, output, tail[:, : router_weight.shape[2]], second[:, 0].astype(jnp.float32), second[:, 1].astype(jnp.float32))
        routers.append(tail[:, :small_width])
        code = second[:, 2 : 2 + codes.shape[1]].reshape(count, -1)[:, :code_count].reshape(count, -1, DEVICE_ROWS, TOPK)
        named = lax.dynamic_index_in_dim(code, sec, 1, keepdims=False).reshape(count * DEVICE_ROWS, TOPK)
        mask = jnp.any(named == me.astype(jnp.bfloat16), axis=-1, keepdims=True)
        return weights, mask

    segment, token_position = layout(micro(lengths[:, 0], 0))
    row_ids = jnp.arange(DEVICE_ROWS, dtype=jnp.int32)
    allowed = (row_ids[:, None] >= row_ids[None, :]) & (segment[:, None] == segment[None, :])
    place = (allowed,) + rotation(token_position)

    weights, masks, stores = [], [], []
    hidden = micro(tokens, 0)
    for layer in range(layers):
        if not fused:
            arrays = gather_all(layer_parts(layer), count, 2, pair=True)
        elif layer == 0:
            arrays = weight_spread(packs[layer], widths, count, 2)
        got, mask = layer_weights(arrays)
        weights.append(got)
        masks.append(mask)
        middle, normed_two, kept = front(hidden.astype(jnp.float32), place, got)
        if not fused:
            mixed, kept_mixture = mixture_forward(normed_two, got[2], mask, experts[layer], count, me)
        else:
            named = mask.astype(jnp.bfloat16).reshape(count, DEVICE_ROWS, 1)
            call = lambda mode, cid, *data, **more: mixture_call(
                mode, count, layer, cid, named, routers[layer], own_expert, partner_expert, *data, **more)
            if layer < layers - 1:
                mixed, everyone, *arrays = call("f", 4, normed_two, following=packs[layer + 1], widths=tuple(widths))
                kept_mixture = (named, everyone)
            else:
                mixed, *kept_mixture = call("fb", 5, normed_two, micro(cotangent, 0))
        hidden = (middle + mixed).astype(jnp.bfloat16)
        stores.append((kept, kept_mixture))
    last = hidden
    grad = micro(cotangent, 0)
    shares, expert_grads = [None] * layers, [None] * layers
    for layer in reversed(range(layers)):
        kept, kept_mixture = stores[layer]
        if not fused:
            mixed, grad_chance, grad_up, grad_down = mixture_backward(grad, masks[layer], kept_mixture, experts[layer], count)
        else:
            if layer < layers - 1:
                named, everyone = kept_mixture
                kept_mixture = mixture_call("b", count, layer, 6, named, routers[layer], own_expert, partner_expert, everyone, grad,
                                            summed=packs[layer + 1])
            mixed, rows, grad_up, grad_down, *more = kept_mixture
            if more:
                shares[layer + 1] = more[0]
            grad_chance = rows[:, 0].T
        expert_grads[layer] = (grad_up, grad_down)
        grad_hidden, parts = front_backward(grad.astype(jnp.float32), mixed, grad_chance, kept, place, weights[layer])
        grad = grad_hidden.astype(jnp.bfloat16)
        tail = small_halves(MODEL_WIDTH, parts[2], jnp.stack([parts[3], parts[4]], axis=1), parts[2][:, :0])
        packed = [parts[0], parts[1], jnp.concatenate(tail, axis=1)]
        packs[layer] = [a.astype(jnp.bfloat16).reshape(count, shard, -1) for a in packed]
        if not fused:
            shares[layer] = reduce_all(packs[layer], count, 3, pair=True)
    if fused:
        *outs, grad_up, grad_down, boundary = closing(packs[0], shares[1], expert_grads[0], expert_grads[1], grad, last, count, 3)
        half = outs[2].shape[1] // 2
        return (
            boundary[None],
            outs[0][None],
            outs[1][None],
            outs[2][None, :, : router_weight.shape[2]],
            outs[2][None, :, half],
            outs[2][None, :, half + 1],
            grad_up[None, None],
            grad_down[None, None],
        )
    outs = []
    for a in range(3):
        kept_half = jnp.where(leading, shares[0][a], shares[1][a])
        got_half = swapped(jnp.where(leading, shares[1][a], shares[0][a]))
        outs.append(jnp.concatenate([jnp.where(leading, kept_half, got_half), jnp.where(leading, got_half, kept_half)], axis=1))
    expert_outs = []
    for a in range(2):
        kept_sum = jnp.where(leading, expert_grads[0][a], expert_grads[1][a])
        got_sum = swapped(jnp.where(leading, expert_grads[1][a], expert_grads[0][a]))
        expert_outs.append((kept_sum + got_sum)[None, None])
    partner = swapped(jnp.where(leading, last, grad))
    boundary = jnp.where(leading, jnp.stack([grad, partner]), jnp.stack([partner, last]))[None]
    half = outs[2].shape[1] // 2
    return (
        boundary,
        outs[0][None],
        outs[1][None],
        outs[2][None, :, : router_weight.shape[2]],
        outs[2][None, :, half],
        outs[2][None, :, half + 1],
        expert_outs[0],
        expert_outs[1],
    )


def solution(mesh):
    return jax.shard_map(
        body,
        mesh=mesh,
        in_specs=(
            P(None, "dp", None),
            P(None, "dp", None),
            P(None, "dp", None),
            P("section", None, "dp", None),
            P("section", "dp", None),
            P("section", "dp", None),
            P("section", "dp", None),
            P("section", "dp"),
            P("section", "dp"),
            P("section", "dp", None, None),
            P("section", "dp", None, None),
        ),
        out_specs=(
            P("section", None, "dp", None),
            P("section", "dp", None),
            P("section", "dp", None),
            P("section", "dp", None),
            P("section", "dp"),
            P("section", "dp"),
            P("section", "dp", None, None),
            P("section", "dp", None, None),
        ),
        check_vma=False,
    )
```

```python
import functools
import jax
import jax.numpy as jnp
from jax import lax
from jax.experimental import pallas as pl
from jax.experimental.pallas import tpu as pltpu
from jax.sharding import PartitionSpec as P

MODEL_WIDTH = 1536
QUERY_HEADS = 24
KEY_VALUE_HEADS = 8
GROUP = QUERY_HEADS // KEY_VALUE_HEADS
HEAD_SIZE = 64
FFE = 512
TOPK = 8
DEVICE_ROWS = 128
NSEQ = 4
QUERY_WIDTH = QUERY_HEADS * HEAD_SIZE
KEY_WIDTH = KEY_VALUE_HEADS * HEAD_SIZE
SCORE_SCALE = HEAD_SIZE ** (-0.5)
norm_epsilon = 1e-06
CHUNK_ROWS = 2048

VMEM_BYTES = 67_000_000


def torus_axes(count):
    side = 1
    while (side + 1) ** 3 <= count:
        side += 1
    assert count % (side * side) == 0
    return [(side * side, count // (side * side)), (1, side), (side, side)]


def offsets(sizes):
    return [(k, j, i) for k in range(sizes[0]) for j in range(sizes[1]) for i in range(sizes[2])]


class Place:
    def __init__(self, axes, order):
        self.me = lax.axis_index("dp")
        self.sec = lax.axis_index("section")
        long, first, second = axes
        if order is None:
            flip = self.sec
            stride_one = first[0] + (second[0] - first[0]) * flip
            stride_two = second[0] + (first[0] - second[0]) * flip
            assert first[1] == second[1]
            self.axes = [long, (stride_one, first[1]), (stride_two, second[1])]
        elif order == 0:
            self.axes = [long, first, second]
        else:
            self.axes = [long, second, first]
        self.sizes = [size for _, size in self.axes]

    def moved(self, steps):
        out = self.me
        for (stride, size), step in zip(self.axes, steps):
            if step % size:
                digit = lax.rem(lax.div(self.me, stride), size)
                out = out + (lax.rem(digit + (step % size), size) - digit) * stride
        return out

    def source(self, offs):
        return self.moved([-o for o in offs])

    def target(self, offs):
        return self.moved(list(offs))

    def flat(self, offs):
        return (offs[0] * self.sizes[1] + offs[1]) * self.sizes[2] + offs[2]


def last_hop(offs):
    for axis in (2, 1, 0):
        if offs[axis]:
            hop = [0, 0, 0]
            hop[axis] = offs[axis]
            base = list(offs)
            base[axis] = 0
            return tuple(hop), tuple(base)
    return None


def greet(axes, pair):
    place = Place(axes, 0)
    barrier = pltpu.get_barrier_semaphore()
    count = 0
    for axis in range(3):
        for step in range(1, place.sizes[axis]):
            hop = [0, 0, 0]
            hop[axis] = step
            pl.semaphore_signal(barrier, inc=1, device_id={"dp": place.target(hop)}, device_id_type=pl.DeviceIdType.MESH)
            count += 1
    if pair:
        pl.semaphore_signal(barrier, inc=1, device_id={"section": 1 - place.sec}, device_id_type=pl.DeviceIdType.MESH)
        count += 1
    pl.semaphore_wait(barrier, count)


def gather_kernel(axes, pair, count, *refs):
    ins, outs = refs[:count], refs[count : 2 * count]
    send, recv, local = refs[2 * count : 2 * count + 3]
    psend, precv = refs[2 * count + 3 :] if pair else (None, None)
    streams = []
    for a in range(count):
        if pair:
            place = Place(axes, None)
            half = ins[a].shape[1]
            cols = pl.ds(pl.multiple_of(place.sec * half, 128), half)
            streams.append((place, ins[a], lambda b, o=outs[a], c=cols: o.at[b, :, c]))
        else:
            half = ins[a].shape[0] // 2
            for h in range(2):
                rows = pl.ds(h * half, half)
                streams.append((Place(axes, h), ins[a].at[rows], lambda b, o=outs[a], r=rows: o.at[b, r]))

    def copy(s, offs):
        place, own, out = streams[s]
        hop, base = last_hop(offs)
        block = place.source(base)
        src = out(block) if any(base) else own
        f = place.flat(offs)
        return pltpu.make_async_remote_copy(
            src_ref=src, dst_ref=out(block), send_sem=send.at[s, f], recv_sem=recv.at[s, f],
            device_id={"dp": place.target(hop)}, device_id_type=pl.DeviceIdType.MESH)

    def share(s, offs):
        place, own, out = streams[s]
        block = place.source(offs)
        src = out(block) if any(offs) else own
        f = place.flat(offs)
        return pltpu.make_async_remote_copy(
            src_ref=src, dst_ref=out(block), send_sem=psend.at[s, f], recv_sem=precv.at[s, f],
            device_id={"section": 1 - place.sec}, device_id_type=pl.DeviceIdType.MESH)

    greet(axes, pair)
    ids = range(len(streams))
    n0, n1, n2 = streams[0][0].sizes
    keep = []
    for s in ids:
        place, own, out = streams[s]
        c = pltpu.make_async_copy(own, out(place.me), local.at[s])
        c.start()
        keep.append(c)
    for k in range(1, n0):
        for s in ids:
            copy(s, (k, 0, 0)).start()

    def first(k):
        for s in ids:
            if k:
                copy(s, (k, 0, 0)).wait_recv()
            for j in range(1, n1):
                copy(s, (k, j, 0)).start()
            for i in range(1, n2):
                copy(s, (k, 0, i)).start()
            if pair:
                share(s, (k, 0, 0)).start()

    def second(k):
        for j in range(1, n1):
            for s in ids:
                copy(s, (k, j, 0)).wait_recv()
                for i in range(1, n2):
                    copy(s, (k, j, i)).start()
                if pair:
                    share(s, (k, j, 0)).start()

    def third(k):
        for j in range(n1):
            for i in range(1, n2):
                for s in ids:
                    copy(s, (k, j, i)).wait_recv()
                    if pair:
                        share(s, (k, j, i)).start()

    for k in range(n0 + 2):
        if k < n0:
            first(k)
        if 0 <= k - 1 < n0:
            second(k - 1)
        if 0 <= k - 2 < n0:
            third(k - 2)
    for s in ids:
        for offs in offsets((n0, n1, n2)):
            if any(offs):
                copy(s, offs).wait_send()
            if pair:
                share(s, offs).wait()
    for c in keep:
        c.wait()


def gather_all(arrays, count, cid, pair=False):
    axes = torus_axes(count)
    streams = len(arrays) * (1 if pair else 2)
    sem = pltpu.SemaphoreType.DMA((streams, count))
    out_shape = [jax.ShapeDtypeStruct((count, a.shape[0], a.shape[1] * (2 if pair else 1)), a.dtype) for a in arrays]
    scratch = [sem, sem, pltpu.SemaphoreType.DMA((streams,))]
    if pair:
        scratch += [sem, sem]
    sent = sum(a.size * a.dtype.itemsize for a in arrays) * (count - 1)
    return pl.pallas_call(
        functools.partial(gather_kernel, axes, pair, len(arrays)),
        out_shape=out_shape,
        in_specs=[pl.BlockSpec(memory_space=pltpu.VMEM)] * len(arrays),
        out_specs=[pl.BlockSpec(memory_space=pl.ANY)] * len(arrays),
        scratch_shapes=scratch,
        compiler_params=pltpu.CompilerParams(collective_id=cid, has_side_effects=True),
        cost_estimate=pl.CostEstimate(flops=0, bytes_accessed=2 * sent, transcendentals=0),
        name="spread" if not pair else "spread_pair",
    )(*arrays)


def reduce_kernel(axes, pair, count, *refs):
    ins, outs = refs[:count], refs[count : 2 * count]
    rest = list(refs[2 * count :])
    send, recv = rest[:2]
    rest = rest[2:]
    if pair:
        psend, precv = rest[:2]
        rest = rest[2:]
    streams = []
    for a in range(count):
        if pair:
            got, held, pgot, psum = rest[:4]
            rest = rest[4:]
            place = Place(axes, None)
            half = outs[a].shape[1]
            mine = pl.ds(pl.multiple_of(place.sec * half, 128), half)
            other = pl.ds(pl.multiple_of((1 - place.sec) * half, 128), half)
            streams.append(dict(place=place, got=got, held=held, pgot=pgot, psum=psum, raw=ins[a], mine=mine, other=other,
                                out=outs[a], rows=outs[a].shape[0]))
        else:
            got, held = rest[:2]
            rest = rest[2:]
            half = outs[a].shape[0] // 2
            for h in range(2):
                rows = pl.ds(h * half, half)
                streams.append(dict(place=Place(axes, h), got=got.at[h], held=held.at[h], raw=ins[a], span=rows,
                                    out=outs[a].at[rows], rows=half))
    step = 8 if streams[0]["rows"] % 16 else 16

    def own_ref(t, offs):
        if pair:
            return t["psum"].at[t["place"].flat(offs)]
        return t["raw"].at[t["place"].target(offs), t["span"]]

    def summed(t, sources, dest):
        def one(r, _):
            rows = pl.ds(pl.multiple_of(r * step, step), step)
            total = sources[0][rows].astype(jnp.float32)
            for source in sources[1:]:
                total = total + source[rows].astype(jnp.float32)
            dest[rows] = total.astype(dest.dtype)
            return 0

        lax.fori_loop(0, t["rows"] // step, one, 0)

    def copy(s, offs):
        t = streams[s]
        place = t["place"]
        hop, base = last_hop(offs)
        f = place.flat(offs)
        src = own_ref(t, offs) if hop[2] else t["held"].at[f // place.sizes[2]]
        return pltpu.make_async_remote_copy(
            src_ref=src, dst_ref=t["got"].at[f], send_sem=send.at[s, f], recv_sem=recv.at[s, f],
            device_id={"dp": place.target(hop)}, device_id_type=pl.DeviceIdType.MESH)

    def share(s, offs):
        t = streams[s]
        place = t["place"]
        f = place.flat(offs)
        return pltpu.make_async_remote_copy(
            src_ref=t["raw"].at[place.target((offs[0], offs[2], offs[1])), :, t["other"]], dst_ref=t["pgot"].at[f],
            send_sem=psend.at[s, f], recv_sem=precv.at[s, f],
            device_id={"section": 1 - place.sec}, device_id_type=pl.DeviceIdType.MESH)

    ids = range(len(streams))
    n0, n1, n2 = streams[0]["place"].sizes
    greet(axes, pair)

    def phase_pair(k):
        for j in reversed(range(n1)):
            for i in reversed(range(n2)):
                for s in ids:
                    share(s, (k, j, i)).start()

    def phase_first(k):
        for j in reversed(range(n1)):
            for i in reversed(range(n2)):
                for s in ids:
                    t = streams[s]
                    if pair:
                        share(s, (k, j, i)).wait_recv()
                        f = t["place"].flat((k, j, i))
                        summed(t, [t["raw"].at[t["place"].target((k, j, i)), :, t["mine"]], t["pgot"].at[f]], t["psum"].at[f])
                    if i:
                        copy(s, (k, j, i)).start()

    def phase_second(k):
        for j in range(1, n1):
            for s in ids:
                t = streams[s]
                for i in range(1, n2):
                    copy(s, (k, j, i)).wait_recv()
                parts = [own_ref(t, (k, j, 0))] + [t["got"].at[t["place"].flat((k, j, i))] for i in range(1, n2)]
                summed(t, parts, t["held"].at[t["place"].flat((k, j, 0)) // n2])
                copy(s, (k, j, 0)).start()

    def gathered_parts(s, k):
        t = streams[s]
        offs = [(k, 0, i) for i in range(1, n2)] + [(k, j, 0) for j in range(1, n1)]
        for o in offs:
            copy(s, o).wait_recv()
        return [own_ref(t, (k, 0, 0))] + [t["got"].at[t["place"].flat(o)] for o in offs]

    def phase_third(k):
        for s in ids:
            t = streams[s]
            parts = gathered_parts(s, k)
            if k:
                summed(t, parts, t["held"].at[t["place"].flat((k, 0, 0)) // n2])
                copy(s, (k, 0, 0)).start()
            else:
                for q in range(1, n0):
                    copy(s, (q, 0, 0)).wait_recv()
                    parts.append(t["got"].at[t["place"].flat((q, 0, 0))])
                summed(t, parts, t["out"])

    chunks = list(range(1, n0)) + [0]
    if pair:
        phase_pair(chunks[0])
    for c in range(n0 + 3):
        if pair and c + 1 < n0:
            phase_pair(chunks[c + 1])
        if c < n0:
            phase_first(chunks[c])
        if 0 <= c - 1 < n0:
            phase_second(chunks[c - 1])
        if 0 <= c - 2 < n0:
            phase_third(chunks[c - 2])
    for s in ids:
        for offs in offsets((n0, n1, n2)):
            if any(offs):
                copy(s, offs).wait_send()
            if pair:
                share(s, offs).wait_send()


def reduce_all(arrays, count, cid, pair=False):
    axes = torus_axes(count)
    streams = len(arrays) * (1 if pair else 2)
    sem = pltpu.SemaphoreType.DMA((streams, count))
    scratch = [sem, sem]
    if pair:
        scratch += [sem, sem]
    groups = count // axes[2][1]
    out_shape = []
    for a in arrays:
        rows, cols = a.shape[1:]
        if pair:
            cols = cols // 2
            scratch += [pltpu.VMEM((count, rows, cols), a.dtype), pltpu.VMEM((groups, rows, cols), a.dtype),
                        pltpu.VMEM((count, rows, cols), a.dtype), pltpu.VMEM((count, rows, cols), a.dtype)]
        else:
            scratch += [pltpu.VMEM((2, count, rows // 2, cols), a.dtype), pltpu.VMEM((2, groups, rows // 2, cols), a.dtype)]
        out_shape.append(jax.ShapeDtypeStruct((rows, cols), jnp.float32))
    sent = sum(a.size * a.dtype.itemsize for a in arrays)
    return pl.pallas_call(
        functools.partial(reduce_kernel, axes, pair, len(arrays)),
        out_shape=out_shape,
        in_specs=[pl.BlockSpec(memory_space=pltpu.VMEM)] * len(arrays),
        out_specs=[pl.BlockSpec(memory_space=pltpu.VMEM)] * len(arrays),
        scratch_shapes=scratch,
        compiler_params=pltpu.CompilerParams(collective_id=cid, has_side_effects=True, vmem_limit_bytes=VMEM_BYTES),
        cost_estimate=pl.CostEstimate(flops=0, bytes_accessed=2 * sent, transcendentals=0),
        name="fold" if not pair else "fold_pair",
    )(*arrays)


ROWS = 128
TILE = 512
STRIP = 16
SPAN = 512
SKIP = set()
PIECE = 256
MESH = pl.DeviceIdType.MESH
ORDERS = ((0, 1, 2), (0, 2, 1), (1, 0, 2), (2, 0, 1))
TOKEN_PARTS = tuple((order, 32 * n, 32) for n, order in enumerate(ORDERS))


class Route:
    def __init__(self, axes, order):
        self.axes, self.order = axes, order
        self.sizes = [size for _, size in axes]
        assert self.sizes == [4, 2, 2]
        self.me = lax.axis_index("dp")
        self.all = offsets(self.sizes)
        self.others = [o for o in self.all if any(o)]
        self.z = lax.div(self.me, axes[0][0])
        self.inner = jnp.logical_and(self.z >= 1, self.z <= 2)
        later = order[order.index(0) + 1 :]
        self.lines = [(j, i) for j in range(2) for i in range(2) if all((0, j, i)[a] == 0 for a in later)]

    def digit(self, axis):
        stride, size = self.axes[axis]
        return lax.rem(lax.div(self.me, stride), size)

    def plane(self, rank):
        z = self.z
        if rank == 1:
            return z + 1 - 2 * lax.rem(z, 2)
        if rank == 2:
            return 2 - lax.div(z, 2)
        if rank == 3:
            return 3 - 3 * lax.div(z, 2)
        return z

    def block(self, offs):
        out = self.me + (self.plane(offs[0]) - self.z) * self.axes[0][0]
        for axis in (1, 2):
            if offs[axis]:
                out = out + (1 - 2 * self.digit(axis)) * self.axes[axis][0]
        return out

    def flat(self, offs):
        return (offs[0] * 2 + offs[1]) * 2 + offs[2]

    def extra(self, line, n):
        return 16 + 2 * self.lines.index(line) + n

    def last_axis(self, offs):
        for axis in reversed(self.order):
            if offs[axis]:
                return axis

    def base(self, offs):
        out = list(offs)
        out[self.last_axis(offs)] = 0
        return tuple(out)

    def across(self, offs):
        return [o for o in self.others if self.last_axis(o) and self.base(o) == offs]


def remote(src, dst, send, recv, peer):
    return pltpu.make_async_remote_copy(src_ref=src, dst_ref=dst, send_sem=send, recv_sem=recv, device_id=peer, device_id_type=MESH)


class Spread:
    def __init__(self, streams, send, recv):
        self.streams, self.send, self.recv = streams, send, recv
        self.ids = range(len(streams))

    def copy(self, s, offs, target, key, slot):
        route, own, out = self.streams[s]
        block = route.block(offs)
        return remote(out(block) if any(offs) else own, out(block), self.send.at[s, slot], self.recv.at[s, route.flat(key)], {"dp": target})

    def arrival(self, s, offs):
        route, own, out = self.streams[s]
        f = route.flat(offs)
        return remote(own, out(route.block(offs)), self.send.at[s, f], self.recv.at[s, f], {"dp": route.block(offs)})

    def onward(self, s, offs):
        route = self.streams[s][0]
        k, line = offs[0], offs[1:]
        out = [(o, False, self.copy(s, offs, route.block((0, *[int(o[a] != offs[a]) for a in (1, 2)])), o, route.flat(o)))
               for o in route.across(offs)]
        if line in route.lines:
            near, facing = route.block((1, 0, 0)), route.block((2, 0, 0))
            if k == 0:
                out.append(((1, *line), False, self.copy(s, offs, near, (1, *line), route.flat((1, *line)))))
                out.append(((2, *line), True, self.copy(s, offs, facing, (2, *line), route.extra(line, 0))))
            elif k == 1:
                out.append(((3, *line), True, self.copy(s, offs, facing, (3, *line), route.extra(line, 1))))
            else:
                out.append((offs, True, self.copy(s, offs, near, offs, route.flat(offs))))
        return out

    def launch(self, items):
        for s, (_, inner, copy) in items:
            if inner:
                pl.when(self.streams[s][0].inner)(copy.start)
            else:
                copy.start()

    def step(self, t):
        if "comm" in SKIP or "ag" in SKIP:
            return
        work = [(offs, s) for s in self.ids for offs in self.streams[s][0].all if offs[0] + offs[1] + offs[2] == t]
        if t == 0:
            first = [(s, item) for offs, s in work for item in self.onward(s, offs)]
            self.launch(sorted(first, key=lambda e: (e[1][0][0], e[1][0], e[0])))
            return
        ends = lambda e: not self.streams[e[1]][0].across(e[0]) and e[0][1:] not in self.streams[e[1]][0].lines
        for offs, s in sorted(work, key=lambda e: (ends(e), -e[0][0], e[0], e[1])):
            self.arrival(s, offs).wait_recv()
            self.launch([(s, item) for item in sorted(self.onward(s, offs), key=lambda e: (e[1], e[0]))])

    def end(self):
        if "comm" in SKIP or "ag" in SKIP:
            return
        for s in self.ids:
            for offs in self.streams[s][0].all:
                for _, inner, copy in self.onward(s, offs):
                    if inner:
                        pl.when(self.streams[s][0].inner)(copy.wait_send)
                    else:
                        copy.wait_send()


SPREAD_STEPS = 6


def add_rows(sources, dest, rows, step=16):
    cols = dest.shape[-1]
    width = 768 if cols % 768 == 0 else cols

    def one(r, _):
        at = pl.ds(pl.multiple_of(r * step, step), step)

        def part(c, _):
            span = pl.ds(pl.multiple_of(c * width, width), width)
            total = sources[0][at, span].astype(jnp.float32)
            for source in sources[1:]:
                total = total + source[at, span].astype(jnp.float32)
            dest[at, span] = total.astype(dest.dtype)
            return 0

        return lax.fori_loop(0, cols // width, part, 0)

    lax.fori_loop(0, rows // step, one, 0)


class Fold:
    def __init__(self, streams, send, recv, ranks):
        self.streams, self.send, self.recv = streams, send, recv
        self.ids = range(len(streams))
        self.turn = {k: c for c, k in enumerate(ranks)}
        self.plan = []
        for s in self.ids:
            route = self.streams[s][0]
            for offs in route.all:
                if offs[0] and offs[1:] in route.lines:
                    self.plan.append((self.ready(route, offs), 1, -offs[0], s, offs, self.outer))
                    self.plan.append((self.passed(route, offs), 2, -offs[0], s, offs, self.middle))
                else:
                    when = self.done(route, offs)
                    rank = 3 if not any(offs) else 1 if self.near(route, offs) or not offs[0] and offs[1:] in route.lines else 0
                    self.plan.append((when, rank, -offs[0], s, offs, self.plain))
        self.plan.sort(key=lambda e: e[:5])

    def near(self, route, offs):
        return [o for o in route.across(offs) if o[0] == offs[0]]

    def ready(self, route, offs):
        return max([self.turn[offs[0]]] + [self.done(route, o) + 1 for o in self.near(route, offs)])

    def passed(self, route, offs):
        line = offs[1:]
        return self.ready(route, offs) + 1 if offs[0] > 1 else max(self.ready(route, offs), self.ready(route, (3, *line)) + 2)

    def done(self, route, offs):
        when = self.ready(route, offs)
        if not offs[0] and offs[1:] in route.lines:
            when = max(when, self.passed(route, (1, *offs[1:])) + 1, self.passed(route, (2, *offs[1:])) + 1)
        return when

    def arrival(self, s, slot):
        route, share, got, _, _ = self.streams[s]
        return remote(share((0, 0, 0)), got(slot), self.send.at[s, slot], self.recv.at[s, slot], {"dp": route.block((1, 0, 0))})

    def copy(self, s, offs):
        route, share, got, _, _ = self.streams[s]
        f = route.flat(offs)
        if route.last_axis(offs):
            hop = [0, 0, 0]
            hop[route.last_axis(offs)] = 1
            return remote(share(offs), got(f), self.send.at[s, f], self.recv.at[s, f], {"dp": route.block(hop)})
        near, facing = route.block((1, 0, 0)), route.block((2, 0, 0))
        if offs[0] == 1:
            return remote(share(offs), got(f), self.send.at[s, f], self.recv.at[s, f], {"dp": near})
        slot = f + (route.extra(offs[1:], offs[0] - 2) - f) * route.inner.astype(jnp.int32)
        return remote(share(offs), got(slot), self.send.at[s, f], self.recv.at[s, slot], {"dp": jnp.where(route.inner, facing, near)})

    def settle(self, s, offs, slots, out=None):
        route, share, got, _, rows = self.streams[s]
        if slots:
            for f in slots:
                self.arrival(s, f).wait_recv()
            own = share(offs)
            add_rows([own] + [got(f) for f in slots], own if out is None else out, rows)

    def outer(self, s, offs):
        route = self.streams[s][0]
        self.settle(s, offs, [route.flat(o) for o in self.near(route, offs)])
        pl.when(jnp.logical_not(route.inner))(self.copy(s, offs).start)

    def middle(self, s, offs):
        route = self.streams[s][0]

        @pl.when(route.inner)
        def _():
            self.settle(s, offs, [route.flat(offs) if offs[0] > 1 else route.extra(offs[1:], 1)])
            self.copy(s, offs).start()

    def plain(self, s, offs):
        route, share, got, out, rows = self.streams[s]
        slots = [route.flat(o) for o in self.near(route, offs)]
        if not offs[0] and offs[1:] in route.lines:
            slots.append(route.flat((1, *offs[1:])))
            facing = route.extra(offs[1:], 0)

            @pl.when(route.inner)
            def _():
                self.settle(s, offs, [facing])

        self.settle(s, offs, slots, None if any(offs) else out)
        if any(offs):
            self.copy(s, offs).start()

    def step(self, t):
        if "comm" in SKIP or "rs" in SKIP:
            return
        for when, _, _, s, offs, action in self.plan:
            if when == t:
                action(s, offs)

    def steps(self):
        return 1 + max(e[0] for e in self.plan)

    def end(self):
        if "comm" in SKIP or "rs" in SKIP:
            return
        for s in self.ids:
            for offs in self.streams[s][0].others:
                self.copy(s, offs).wait_send()


def meet(axes, everyone, pair):
    route = Route(axes, ORDERS[0])
    barrier = pltpu.get_barrier_semaphore()
    if everyone:
        for offs in route.others:
            pl.semaphore_signal(barrier, inc=1, device_id={"dp": route.block(offs)}, device_id_type=MESH)
    else:
        for offs in ((0, 0, 1), (0, 1, 0), (1, 0, 0)):
            pl.semaphore_signal(barrier, inc=1, device_id={"dp": route.block(offs)}, device_id_type=MESH)

        @pl.when(route.inner)
        def _():
            pl.semaphore_signal(barrier, inc=1, device_id={"dp": route.block((2, 0, 0))}, device_id_type=MESH)

    if pair:
        pl.semaphore_signal(barrier, inc=1, device_id={"section": 1 - lax.axis_index("section")}, device_id_type=MESH)
    pl.semaphore_wait(barrier, (len(route.others) if everyone else 3 + route.inner.astype(jnp.int32)) + (1 if pair else 0))


def contract(left, right, dims):
    return lax.dot_general(left, right, ((dims[:1], dims[1:]), ((), ())), preferred_element_type=jnp.float32)


def weight_parts(rows):
    third = rows // 3
    sizes = (third, third, third // 2, third // 2)
    return tuple((order, sum(sizes[:n]), sizes[n]) for n, order in enumerate(ORDERS))


def weight_columns(half):
    sec = lax.axis_index("section")
    return pl.ds(pl.multiple_of(sec * half, 128), half), pl.ds(pl.multiple_of((1 - sec) * half, 128), half)


def packed_columns(widths):
    return [pl.ds(sum(widths[:n]), w) for n, w in enumerate(widths)]


class WeightSpread:
    def __init__(self, axes, own, full, outs, sems):
        send, recv, self.psend, self.precv, self.local = sems
        self.own, self.full, self.outs = own, full, outs
        self.route = Route(axes, ORDERS[0])
        streams = []
        for order, at, size in weight_parts(own.shape[0]):
            rows = pl.ds(at, size)
            streams.append((Route(axes, order), own.at[rows], lambda b, r=rows: full.at[b, r]))
        self.spread = Spread(streams, send, recv)
        self.widths = [out.shape[2] // 2 for out in outs]

    def deliveries(self, offs):
        block, f = self.route.block(offs), self.route.flat(offs)
        for a, cols in enumerate(packed_columns(self.widths)):
            src = self.full.at[block, :, cols] if any(offs) else self.own.at[:, cols]
            dst = self.outs[a].at[block, :, weight_columns(self.widths[a])[0]]
            yield pltpu.make_async_copy(src, dst, self.local.at[a, f])
            yield remote(src, dst, self.psend.at[a, f], self.precv.at[a, f], {"section": 1 - lax.axis_index("section")})

    def step(self, t):
        self.spread.step(t)
        for offs in self.route.all:
            if sum(offs) == t:
                for copy in self.deliveries(offs):
                    copy.start()

    def end(self):
        self.spread.end()
        for offs in self.route.all:
            for copy in self.deliveries(offs):
                copy.wait()


def weight_shapes(pack, widths, count):
    return [jax.ShapeDtypeStruct((count, pack.shape[0], 2 * w), pack.dtype) for w in widths]


def weight_scratch(pack, widths, count):
    dma = pltpu.SemaphoreType.DMA
    return [pltpu.VMEM((count, *pack.shape), pack.dtype)] + [dma((len(ORDERS), count + 4))] * 2 + [dma((len(widths), count))] * 3


def weight_spread_kernel(axes, arrays, *refs):
    own, outs, full, sems = refs[0], refs[1 : 1 + arrays], refs[1 + arrays], refs[2 + arrays :]
    meet(axes, False, True)
    spread = WeightSpread(axes, own, full, outs, sems)
    for t in range(SPREAD_STEPS):
        spread.step(t)
    spread.end()


def weight_spread(pack, widths, count, cid):
    return pl.pallas_call(
        functools.partial(weight_spread_kernel, torus_axes(count), len(widths)),
        out_shape=weight_shapes(pack, widths, count),
        in_specs=[pl.BlockSpec(memory_space=pltpu.VMEM)],
        out_specs=[pl.BlockSpec(memory_space=pl.ANY)] * len(widths),
        scratch_shapes=weight_scratch(pack, widths, count),
        compiler_params=pltpu.CompilerParams(collective_id=cid, has_side_effects=True),
        name="weight_spread",
    )(pack)


class WeightFold:
    def __init__(self, axes, raws, total, got, load, out, sems, ranks):
        send, recv, self.psend, self.precv, self.local = sems
        self.raws, self.total, self.held, self.rows = raws, total, load, out.shape[0]
        self.widths = [raw.shape[2] // 2 for raw in raws]
        self.ranks = ranks
        streams = []
        for order, at, size in weight_parts(self.rows):
            rows, route = pl.ds(at, size), Route(axes, order)
            streams.append((route, lambda o, r=rows, w=route: total.at[w.flat(o), r], lambda f, r=rows: got.at[f, r], out.at[rows], size))
        self.route = Route(axes, ORDERS[0])
        self.fold = Fold(streams, send, recv, ranks)

    def pieces(self, c):
        cols = packed_columns(self.widths)
        return [(o, a, cols[a]) for o in self.route.all if o[0] == self.ranks[c] for a in range(len(self.raws))]

    def give(self, offs, a, cols):
        f = self.route.flat(offs)
        src = self.raws[a].at[self.route.block(offs), :, weight_columns(self.widths[a])[1]]
        return remote(src, self.total.at[f, :, cols], self.psend.at[a, f], self.precv.at[a, f], {"section": 1 - lax.axis_index("section")})

    def load(self, offs, a, cols):
        src = self.raws[a].at[self.route.block(offs), :, weight_columns(self.widths[a])[0]]
        return pltpu.make_async_copy(src, self.held.at[offs[1] * 2 + offs[2], :, cols], self.local.at[a, self.route.flat(offs)])

    def begin(self):
        for c in range(len(self.ranks)):
            for piece in self.pieces(c):
                self.give(*piece).start()
                if c == 0:
                    self.load(*piece).start()

    def step(self, t):
        if t < len(self.ranks):
            for piece in self.pieces(t):
                self.load(*piece).wait()
                self.give(*piece).wait_recv()
            for offs in self.route.all:
                if offs[0] == self.ranks[t]:
                    here = self.total.at[self.route.flat(offs)]
                    add_rows([self.held.at[offs[1] * 2 + offs[2]], here], here, self.rows)
            if t + 1 < len(self.ranks):
                for piece in self.pieces(t + 1):
                    self.load(*piece).start()
        self.fold.step(t)

    def steps(self):
        return self.fold.steps()

    def end(self):
        self.fold.end()
        for c in range(len(self.ranks)):
            for piece in self.pieces(c):
                self.give(*piece).wait_send()


def fold_shape(arrays):
    return jax.ShapeDtypeStruct((arrays[0].shape[1], sum(a.shape[2] // 2 for a in arrays)), jnp.float32)


def fold_scratch(arrays, axes):
    count, dma, block = arrays[0].shape[0], pltpu.SemaphoreType.DMA, fold_shape(arrays).shape
    blocks = [pltpu.VMEM((n, *block), jnp.bfloat16) for n in (count, count + 4, axes[1][1] * axes[2][1])]
    return blocks + [dma((len(ORDERS), count + 4))] * 2 + [dma((len(arrays), count))] * 3


def closing_kernel(axes, count, *refs):
    refs = list(refs)
    take = lambda n: [refs.pop(0) for _ in range(n)]
    raws = take(count)
    other = take(1)[0]
    first_up, first_down, last_up, last_down, grad_in, last_in = take(6)
    outs = take(count)
    up_out, down_out, edge_out = take(3)
    blocks, sems = take(3), take(5)
    result, given, taken = take(3)
    own_up, own_down, got_up, got_down, edge_give, edge_got, x_send, x_recv, x_local, h_send, h_recv = take(11)
    sec = lax.axis_index("section")
    partner = {"section": 1 - sec}
    chunks = [axes[0][1] - 1 - c for c in range(axes[0][1])]
    meet(axes, False, True)
    fold = WeightFold(axes, raws, *blocks, result, sems, chunks)
    fold.begin()
    leading = sec == 0

    def cross(src, dst, n):
        return remote(src, dst, x_send.at[n], x_recv.at[n], partner)

    edge_give[...] = jnp.where(leading, last_in[...], grad_in[...])
    edge = cross(edge_give, edge_got, 2)
    edge.start()
    edge_out[sec] = jnp.where(leading, grad_in[...], last_in[...])

    @pl.when(leading)
    def _():
        cross(last_up, got_up, 0).start()
        cross(last_down, got_down, 1).start()
        pltpu.make_async_copy(first_up, own_up, x_local.at[0]).start()
        pltpu.make_async_copy(first_down, own_down, x_local.at[1]).start()

    @pl.when(jnp.logical_not(leading))
    def _():
        cross(first_up, got_up, 0).start()
        cross(first_down, got_down, 1).start()
        pltpu.make_async_copy(last_up, own_up, x_local.at[0]).start()
        pltpu.make_async_copy(last_down, own_down, x_local.at[1]).start()

    steps = fold.steps()
    for t in range(steps - 1):
        fold.step(t)
        for n, (own, got, out, src) in enumerate(((own_up, got_up, up_out, first_up), (own_down, got_down, down_out, first_down))):
            if t == 3:
                pltpu.make_async_copy(src, own, x_local.at[n]).wait()
                cross(src, got, n).wait_recv()
            if t in (3, 4):
                size = own.shape[0] // 2
                rows = pl.ds((t - 3) * size, size)
                add_rows([own.at[rows], got.at[rows]], own.at[rows], size, 8)
            if t == 4:
                pltpu.make_async_copy(own, out, x_local.at[n]).start()
        if t == 2:
            edge.wait_recv()
            edge_out[1 - sec] = edge_got[...]
    assert steps > 5
    fold.step(steps - 1)
    given[...] = jnp.where(leading, other[...], result[...])
    hand = remote(given, taken, h_send.at[0], h_recv.at[0], partner)
    hand.start()
    packed = packed_columns(fold.widths)
    for a in range(count):
        outs[a][:, weight_columns(fold.widths[a])[0]] = jnp.where(leading, result[:, packed[a]], other[:, packed[a]])
    fold.end()
    edge.wait_send()
    for n, (own, got, out, src) in enumerate(((own_up, got_up, up_out, first_up), (own_down, got_down, down_out, first_down))):
        cross(src, got, n).wait_send()
        pltpu.make_async_copy(own, out, x_local.at[n]).wait()
    hand.wait()
    for a in range(count):
        outs[a][:, weight_columns(fold.widths[a])[1]] = taken[:, packed[a]]


def closing(raws, other, first, last, grad, final, count, cid):
    axes, n = torus_axes(count), len(raws)
    vmem, anywhere = pl.BlockSpec(memory_space=pltpu.VMEM), pl.BlockSpec(memory_space=pl.ANY)
    dma, f32 = pltpu.SemaphoreType.DMA, jnp.float32
    half = pltpu.VMEM(fold_shape(raws).shape, f32)
    experts = [pltpu.VMEM(w.shape, f32) for w in first]
    block = pltpu.VMEM(grad.shape, grad.dtype)
    return pl.pallas_call(
        functools.partial(closing_kernel, axes, n),
        out_shape=[jax.ShapeDtypeStruct(a.shape[1:], f32) for a in raws] + [jax.ShapeDtypeStruct(w.shape, f32) for w in first]
        + [jax.ShapeDtypeStruct((2, *grad.shape), grad.dtype)],
        in_specs=[anywhere] * n + [vmem] + [anywhere] * 4 + [vmem] * 2,
        out_specs=[vmem] * n + [anywhere] * 2 + [vmem],
        scratch_shapes=fold_scratch(raws, axes) + [half] * 3 + experts * 2 + [block, block, dma((3,)), dma((3,)), dma((2,)), dma((1,)), dma((1,))],
        compiler_params=pltpu.CompilerParams(collective_id=cid, has_side_effects=True, vmem_limit_bytes=VMEM_BYTES),
        cost_estimate=pl.CostEstimate(flops=0, bytes_accessed=100_000_000, transcendentals=0),
        name="closing",
    )(*raws, other, *first, *last, grad, final)


def mixture_kernel(mode, axes, count, layer, extra, folded, *refs):
    fore, back = "f" in mode, "b" in mode
    refs = list(refs)
    take = lambda n: [refs.pop(0) for _ in range(n)]
    mask_ref, router_ref, up_own, up_other, down_own, down_other, x_in = take(7)
    g_in = take(1)[0] if back else None
    next_in = take(1)[0] if extra else None
    raws = take(folded)
    mixed_out = take(1)[0] if fore else None
    saved_out = take(1)[0] if mode == "f" else None
    if back:
        grad_out, chance_out, up_grad_out, down_grad_out = take(4)
    next_out = take(extra)
    raw_out = take(1)[0] if folded else None
    up, down, xg, gates_at, weight_at, local = take(6)
    ag_send, ag_recv, rs_send, rs_recv = take(4)
    gathers, folds = [], []
    if fore:
        share_f, got_f, act_at = take(3)
        gathers.append((x_in, xg))
        folds.append((share_f, got_f, mixed_out))
    if back:
        (gg, share_b, got_b, plain_at, ggu_at, actw_at, high_at, low_at, up_sum, down_sum, chance_row, chance_got, c_send, c_recv,
         out_sem) = take(15)
        gathers.append((g_in, gg))
        folds.append((share_b, got_b, grad_out))
    me, sec = lax.axis_index("dp"), lax.axis_index("section")
    n0, n1, n2 = [size for _, size in axes]
    plane = n1 * n2
    assert n0 == 4
    meet(axes, back, bool(extra or folded))
    spread_streams, fold_streams = [], []
    for own, full in gathers:
        for order, at, size in TOKEN_PARTS:
            rows = pl.ds(at, size)
            spread_streams.append((Route(axes, order), own.at[rows], lambda b, f=full, r=rows: f.at[b, r]))
    for share, got, out in folds:
        for order, at, size in TOKEN_PARTS:
            rows, route = pl.ds(at, size), Route(axes, order)
            fold_streams.append((route, lambda o, a=share, r=rows, w=route: a.at[w.block(o), r], lambda f, g=got, r=rows: g.at[f, r],
                                 out.at[rows], size))
    spread = Spread(spread_streams, ag_send, ag_recv)
    ranks = [3, 2, 1, 0]
    fold = Fold(fold_streams, rs_send, rs_recv, ranks)
    spread.step(0)
    if extra:
        other = WeightSpread(axes, next_in, take(1)[0], next_out, take(5))
    if folded:
        aside = WeightFold(axes, raws, *take(3), raw_out, take(5), ranks)
        aside.begin()

    @pl.when(sec == layer)
    def _():
        pltpu.make_async_copy(up_own, up, local.at[0]).start()
        pltpu.make_async_copy(down_own, down, local.at[1]).start()

    @pl.when(sec != layer)
    def _():
        pltpu.make_async_copy(up_other, up, local.at[0]).start()
        pltpu.make_async_copy(down_other, down, local.at[1]).start()

    if not fore:
        bring = pltpu.make_async_copy(x_in, xg, local.at[2])
        bring.start()
    else:
        xg[me] = x_in[...]
    if back:
        gg[me] = g_in[...]
    pltpu.make_async_copy(up_own, up, local.at[0]).wait()
    pltpu.make_async_copy(down_own, down, local.at[1]).wait()
    if not fore:
        bring.wait()

    def span(n, size=SPAN):
        return pl.ds(pl.multiple_of(n * size, size), size)

    def tile(b0):
        blocks = pl.ds(b0, TILE // ROWS)
        here = pl.ds(pl.multiple_of(b0 * ROWS, TILE), TILE)
        x = xg[blocks].reshape(TILE, MODEL_WIDTH)
        lane = lax.broadcasted_iota(jnp.int32, (TILE, router_ref.shape[1]), 1)
        chance = jnp.where(lane < count, jnp.exp(dot(x, router_ref[...])), 0.0)
        total = jnp.sum(chance, axis=1, keepdims=True)
        ones = jnp.ones((8, 128), jnp.bfloat16)
        named = jnp.concatenate([contract(mask_ref[b0 + b], ones, (0, 0)) for b in range(TILE // ROWS)], axis=0)
        weight = jnp.sum(jnp.where(lane == me, chance, 0.0), axis=1, keepdims=True) / total
        weight_at[...] = jnp.where(lane[:, :128] == 0, weight * named, named)

        def gate_step(n, _):
            gates_at[:, span(n)] = dot(xg[blocks].reshape(TILE, MODEL_WIDTH), up[:, span(n)])
            return 0

        lax.fori_loop(0, 2 * FFE // SPAN, gate_step, 0)
        if back:
            def plain_step(n, _):
                plain_at[:, span(n)] = contract(gg[blocks].reshape(TILE, MODEL_WIDTH), down[span(n), :], (1, 1))
                return 0

            lax.fori_loop(0, FFE // SPAN, plain_step, 0)

        def strip(r, _):
            at = pl.ds(pl.multiple_of(r * STRIP, STRIP), STRIP)
            gate, raise_ = gates_at[at, :FFE], gates_at[at, FFE:]
            sigmoid = 1.0 / (1.0 + jnp.exp(-gate))
            silu = gate * sigmoid
            activated = silu * raise_
            if fore:
                act_at[at] = activated.astype(jnp.bfloat16)
            if back:
                row = pl.ds(pl.multiple_of(b0 * ROWS + r * STRIP, STRIP), STRIP)
                w, m = weight_at[at, 0:1], weight_at[at, 1:2]
                plain = plain_at[at]
                grad_act = plain * w
                ggu_at[row, :FFE] = (grad_act * raise_ * sigmoid * (1.0 + gate * (1.0 - sigmoid))).astype(jnp.bfloat16)
                ggu_at[row, FFE:] = (grad_act * silu).astype(jnp.bfloat16)
                actw_at[row] = (activated * w).astype(jnp.bfloat16)
                product = activated * plain * m
                high = product.astype(jnp.bfloat16)
                high_at[at] = high
                low_at[at] = (product - high.astype(jnp.float32)).astype(jnp.bfloat16)
            return 0

        lax.fori_loop(0, TILE // STRIP, strip, 0)
        if back:
            def back_step(n, _):
                part = contract(ggu_at[here], up[span(n), :], (1, 1))
                share_b[blocks, :, span(n)] = part.astype(jnp.bfloat16).reshape(TILE // ROWS, ROWS, SPAN)
                return 0

            lax.fori_loop(0, MODEL_WIDTH // SPAN, back_step, 0)
        if fore:
            def share_step(n, _):
                part = dot(act_at[...], down[:, span(n)]) * weight_at[:, 0:1]
                share_f[blocks, :, span(n)] = part.astype(jnp.bfloat16).reshape(TILE // ROWS, ROWS, SPAN)
                return 0

            lax.fori_loop(0, MODEL_WIDTH // SPAN, share_step, 0)
        if back:
            ones = jnp.ones((8, FFE), jnp.bfloat16)
            row = contract(ones, high_at[...], (1, 1)) + contract(ones, low_at[...], (1, 1))
            for b in range(TILE // ROWS):
                chance_row[b0 + b] = row[:, b * ROWS : (b + 1) * ROWS]

    for t in range(1, SPREAD_STEPS):
        spread.step(t)
        if folded:
            aside.step(t - 1)
    if extra:
        other.step(0)
    route = Route(axes, ORDERS[0])
    sources = [route.plane(k) for k in ranks]

    def chunk(c, _):
        source = sources[0]
        for v in range(1, n0):
            source = jnp.where(c == v, sources[v], source)

        def step(q, _):
            if "tile" not in SKIP:
                tile(source * plane + q * (TILE // ROWS))
            return 0

        lax.fori_loop(0, plane * ROWS // TILE, step, 0)
        for v in range(n0):
            @pl.when(c == v)
            def _(v=v):
                fold.step(v)
                if extra and v:
                    other.step(v)
                if folded:
                    aside.step(SPREAD_STEPS - 1 + v)
        return 0

    lax.fori_loop(0, n0, chunk, 0)
    if back:

        def chance_copy(offs, sender):
            block = route.block(offs)
            return remote(chance_row.at[block], chance_got.at[sender], c_send.at[route.flat(offs)], c_recv.at[sender], {"dp": block})

        for offs in route.others:
            chance_copy(offs, me).start()
        chance_got[me] = chance_row[me]

        def up_piece(n):
            return pltpu.make_async_copy(up_sum.at[0], up_grad_out.at[pl.ds(n * PIECE, PIECE)], out_sem.at[0, 0])

        def down_piece(n):
            return pltpu.make_async_copy(down_sum.at[0], down_grad_out.at[pl.ds(n * PIECE, PIECE)], out_sem.at[1, 0])

        ups, downs = MODEL_WIDTH // PIECE, FFE // PIECE

        def gradient(n):
            if n < ups:
                if n:
                    up_piece(n - 1).wait()
                left = xg[:, :, n * PIECE : (n + 1) * PIECE].reshape(count * ROWS, PIECE)
                up_sum[0] = contract(left, ggu_at[...], (0, 0))
                up_piece(n).start()
            else:
                n -= ups
                if n:
                    down_piece(n - 1).wait()
                down_sum[0] = contract(actw_at[:, n * PIECE : (n + 1) * PIECE], gg[...].reshape(count * ROWS, MODEL_WIDTH), (0, 0))
                down_piece(n).start()

        work = list(range(ups + downs))
    else:
        work = []
    if saved_out is not None:
        save = pltpu.make_async_copy(xg, saved_out, local.at[2])
        save.start()
    last = fold.steps()
    for t in range(n0, last):
        share = -(-len(work) // (last - t))
        for _ in range(share):
            n = work.pop(0)
            if "grad" not in SKIP:
                gradient(n)
        fold.step(t)
        if extra:
            other.step(t)
        if folded:
            aside.step(SPREAD_STEPS - 1 + t)
    if folded:
        assert aside.steps() <= SPREAD_STEPS - 1 + last
        aside.end()
    if extra:
        assert last >= SPREAD_STEPS
        other.end()
    spread.end()
    fold.end()
    if back:
        for n in range(ups - 1, ups) if "grad" not in SKIP else ():
            up_piece(n).wait()
        for n in range(downs - 1, downs) if "grad" not in SKIP else ():
            down_piece(n).wait()
        for offs in route.others:
            chance_copy(offs, route.block(offs)).wait()
        chance_out[...] = chance_got[...]
    if saved_out is not None:
        save.wait()


def mixture_call(mode, count, layer, cid, mask, router, expert, partner, x, g=None, following=None, widths=(), summed=()):
    axes = torus_axes(count)
    fore, back = "f" in mode, "b" in mode
    vmem, anywhere = pl.BlockSpec(memory_space=pltpu.VMEM), pl.BlockSpec(memory_space=pl.ANY)
    args = [mask, router, expert[0], partner[0], expert[1], partner[1], x]
    in_specs = [vmem, vmem] + [anywhere] * 4 + [vmem if fore else anywhere]
    if back:
        args.append(g)
        in_specs.append(vmem)
    args += ([following] if widths else []) + list(summed)
    in_specs += ([vmem] if widths else []) + [anywhere] * len(summed)
    whole = (count, ROWS, MODEL_WIDTH)
    out_shape, out_specs = [], []
    block = jax.ShapeDtypeStruct((ROWS, MODEL_WIDTH), jnp.float32)
    if fore:
        out_shape.append(block)
        out_specs.append(vmem)
    if mode == "f":
        out_shape.append(jax.ShapeDtypeStruct(whole, jnp.bfloat16))
        out_specs.append(anywhere)
    if back:
        out_shape += [block, jax.ShapeDtypeStruct((count, 8, ROWS), jnp.float32)]
        out_shape += [jax.ShapeDtypeStruct(w.shape, jnp.float32) for w in expert]
        out_specs += [vmem, vmem, anywhere, anywhere]
    if widths:
        out_shape += weight_shapes(following, widths, count)
        out_specs += [anywhere] * len(widths)
    if summed:
        out_shape.append(fold_shape(summed))
        out_specs.append(vmem)
    dma = pltpu.SemaphoreType.DMA
    scratch = [pltpu.VMEM(expert[0].shape, jnp.bfloat16), pltpu.VMEM(expert[1].shape, jnp.bfloat16), pltpu.VMEM(whole, jnp.bfloat16),
               pltpu.VMEM((TILE, 2 * FFE), jnp.float32), pltpu.VMEM((TILE, 128), jnp.float32), dma((3,))]
    parts = len(TOKEN_PARTS)
    ag, rs = parts * (1 if mode == "b" else fore + back), parts * (fore + back)
    scratch += [dma((ag, count + 4)), dma((ag, count + 4)), dma((rs, count + 4)), dma((rs, count + 4))]
    blocks = pltpu.VMEM(whole, jnp.bfloat16)
    arrivals = pltpu.VMEM((count + 4, *whole[1:]), jnp.bfloat16)
    low = lambda rows, width: pltpu.VMEM((rows, width), jnp.bfloat16)
    if fore:
        scratch += [blocks, arrivals, low(TILE, FFE)]
    if back:
        scratch += [blocks, blocks, arrivals, pltpu.VMEM((TILE, FFE), jnp.float32),
                    low(count * ROWS, 2 * FFE), low(count * ROWS, FFE), low(TILE, FFE), low(TILE, FFE),
                    pltpu.VMEM((1, PIECE, 2 * FFE), jnp.float32), pltpu.VMEM((1, PIECE, MODEL_WIDTH), jnp.float32),
                    pltpu.VMEM((count, 8, ROWS), jnp.float32), pltpu.VMEM((count, 8, ROWS), jnp.float32), dma((count,)), dma((count,)),
                    dma((2, 2))]
    if widths:
        scratch += weight_scratch(following, widths, count)
    if summed:
        scratch += fold_scratch(summed, axes)
    rows = count * ROWS
    flops = rows * 6 * MODEL_WIDTH * FFE * (fore + 2 * back + (mode == "b"))
    return pl.pallas_call(
        functools.partial(mixture_kernel, mode, axes, count, layer, len(widths), len(summed)),
        out_shape=out_shape,
        in_specs=in_specs,
        out_specs=out_specs,
        scratch_shapes=scratch,
        compiler_params=pltpu.CompilerParams(collective_id=cid, has_side_effects=True, vmem_limit_bytes=VMEM_BYTES),
        cost_estimate=pl.CostEstimate(flops=flops, bytes_accessed=4 * rows * MODEL_WIDTH, transcendentals=rows * FFE),
        name="mixture_" + mode,
    )(*args)

def swapped(value):
    return lax.ppermute(value, "section", [(0, 1), (1, 0)])


def layout(length_row):
    seq_ends = jnp.cumsum(length_row)
    seq_starts = seq_ends - length_row
    row_ids = jnp.arange(DEVICE_ROWS, dtype=jnp.int32)
    segment = jnp.sum((row_ids[:, None] >= seq_ends[None, :]).astype(jnp.int32), axis=-1)
    member = (segment[:, None] == jnp.arange(NSEQ, dtype=jnp.int32)[None, :]).astype(jnp.int32)
    token_position = row_ids - jnp.sum(member * seq_starts[None, :], axis=-1)
    return segment, token_position


def rotation(token_position):
    half_width = HEAD_SIZE // 2
    frequency = 10000.0 ** (-2.0 * jnp.arange(half_width, dtype=jnp.float32) / HEAD_SIZE)
    angles = token_position.astype(jnp.float32)[:, None] * frequency
    return jnp.cos(angles)[:, None, :], jnp.sin(angles)[:, None, :]


def rotary_embedding(values, cosine, sine):
    half_width = HEAD_SIZE // 2
    former, latter = values[..., :half_width], values[..., half_width:]
    return jnp.concatenate([former * cosine - latter * sine, latter * cosine + former * sine], axis=-1)


def dot(left, right):
    return jnp.dot(left, right, preferred_element_type=jnp.float32)


def dot_rows(left, right):
    return lax.dot_general(left, right, (((0,), (0,)), ((), ())), preferred_element_type=jnp.float32)


def dot_columns(left, right):
    return lax.dot_general(left, right, (((1,), (1,)), ((), ())), preferred_element_type=jnp.float32)


def router_chances(normed_two, router):
    chance = jnp.exp(dot(normed_two, router))
    return chance / jnp.sum(chance, axis=-1, keepdims=True)


def front(hidden, place, weights):
    joint, result_output, router, gain_attention, gain_mixture = weights
    allowed, cosine, sine = place
    rows = hidden.shape[0]
    inverse_one = lax.rsqrt(jnp.mean(hidden * hidden, axis=-1, keepdims=True) + norm_epsilon)
    scaled_one = hidden * inverse_one
    normed = (scaled_one * gain_attention).astype(jnp.bfloat16)
    projected = dot(normed, joint)
    query = rotary_embedding(projected[:, :QUERY_WIDTH].reshape(rows, QUERY_HEADS, HEAD_SIZE), cosine, sine)
    query = query.astype(jnp.bfloat16).reshape(rows, KEY_VALUE_HEADS, GROUP, HEAD_SIZE)
    key = rotary_embedding(projected[:, QUERY_WIDTH : QUERY_WIDTH + KEY_WIDTH].reshape(rows, KEY_VALUE_HEADS, HEAD_SIZE), cosine, sine)
    key = key.astype(jnp.bfloat16)
    value = projected[:, QUERY_WIDTH + KEY_WIDTH :].reshape(rows, KEY_VALUE_HEADS, HEAD_SIZE).astype(jnp.bfloat16)
    scores = jnp.einsum("qhgd,khd->hgqk", query, key, preferred_element_type=jnp.float32) * SCORE_SCALE
    exponent = jnp.where(allowed, jnp.exp(scores), 0.0)
    attention = exponent / jnp.sum(exponent, axis=-1, keepdims=True)
    context = jnp.einsum("hgqk,khd->qhgd", attention.astype(jnp.bfloat16), value, preferred_element_type=jnp.float32)
    context = context.reshape(rows, QUERY_WIDTH).astype(jnp.bfloat16)
    middle = hidden + dot(context, result_output)
    inverse_two = lax.rsqrt(jnp.mean(middle * middle, axis=-1, keepdims=True) + norm_epsilon)
    scaled_two = middle * inverse_two
    normed_two = (scaled_two * gain_mixture).astype(jnp.bfloat16)
    kept = (inverse_one, scaled_one, normed, query, key, value, attention, context, inverse_two, scaled_two, normed_two)
    return middle, normed_two, kept


def gates(everyone, up_weight):
    both = dot(everyone, up_weight)
    return both[:, :FFE], both[:, FFE:]


def expert_forward(everyone, mask, router, expert, count, me):
    up_weight, down_weight = expert
    chance = router_chances(everyone, router)
    own = jnp.arange(count, dtype=jnp.int32) == me
    weight = jnp.sum(jnp.where(own[None, :] & mask, chance, 0.0), axis=-1)
    gate, up = gates(everyone, up_weight)
    activated = (jax.nn.silu(gate) * up).astype(jnp.bfloat16)
    share = (dot(activated, down_weight) * weight[:, None]).astype(jnp.bfloat16)
    return share, weight, (gate, up)


def expert_backward(grads, everyone, weight, mask, held, expert):
    up_weight, down_weight = expert
    gate, up = held if held is not None else gates(everyone, up_weight)
    sigmoid = jax.nn.sigmoid(gate)
    silu = gate * sigmoid
    activated = silu * up
    grad_plain = dot_columns(grads, down_weight)
    grad_weight = jnp.where(mask[:, 0], jnp.sum(activated * grad_plain, axis=-1), 0.0)
    grad_act = grad_plain * weight[:, None]
    grad_gate = grad_act * up * sigmoid * (1.0 + gate * (1.0 - sigmoid))
    grad_gate_up = jnp.concatenate([grad_gate, grad_act * silu], axis=-1).astype(jnp.bfloat16)
    grad_down = dot_rows((activated * weight[:, None]).astype(jnp.bfloat16), grads)
    grad_up_weight = dot_rows(everyone, grad_gate_up)
    share = dot_columns(grad_gate_up, up_weight).astype(jnp.bfloat16)
    return share, grad_weight, grad_up_weight, grad_down


def pieces(value):
    return value.reshape(-1, CHUNK_ROWS, *value.shape[1:])


def mixture_forward(normed_two, router, mask, expert, count, me):
    (spread,) = gather_all([normed_two], count, 0)
    everyone = spread.reshape(-1, MODEL_WIDTH)
    if everyone.shape[0] <= CHUNK_ROWS:
        share, weight, held = expert_forward(everyone, mask, router, expert, count, me)
    else:
        share, weight = lax.map(
            lambda part: expert_forward(part[0], part[1], router, expert, count, me)[:2], (pieces(everyone), pieces(mask)))
        held = None
    (mixed,) = reduce_all([share.reshape(spread.shape)], count, 1)
    return mixed, (everyone, weight.reshape(-1), held)


def mixture_backward(grad_out, mask, kept, expert, count):
    everyone, weight, held = kept
    (spread,) = gather_all([grad_out], count, 0)
    grads = spread.reshape(-1, MODEL_WIDTH)
    if grads.shape[0] <= CHUNK_ROWS:
        share, grad_weight, grad_up, grad_down = expert_backward(grads, everyone, weight, mask, held, expert)
    else:
        def step(sums, part):
            share, grad_weight, grad_up, grad_down = expert_backward(*part, None, expert)
            return (sums[0] + grad_up, sums[1] + grad_down), (share, grad_weight)

        zero = tuple(jnp.zeros(w.shape, jnp.float32) for w in expert)
        (grad_up, grad_down), (share, grad_weight) = lax.scan(
            step, zero, (pieces(grads), pieces(everyone), pieces(weight), pieces(mask)))
    grad_chance = lax.all_to_all(grad_weight.reshape(count, DEVICE_ROWS), "dp", split_axis=0, concat_axis=0, tiled=True)
    (mixed,) = reduce_all([share.reshape(spread.shape)], count, 1)
    return mixed, grad_chance.T, grad_up, grad_down


def front_backward(grad_out, grad_mixed, grad_chance, kept, place, weights):
    joint, result_output, router, gain_attention, gain_mixture = weights
    allowed, cosine, sine = place
    inverse_one, scaled_one, normed, query, key, value, attention, context, inverse_two, scaled_two, normed_two = kept
    rows = normed.shape[0]
    chance = router_chances(normed_two, router)
    grad_logit = (chance * (grad_chance - jnp.sum(grad_chance * chance, axis=-1, keepdims=True))).astype(jnp.bfloat16)
    grad_router = dot_rows(normed_two, grad_logit)
    grad_normed_two = grad_mixed + dot_columns(grad_logit, router)
    grad_gain_two = jnp.sum(grad_normed_two * scaled_two, axis=0)
    scaled_grad_two = grad_normed_two * gain_mixture
    grad_middle = grad_out + inverse_two * (scaled_grad_two - scaled_two * jnp.mean(scaled_grad_two * scaled_two, axis=-1, keepdims=True))
    branch = grad_middle.astype(jnp.bfloat16)
    grad_output = dot_rows(context, branch)
    grad_context = dot_columns(branch, result_output).astype(jnp.bfloat16).reshape(rows, KEY_VALUE_HEADS, GROUP, HEAD_SIZE)
    grad_attention = jnp.einsum("qhgd,khd->hgqk", grad_context, value, preferred_element_type=jnp.float32)
    grad_value = jnp.einsum("hgqk,qhgd->khd", attention.astype(jnp.bfloat16), grad_context, preferred_element_type=jnp.float32)
    grad_scores = (attention * (grad_attention - jnp.sum(grad_attention * attention, axis=-1, keepdims=True))).astype(jnp.bfloat16)
    grad_query = jnp.einsum("hgqk,khd->qhgd", grad_scores, key, preferred_element_type=jnp.float32).reshape(rows, QUERY_HEADS, HEAD_SIZE)
    grad_key = jnp.einsum("hgqk,qhgd->khd", grad_scores, query, preferred_element_type=jnp.float32)
    grad_query = rotary_embedding(grad_query * SCORE_SCALE, cosine, -sine)
    grad_key = rotary_embedding(grad_key * SCORE_SCALE, cosine, -sine)
    grad_projected = jnp.concatenate(
        [grad_query.reshape(rows, -1), grad_key.reshape(rows, -1), grad_value.reshape(rows, -1)], axis=-1).astype(jnp.bfloat16)
    grad_joint = dot_rows(normed, grad_projected)
    grad_normed = dot_columns(grad_projected, joint)
    grad_gain_one = jnp.sum(grad_normed * scaled_one, axis=0)
    scaled_grad_one = grad_normed * gain_attention
    grad_hidden = grad_middle + inverse_one * (scaled_grad_one - scaled_one * jnp.mean(scaled_grad_one * scaled_one, axis=-1, keepdims=True))
    return grad_hidden, (grad_joint, grad_output, grad_router, grad_gain_one, grad_gain_two)


def small_halves(rows, router, gains, codes):
    second = jnp.concatenate([gains, codes], axis=1)
    width = -(-max(router.shape[1], second.shape[1]) // 128) * 128
    pad = lambda v: jnp.pad(v, ((0, 0), (0, width - v.shape[1])))
    return pad(router), pad(second)


def body(tokens, cotangent, lengths, routes, combined_weight, output_weight, router_weight, attention_gain, mixture_gain,
         expert_gate_up, expert_down):
    count = lax.axis_size("dp")
    me, sec = lax.axis_index("dp"), lax.axis_index("section")
    layers = lax.axis_size("section")
    leading = sec == 0
    shard = combined_weight.shape[1]
    micro = lambda a, axis: lax.dynamic_index_in_dim(a, sec, axis, keepdims=False)

    gains = jnp.stack([attention_gain[0], mixture_gain[0]], axis=1)
    codes = routes[0].astype(jnp.bfloat16).reshape(-1)
    code_count = codes.shape[0]
    codes = jnp.pad(codes, (0, -code_count % shard)).reshape(shard, -1)
    fused = count * DEVICE_ROWS <= CHUNK_ROWS
    if fused:
        member = jnp.any(routes[0][:, None] == jnp.arange(count, dtype=jnp.int32)[None, :, None, None], axis=-1)
        member = member.astype(jnp.bfloat16).reshape(-1, DEVICE_ROWS)
        small = small_halves(shard, jnp.concatenate([router_weight[0], gains], axis=1), gains[:, :0], gains[:, :0])
        small = (small[0], jnp.pad(member, ((0, shard - member.shape[0]), (0, 0))))
    else:
        small = small_halves(shard, router_weight[0], gains, codes)
    small_width = small[0].shape[1]
    halves = [
        (combined_weight[0, :, : combined_weight.shape[2] // 2], combined_weight[0, :, combined_weight.shape[2] // 2 :]),
        (output_weight[0, :, : output_weight.shape[2] // 2], output_weight[0, :, output_weight.shape[2] // 2 :]),
        small,
    ]
    widths = [h[0].shape[1] for h in halves]
    mine = jnp.concatenate([jnp.where(leading, a, b) for a, b in halves], axis=1)
    given = swapped(jnp.concatenate([jnp.where(leading, b, a) for a, b in halves], axis=1))
    packs = [jnp.where(leading, mine, given), jnp.where(leading, given, mine)]
    partner_expert = tuple(swapped(w[0, 0]) for w in (expert_gate_up, expert_down))
    own_expert = (expert_gate_up[0, 0], expert_down[0, 0])
    experts, routers = [], []
    for layer in range(0 if fused else layers):
        keep = sec == layer
        experts.append((jnp.where(keep, expert_gate_up[0, 0], partner_expert[0]), jnp.where(keep, expert_down[0, 0], partner_expert[1])))

    def layer_parts(layer):
        at, parts = 0, []
        for w in widths:
            parts.append(packs[layer][:, at : at + w])
            at += w
        return parts

    def layer_weights(arrays):
        joint, output, tail = [a.reshape(MODEL_WIDTH, -1) for a in arrays]
        experts_wide = router_weight.shape[2]
        second = tail[:, small_width:] if not fused else tail[:, experts_wide:]
        weights = (joint, output, tail[:, :experts_wide], second[:, 0].astype(jnp.float32), second[:, 1].astype(jnp.float32))
        routers.append(tail[:, :small_width])
        if fused:
            rows = lax.dynamic_slice(arrays[2], (0, sec * count + me, small_width), (count, 1, DEVICE_ROWS))
            return weights, jnp.pad(rows, ((0, 0), (0, 7), (0, 0)))
        code = second[:, 2 : 2 + codes.shape[1]].reshape(count, -1)[:, :code_count].reshape(count, -1, DEVICE_ROWS, TOPK)
        named = lax.dynamic_index_in_dim(code, sec, 1, keepdims=False).reshape(count * DEVICE_ROWS, TOPK)
        mask = jnp.any(named == me.astype(jnp.bfloat16), axis=-1, keepdims=True)
        return weights, mask

    segment, token_position = layout(micro(lengths[:, 0], 0))
    row_ids = jnp.arange(DEVICE_ROWS, dtype=jnp.int32)
    allowed = (row_ids[:, None] >= row_ids[None, :]) & (segment[:, None] == segment[None, :])
    place = (allowed,) + rotation(token_position)

    weights, masks, stores = [], [], []
    hidden = micro(tokens, 0)
    for layer in range(layers):
        if not fused:
            arrays = gather_all(layer_parts(layer), count, 2, pair=True)
        elif layer == 0:
            arrays = weight_spread(packs[layer], widths, count, 2)
        got, mask = layer_weights(arrays)
        weights.append(got)
        masks.append(mask)
        middle, normed_two, kept = front(hidden.astype(jnp.float32), place, got)
        if not fused:
            mixed, kept_mixture = mixture_forward(normed_two, got[2], mask, experts[layer], count, me)
        else:
            named = mask
            call = lambda mode, cid, *data, **more: mixture_call(
                mode, count, layer, cid, named, routers[layer], own_expert, partner_expert, *data, **more)
            if layer < layers - 1:
                mixed, everyone, *arrays = call("f", 4, normed_two, following=packs[layer + 1], widths=tuple(widths))
                kept_mixture = (named, everyone)
            else:
                mixed, *kept_mixture = call("fb", 5, normed_two, micro(cotangent, 0))
        hidden = (middle + mixed).astype(jnp.bfloat16)
        stores.append((kept, kept_mixture))
    last = hidden
    grad = micro(cotangent, 0)
    shares, expert_grads = [None] * layers, [None] * layers
    for layer in reversed(range(layers)):
        kept, kept_mixture = stores[layer]
        if not fused:
            mixed, grad_chance, grad_up, grad_down = mixture_backward(grad, masks[layer], kept_mixture, experts[layer], count)
        else:
            if layer < layers - 1:
                named, everyone = kept_mixture
                kept_mixture = mixture_call("b", count, layer, 6, named, routers[layer], own_expert, partner_expert, everyone, grad,
                                            summed=packs[layer + 1])
            mixed, rows, grad_up, grad_down, *more = kept_mixture
            if more:
                shares[layer + 1] = more[0]
            grad_chance = rows[:, 0].T
        expert_grads[layer] = (grad_up, grad_down)
        grad_hidden, parts = front_backward(grad.astype(jnp.float32), mixed, grad_chance, kept, place, weights[layer])
        grad = grad_hidden.astype(jnp.bfloat16)
        tail = small_halves(MODEL_WIDTH, parts[2], jnp.stack([parts[3], parts[4]], axis=1), parts[2][:, :0])
        packed = [parts[0], parts[1], jnp.concatenate(tail, axis=1)]
        packs[layer] = [a.astype(jnp.bfloat16).reshape(count, shard, -1) for a in packed]
        if not fused:
            shares[layer] = reduce_all(packs[layer], count, 3, pair=True)
    if fused:
        *outs, grad_up, grad_down, boundary = closing(packs[0], shares[1], expert_grads[0], expert_grads[1], grad, last, count, 3)
        half = outs[2].shape[1] // 2
        return (
            boundary[None],
            outs[0][None],
            outs[1][None],
            outs[2][None, :, : router_weight.shape[2]],
            outs[2][None, :, half],
            outs[2][None, :, half + 1],
            grad_up[None, None],
            grad_down[None, None],
        )
    outs = []
    for a in range(3):
        kept_half = jnp.where(leading, shares[0][a], shares[1][a])
        got_half = swapped(jnp.where(leading, shares[1][a], shares[0][a]))
        outs.append(jnp.concatenate([jnp.where(leading, kept_half, got_half), jnp.where(leading, got_half, kept_half)], axis=1))
    expert_outs = []
    for a in range(2):
        kept_sum = jnp.where(leading, expert_grads[0][a], expert_grads[1][a])
        got_sum = swapped(jnp.where(leading, expert_grads[1][a], expert_grads[0][a]))
        expert_outs.append((kept_sum + got_sum)[None, None])
    partner = swapped(jnp.where(leading, last, grad))
    boundary = jnp.where(leading, jnp.stack([grad, partner]), jnp.stack([partner, last]))[None]
    half = outs[2].shape[1] // 2
    return (
        boundary,
        outs[0][None],
        outs[1][None],
        outs[2][None, :, : router_weight.shape[2]],
        outs[2][None, :, half],
        outs[2][None, :, half + 1],
        expert_outs[0],
        expert_outs[1],
    )


def solution(mesh):
    return jax.shard_map(
        body,
        mesh=mesh,
        in_specs=(
            P(None, "dp", None),
            P(None, "dp", None),
            P(None, "dp", None),
            P("section", None, "dp", None),
            P("section", "dp", None),
            P("section", "dp", None),
            P("section", "dp", None),
            P("section", "dp"),
            P("section", "dp"),
            P("section", "dp", None, None),
            P("section", "dp", None, None),
        ),
        out_specs=(
            P("section", None, "dp", None),
            P("section", "dp", None),
            P("section", "dp", None),
            P("section", "dp", None),
            P("section", "dp"),
            P("section", "dp"),
            P("section", "dp", None, None),
            P("section", "dp", None, None),
        ),
        check_vma=False,
    )
```

```python
import functools
import jax
import jax.numpy as jnp
from jax import lax
from jax.experimental import pallas as pl
from jax.experimental.pallas import tpu as pltpu
from jax.sharding import PartitionSpec as P

MODEL_WIDTH = 1536
QUERY_HEADS = 24
KEY_VALUE_HEADS = 8
GROUP = QUERY_HEADS // KEY_VALUE_HEADS
HEAD_SIZE = 64
FFE = 512
TOPK = 8
DEVICE_ROWS = 128
NSEQ = 4
QUERY_WIDTH = QUERY_HEADS * HEAD_SIZE
KEY_WIDTH = KEY_VALUE_HEADS * HEAD_SIZE
SCORE_SCALE = HEAD_SIZE ** (-0.5)
norm_epsilon = 1e-06
CHUNK_ROWS = 2048

VMEM_BYTES = 67_000_000


def torus_axes(count):
    side = 1
    while (side + 1) ** 3 <= count:
        side += 1
    assert count % (side * side) == 0
    return [(side * side, count // (side * side)), (1, side), (side, side)]


def offsets(sizes):
    return [(k, j, i) for k in range(sizes[0]) for j in range(sizes[1]) for i in range(sizes[2])]


class Place:
    def __init__(self, axes, order):
        self.me = lax.axis_index("dp")
        self.sec = lax.axis_index("section")
        long, first, second = axes
        if order is None:
            flip = self.sec
            stride_one = first[0] + (second[0] - first[0]) * flip
            stride_two = second[0] + (first[0] - second[0]) * flip
            assert first[1] == second[1]
            self.axes = [long, (stride_one, first[1]), (stride_two, second[1])]
        elif order == 0:
            self.axes = [long, first, second]
        else:
            self.axes = [long, second, first]
        self.sizes = [size for _, size in self.axes]

    def moved(self, steps):
        out = self.me
        for (stride, size), step in zip(self.axes, steps):
            if step % size:
                digit = lax.rem(lax.div(self.me, stride), size)
                out = out + (lax.rem(digit + (step % size), size) - digit) * stride
        return out

    def source(self, offs):
        return self.moved([-o for o in offs])

    def target(self, offs):
        return self.moved(list(offs))

    def flat(self, offs):
        return (offs[0] * self.sizes[1] + offs[1]) * self.sizes[2] + offs[2]


def last_hop(offs):
    for axis in (2, 1, 0):
        if offs[axis]:
            hop = [0, 0, 0]
            hop[axis] = offs[axis]
            base = list(offs)
            base[axis] = 0
            return tuple(hop), tuple(base)
    return None


def greet(axes, pair):
    place = Place(axes, 0)
    barrier = pltpu.get_barrier_semaphore()
    count = 0
    for axis in range(3):
        for step in range(1, place.sizes[axis]):
            hop = [0, 0, 0]
            hop[axis] = step
            pl.semaphore_signal(barrier, inc=1, device_id={"dp": place.target(hop)}, device_id_type=pl.DeviceIdType.MESH)
            count += 1
    if pair:
        pl.semaphore_signal(barrier, inc=1, device_id={"section": 1 - place.sec}, device_id_type=pl.DeviceIdType.MESH)
        count += 1
    pl.semaphore_wait(barrier, count)


def gather_kernel(axes, pair, count, *refs):
    ins, outs = refs[:count], refs[count : 2 * count]
    send, recv, local = refs[2 * count : 2 * count + 3]
    psend, precv = refs[2 * count + 3 :] if pair else (None, None)
    streams = []
    for a in range(count):
        if pair:
            place = Place(axes, None)
            half = ins[a].shape[1]
            cols = pl.ds(pl.multiple_of(place.sec * half, 128), half)
            streams.append((place, ins[a], lambda b, o=outs[a], c=cols: o.at[b, :, c]))
        else:
            half = ins[a].shape[0] // 2
            for h in range(2):
                rows = pl.ds(h * half, half)
                streams.append((Place(axes, h), ins[a].at[rows], lambda b, o=outs[a], r=rows: o.at[b, r]))

    def copy(s, offs):
        place, own, out = streams[s]
        hop, base = last_hop(offs)
        block = place.source(base)
        src = out(block) if any(base) else own
        f = place.flat(offs)
        return pltpu.make_async_remote_copy(
            src_ref=src, dst_ref=out(block), send_sem=send.at[s, f], recv_sem=recv.at[s, f],
            device_id={"dp": place.target(hop)}, device_id_type=pl.DeviceIdType.MESH)

    def share(s, offs):
        place, own, out = streams[s]
        block = place.source(offs)
        src = out(block) if any(offs) else own
        f = place.flat(offs)
        return pltpu.make_async_remote_copy(
            src_ref=src, dst_ref=out(block), send_sem=psend.at[s, f], recv_sem=precv.at[s, f],
            device_id={"section": 1 - place.sec}, device_id_type=pl.DeviceIdType.MESH)

    greet(axes, pair)
    ids = range(len(streams))
    n0, n1, n2 = streams[0][0].sizes
    keep = []
    for s in ids:
        place, own, out = streams[s]
        c = pltpu.make_async_copy(own, out(place.me), local.at[s])
        c.start()
        keep.append(c)
    for k in range(1, n0):
        for s in ids:
            copy(s, (k, 0, 0)).start()

    def first(k):
        for s in ids:
            if k:
                copy(s, (k, 0, 0)).wait_recv()
            for j in range(1, n1):
                copy(s, (k, j, 0)).start()
            for i in range(1, n2):
                copy(s, (k, 0, i)).start()
            if pair:
                share(s, (k, 0, 0)).start()

    def second(k):
        for j in range(1, n1):
            for s in ids:
                copy(s, (k, j, 0)).wait_recv()
                for i in range(1, n2):
                    copy(s, (k, j, i)).start()
                if pair:
                    share(s, (k, j, 0)).start()

    def third(k):
        for j in range(n1):
            for i in range(1, n2):
                for s in ids:
                    copy(s, (k, j, i)).wait_recv()
                    if pair:
                        share(s, (k, j, i)).start()

    for k in range(n0 + 2):
        if k < n0:
            first(k)
        if 0 <= k - 1 < n0:
            second(k - 1)
        if 0 <= k - 2 < n0:
            third(k - 2)
    for s in ids:
        for offs in offsets((n0, n1, n2)):
            if any(offs):
                copy(s, offs).wait_send()
            if pair:
                share(s, offs).wait()
    for c in keep:
        c.wait()


def gather_all(arrays, count, cid, pair=False):
    axes = torus_axes(count)
    streams = len(arrays) * (1 if pair else 2)
    sem = pltpu.SemaphoreType.DMA((streams, count))
    out_shape = [jax.ShapeDtypeStruct((count, a.shape[0], a.shape[1] * (2 if pair else 1)), a.dtype) for a in arrays]
    scratch = [sem, sem, pltpu.SemaphoreType.DMA((streams,))]
    if pair:
        scratch += [sem, sem]
    sent = sum(a.size * a.dtype.itemsize for a in arrays) * (count - 1)
    return pl.pallas_call(
        functools.partial(gather_kernel, axes, pair, len(arrays)),
        out_shape=out_shape,
        in_specs=[pl.BlockSpec(memory_space=pltpu.VMEM)] * len(arrays),
        out_specs=[pl.BlockSpec(memory_space=pl.ANY)] * len(arrays),
        scratch_shapes=scratch,
        compiler_params=pltpu.CompilerParams(collective_id=cid, has_side_effects=True),
        cost_estimate=pl.CostEstimate(flops=0, bytes_accessed=2 * sent, transcendentals=0),
        name="spread" if not pair else "spread_pair",
    )(*arrays)


def reduce_kernel(axes, pair, count, *refs):
    ins, outs = refs[:count], refs[count : 2 * count]
    rest = list(refs[2 * count :])
    send, recv = rest[:2]
    rest = rest[2:]
    if pair:
        psend, precv = rest[:2]
        rest = rest[2:]
    streams = []
    for a in range(count):
        if pair:
            got, held, pgot, psum = rest[:4]
            rest = rest[4:]
            place = Place(axes, None)
            half = outs[a].shape[1]
            mine = pl.ds(pl.multiple_of(place.sec * half, 128), half)
            other = pl.ds(pl.multiple_of((1 - place.sec) * half, 128), half)
            streams.append(dict(place=place, got=got, held=held, pgot=pgot, psum=psum, raw=ins[a], mine=mine, other=other,
                                out=outs[a], rows=outs[a].shape[0]))
        else:
            got, held = rest[:2]
            rest = rest[2:]
            half = outs[a].shape[0] // 2
            for h in range(2):
                rows = pl.ds(h * half, half)
                streams.append(dict(place=Place(axes, h), got=got.at[h], held=held.at[h], raw=ins[a], span=rows,
                                    out=outs[a].at[rows], rows=half))
    step = 8 if streams[0]["rows"] % 16 else 16

    def own_ref(t, offs):
        if pair:
            return t["psum"].at[t["place"].flat(offs)]
        return t["raw"].at[t["place"].target(offs), t["span"]]

    def summed(t, sources, dest):
        def one(r, _):
            rows = pl.ds(pl.multiple_of(r * step, step), step)
            total = sources[0][rows].astype(jnp.float32)
            for source in sources[1:]:
                total = total + source[rows].astype(jnp.float32)
            dest[rows] = total.astype(dest.dtype)
            return 0

        lax.fori_loop(0, t["rows"] // step, one, 0)

    def copy(s, offs):
        t = streams[s]
        place = t["place"]
        hop, base = last_hop(offs)
        f = place.flat(offs)
        src = own_ref(t, offs) if hop[2] else t["held"].at[f // place.sizes[2]]
        return pltpu.make_async_remote_copy(
            src_ref=src, dst_ref=t["got"].at[f], send_sem=send.at[s, f], recv_sem=recv.at[s, f],
            device_id={"dp": place.target(hop)}, device_id_type=pl.DeviceIdType.MESH)

    def share(s, offs):
        t = streams[s]
        place = t["place"]
        f = place.flat(offs)
        return pltpu.make_async_remote_copy(
            src_ref=t["raw"].at[place.target((offs[0], offs[2], offs[1])), :, t["other"]], dst_ref=t["pgot"].at[f],
            send_sem=psend.at[s, f], recv_sem=precv.at[s, f],
            device_id={"section": 1 - place.sec}, device_id_type=pl.DeviceIdType.MESH)

    ids = range(len(streams))
    n0, n1, n2 = streams[0]["place"].sizes
    greet(axes, pair)

    def phase_pair(k):
        for j in reversed(range(n1)):
            for i in reversed(range(n2)):
                for s in ids:
                    share(s, (k, j, i)).start()

    def phase_first(k):
        for j in reversed(range(n1)):
            for i in reversed(range(n2)):
                for s in ids:
                    t = streams[s]
                    if pair:
                        share(s, (k, j, i)).wait_recv()
                        f = t["place"].flat((k, j, i))
                        summed(t, [t["raw"].at[t["place"].target((k, j, i)), :, t["mine"]], t["pgot"].at[f]], t["psum"].at[f])
                    if i:
                        copy(s, (k, j, i)).start()

    def phase_second(k):
        for j in range(1, n1):
            for s in ids:
                t = streams[s]
                for i in range(1, n2):
                    copy(s, (k, j, i)).wait_recv()
                parts = [own_ref(t, (k, j, 0))] + [t["got"].at[t["place"].flat((k, j, i))] for i in range(1, n2)]
                summed(t, parts, t["held"].at[t["place"].flat((k, j, 0)) // n2])
                copy(s, (k, j, 0)).start()

    def gathered_parts(s, k):
        t = streams[s]
        offs = [(k, 0, i) for i in range(1, n2)] + [(k, j, 0) for j in range(1, n1)]
        for o in offs:
            copy(s, o).wait_recv()
        return [own_ref(t, (k, 0, 0))] + [t["got"].at[t["place"].flat(o)] for o in offs]

    def phase_third(k):
        for s in ids:
            t = streams[s]
            parts = gathered_parts(s, k)
            if k:
                summed(t, parts, t["held"].at[t["place"].flat((k, 0, 0)) // n2])
                copy(s, (k, 0, 0)).start()
            else:
                for q in range(1, n0):
                    copy(s, (q, 0, 0)).wait_recv()
                    parts.append(t["got"].at[t["place"].flat((q, 0, 0))])
                summed(t, parts, t["out"])

    chunks = list(range(1, n0)) + [0]
    if pair:
        phase_pair(chunks[0])
    for c in range(n0 + 3):
        if pair and c + 1 < n0:
            phase_pair(chunks[c + 1])
        if c < n0:
            phase_first(chunks[c])
        if 0 <= c - 1 < n0:
            phase_second(chunks[c - 1])
        if 0 <= c - 2 < n0:
            phase_third(chunks[c - 2])
    for s in ids:
        for offs in offsets((n0, n1, n2)):
            if any(offs):
                copy(s, offs).wait_send()
            if pair:
                share(s, offs).wait_send()


def reduce_all(arrays, count, cid, pair=False):
    axes = torus_axes(count)
    streams = len(arrays) * (1 if pair else 2)
    sem = pltpu.SemaphoreType.DMA((streams, count))
    scratch = [sem, sem]
    if pair:
        scratch += [sem, sem]
    groups = count // axes[2][1]
    out_shape = []
    for a in arrays:
        rows, cols = a.shape[1:]
        if pair:
            cols = cols // 2
            scratch += [pltpu.VMEM((count, rows, cols), a.dtype), pltpu.VMEM((groups, rows, cols), a.dtype),
                        pltpu.VMEM((count, rows, cols), a.dtype), pltpu.VMEM((count, rows, cols), a.dtype)]
        else:
            scratch += [pltpu.VMEM((2, count, rows // 2, cols), a.dtype), pltpu.VMEM((2, groups, rows // 2, cols), a.dtype)]
        out_shape.append(jax.ShapeDtypeStruct((rows, cols), jnp.float32))
    sent = sum(a.size * a.dtype.itemsize for a in arrays)
    return pl.pallas_call(
        functools.partial(reduce_kernel, axes, pair, len(arrays)),
        out_shape=out_shape,
        in_specs=[pl.BlockSpec(memory_space=pltpu.VMEM)] * len(arrays),
        out_specs=[pl.BlockSpec(memory_space=pltpu.VMEM)] * len(arrays),
        scratch_shapes=scratch,
        compiler_params=pltpu.CompilerParams(collective_id=cid, has_side_effects=True, vmem_limit_bytes=VMEM_BYTES),
        cost_estimate=pl.CostEstimate(flops=0, bytes_accessed=2 * sent, transcendentals=0),
        name="fold" if not pair else "fold_pair",
    )(*arrays)


ROWS = 128
TILE = 512
STRIP = 16
SPAN = 512
SKIP = set()
PIECE = 256
MESH = pl.DeviceIdType.MESH
ORDERS = ((0, 1, 2), (0, 2, 1), (1, 0, 2), (2, 0, 1))
TOKEN_PARTS = tuple((order, 32 * n, 32) for n, order in enumerate(ORDERS))


class Route:
    def __init__(self, axes, order):
        self.axes, self.order = axes, order
        self.sizes = [size for _, size in axes]
        assert self.sizes == [4, 2, 2]
        self.me = lax.axis_index("dp")
        self.all = offsets(self.sizes)
        self.others = [o for o in self.all if any(o)]
        self.z = lax.div(self.me, axes[0][0])
        self.inner = jnp.logical_and(self.z >= 1, self.z <= 2)
        later = order[order.index(0) + 1 :]
        self.lines = [(j, i) for j in range(2) for i in range(2) if all((0, j, i)[a] == 0 for a in later)]

    def digit(self, axis):
        stride, size = self.axes[axis]
        return lax.rem(lax.div(self.me, stride), size)

    def plane(self, rank):
        z = self.z
        if rank == 1:
            return z + 1 - 2 * lax.rem(z, 2)
        if rank == 2:
            return 2 - lax.div(z, 2)
        if rank == 3:
            return 3 - 3 * lax.div(z, 2)
        return z

    def block(self, offs):
        out = self.me + (self.plane(offs[0]) - self.z) * self.axes[0][0]
        for axis in (1, 2):
            if offs[axis]:
                out = out + (1 - 2 * self.digit(axis)) * self.axes[axis][0]
        return out

    def flat(self, offs):
        return (offs[0] * 2 + offs[1]) * 2 + offs[2]

    def extra(self, line, n):
        return 16 + 2 * self.lines.index(line) + n

    def last_axis(self, offs):
        for axis in reversed(self.order):
            if offs[axis]:
                return axis

    def base(self, offs):
        out = list(offs)
        out[self.last_axis(offs)] = 0
        return tuple(out)

    def across(self, offs):
        return [o for o in self.others if self.last_axis(o) and self.base(o) == offs]


def remote(src, dst, send, recv, peer):
    return pltpu.make_async_remote_copy(src_ref=src, dst_ref=dst, send_sem=send, recv_sem=recv, device_id=peer, device_id_type=MESH)


class Spread:
    def __init__(self, streams, send, recv):
        self.streams, self.send, self.recv = streams, send, recv
        self.ids = range(len(streams))

    def copy(self, s, offs, target, key, slot):
        route, own, out = self.streams[s]
        block = route.block(offs)
        return remote(out(block) if any(offs) else own, out(block), self.send.at[s, slot], self.recv.at[s, route.flat(key)], {"dp": target})

    def arrival(self, s, offs):
        route, own, out = self.streams[s]
        f = route.flat(offs)
        return remote(own, out(route.block(offs)), self.send.at[s, f], self.recv.at[s, f], {"dp": route.block(offs)})

    def onward(self, s, offs):
        route = self.streams[s][0]
        k, line = offs[0], offs[1:]
        out = [(o, False, self.copy(s, offs, route.block((0, *[int(o[a] != offs[a]) for a in (1, 2)])), o, route.flat(o)))
               for o in route.across(offs)]
        if line in route.lines:
            near, facing = route.block((1, 0, 0)), route.block((2, 0, 0))
            if k == 0:
                out.append(((1, *line), False, self.copy(s, offs, near, (1, *line), route.flat((1, *line)))))
                out.append(((2, *line), True, self.copy(s, offs, facing, (2, *line), route.extra(line, 0))))
            elif k == 1:
                out.append(((3, *line), True, self.copy(s, offs, facing, (3, *line), route.extra(line, 1))))
            else:
                out.append((offs, True, self.copy(s, offs, near, offs, route.flat(offs))))
        return out

    def launch(self, items):
        for s, (_, inner, copy) in items:
            if inner:
                pl.when(self.streams[s][0].inner)(copy.start)
            else:
                copy.start()

    def step(self, t):
        if "comm" in SKIP or "ag" in SKIP:
            return
        work = [(offs, s) for s in self.ids for offs in self.streams[s][0].all if offs[0] + offs[1] + offs[2] == t]
        if t == 0:
            first = [(s, item) for offs, s in work for item in self.onward(s, offs)]
            self.launch(sorted(first, key=lambda e: (e[1][0][0], e[1][0], e[0])))
            return
        ends = lambda e: not self.streams[e[1]][0].across(e[0]) and e[0][1:] not in self.streams[e[1]][0].lines
        for offs, s in sorted(work, key=lambda e: (ends(e), -e[0][0], e[0], e[1])):
            self.arrival(s, offs).wait_recv()
            self.launch([(s, item) for item in sorted(self.onward(s, offs), key=lambda e: (e[1], e[0]))])

    def end(self):
        if "comm" in SKIP or "ag" in SKIP:
            return
        for s in self.ids:
            for offs in self.streams[s][0].all:
                for _, inner, copy in self.onward(s, offs):
                    if inner:
                        pl.when(self.streams[s][0].inner)(copy.wait_send)
                    else:
                        copy.wait_send()


SPREAD_STEPS = 6


def add_rows(sources, dest, rows, step=16):
    cols = dest.shape[-1]
    width = 768 if cols % 768 == 0 else cols

    def one(r, _):
        at = pl.ds(pl.multiple_of(r * step, step), step)

        def part(c, _):
            span = pl.ds(pl.multiple_of(c * width, width), width)
            total = sources[0][at, span].astype(jnp.float32)
            for source in sources[1:]:
                total = total + source[at, span].astype(jnp.float32)
            dest[at, span] = total.astype(dest.dtype)
            return 0

        return lax.fori_loop(0, cols // width, part, 0)

    lax.fori_loop(0, rows // step, one, 0)


class Fold:
    def __init__(self, streams, send, recv, ranks):
        self.streams, self.send, self.recv = streams, send, recv
        self.ids = range(len(streams))
        self.turn = {k: c for c, k in enumerate(ranks)}
        self.plan = []
        for s in self.ids:
            route = self.streams[s][0]
            for offs in route.all:
                if offs[0] and offs[1:] in route.lines:
                    self.plan.append((self.ready(route, offs), 1, -offs[0], s, offs, self.outer))
                    self.plan.append((self.passed(route, offs), 2, -offs[0], s, offs, self.middle))
                else:
                    when = self.done(route, offs)
                    rank = 3 if not any(offs) else 1 if self.near(route, offs) or not offs[0] and offs[1:] in route.lines else 0
                    self.plan.append((when, rank, -offs[0], s, offs, self.plain))
        self.plan.sort(key=lambda e: e[:5])

    def near(self, route, offs):
        return [o for o in route.across(offs) if o[0] == offs[0]]

    def ready(self, route, offs):
        return max([self.turn[offs[0]]] + [self.done(route, o) + 1 for o in self.near(route, offs)])

    def passed(self, route, offs):
        line = offs[1:]
        return self.ready(route, offs) + 1 if offs[0] > 1 else max(self.ready(route, offs), self.ready(route, (3, *line)) + 2)

    def done(self, route, offs):
        when = self.ready(route, offs)
        if not offs[0] and offs[1:] in route.lines:
            when = max(when, self.passed(route, (1, *offs[1:])) + 1, self.passed(route, (2, *offs[1:])) + 1)
        return when

    def arrival(self, s, slot):
        route, share, got, _, _ = self.streams[s]
        return remote(share((0, 0, 0)), got(slot), self.send.at[s, slot], self.recv.at[s, slot], {"dp": route.block((1, 0, 0))})

    def copy(self, s, offs):
        route, share, got, _, _ = self.streams[s]
        f = route.flat(offs)
        if route.last_axis(offs):
            hop = [0, 0, 0]
            hop[route.last_axis(offs)] = 1
            return remote(share(offs), got(f), self.send.at[s, f], self.recv.at[s, f], {"dp": route.block(hop)})
        near, facing = route.block((1, 0, 0)), route.block((2, 0, 0))
        if offs[0] == 1:
            return remote(share(offs), got(f), self.send.at[s, f], self.recv.at[s, f], {"dp": near})
        slot = f + (route.extra(offs[1:], offs[0] - 2) - f) * route.inner.astype(jnp.int32)
        return remote(share(offs), got(slot), self.send.at[s, f], self.recv.at[s, slot], {"dp": jnp.where(route.inner, facing, near)})

    def settle(self, s, offs, slots, out=None):
        route, share, got, _, rows = self.streams[s]
        if slots:
            for f in slots:
                self.arrival(s, f).wait_recv()
            own = share(offs)
            add_rows([own] + [got(f) for f in slots], own if out is None else out, rows)

    def outer(self, s, offs):
        route = self.streams[s][0]
        self.settle(s, offs, [route.flat(o) for o in self.near(route, offs)])
        pl.when(jnp.logical_not(route.inner))(self.copy(s, offs).start)

    def middle(self, s, offs):
        route = self.streams[s][0]

        @pl.when(route.inner)
        def _():
            self.settle(s, offs, [route.flat(offs) if offs[0] > 1 else route.extra(offs[1:], 1)])
            self.copy(s, offs).start()

    def plain(self, s, offs):
        route, share, got, out, rows = self.streams[s]
        slots = [route.flat(o) for o in self.near(route, offs)]
        if not offs[0] and offs[1:] in route.lines:
            slots.append(route.flat((1, *offs[1:])))
            facing = route.extra(offs[1:], 0)

            @pl.when(route.inner)
            def _():
                self.settle(s, offs, [facing])

        self.settle(s, offs, slots, None if any(offs) else out)
        if any(offs):
            self.copy(s, offs).start()

    def step(self, t):
        if "comm" in SKIP or "rs" in SKIP:
            return
        for when, _, _, s, offs, action in self.plan:
            if when == t:
                action(s, offs)

    def steps(self):
        return 1 + max(e[0] for e in self.plan)

    def end(self):
        if "comm" in SKIP or "rs" in SKIP:
            return
        for s in self.ids:
            for offs in self.streams[s][0].others:
                self.copy(s, offs).wait_send()


def meet(axes, everyone, pair):
    route = Route(axes, ORDERS[0])
    barrier = pltpu.get_barrier_semaphore()
    if everyone:
        for offs in route.others:
            pl.semaphore_signal(barrier, inc=1, device_id={"dp": route.block(offs)}, device_id_type=MESH)
    else:
        for offs in ((0, 0, 1), (0, 1, 0), (1, 0, 0)):
            pl.semaphore_signal(barrier, inc=1, device_id={"dp": route.block(offs)}, device_id_type=MESH)

        @pl.when(route.inner)
        def _():
            pl.semaphore_signal(barrier, inc=1, device_id={"dp": route.block((2, 0, 0))}, device_id_type=MESH)

    if pair:
        pl.semaphore_signal(barrier, inc=1, device_id={"section": 1 - lax.axis_index("section")}, device_id_type=MESH)
    pl.semaphore_wait(barrier, (len(route.others) if everyone else 3 + route.inner.astype(jnp.int32)) + (1 if pair else 0))


def contract(left, right, dims):
    return lax.dot_general(left, right, ((dims[:1], dims[1:]), ((), ())), preferred_element_type=jnp.float32)


def weight_parts(rows):
    third = rows // 3
    sizes = (third, third, third // 2, third // 2)
    return tuple((order, sum(sizes[:n]), sizes[n]) for n, order in enumerate(ORDERS))


def weight_columns(half):
    sec = lax.axis_index("section")
    return pl.ds(pl.multiple_of(sec * half, 128), half), pl.ds(pl.multiple_of((1 - sec) * half, 128), half)


def packed_columns(widths):
    return [pl.ds(sum(widths[:n]), w) for n, w in enumerate(widths)]


class WeightSpread:
    def __init__(self, axes, own, full, outs, sems):
        send, recv, self.psend, self.precv, self.local = sems
        self.own, self.full, self.outs = own, full, outs
        self.route = Route(axes, ORDERS[0])
        streams = []
        for order, at, size in weight_parts(own.shape[0]):
            rows = pl.ds(at, size)
            streams.append((Route(axes, order), own.at[rows], lambda b, r=rows: full.at[b, r]))
        self.spread = Spread(streams, send, recv)
        self.widths = [out.shape[2] // 2 for out in outs]

    def deliveries(self, offs):
        block, f = self.route.block(offs), self.route.flat(offs)
        for a, cols in enumerate(packed_columns(self.widths)):
            src = self.full.at[block, :, cols] if any(offs) else self.own.at[:, cols]
            dst = self.outs[a].at[block, :, weight_columns(self.widths[a])[0]]
            yield pltpu.make_async_copy(src, dst, self.local.at[a, f])
            yield remote(src, dst, self.psend.at[a, f], self.precv.at[a, f], {"section": 1 - lax.axis_index("section")})

    def step(self, t):
        self.spread.step(t)
        for offs in self.route.all:
            if sum(offs) == t:
                for copy in self.deliveries(offs):
                    copy.start()

    def end(self):
        self.spread.end()
        for offs in self.route.all:
            for copy in self.deliveries(offs):
                copy.wait()


def weight_shapes(pack, widths, count):
    return [jax.ShapeDtypeStruct((count, pack.shape[0], 2 * w), pack.dtype) for w in widths]


def weight_scratch(pack, widths, count):
    dma = pltpu.SemaphoreType.DMA
    return [pltpu.VMEM((count, *pack.shape), pack.dtype)] + [dma((len(ORDERS), count + 4))] * 2 + [dma((len(widths), count))] * 3


def weight_spread_kernel(axes, arrays, *refs):
    own, outs, full, sems = refs[0], refs[1 : 1 + arrays], refs[1 + arrays], refs[2 + arrays :]
    meet(axes, False, True)
    spread = WeightSpread(axes, own, full, outs, sems)
    for t in range(SPREAD_STEPS):
        spread.step(t)
    spread.end()


def weight_spread(pack, widths, count, cid):
    return pl.pallas_call(
        functools.partial(weight_spread_kernel, torus_axes(count), len(widths)),
        out_shape=weight_shapes(pack, widths, count),
        in_specs=[pl.BlockSpec(memory_space=pltpu.VMEM)],
        out_specs=[pl.BlockSpec(memory_space=pl.ANY)] * len(widths),
        scratch_shapes=weight_scratch(pack, widths, count),
        compiler_params=pltpu.CompilerParams(collective_id=cid, has_side_effects=True),
        name="weight_spread",
    )(pack)


class WeightFold:
    def __init__(self, axes, data, total, got, made, tail, out, sems, ranks):
        send, recv, self.psend, self.precv, self.local = sems
        self.lefts, self.rights, self.small = data[:2], data[2:4], data[4]
        self.total, self.made, self.tail, self.rows, self.ranks = total, made, tail, out.shape[0], ranks
        self.widths = fold_widths(data)
        self.columns = packed_columns(self.widths)
        streams = []
        for order, at, size in weight_parts(self.rows):
            rows, route = pl.ds(at, size), Route(axes, order)
            streams.append((route, lambda o, r=rows, w=route: total.at[w.flat(o), r], lambda f, r=rows: got.at[f, r], out.at[rows], size))
        self.route = Route(axes, ORDERS[0])
        self.fold = Fold(streams, send, recv, ranks)

    def place(self, c, q):
        k, route = self.ranks[c], self.route
        j = lax.rem(q + route.digit(1), 2)
        i = lax.rem(lax.div(q, 2) + route.digit(2), 2)
        return route.plane(k) * 4 + q, (k * 2 + j) * 2 + i

    def product(self, a, block, other):
        rows = pl.ds(pl.multiple_of(block * self.rows, 32), self.rows)
        return dot(self.lefts[a][rows, :], self.rights[a][:, weight_columns(self.widths[a])[other]])

    def give(self, c, q):
        block, f = self.place(c, q)
        partner = {"section": 1 - lax.axis_index("section")}
        main = pl.ds(0, sum(self.widths[:2]))
        return (remote(self.made.at[q], self.total.at[f, :, main], self.psend.at[0, f], self.precv.at[0, f], partner),
                remote(self.small.at[block, :, weight_columns(self.widths[2])[1]], self.total.at[f, :, self.columns[2]],
                       self.psend.at[1, f], self.precv.at[1, f], partner))

    def load(self, c, q):
        block, f = self.place(c, q)
        return pltpu.make_async_copy(self.small.at[block, :, weight_columns(self.widths[2])[0]], self.tail.at[q], self.local.at[f])

    def produce(self, c):
        def one(q, _):
            block, _ = self.place(c, q)
            for a in range(2):
                self.made[q, :, self.columns[a]] = self.product(a, block, 1).astype(jnp.bfloat16)
            for copy in self.give(c, q):
                copy.start()
            self.load(c, q).start()
            return 0

        lax.fori_loop(0, 4, one, 0)

    def begin(self):
        self.produce(0)

    def step(self, t):
        if t < len(self.ranks):
            def own(q, _):
                block, f = self.place(t, q)
                for copy in self.give(t, q):
                    copy.wait_recv()
                for a in range(2):
                    cols = self.columns[a]
                    self.total[f, :, cols] = (self.total[f, :, cols].astype(jnp.float32) + self.product(a, block, 0)).astype(jnp.bfloat16)
                cols = self.columns[2]
                self.total[f, :, cols] = (self.total[f, :, cols].astype(jnp.float32) + self.tail[q].astype(jnp.float32)).astype(jnp.bfloat16)
                return 0

            def settled(q, _):
                for copy in self.give(t, q):
                    copy.wait_send()
                self.load(t, q).wait()
                return 0

            lax.fori_loop(0, 4, settled, 0)
            lax.fori_loop(0, 4, own, 0)
            if t + 1 < len(self.ranks):
                self.produce(t + 1)
        self.fold.step(t)

    def steps(self):
        return self.fold.steps()

    def end(self):
        self.fold.end()


def fold_widths(data):
    return [a.shape[-1] // 2 for a in data[2:]]


def fold_shape(data):
    return jax.ShapeDtypeStruct((data[4].shape[1], sum(fold_widths(data))), jnp.float32)


def fold_specs():
    return [pl.BlockSpec(memory_space=pltpu.VMEM)] * 4 + [pl.BlockSpec(memory_space=pl.ANY)]


def fold_scratch(data):
    (rows, cols), count, dma = fold_shape(data).shape, data[4].shape[0], pltpu.SemaphoreType.DMA
    small = fold_widths(data)[2]
    blocks = [pltpu.VMEM(shape, jnp.bfloat16) for shape in ((count, rows, cols), (count + 4, rows, cols), (4, rows, cols - small), (4, rows, small))]
    return blocks + [dma((len(ORDERS), count + 4))] * 2 + [dma((2, count))] * 2 + [dma((count,))]


def closing_kernel(axes, *refs):
    refs = list(refs)
    take = lambda n: [refs.pop(0) for _ in range(n)]
    data = take(5)
    count = 3
    other = take(1)[0]
    first_up, first_down, last_up, last_down, grad_in, last_in = take(6)
    outs = take(count)
    up_out, down_out, edge_out = take(3)
    blocks, sems = take(4), take(5)
    result, given, taken = take(3)
    own_up, own_down, got_up, got_down, edge_give, edge_got, x_send, x_recv, x_local, h_send, h_recv = take(11)
    sec = lax.axis_index("section")
    partner = {"section": 1 - sec}
    chunks = [axes[0][1] - 1 - c for c in range(axes[0][1])]
    meet(axes, False, True)
    fold = WeightFold(axes, data, *blocks, result, sems, chunks)
    fold.begin()
    leading = sec == 0

    def cross(src, dst, n):
        return remote(src, dst, x_send.at[n], x_recv.at[n], partner)

    edge_give[...] = jnp.where(leading, last_in[...], grad_in[...])
    edge = cross(edge_give, edge_got, 2)
    edge.start()
    edge_out[sec] = jnp.where(leading, grad_in[...], last_in[...])

    @pl.when(leading)
    def _():
        cross(last_up, got_up, 0).start()
        cross(last_down, got_down, 1).start()
        pltpu.make_async_copy(first_up, own_up, x_local.at[0]).start()
        pltpu.make_async_copy(first_down, own_down, x_local.at[1]).start()

    @pl.when(jnp.logical_not(leading))
    def _():
        cross(first_up, got_up, 0).start()
        cross(first_down, got_down, 1).start()
        pltpu.make_async_copy(last_up, own_up, x_local.at[0]).start()
        pltpu.make_async_copy(last_down, own_down, x_local.at[1]).start()

    steps = fold.steps()
    for t in range(steps - 1):
        fold.step(t)
        for n, (own, got, out, src) in enumerate(((own_up, got_up, up_out, first_up), (own_down, got_down, down_out, first_down))):
            if t == 3:
                pltpu.make_async_copy(src, own, x_local.at[n]).wait()
                cross(src, got, n).wait_recv()
            if t in (3, 4):
                size = own.shape[0] // 2
                rows = pl.ds((t - 3) * size, size)
                add_rows([own.at[rows], got.at[rows]], own.at[rows], size, 8)
            if t == 4:
                pltpu.make_async_copy(own, out, x_local.at[n]).start()
        if t == 2:
            edge.wait_recv()
            edge_out[1 - sec] = edge_got[...]
    assert steps > 5
    fold.step(steps - 1)
    given[...] = jnp.where(leading, other[...], result[...])
    hand = remote(given, taken, h_send.at[0], h_recv.at[0], partner)
    hand.start()
    packed = packed_columns(fold.widths)
    for a in range(count):
        outs[a][:, weight_columns(fold.widths[a])[0]] = jnp.where(leading, result[:, packed[a]], other[:, packed[a]])
    fold.end()
    edge.wait_send()
    for n, (own, got, out, src) in enumerate(((own_up, got_up, up_out, first_up), (own_down, got_down, down_out, first_down))):
        cross(src, got, n).wait_send()
        pltpu.make_async_copy(own, out, x_local.at[n]).wait()
    hand.wait()
    for a in range(count):
        outs[a][:, weight_columns(fold.widths[a])[1]] = taken[:, packed[a]]


def closing(data, other, first, last, grad, final, count, cid):
    axes, n = torus_axes(count), 3
    vmem, anywhere = pl.BlockSpec(memory_space=pltpu.VMEM), pl.BlockSpec(memory_space=pl.ANY)
    dma, f32 = pltpu.SemaphoreType.DMA, jnp.float32
    rows = fold_shape(data).shape[0]
    half = pltpu.VMEM(fold_shape(data).shape, f32)
    experts = [pltpu.VMEM(w.shape, f32) for w in first]
    block = pltpu.VMEM(grad.shape, grad.dtype)
    return pl.pallas_call(
        functools.partial(closing_kernel, axes),
        out_shape=[jax.ShapeDtypeStruct((rows, 2 * w), f32) for w in fold_widths(data)] + [jax.ShapeDtypeStruct(w.shape, f32) for w in first]
        + [jax.ShapeDtypeStruct((2, *grad.shape), grad.dtype)],
        in_specs=fold_specs() + [vmem] + [anywhere] * 4 + [vmem] * 2,
        out_specs=[vmem] * n + [anywhere] * 2 + [vmem],
        scratch_shapes=fold_scratch(data) + [half] * 3 + experts * 2 + [block, block, dma((3,)), dma((3,)), dma((2,)), dma((1,)), dma((1,))],
        compiler_params=pltpu.CompilerParams(collective_id=cid, has_side_effects=True, vmem_limit_bytes=VMEM_BYTES),
        cost_estimate=pl.CostEstimate(flops=0, bytes_accessed=100_000_000, transcendentals=0),
        name="closing",
    )(*data, other, *first, *last, grad, final)


def mixture_kernel(mode, axes, count, layer, extra, folded, *refs):
    fore, back = "f" in mode, "b" in mode
    refs = list(refs)
    take = lambda n: [refs.pop(0) for _ in range(n)]
    mask_ref, router_ref, up_own, up_other, down_own, down_other, x_in = take(7)
    g_in = take(1)[0] if back else None
    next_in = take(1)[0] if extra else None
    data = take(folded)
    mixed_out = take(1)[0] if fore else None
    saved_out = take(1)[0] if mode == "f" else None
    if back:
        grad_out, chance_out, up_grad_out, down_grad_out = take(4)
    next_out = take(extra)
    raw_out = take(1)[0] if folded else None
    up, down, xg, gates_at, weight_at, local = take(6)
    ag_send, ag_recv, rs_send, rs_recv = take(4)
    gathers, folds = [], []
    if fore:
        share_f, got_f, act_at = take(3)
        gathers.append((x_in, xg))
        folds.append((share_f, got_f, mixed_out))
    if back:
        (gg, share_b, got_b, plain_at, ggu_at, actw_at, high_at, low_at, chance_row, chance_got, c_send, c_recv, out_sem) = take(13)
        gathers.append((g_in, gg))
        folds.append((share_b, got_b, grad_out))
    me, sec = lax.axis_index("dp"), lax.axis_index("section")
    n0, n1, n2 = [size for _, size in axes]
    plane = n1 * n2
    assert n0 == 4
    meet(axes, back, bool(extra or folded))
    spread_streams, fold_streams = [], []
    for own, full in gathers:
        for order, at, size in TOKEN_PARTS:
            rows = pl.ds(at, size)
            spread_streams.append((Route(axes, order), own.at[rows], lambda b, f=full, r=rows: f.at[b, r]))
    for share, got, out in folds:
        for order, at, size in TOKEN_PARTS:
            rows, route = pl.ds(at, size), Route(axes, order)
            fold_streams.append((route, lambda o, a=share, r=rows, w=route: a.at[w.block(o), r], lambda f, g=got, r=rows: g.at[f, r],
                                 out.at[rows], size))
    spread = Spread(spread_streams, ag_send, ag_recv)
    ranks = [3, 2, 1, 0]
    fold = Fold(fold_streams, rs_send, rs_recv, ranks)
    spread.step(0)
    if extra:
        other = WeightSpread(axes, next_in, take(1)[0], next_out, take(5))
    if folded:
        aside = WeightFold(axes, data, *take(4), raw_out, take(5), ranks)
        aside.begin()

    @pl.when(sec == layer)
    def _():
        pltpu.make_async_copy(up_own, up, local.at[0]).start()
        pltpu.make_async_copy(down_own, down, local.at[1]).start()

    @pl.when(sec != layer)
    def _():
        pltpu.make_async_copy(up_other, up, local.at[0]).start()
        pltpu.make_async_copy(down_other, down, local.at[1]).start()

    if not fore:
        bring = pltpu.make_async_copy(x_in, xg, local.at[2])
        bring.start()
    else:
        xg[me] = x_in[...]
    if back:
        gg[me] = g_in[...]
    pltpu.make_async_copy(up_own, up, local.at[0]).wait()
    pltpu.make_async_copy(down_own, down, local.at[1]).wait()
    if not fore:
        bring.wait()

    def span(n, size=SPAN):
        return pl.ds(pl.multiple_of(n * size, size), size)

    def tile(b0):
        blocks = pl.ds(b0, TILE // ROWS)
        here = pl.ds(pl.multiple_of(b0 * ROWS, TILE), TILE)
        x = xg[blocks].reshape(TILE, MODEL_WIDTH)
        lane = lax.broadcasted_iota(jnp.int32, (TILE, router_ref.shape[1]), 1)
        chance = jnp.where(lane < count, jnp.exp(dot(x, router_ref[...])), 0.0)
        total = jnp.sum(chance, axis=1, keepdims=True)
        ones = jnp.ones((8, 128), jnp.bfloat16)
        named = jnp.concatenate([contract(mask_ref[b0 + b], ones, (0, 0)) for b in range(TILE // ROWS)], axis=0)
        weight = jnp.sum(jnp.where(lane == me, chance, 0.0), axis=1, keepdims=True) / total
        weight_at[...] = jnp.where(lane[:, :128] == 0, weight * named, named)

        def gate_step(n, _):
            gates_at[:, span(n)] = dot(xg[blocks].reshape(TILE, MODEL_WIDTH), up[:, span(n)])
            return 0

        lax.fori_loop(0, 2 * FFE // SPAN, gate_step, 0)
        if back:
            def plain_step(n, _):
                plain_at[:, span(n)] = contract(gg[blocks].reshape(TILE, MODEL_WIDTH), down[span(n), :], (1, 1))
                return 0

            lax.fori_loop(0, FFE // SPAN, plain_step, 0)

        def strip(r, _):
            at = pl.ds(pl.multiple_of(r * STRIP, STRIP), STRIP)
            gate, raise_ = gates_at[at, :FFE], gates_at[at, FFE:]
            sigmoid = 1.0 / (1.0 + jnp.exp(-gate))
            silu = gate * sigmoid
            activated = silu * raise_
            if fore:
                act_at[at] = activated.astype(jnp.bfloat16)
            if back:
                row = pl.ds(pl.multiple_of(b0 * ROWS + r * STRIP, STRIP), STRIP)
                w, m = weight_at[at, 0:1], weight_at[at, 1:2]
                plain = plain_at[at]
                grad_act = plain * w
                ggu_at[row, :FFE] = (grad_act * raise_ * sigmoid * (1.0 + gate * (1.0 - sigmoid))).astype(jnp.bfloat16)
                ggu_at[row, FFE:] = (grad_act * silu).astype(jnp.bfloat16)
                actw_at[row] = (activated * w).astype(jnp.bfloat16)
                product = activated * plain * m
                high = product.astype(jnp.bfloat16)
                high_at[at] = high
                low_at[at] = (product - high.astype(jnp.float32)).astype(jnp.bfloat16)
            return 0

        lax.fori_loop(0, TILE // STRIP, strip, 0)
        if back:
            def back_step(n, _):
                part = contract(ggu_at[here], up[span(n), :], (1, 1))
                share_b[blocks, :, span(n)] = part.astype(jnp.bfloat16).reshape(TILE // ROWS, ROWS, SPAN)
                return 0

            lax.fori_loop(0, MODEL_WIDTH // SPAN, back_step, 0)
        if fore:
            def share_step(n, _):
                part = dot(act_at[...], down[:, span(n)]) * weight_at[:, 0:1]
                share_f[blocks, :, span(n)] = part.astype(jnp.bfloat16).reshape(TILE // ROWS, ROWS, SPAN)
                return 0

            lax.fori_loop(0, MODEL_WIDTH // SPAN, share_step, 0)
        if back:
            ones = jnp.ones((8, FFE), jnp.bfloat16)
            row = contract(ones, high_at[...], (1, 1)) + contract(ones, low_at[...], (1, 1))
            for b in range(TILE // ROWS):
                chance_row[b0 + b] = row[:, b * ROWS : (b + 1) * ROWS]

    for t in range(1, SPREAD_STEPS):
        spread.step(t)
        if folded:
            aside.step(t - 1)
    if extra:
        other.step(0)
    route = Route(axes, ORDERS[0])
    sources = [route.plane(k) for k in ranks]

    def chunk(c, _):
        source = sources[0]
        for v in range(1, n0):
            source = jnp.where(c == v, sources[v], source)

        def step(q, _):
            if "tile" not in SKIP:
                tile(source * plane + q * (TILE // ROWS))
            return 0

        lax.fori_loop(0, plane * ROWS // TILE, step, 0)

        for v in range(n0):
            @pl.when(c == v)
            def _(v=v):
                fold.step(v)
                if extra and v:
                    other.step(v)
                if folded:
                    aside.step(SPREAD_STEPS - 1 + v)
        return 0

    lax.fori_loop(0, n0, chunk, 0)
    if back:

        def chance_copy(offs, sender):
            block = route.block(offs)
            return remote(chance_row.at[block], chance_got.at[sender], c_send.at[route.flat(offs)], c_recv.at[sender], {"dp": block})

        for offs in route.others:
            chance_copy(offs, me).start()
        chance_got[me] = chance_row[me]

        up_held = gates_at.at[pl.ds(0, PIECE)]
        down_held = (gates_at.at[pl.ds(PIECE, PIECE)], plain_at.at[pl.ds(0, PIECE)])
        down_parts = ((0, 2 * FFE), (2 * FFE, MODEL_WIDTH - 2 * FFE))

        def put_up(n):
            return pltpu.make_async_copy(up_held, up_grad_out.at[span(n, PIECE)], out_sem.at[0, 0])

        def put_down(n, p):
            cols = pl.ds(*down_parts[p])
            return pltpu.make_async_copy(down_held[p], down_grad_out.at[span(n, PIECE), cols], out_sem.at[1, p])

        def up_gradient(n, _):
            @pl.when(n > 0)
            def _():
                put_up(n).wait()

            left = xg[:, :, span(n, PIECE)].reshape(count * ROWS, PIECE)
            up_held[...] = contract(left, ggu_at[...], (0, 0))
            put_up(n).start()
            return 0

        def down_gradient(n, _):
            @pl.when(n > 0)
            def _():
                put_down(n, 0).wait()
                put_down(n, 1).wait()

            for p, (at, width) in enumerate(down_parts):
                right = gg[:, :, at : at + width].reshape(count * ROWS, width)
                down_held[p][...] = contract(actw_at[:, span(n, PIECE)], right, (0, 0))
                put_down(n, p).start()
            return 0

    if saved_out is not None:
        save = pltpu.make_async_copy(xg, saved_out, local.at[2])
        save.start()
    last = fold.steps()
    assert last == 6
    for t in range(n0, last):
        if back and t == n0:
            lax.fori_loop(0, MODEL_WIDTH // PIECE, up_gradient, 0)
        elif back:
            lax.fori_loop(0, FFE // PIECE, down_gradient, 0)
        fold.step(t)
        if extra:
            other.step(t)
    if folded:
        assert aside.steps() == 6
        aside.end()
    if extra:
        other.end()
    spread.end()
    fold.end()
    if back:
        put_up(0).wait()
        put_down(0, 0).wait()
        put_down(0, 1).wait()
        for offs in route.others:
            chance_copy(offs, route.block(offs)).wait()
        chance_out[...] = chance_got[...]
    if saved_out is not None:
        save.wait()


def mixture_call(mode, count, layer, cid, mask, router, expert, partner, x, g=None, following=None, widths=(), summed=()):
    axes = torus_axes(count)
    fore, back = "f" in mode, "b" in mode
    vmem, anywhere = pl.BlockSpec(memory_space=pltpu.VMEM), pl.BlockSpec(memory_space=pl.ANY)
    args = [mask, router, expert[0], partner[0], expert[1], partner[1], x]
    in_specs = [vmem, vmem] + [anywhere] * 4 + [vmem if fore else anywhere]
    if back:
        args.append(g)
        in_specs.append(vmem)
    args += ([following] if widths else []) + list(summed)
    in_specs += ([vmem] if widths else []) + (fold_specs() if summed else [])
    whole = (count, ROWS, MODEL_WIDTH)
    out_shape, out_specs = [], []
    block = jax.ShapeDtypeStruct((ROWS, MODEL_WIDTH), jnp.float32)
    if fore:
        out_shape.append(block)
        out_specs.append(vmem)
    if mode == "f":
        out_shape.append(jax.ShapeDtypeStruct(whole, jnp.bfloat16))
        out_specs.append(anywhere)
    if back:
        out_shape += [block, jax.ShapeDtypeStruct((count, 8, ROWS), jnp.float32)]
        out_shape += [jax.ShapeDtypeStruct(w.shape, jnp.float32) for w in expert]
        out_specs += [vmem, vmem, anywhere, anywhere]
    if widths:
        out_shape += weight_shapes(following, widths, count)
        out_specs += [anywhere] * len(widths)
    if summed:
        out_shape.append(fold_shape(summed))
        out_specs.append(vmem)
    dma = pltpu.SemaphoreType.DMA
    scratch = [pltpu.VMEM(expert[0].shape, jnp.bfloat16), pltpu.VMEM(expert[1].shape, jnp.bfloat16), pltpu.VMEM(whole, jnp.bfloat16),
               pltpu.VMEM((TILE, 2 * FFE), jnp.float32), pltpu.VMEM((TILE, 128), jnp.float32), dma((3,))]
    parts = len(TOKEN_PARTS)
    ag, rs = parts * (1 if mode == "b" else fore + back), parts * (fore + back)
    scratch += [dma((ag, count + 4)), dma((ag, count + 4)), dma((rs, count + 4)), dma((rs, count + 4))]
    blocks = pltpu.VMEM(whole, jnp.bfloat16)
    arrivals = pltpu.VMEM((count + 4, *whole[1:]), jnp.bfloat16)
    low = lambda rows, width: pltpu.VMEM((rows, width), jnp.bfloat16)
    if fore:
        scratch += [blocks, arrivals, low(TILE, FFE)]
    if back:
        scratch += [blocks, blocks, arrivals, pltpu.VMEM((TILE, FFE), jnp.float32),
                    low(count * ROWS, 2 * FFE), low(count * ROWS, FFE), low(TILE, FFE), low(TILE, FFE),
                    pltpu.VMEM((count, 8, ROWS), jnp.float32), pltpu.VMEM((count, 8, ROWS), jnp.float32), dma((count,)), dma((count,)),
                    dma((2, 2))]
    if widths:
        scratch += weight_scratch(following, widths, count)
    if summed:
        scratch += fold_scratch(summed)
    rows = count * ROWS
    flops = rows * 6 * MODEL_WIDTH * FFE * (fore + 2 * back + (mode == "b"))
    return pl.pallas_call(
        functools.partial(mixture_kernel, mode, axes, count, layer, len(widths), len(summed)),
        out_shape=out_shape,
        in_specs=in_specs,
        out_specs=out_specs,
        scratch_shapes=scratch,
        compiler_params=pltpu.CompilerParams(collective_id=cid, has_side_effects=True, vmem_limit_bytes=VMEM_BYTES),
        cost_estimate=pl.CostEstimate(flops=flops, bytes_accessed=4 * rows * MODEL_WIDTH, transcendentals=rows * FFE),
        name="mixture_" + mode,
    )(*args)

def swapped(value):
    return lax.ppermute(value, "section", [(0, 1), (1, 0)])


def layout(length_row):
    seq_ends = jnp.cumsum(length_row)
    seq_starts = seq_ends - length_row
    row_ids = jnp.arange(DEVICE_ROWS, dtype=jnp.int32)
    segment = jnp.sum((row_ids[:, None] >= seq_ends[None, :]).astype(jnp.int32), axis=-1)
    member = (segment[:, None] == jnp.arange(NSEQ, dtype=jnp.int32)[None, :]).astype(jnp.int32)
    token_position = row_ids - jnp.sum(member * seq_starts[None, :], axis=-1)
    return segment, token_position


def rotation(token_position):
    half_width = HEAD_SIZE // 2
    frequency = 10000.0 ** (-2.0 * jnp.arange(half_width, dtype=jnp.float32) / HEAD_SIZE)
    angles = token_position.astype(jnp.float32)[:, None] * frequency
    return jnp.cos(angles)[:, None, :], jnp.sin(angles)[:, None, :]


def rotary_embedding(values, cosine, sine):
    half_width = HEAD_SIZE // 2
    former, latter = values[..., :half_width], values[..., half_width:]
    return jnp.concatenate([former * cosine - latter * sine, latter * cosine + former * sine], axis=-1)


def dot(left, right):
    return jnp.dot(left, right, preferred_element_type=jnp.float32)


def dot_rows(left, right):
    return lax.dot_general(left, right, (((0,), (0,)), ((), ())), preferred_element_type=jnp.float32)


def dot_columns(left, right):
    return lax.dot_general(left, right, (((1,), (1,)), ((), ())), preferred_element_type=jnp.float32)


def router_chances(normed_two, router):
    chance = jnp.exp(dot(normed_two, router))
    return chance / jnp.sum(chance, axis=-1, keepdims=True)


def front(hidden, place, weights):
    joint, result_output, router, gain_attention, gain_mixture = weights
    allowed, cosine, sine = place
    rows = hidden.shape[0]
    inverse_one = lax.rsqrt(jnp.mean(hidden * hidden, axis=-1, keepdims=True) + norm_epsilon)
    scaled_one = hidden * inverse_one
    normed = (scaled_one * gain_attention).astype(jnp.bfloat16)
    projected = dot(normed, joint)
    query = rotary_embedding(projected[:, :QUERY_WIDTH].reshape(rows, QUERY_HEADS, HEAD_SIZE), cosine, sine)
    query = query.astype(jnp.bfloat16).reshape(rows, KEY_VALUE_HEADS, GROUP, HEAD_SIZE)
    key = rotary_embedding(projected[:, QUERY_WIDTH : QUERY_WIDTH + KEY_WIDTH].reshape(rows, KEY_VALUE_HEADS, HEAD_SIZE), cosine, sine)
    key = key.astype(jnp.bfloat16)
    value = projected[:, QUERY_WIDTH + KEY_WIDTH :].reshape(rows, KEY_VALUE_HEADS, HEAD_SIZE).astype(jnp.bfloat16)
    scores = jnp.einsum("qhgd,khd->hgqk", query, key, preferred_element_type=jnp.float32) * SCORE_SCALE
    exponent = jnp.where(allowed, jnp.exp(scores), 0.0)
    attention = exponent / jnp.sum(exponent, axis=-1, keepdims=True)
    context = jnp.einsum("hgqk,khd->qhgd", attention.astype(jnp.bfloat16), value, preferred_element_type=jnp.float32)
    context = context.reshape(rows, QUERY_WIDTH).astype(jnp.bfloat16)
    middle = hidden + dot(context, result_output)
    inverse_two = lax.rsqrt(jnp.mean(middle * middle, axis=-1, keepdims=True) + norm_epsilon)
    scaled_two = middle * inverse_two
    normed_two = (scaled_two * gain_mixture).astype(jnp.bfloat16)
    kept = (inverse_one, scaled_one, normed, query, key, value, attention, context, inverse_two, scaled_two, normed_two)
    return middle, normed_two, kept


def gates(everyone, up_weight):
    both = dot(everyone, up_weight)
    return both[:, :FFE], both[:, FFE:]


def expert_forward(everyone, mask, router, expert, count, me):
    up_weight, down_weight = expert
    chance = router_chances(everyone, router)
    own = jnp.arange(count, dtype=jnp.int32) == me
    weight = jnp.sum(jnp.where(own[None, :] & mask, chance, 0.0), axis=-1)
    gate, up = gates(everyone, up_weight)
    activated = (jax.nn.silu(gate) * up).astype(jnp.bfloat16)
    share = (dot(activated, down_weight) * weight[:, None]).astype(jnp.bfloat16)
    return share, weight, (gate, up)


def expert_backward(grads, everyone, weight, mask, held, expert):
    up_weight, down_weight = expert
    gate, up = held if held is not None else gates(everyone, up_weight)
    sigmoid = jax.nn.sigmoid(gate)
    silu = gate * sigmoid
    activated = silu * up
    grad_plain = dot_columns(grads, down_weight)
    grad_weight = jnp.where(mask[:, 0], jnp.sum(activated * grad_plain, axis=-1), 0.0)
    grad_act = grad_plain * weight[:, None]
    grad_gate = grad_act * up * sigmoid * (1.0 + gate * (1.0 - sigmoid))
    grad_gate_up = jnp.concatenate([grad_gate, grad_act * silu], axis=-1).astype(jnp.bfloat16)
    grad_down = dot_rows((activated * weight[:, None]).astype(jnp.bfloat16), grads)
    grad_up_weight = dot_rows(everyone, grad_gate_up)
    share = dot_columns(grad_gate_up, up_weight).astype(jnp.bfloat16)
    return share, grad_weight, grad_up_weight, grad_down


def pieces(value):
    return value.reshape(-1, CHUNK_ROWS, *value.shape[1:])


def mixture_forward(normed_two, router, mask, expert, count, me):
    (spread,) = gather_all([normed_two], count, 0)
    everyone = spread.reshape(-1, MODEL_WIDTH)
    if everyone.shape[0] <= CHUNK_ROWS:
        share, weight, held = expert_forward(everyone, mask, router, expert, count, me)
    else:
        share, weight = lax.map(
            lambda part: expert_forward(part[0], part[1], router, expert, count, me)[:2], (pieces(everyone), pieces(mask)))
        held = None
    (mixed,) = reduce_all([share.reshape(spread.shape)], count, 1)
    return mixed, (everyone, weight.reshape(-1), held)


def mixture_backward(grad_out, mask, kept, expert, count):
    everyone, weight, held = kept
    (spread,) = gather_all([grad_out], count, 0)
    grads = spread.reshape(-1, MODEL_WIDTH)
    if grads.shape[0] <= CHUNK_ROWS:
        share, grad_weight, grad_up, grad_down = expert_backward(grads, everyone, weight, mask, held, expert)
    else:
        def step(sums, part):
            share, grad_weight, grad_up, grad_down = expert_backward(*part, None, expert)
            return (sums[0] + grad_up, sums[1] + grad_down), (share, grad_weight)

        zero = tuple(jnp.zeros(w.shape, jnp.float32) for w in expert)
        (grad_up, grad_down), (share, grad_weight) = lax.scan(
            step, zero, (pieces(grads), pieces(everyone), pieces(weight), pieces(mask)))
    grad_chance = lax.all_to_all(grad_weight.reshape(count, DEVICE_ROWS), "dp", split_axis=0, concat_axis=0, tiled=True)
    (mixed,) = reduce_all([share.reshape(spread.shape)], count, 1)
    return mixed, grad_chance.T, grad_up, grad_down


def front_backward(grad_out, grad_mixed, grad_chance, kept, place, weights, fused):
    joint, result_output, router, gain_attention, gain_mixture = weights
    allowed, cosine, sine = place
    inverse_one, scaled_one, normed, query, key, value, attention, context, inverse_two, scaled_two, normed_two = kept
    rows = normed.shape[0]
    chance = router_chances(normed_two, router)
    grad_logit = (chance * (grad_chance - jnp.sum(grad_chance * chance, axis=-1, keepdims=True))).astype(jnp.bfloat16)
    grad_router = dot_rows(normed_two, grad_logit)
    grad_normed_two = grad_mixed + dot_columns(grad_logit, router)
    grad_gain_two = jnp.sum(grad_normed_two * scaled_two, axis=0)
    scaled_grad_two = grad_normed_two * gain_mixture
    grad_middle = grad_out + inverse_two * (scaled_grad_two - scaled_two * jnp.mean(scaled_grad_two * scaled_two, axis=-1, keepdims=True))
    branch = grad_middle.astype(jnp.bfloat16)
    grad_context = dot_columns(branch, result_output).astype(jnp.bfloat16).reshape(rows, KEY_VALUE_HEADS, GROUP, HEAD_SIZE)
    grad_attention = jnp.einsum("qhgd,khd->hgqk", grad_context, value, preferred_element_type=jnp.float32)
    grad_value = jnp.einsum("hgqk,qhgd->khd", attention.astype(jnp.bfloat16), grad_context, preferred_element_type=jnp.float32)
    grad_scores = (attention * (grad_attention - jnp.sum(grad_attention * attention, axis=-1, keepdims=True))).astype(jnp.bfloat16)
    grad_query = jnp.einsum("hgqk,khd->qhgd", grad_scores, key, preferred_element_type=jnp.float32).reshape(rows, QUERY_HEADS, HEAD_SIZE)
    grad_key = jnp.einsum("hgqk,qhgd->khd", grad_scores, query, preferred_element_type=jnp.float32)
    grad_query = rotary_embedding(grad_query * SCORE_SCALE, cosine, -sine)
    grad_key = rotary_embedding(grad_key * SCORE_SCALE, cosine, -sine)
    grad_projected = jnp.concatenate(
        [grad_query.reshape(rows, -1), grad_key.reshape(rows, -1), grad_value.reshape(rows, -1)], axis=-1).astype(jnp.bfloat16)
    pairs = (normed, context, grad_projected, branch)
    products = (pairs[0].T, pairs[1].T, *pairs[2:]) if fused else (dot_rows(normed, grad_projected), dot_rows(context, branch))
    grad_normed = dot_columns(grad_projected, joint)
    grad_gain_one = jnp.sum(grad_normed * scaled_one, axis=0)
    scaled_grad_one = grad_normed * gain_attention
    grad_hidden = grad_middle + inverse_one * (scaled_grad_one - scaled_one * jnp.mean(scaled_grad_one * scaled_one, axis=-1, keepdims=True))
    return grad_hidden, (products, None, grad_router, grad_gain_one, grad_gain_two)


def small_halves(rows, router, gains, codes):
    second = jnp.concatenate([gains, codes], axis=1)
    width = -(-max(router.shape[1], second.shape[1]) // 128) * 128
    pad = lambda v: jnp.pad(v, ((0, 0), (0, width - v.shape[1])))
    return pad(router), pad(second)


def body(tokens, cotangent, lengths, routes, combined_weight, output_weight, router_weight, attention_gain, mixture_gain,
         expert_gate_up, expert_down):
    count = lax.axis_size("dp")
    me, sec = lax.axis_index("dp"), lax.axis_index("section")
    layers = lax.axis_size("section")
    leading = sec == 0
    shard = combined_weight.shape[1]
    micro = lambda a, axis: lax.dynamic_index_in_dim(a, sec, axis, keepdims=False)

    gains = jnp.stack([attention_gain[0], mixture_gain[0]], axis=1)
    codes = routes[0].astype(jnp.bfloat16).reshape(-1)
    code_count = codes.shape[0]
    codes = jnp.pad(codes, (0, -code_count % shard)).reshape(shard, -1)
    fused = count * DEVICE_ROWS <= CHUNK_ROWS
    if fused:
        member = jnp.any(routes[0][:, None] == jnp.arange(count, dtype=jnp.int32)[None, :, None, None], axis=-1)
        member = member.astype(jnp.bfloat16).reshape(-1, DEVICE_ROWS)
        small = small_halves(shard, jnp.concatenate([router_weight[0], gains], axis=1), gains[:, :0], gains[:, :0])
        small = (small[0], jnp.pad(member, ((0, shard - member.shape[0]), (0, 0))))
    else:
        small = small_halves(shard, router_weight[0], gains, codes)
    small_width = small[0].shape[1]
    halves = [
        (combined_weight[0, :, : combined_weight.shape[2] // 2], combined_weight[0, :, combined_weight.shape[2] // 2 :]),
        (output_weight[0, :, : output_weight.shape[2] // 2], output_weight[0, :, output_weight.shape[2] // 2 :]),
        small,
    ]
    widths = [h[0].shape[1] for h in halves]
    mine = jnp.concatenate([jnp.where(leading, a, b) for a, b in halves], axis=1)
    given = swapped(jnp.concatenate([jnp.where(leading, b, a) for a, b in halves], axis=1))
    packs = [jnp.where(leading, mine, given), jnp.where(leading, given, mine)]
    partner_expert = tuple(swapped(w[0, 0]) for w in (expert_gate_up, expert_down))
    own_expert = (expert_gate_up[0, 0], expert_down[0, 0])
    experts, routers = [], []
    for layer in range(0 if fused else layers):
        keep = sec == layer
        experts.append((jnp.where(keep, expert_gate_up[0, 0], partner_expert[0]), jnp.where(keep, expert_down[0, 0], partner_expert[1])))

    def layer_parts(layer):
        at, parts = 0, []
        for w in widths:
            parts.append(packs[layer][:, at : at + w])
            at += w
        return parts

    def layer_weights(arrays):
        joint, output, tail = [a.reshape(MODEL_WIDTH, -1) for a in arrays]
        experts_wide = router_weight.shape[2]
        second = tail[:, small_width:] if not fused else tail[:, experts_wide:]
        weights = (joint, output, tail[:, :experts_wide], second[:, 0].astype(jnp.float32), second[:, 1].astype(jnp.float32))
        routers.append(tail[:, :small_width])
        if fused:
            rows = lax.dynamic_slice(arrays[2], (0, sec * count + me, small_width), (count, 1, DEVICE_ROWS))
            return weights, jnp.pad(rows, ((0, 0), (0, 7), (0, 0)))
        code = second[:, 2 : 2 + codes.shape[1]].reshape(count, -1)[:, :code_count].reshape(count, -1, DEVICE_ROWS, TOPK)
        named = lax.dynamic_index_in_dim(code, sec, 1, keepdims=False).reshape(count * DEVICE_ROWS, TOPK)
        mask = jnp.any(named == me.astype(jnp.bfloat16), axis=-1, keepdims=True)
        return weights, mask

    segment, token_position = layout(micro(lengths[:, 0], 0))
    row_ids = jnp.arange(DEVICE_ROWS, dtype=jnp.int32)
    allowed = (row_ids[:, None] >= row_ids[None, :]) & (segment[:, None] == segment[None, :])
    place = (allowed,) + rotation(token_position)

    weights, masks, stores = [], [], []
    hidden = micro(tokens, 0)
    for layer in range(layers):
        if not fused:
            arrays = gather_all(layer_parts(layer), count, 2, pair=True)
        elif layer == 0:
            arrays = weight_spread(packs[layer], widths, count, 2)
        got, mask = layer_weights(arrays)
        weights.append(got)
        masks.append(mask)
        middle, normed_two, kept = front(hidden.astype(jnp.float32), place, got)
        if not fused:
            mixed, kept_mixture = mixture_forward(normed_two, got[2], mask, experts[layer], count, me)
        else:
            named = mask
            call = lambda mode, cid, *data, **more: mixture_call(
                mode, count, layer, cid, named, routers[layer], own_expert, partner_expert, *data, **more)
            if layer < layers - 1:
                mixed, everyone, *arrays = call("f", 4, normed_two, following=packs[layer + 1], widths=tuple(widths))
                kept_mixture = (named, everyone)
            else:
                mixed, *kept_mixture = call("fb", 5, normed_two, micro(cotangent, 0))
        hidden = (middle + mixed).astype(jnp.bfloat16)
        stores.append((kept, kept_mixture))
    last = hidden
    grad = micro(cotangent, 0)
    shares, expert_grads = [None] * layers, [None] * layers
    for layer in reversed(range(layers)):
        kept, kept_mixture = stores[layer]
        if not fused:
            mixed, grad_chance, grad_up, grad_down = mixture_backward(grad, masks[layer], kept_mixture, experts[layer], count)
        else:
            if layer < layers - 1:
                named, everyone = kept_mixture
                kept_mixture = mixture_call("b", count, layer, 6, named, routers[layer], own_expert, partner_expert, everyone, grad,
                                            summed=packs[layer + 1])
            mixed, rows, grad_up, grad_down, *more = kept_mixture
            if more:
                shares[layer + 1] = more[0]
            grad_chance = rows[:, 0].T
        expert_grads[layer] = (grad_up, grad_down)
        grad_hidden, parts = front_backward(grad.astype(jnp.float32), mixed, grad_chance, kept, place, weights[layer], fused)
        grad = grad_hidden.astype(jnp.bfloat16)
        tail = small_halves(MODEL_WIDTH, parts[2], jnp.stack([parts[3], parts[4]], axis=1), parts[2][:, :0])
        small = jnp.concatenate(tail, axis=1).astype(jnp.bfloat16).reshape(count, shard, -1)
        if fused:
            packs[layer] = [*parts[0], small]
        else:
            packed = [a.astype(jnp.bfloat16).reshape(count, shard, -1) for a in parts[0]] + [small]
            shares[layer] = reduce_all(packed, count, 3, pair=True)
    if fused:
        *outs, grad_up, grad_down, boundary = closing(packs[0], shares[1], expert_grads[0], expert_grads[1], grad, last, count, 3)
        half = outs[2].shape[1] // 2
        return (
            boundary[None],
            outs[0][None],
            outs[1][None],
            outs[2][None, :, : router_weight.shape[2]],
            outs[2][None, :, half],
            outs[2][None, :, half + 1],
            grad_up[None, None],
            grad_down[None, None],
        )
    outs = []
    for a in range(3):
        kept_half = jnp.where(leading, shares[0][a], shares[1][a])
        got_half = swapped(jnp.where(leading, shares[1][a], shares[0][a]))
        outs.append(jnp.concatenate([jnp.where(leading, kept_half, got_half), jnp.where(leading, got_half, kept_half)], axis=1))
    expert_outs = []
    for a in range(2):
        kept_sum = jnp.where(leading, expert_grads[0][a], expert_grads[1][a])
        got_sum = swapped(jnp.where(leading, expert_grads[1][a], expert_grads[0][a]))
        expert_outs.append((kept_sum + got_sum)[None, None])
    partner = swapped(jnp.where(leading, last, grad))
    boundary = jnp.where(leading, jnp.stack([grad, partner]), jnp.stack([partner, last]))[None]
    half = outs[2].shape[1] // 2
    return (
        boundary,
        outs[0][None],
        outs[1][None],
        outs[2][None, :, : router_weight.shape[2]],
        outs[2][None, :, half],
        outs[2][None, :, half + 1],
        expert_outs[0],
        expert_outs[1],
    )


def solution(mesh):
    return jax.shard_map(
        body,
        mesh=mesh,
        in_specs=(
            P(None, "dp", None),
            P(None, "dp", None),
            P(None, "dp", None),
            P("section", None, "dp", None),
            P("section", "dp", None),
            P("section", "dp", None),
            P("section", "dp", None),
            P("section", "dp"),
            P("section", "dp"),
            P("section", "dp", None, None),
            P("section", "dp", None, None),
        ),
        out_specs=(
            P("section", None, "dp", None),
            P("section", "dp", None),
            P("section", "dp", None),
            P("section", "dp", None),
            P("section", "dp"),
            P("section", "dp"),
            P("section", "dp", None, None),
            P("section", "dp", None, None),
        ),
        check_vma=False,
    )
```

```python
import functools
import jax
import jax.numpy as jnp
from jax import lax
from jax.experimental import pallas as pl
from jax.experimental.pallas import tpu as pltpu
from jax.sharding import PartitionSpec as P

MODEL_WIDTH = 1536
QUERY_HEADS = 24
KEY_VALUE_HEADS = 8
GROUP = QUERY_HEADS // KEY_VALUE_HEADS
HEAD_SIZE = 64
FFE = 512
TOPK = 8
DEVICE_ROWS = 128
NSEQ = 4
QUERY_WIDTH = QUERY_HEADS * HEAD_SIZE
KEY_WIDTH = KEY_VALUE_HEADS * HEAD_SIZE
SCORE_SCALE = HEAD_SIZE ** (-0.5)
norm_epsilon = 1e-06
CHUNK_ROWS = 2048

VMEM_BYTES = 67_000_000


def torus_axes(count):
    side = 1
    while (side + 1) ** 3 <= count:
        side += 1
    assert count % (side * side) == 0
    return [(side * side, count // (side * side)), (1, side), (side, side)]


def offsets(sizes):
    return [(k, j, i) for k in range(sizes[0]) for j in range(sizes[1]) for i in range(sizes[2])]


class Place:
    def __init__(self, axes, order):
        self.me = lax.axis_index("dp")
        self.sec = lax.axis_index("section")
        long, first, second = axes
        if order is None:
            flip = self.sec
            stride_one = first[0] + (second[0] - first[0]) * flip
            stride_two = second[0] + (first[0] - second[0]) * flip
            assert first[1] == second[1]
            self.axes = [long, (stride_one, first[1]), (stride_two, second[1])]
        elif order == 0:
            self.axes = [long, first, second]
        else:
            self.axes = [long, second, first]
        self.sizes = [size for _, size in self.axes]

    def moved(self, steps):
        out = self.me
        for (stride, size), step in zip(self.axes, steps):
            if step % size:
                digit = lax.rem(lax.div(self.me, stride), size)
                out = out + (lax.rem(digit + (step % size), size) - digit) * stride
        return out

    def source(self, offs):
        return self.moved([-o for o in offs])

    def target(self, offs):
        return self.moved(list(offs))

    def flat(self, offs):
        return (offs[0] * self.sizes[1] + offs[1]) * self.sizes[2] + offs[2]


def last_hop(offs):
    for axis in (2, 1, 0):
        if offs[axis]:
            hop = [0, 0, 0]
            hop[axis] = offs[axis]
            base = list(offs)
            base[axis] = 0
            return tuple(hop), tuple(base)
    return None


def greet(axes, pair):
    place = Place(axes, 0)
    barrier = pltpu.get_barrier_semaphore()
    count = 0
    for axis in range(3):
        for step in range(1, place.sizes[axis]):
            hop = [0, 0, 0]
            hop[axis] = step
            pl.semaphore_signal(barrier, inc=1, device_id={"dp": place.target(hop)}, device_id_type=pl.DeviceIdType.MESH)
            count += 1
    if pair:
        pl.semaphore_signal(barrier, inc=1, device_id={"section": 1 - place.sec}, device_id_type=pl.DeviceIdType.MESH)
        count += 1
    pl.semaphore_wait(barrier, count)


def gather_kernel(axes, pair, count, *refs):
    ins, outs = refs[:count], refs[count : 2 * count]
    send, recv, local = refs[2 * count : 2 * count + 3]
    psend, precv = refs[2 * count + 3 :] if pair else (None, None)
    streams = []
    for a in range(count):
        if pair:
            place = Place(axes, None)
            half = ins[a].shape[1]
            cols = pl.ds(pl.multiple_of(place.sec * half, 128), half)
            streams.append((place, ins[a], lambda b, o=outs[a], c=cols: o.at[b, :, c]))
        else:
            half = ins[a].shape[0] // 2
            for h in range(2):
                rows = pl.ds(h * half, half)
                streams.append((Place(axes, h), ins[a].at[rows], lambda b, o=outs[a], r=rows: o.at[b, r]))

    def copy(s, offs):
        place, own, out = streams[s]
        hop, base = last_hop(offs)
        block = place.source(base)
        src = out(block) if any(base) else own
        f = place.flat(offs)
        return pltpu.make_async_remote_copy(
            src_ref=src, dst_ref=out(block), send_sem=send.at[s, f], recv_sem=recv.at[s, f],
            device_id={"dp": place.target(hop)}, device_id_type=pl.DeviceIdType.MESH)

    def share(s, offs):
        place, own, out = streams[s]
        block = place.source(offs)
        src = out(block) if any(offs) else own
        f = place.flat(offs)
        return pltpu.make_async_remote_copy(
            src_ref=src, dst_ref=out(block), send_sem=psend.at[s, f], recv_sem=precv.at[s, f],
            device_id={"section": 1 - place.sec}, device_id_type=pl.DeviceIdType.MESH)

    greet(axes, pair)
    ids = range(len(streams))
    n0, n1, n2 = streams[0][0].sizes
    keep = []
    for s in ids:
        place, own, out = streams[s]
        c = pltpu.make_async_copy(own, out(place.me), local.at[s])
        c.start()
        keep.append(c)
    for k in range(1, n0):
        for s in ids:
            copy(s, (k, 0, 0)).start()

    def first(k):
        for s in ids:
            if k:
                copy(s, (k, 0, 0)).wait_recv()
            for j in range(1, n1):
                copy(s, (k, j, 0)).start()
            for i in range(1, n2):
                copy(s, (k, 0, i)).start()
            if pair:
                share(s, (k, 0, 0)).start()

    def second(k):
        for j in range(1, n1):
            for s in ids:
                copy(s, (k, j, 0)).wait_recv()
                for i in range(1, n2):
                    copy(s, (k, j, i)).start()
                if pair:
                    share(s, (k, j, 0)).start()

    def third(k):
        for j in range(n1):
            for i in range(1, n2):
                for s in ids:
                    copy(s, (k, j, i)).wait_recv()
                    if pair:
                        share(s, (k, j, i)).start()

    for k in range(n0 + 2):
        if k < n0:
            first(k)
        if 0 <= k - 1 < n0:
            second(k - 1)
        if 0 <= k - 2 < n0:
            third(k - 2)
    for s in ids:
        for offs in offsets((n0, n1, n2)):
            if any(offs):
                copy(s, offs).wait_send()
            if pair:
                share(s, offs).wait()
    for c in keep:
        c.wait()


def gather_all(arrays, count, cid, pair=False):
    axes = torus_axes(count)
    streams = len(arrays) * (1 if pair else 2)
    sem = pltpu.SemaphoreType.DMA((streams, count))
    out_shape = [jax.ShapeDtypeStruct((count, a.shape[0], a.shape[1] * (2 if pair else 1)), a.dtype) for a in arrays]
    scratch = [sem, sem, pltpu.SemaphoreType.DMA((streams,))]
    if pair:
        scratch += [sem, sem]
    sent = sum(a.size * a.dtype.itemsize for a in arrays) * (count - 1)
    return pl.pallas_call(
        functools.partial(gather_kernel, axes, pair, len(arrays)),
        out_shape=out_shape,
        in_specs=[pl.BlockSpec(memory_space=pltpu.VMEM)] * len(arrays),
        out_specs=[pl.BlockSpec(memory_space=pl.ANY)] * len(arrays),
        scratch_shapes=scratch,
        compiler_params=pltpu.CompilerParams(collective_id=cid, has_side_effects=True),
        cost_estimate=pl.CostEstimate(flops=0, bytes_accessed=2 * sent, transcendentals=0),
        name="spread" if not pair else "spread_pair",
    )(*arrays)


def reduce_kernel(axes, pair, count, *refs):
    ins, outs = refs[:count], refs[count : 2 * count]
    rest = list(refs[2 * count :])
    send, recv = rest[:2]
    rest = rest[2:]
    if pair:
        psend, precv = rest[:2]
        rest = rest[2:]
    streams = []
    for a in range(count):
        if pair:
            got, held, pgot, psum = rest[:4]
            rest = rest[4:]
            place = Place(axes, None)
            half = outs[a].shape[1]
            mine = pl.ds(pl.multiple_of(place.sec * half, 128), half)
            other = pl.ds(pl.multiple_of((1 - place.sec) * half, 128), half)
            streams.append(dict(place=place, got=got, held=held, pgot=pgot, psum=psum, raw=ins[a], mine=mine, other=other,
                                out=outs[a], rows=outs[a].shape[0]))
        else:
            got, held = rest[:2]
            rest = rest[2:]
            half = outs[a].shape[0] // 2
            for h in range(2):
                rows = pl.ds(h * half, half)
                streams.append(dict(place=Place(axes, h), got=got.at[h], held=held.at[h], raw=ins[a], span=rows,
                                    out=outs[a].at[rows], rows=half))
    step = 8 if streams[0]["rows"] % 16 else 16

    def own_ref(t, offs):
        if pair:
            return t["psum"].at[t["place"].flat(offs)]
        return t["raw"].at[t["place"].target(offs), t["span"]]

    def summed(t, sources, dest):
        def one(r, _):
            rows = pl.ds(pl.multiple_of(r * step, step), step)
            total = sources[0][rows].astype(jnp.float32)
            for source in sources[1:]:
                total = total + source[rows].astype(jnp.float32)
            dest[rows] = total.astype(dest.dtype)
            return 0

        lax.fori_loop(0, t["rows"] // step, one, 0)

    def copy(s, offs):
        t = streams[s]
        place = t["place"]
        hop, base = last_hop(offs)
        f = place.flat(offs)
        src = own_ref(t, offs) if hop[2] else t["held"].at[f // place.sizes[2]]
        return pltpu.make_async_remote_copy(
            src_ref=src, dst_ref=t["got"].at[f], send_sem=send.at[s, f], recv_sem=recv.at[s, f],
            device_id={"dp": place.target(hop)}, device_id_type=pl.DeviceIdType.MESH)

    def share(s, offs):
        t = streams[s]
        place = t["place"]
        f = place.flat(offs)
        return pltpu.make_async_remote_copy(
            src_ref=t["raw"].at[place.target((offs[0], offs[2], offs[1])), :, t["other"]], dst_ref=t["pgot"].at[f],
            send_sem=psend.at[s, f], recv_sem=precv.at[s, f],
            device_id={"section": 1 - place.sec}, device_id_type=pl.DeviceIdType.MESH)

    ids = range(len(streams))
    n0, n1, n2 = streams[0]["place"].sizes
    greet(axes, pair)

    def phase_pair(k):
        for j in reversed(range(n1)):
            for i in reversed(range(n2)):
                for s in ids:
                    share(s, (k, j, i)).start()

    def phase_first(k):
        for j in reversed(range(n1)):
            for i in reversed(range(n2)):
                for s in ids:
                    t = streams[s]
                    if pair:
                        share(s, (k, j, i)).wait_recv()
                        f = t["place"].flat((k, j, i))
                        summed(t, [t["raw"].at[t["place"].target((k, j, i)), :, t["mine"]], t["pgot"].at[f]], t["psum"].at[f])
                    if i:
                        copy(s, (k, j, i)).start()

    def phase_second(k):
        for j in range(1, n1):
            for s in ids:
                t = streams[s]
                for i in range(1, n2):
                    copy(s, (k, j, i)).wait_recv()
                parts = [own_ref(t, (k, j, 0))] + [t["got"].at[t["place"].flat((k, j, i))] for i in range(1, n2)]
                summed(t, parts, t["held"].at[t["place"].flat((k, j, 0)) // n2])
                copy(s, (k, j, 0)).start()

    def gathered_parts(s, k):
        t = streams[s]
        offs = [(k, 0, i) for i in range(1, n2)] + [(k, j, 0) for j in range(1, n1)]
        for o in offs:
            copy(s, o).wait_recv()
        return [own_ref(t, (k, 0, 0))] + [t["got"].at[t["place"].flat(o)] for o in offs]

    def phase_third(k):
        for s in ids:
            t = streams[s]
            parts = gathered_parts(s, k)
            if k:
                summed(t, parts, t["held"].at[t["place"].flat((k, 0, 0)) // n2])
                copy(s, (k, 0, 0)).start()
            else:
                for q in range(1, n0):
                    copy(s, (q, 0, 0)).wait_recv()
                    parts.append(t["got"].at[t["place"].flat((q, 0, 0))])
                summed(t, parts, t["out"])

    chunks = list(range(1, n0)) + [0]
    if pair:
        phase_pair(chunks[0])
    for c in range(n0 + 3):
        if pair and c + 1 < n0:
            phase_pair(chunks[c + 1])
        if c < n0:
            phase_first(chunks[c])
        if 0 <= c - 1 < n0:
            phase_second(chunks[c - 1])
        if 0 <= c - 2 < n0:
            phase_third(chunks[c - 2])
    for s in ids:
        for offs in offsets((n0, n1, n2)):
            if any(offs):
                copy(s, offs).wait_send()
            if pair:
                share(s, offs).wait_send()


def reduce_all(arrays, count, cid, pair=False):
    axes = torus_axes(count)
    streams = len(arrays) * (1 if pair else 2)
    sem = pltpu.SemaphoreType.DMA((streams, count))
    scratch = [sem, sem]
    if pair:
        scratch += [sem, sem]
    groups = count // axes[2][1]
    out_shape = []
    for a in arrays:
        rows, cols = a.shape[1:]
        if pair:
            cols = cols // 2
            scratch += [pltpu.VMEM((count, rows, cols), a.dtype), pltpu.VMEM((groups, rows, cols), a.dtype),
                        pltpu.VMEM((count, rows, cols), a.dtype), pltpu.VMEM((count, rows, cols), a.dtype)]
        else:
            scratch += [pltpu.VMEM((2, count, rows // 2, cols), a.dtype), pltpu.VMEM((2, groups, rows // 2, cols), a.dtype)]
        out_shape.append(jax.ShapeDtypeStruct((rows, cols), jnp.float32))
    sent = sum(a.size * a.dtype.itemsize for a in arrays)
    return pl.pallas_call(
        functools.partial(reduce_kernel, axes, pair, len(arrays)),
        out_shape=out_shape,
        in_specs=[pl.BlockSpec(memory_space=pltpu.VMEM)] * len(arrays),
        out_specs=[pl.BlockSpec(memory_space=pltpu.VMEM)] * len(arrays),
        scratch_shapes=scratch,
        compiler_params=pltpu.CompilerParams(collective_id=cid, has_side_effects=True, vmem_limit_bytes=VMEM_BYTES),
        cost_estimate=pl.CostEstimate(flops=0, bytes_accessed=2 * sent, transcendentals=0),
        name="fold" if not pair else "fold_pair",
    )(*arrays)


ROWS = 128
TILE = 512
STRIP = 16
SPAN = 512
PIECE = 256
MESH = pl.DeviceIdType.MESH
ORDERS = ((0, 1, 2), (0, 2, 1), (1, 0, 2), (2, 0, 1))
TOKEN_PARTS = tuple((order, 32 * n, 32) for n, order in enumerate(ORDERS))


class Route:
    def __init__(self, axes, order):
        self.axes, self.order = axes, order
        self.sizes = [size for _, size in axes]
        assert self.sizes == [4, 2, 2]
        self.me = lax.axis_index("dp")
        self.all = offsets(self.sizes)
        self.others = [o for o in self.all if any(o)]
        self.z = lax.div(self.me, axes[0][0])
        self.inner = jnp.logical_and(self.z >= 1, self.z <= 2)
        later = order[order.index(0) + 1 :]
        self.lines = [(j, i) for j in range(2) for i in range(2) if all((0, j, i)[a] == 0 for a in later)]

    def digit(self, axis):
        stride, size = self.axes[axis]
        return lax.rem(lax.div(self.me, stride), size)

    def plane(self, rank):
        z = self.z
        if rank == 1:
            return z + 1 - 2 * lax.rem(z, 2)
        if rank == 2:
            return 2 - lax.div(z, 2)
        if rank == 3:
            return 3 - 3 * lax.div(z, 2)
        return z

    def block(self, offs):
        out = self.me + (self.plane(offs[0]) - self.z) * self.axes[0][0]
        for axis in (1, 2):
            if offs[axis]:
                out = out + (1 - 2 * self.digit(axis)) * self.axes[axis][0]
        return out

    def flat(self, offs):
        return (offs[0] * 2 + offs[1]) * 2 + offs[2]

    def extra(self, line, n):
        return 16 + 2 * self.lines.index(line) + n

    def last_axis(self, offs):
        for axis in reversed(self.order):
            if offs[axis]:
                return axis

    def base(self, offs):
        out = list(offs)
        out[self.last_axis(offs)] = 0
        return tuple(out)

    def across(self, offs):
        return [o for o in self.others if self.last_axis(o) and self.base(o) == offs]


def remote(src, dst, send, recv, peer):
    return pltpu.make_async_remote_copy(src_ref=src, dst_ref=dst, send_sem=send, recv_sem=recv, device_id=peer, device_id_type=MESH)


class Spread:
    def __init__(self, streams, send, recv):
        self.streams, self.send, self.recv = streams, send, recv
        self.ids = range(len(streams))

    def copy(self, s, offs, target, key, slot):
        route, own, out = self.streams[s]
        block = route.block(offs)
        return remote(out(block) if any(offs) else own, out(block), self.send.at[s, slot], self.recv.at[s, route.flat(key)], {"dp": target})

    def arrival(self, s, offs):
        route, own, out = self.streams[s]
        f = route.flat(offs)
        return remote(own, out(route.block(offs)), self.send.at[s, f], self.recv.at[s, f], {"dp": route.block(offs)})

    def onward(self, s, offs):
        route = self.streams[s][0]
        k, line = offs[0], offs[1:]
        out = [(o, False, self.copy(s, offs, route.block((0, *[int(o[a] != offs[a]) for a in (1, 2)])), o, route.flat(o)))
               for o in route.across(offs)]
        if line in route.lines:
            near, facing = route.block((1, 0, 0)), route.block((2, 0, 0))
            if k == 0:
                out.append(((1, *line), False, self.copy(s, offs, near, (1, *line), route.flat((1, *line)))))
                out.append(((2, *line), True, self.copy(s, offs, facing, (2, *line), route.extra(line, 0))))
            elif k == 1:
                out.append(((3, *line), True, self.copy(s, offs, facing, (3, *line), route.extra(line, 1))))
            else:
                out.append((offs, True, self.copy(s, offs, near, offs, route.flat(offs))))
        return out

    def launch(self, items):
        for s, (_, inner, copy) in items:
            if inner:
                pl.when(self.streams[s][0].inner)(copy.start)
            else:
                copy.start()

    def step(self, t):
        work = [(offs, s) for s in self.ids for offs in self.streams[s][0].all if offs[0] + offs[1] + offs[2] == t]
        if t == 0:
            first = [(s, item) for offs, s in work for item in self.onward(s, offs)]
            self.launch(sorted(first, key=lambda e: (e[1][0][0], e[1][0], e[0])))
            return
        ends = lambda e: not self.streams[e[1]][0].across(e[0]) and e[0][1:] not in self.streams[e[1]][0].lines
        for offs, s in sorted(work, key=lambda e: (ends(e), -e[0][0], e[0], e[1])):
            self.arrival(s, offs).wait_recv()
            self.launch([(s, item) for item in sorted(self.onward(s, offs), key=lambda e: (e[1], e[0]))])

    def end(self):
        for s in self.ids:
            for offs in self.streams[s][0].all:
                for _, inner, copy in self.onward(s, offs):
                    if inner:
                        pl.when(self.streams[s][0].inner)(copy.wait_send)
                    else:
                        copy.wait_send()


SPREAD_STEPS = 6


def add_rows(sources, dest, rows, step=16):
    cols = dest.shape[-1]
    width = 768 if cols % 768 == 0 else cols

    def one(r, _):
        at = pl.ds(pl.multiple_of(r * step, step), step)

        def part(c, _):
            span = pl.ds(pl.multiple_of(c * width, width), width)
            total = sources[0][at, span].astype(jnp.float32)
            for source in sources[1:]:
                total = total + source[at, span].astype(jnp.float32)
            dest[at, span] = total.astype(dest.dtype)
            return 0

        return lax.fori_loop(0, cols // width, part, 0)

    lax.fori_loop(0, rows // step, one, 0)


class Fold:
    def __init__(self, streams, send, recv, ranks):
        self.streams, self.send, self.recv = streams, send, recv
        self.ids = range(len(streams))
        self.turn = {k: c for c, k in enumerate(ranks)}
        self.plan = []
        for s in self.ids:
            route = self.streams[s][0]
            for offs in route.all:
                if offs[0] and offs[1:] in route.lines:
                    self.plan.append((self.ready(route, offs), 1, -offs[0], s, offs, self.outer))
                    self.plan.append((self.passed(route, offs), 2, -offs[0], s, offs, self.middle))
                else:
                    when = self.done(route, offs)
                    rank = 3 if not any(offs) else 1 if self.near(route, offs) or not offs[0] and offs[1:] in route.lines else 0
                    self.plan.append((when, rank, -offs[0], s, offs, self.plain))
        self.plan.sort(key=lambda e: e[:5])

    def near(self, route, offs):
        return [o for o in route.across(offs) if o[0] == offs[0]]

    def ready(self, route, offs):
        return max([self.turn[offs[0]]] + [self.done(route, o) + 1 for o in self.near(route, offs)])

    def passed(self, route, offs):
        line = offs[1:]
        return self.ready(route, offs) + 1 if offs[0] > 1 else max(self.ready(route, offs), self.ready(route, (3, *line)) + 2)

    def done(self, route, offs):
        when = self.ready(route, offs)
        if not offs[0] and offs[1:] in route.lines:
            when = max(when, self.passed(route, (1, *offs[1:])) + 1, self.passed(route, (2, *offs[1:])) + 1)
        return when

    def arrival(self, s, slot):
        route, share, got, _, _ = self.streams[s]
        return remote(share((0, 0, 0)), got(slot), self.send.at[s, slot], self.recv.at[s, slot], {"dp": route.block((1, 0, 0))})

    def copy(self, s, offs):
        route, share, got, _, _ = self.streams[s]
        f = route.flat(offs)
        if route.last_axis(offs):
            hop = [0, 0, 0]
            hop[route.last_axis(offs)] = 1
            return remote(share(offs), got(f), self.send.at[s, f], self.recv.at[s, f], {"dp": route.block(hop)})
        near, facing = route.block((1, 0, 0)), route.block((2, 0, 0))
        if offs[0] == 1:
            return remote(share(offs), got(f), self.send.at[s, f], self.recv.at[s, f], {"dp": near})
        slot = f + (route.extra(offs[1:], offs[0] - 2) - f) * route.inner.astype(jnp.int32)
        return remote(share(offs), got(slot), self.send.at[s, f], self.recv.at[s, slot], {"dp": jnp.where(route.inner, facing, near)})

    def settle(self, s, offs, slots, out=None):
        route, share, got, _, rows = self.streams[s]
        if slots:
            for f in slots:
                self.arrival(s, f).wait_recv()
            own = share(offs)
            add_rows([own] + [got(f) for f in slots], own if out is None else out, rows)

    def outer(self, s, offs):
        route = self.streams[s][0]
        self.settle(s, offs, [route.flat(o) for o in self.near(route, offs)])
        pl.when(jnp.logical_not(route.inner))(self.copy(s, offs).start)

    def middle(self, s, offs):
        route = self.streams[s][0]

        @pl.when(route.inner)
        def _():
            self.settle(s, offs, [route.flat(offs) if offs[0] > 1 else route.extra(offs[1:], 1)])
            self.copy(s, offs).start()

    def plain(self, s, offs):
        route, share, got, out, rows = self.streams[s]
        slots = [route.flat(o) for o in self.near(route, offs)]
        if not offs[0] and offs[1:] in route.lines:
            slots.append(route.flat((1, *offs[1:])))
            facing = route.extra(offs[1:], 0)

            @pl.when(route.inner)
            def _():
                self.settle(s, offs, [facing])

        self.settle(s, offs, slots, None if any(offs) else out)
        if any(offs):
            self.copy(s, offs).start()

    def step(self, t):
        for when, _, _, s, offs, action in self.plan:
            if when == t:
                action(s, offs)

    def steps(self):
        return 1 + max(e[0] for e in self.plan)

    def end(self):
        for s in self.ids:
            for offs in self.streams[s][0].others:
                self.copy(s, offs).wait_send()


def meet(axes, everyone, pair):
    route = Route(axes, ORDERS[0])
    barrier = pltpu.get_barrier_semaphore()
    if everyone:
        for offs in route.others:
            pl.semaphore_signal(barrier, inc=1, device_id={"dp": route.block(offs)}, device_id_type=MESH)
    else:
        for offs in ((0, 0, 1), (0, 1, 0), (1, 0, 0)):
            pl.semaphore_signal(barrier, inc=1, device_id={"dp": route.block(offs)}, device_id_type=MESH)

        @pl.when(route.inner)
        def _():
            pl.semaphore_signal(barrier, inc=1, device_id={"dp": route.block((2, 0, 0))}, device_id_type=MESH)

    if pair:
        pl.semaphore_signal(barrier, inc=1, device_id={"section": 1 - lax.axis_index("section")}, device_id_type=MESH)
    pl.semaphore_wait(barrier, (len(route.others) if everyone else 3 + route.inner.astype(jnp.int32)) + (1 if pair else 0))


def contract(left, right, dims):
    return lax.dot_general(left, right, ((dims[:1], dims[1:]), ((), ())), preferred_element_type=jnp.float32)


def weight_parts(rows):
    third = rows // 3
    sizes = (third, third, third // 2, third // 2)
    return tuple((order, sum(sizes[:n]), sizes[n]) for n, order in enumerate(ORDERS))


def weight_columns(half):
    sec = lax.axis_index("section")
    return pl.ds(pl.multiple_of(sec * half, 128), half), pl.ds(pl.multiple_of((1 - sec) * half, 128), half)


def packed_columns(widths):
    return [pl.ds(sum(widths[:n]), w) for n, w in enumerate(widths)]


class WeightSpread:
    def __init__(self, axes, own, full, outs, sems):
        send, recv, self.psend, self.precv, self.local = sems
        self.own, self.full, self.outs = own, full, outs
        self.route = Route(axes, ORDERS[0])
        streams = []
        for order, at, size in weight_parts(own.shape[0]):
            rows = pl.ds(at, size)
            streams.append((Route(axes, order), own.at[rows], lambda b, r=rows: full.at[b, r]))
        self.spread = Spread(streams, send, recv)
        self.widths = [out.shape[2] // 2 for out in outs]

    def deliveries(self, offs):
        block, f = self.route.block(offs), self.route.flat(offs)
        for a, cols in enumerate(packed_columns(self.widths)):
            src = self.full.at[block, :, cols] if any(offs) else self.own.at[:, cols]
            dst = self.outs[a].at[block, :, weight_columns(self.widths[a])[0]]
            yield pltpu.make_async_copy(src, dst, self.local.at[a, f])
            yield remote(src, dst, self.psend.at[a, f], self.precv.at[a, f], {"section": 1 - lax.axis_index("section")})

    def step(self, t):
        self.spread.step(t)
        for offs in self.route.all:
            if sum(offs) == t:
                for copy in self.deliveries(offs):
                    copy.start()

    def end(self):
        self.spread.end()
        for offs in self.route.all:
            for copy in self.deliveries(offs):
                copy.wait()


def weight_shapes(pack, widths, count):
    return [jax.ShapeDtypeStruct((count, pack.shape[0], 2 * w), pack.dtype) for w in widths]


def weight_scratch(pack, widths, count):
    dma = pltpu.SemaphoreType.DMA
    return [pltpu.VMEM((count, *pack.shape), pack.dtype)] + [dma((len(ORDERS), count + 4))] * 2 + [dma((len(widths), count))] * 3


def weight_spread_kernel(axes, arrays, *refs):
    own, outs, full, sems = refs[0], refs[1 : 1 + arrays], refs[1 + arrays], refs[2 + arrays :]
    meet(axes, False, True)
    spread = WeightSpread(axes, own, full, outs, sems)
    for t in range(SPREAD_STEPS):
        spread.step(t)
    spread.end()


def weight_spread(pack, widths, count, cid):
    return pl.pallas_call(
        functools.partial(weight_spread_kernel, torus_axes(count), len(widths)),
        out_shape=weight_shapes(pack, widths, count),
        in_specs=[pl.BlockSpec(memory_space=pltpu.VMEM)],
        out_specs=[pl.BlockSpec(memory_space=pl.ANY)] * len(widths),
        scratch_shapes=weight_scratch(pack, widths, count),
        compiler_params=pltpu.CompilerParams(collective_id=cid, has_side_effects=True),
        name="weight_spread",
    )(pack)


class WeightFold:
    def __init__(self, axes, data, total, got, made, tail, out, sems, ranks):
        send, recv, self.psend, self.precv, self.local = sems
        self.lefts, self.rights, self.small = data[:2], data[2:4], data[4]
        self.total, self.made, self.tail, self.rows, self.ranks = total, made, tail, out.shape[0], ranks
        self.widths = fold_widths(data)
        self.columns = packed_columns(self.widths)
        streams = []
        for order, at, size in weight_parts(self.rows):
            rows, route = pl.ds(at, size), Route(axes, order)
            streams.append((route, lambda o, r=rows, w=route: total.at[w.flat(o), r], lambda f, r=rows: got.at[f, r], out.at[rows], size))
        self.route = Route(axes, ORDERS[0])
        self.fold = Fold(streams, send, recv, ranks)

    def place(self, c, q):
        k, route = self.ranks[c], self.route
        j = lax.rem(q + route.digit(1), 2)
        i = lax.rem(lax.div(q, 2) + route.digit(2), 2)
        return route.plane(k) * 4 + q, (k * 2 + j) * 2 + i

    def product(self, a, block, other):
        rows = pl.ds(pl.multiple_of(block * self.rows, 32), self.rows)
        return dot(self.lefts[a][rows, :], self.rights[a][:, weight_columns(self.widths[a])[other]])

    def give(self, c, q):
        block, f = self.place(c, q)
        partner = {"section": 1 - lax.axis_index("section")}
        main = pl.ds(0, sum(self.widths[:2]))
        return (remote(self.made.at[q], self.total.at[f, :, main], self.psend.at[0, f], self.precv.at[0, f], partner),
                remote(self.small.at[block, :, weight_columns(self.widths[2])[1]], self.total.at[f, :, self.columns[2]],
                       self.psend.at[1, f], self.precv.at[1, f], partner))

    def load(self, c, q):
        block, f = self.place(c, q)
        return pltpu.make_async_copy(self.small.at[block, :, weight_columns(self.widths[2])[0]], self.tail.at[q], self.local.at[f])

    def produce(self, c):
        def one(q, _):
            block, _ = self.place(c, q)
            for a in range(2):
                self.made[q, :, self.columns[a]] = self.product(a, block, 1).astype(jnp.bfloat16)
            for copy in self.give(c, q):
                copy.start()
            self.load(c, q).start()
            return 0

        lax.fori_loop(0, 4, one, 0)

    def begin(self):
        self.produce(0)

    def step(self, t):
        if t < len(self.ranks):
            def own(q, _):
                block, f = self.place(t, q)
                for copy in self.give(t, q):
                    copy.wait_recv()
                for a in range(2):
                    cols = self.columns[a]
                    self.total[f, :, cols] = (self.total[f, :, cols].astype(jnp.float32) + self.product(a, block, 0)).astype(jnp.bfloat16)
                cols = self.columns[2]
                self.total[f, :, cols] = (self.total[f, :, cols].astype(jnp.float32) + self.tail[q].astype(jnp.float32)).astype(jnp.bfloat16)
                return 0

            def settled(q, _):
                for copy in self.give(t, q):
                    copy.wait_send()
                self.load(t, q).wait()
                return 0

            lax.fori_loop(0, 4, settled, 0)
            lax.fori_loop(0, 4, own, 0)
            if t + 1 < len(self.ranks):
                self.produce(t + 1)
        self.fold.step(t)

    def steps(self):
        return self.fold.steps()

    def end(self):
        self.fold.end()


def fold_widths(data):
    return [a.shape[-1] // 2 for a in data[2:]]


def fold_shape(data):
    return jax.ShapeDtypeStruct((data[4].shape[1], sum(fold_widths(data))), jnp.float32)


def fold_specs():
    return [pl.BlockSpec(memory_space=pltpu.VMEM)] * 4 + [pl.BlockSpec(memory_space=pl.ANY)]


def fold_scratch(data):
    (rows, cols), count, dma = fold_shape(data).shape, data[4].shape[0], pltpu.SemaphoreType.DMA
    small = fold_widths(data)[2]
    blocks = [pltpu.VMEM(shape, jnp.bfloat16) for shape in ((count, rows, cols), (count + 4, rows, cols), (4, rows, cols - small), (4, rows, small))]
    return blocks + [dma((len(ORDERS), count + 4))] * 2 + [dma((2, count))] * 2 + [dma((count,))]


def closing_kernel(axes, *refs):
    refs = list(refs)
    take = lambda n: [refs.pop(0) for _ in range(n)]
    data = take(5)
    count = 3
    other = take(1)[0]
    first_up, first_down, last_up, last_down, grad_in, last_in = take(6)
    outs = take(count)
    up_out, down_out, edge_out = take(3)
    blocks, sems = take(4), take(5)
    result, given, taken = take(3)
    own_up, own_down, got_up, got_down, edge_give, edge_got, x_send, x_recv, x_local, h_send, h_recv = take(11)
    sec = lax.axis_index("section")
    partner = {"section": 1 - sec}
    chunks = [axes[0][1] - 1 - c for c in range(axes[0][1])]
    meet(axes, False, True)
    fold = WeightFold(axes, data, *blocks, result, sems, chunks)
    fold.begin()
    leading = sec == 0

    def cross(src, dst, n):
        return remote(src, dst, x_send.at[n], x_recv.at[n], partner)

    edge_give[...] = jnp.where(leading, last_in[...], grad_in[...])
    edge = cross(edge_give, edge_got, 2)
    edge.start()
    edge_out[sec] = jnp.where(leading, grad_in[...], last_in[...])

    @pl.when(leading)
    def _():
        cross(last_up, got_up, 0).start()
        cross(last_down, got_down, 1).start()
        pltpu.make_async_copy(first_up, own_up, x_local.at[0]).start()
        pltpu.make_async_copy(first_down, own_down, x_local.at[1]).start()

    @pl.when(jnp.logical_not(leading))
    def _():
        cross(first_up, got_up, 0).start()
        cross(first_down, got_down, 1).start()
        pltpu.make_async_copy(last_up, own_up, x_local.at[0]).start()
        pltpu.make_async_copy(last_down, own_down, x_local.at[1]).start()

    steps = fold.steps()
    for t in range(steps - 1):
        fold.step(t)
        for n, (own, got, out, src) in enumerate(((own_up, got_up, up_out, first_up), (own_down, got_down, down_out, first_down))):
            if t == 3:
                pltpu.make_async_copy(src, own, x_local.at[n]).wait()
                cross(src, got, n).wait_recv()
            if t in (3, 4):
                size = own.shape[0] // 2
                rows = pl.ds((t - 3) * size, size)
                add_rows([own.at[rows], got.at[rows]], own.at[rows], size, 8)
            if t == 4:
                pltpu.make_async_copy(own, out, x_local.at[n]).start()
        if t == 2:
            edge.wait_recv()
            edge_out[1 - sec] = edge_got[...]
    assert steps > 5
    fold.step(steps - 1)
    given[...] = jnp.where(leading, other[...], result[...])
    hand = remote(given, taken, h_send.at[0], h_recv.at[0], partner)
    hand.start()
    packed = packed_columns(fold.widths)
    for a in range(count):
        outs[a][:, weight_columns(fold.widths[a])[0]] = jnp.where(leading, result[:, packed[a]], other[:, packed[a]])
    fold.end()
    edge.wait_send()
    for n, (own, got, out, src) in enumerate(((own_up, got_up, up_out, first_up), (own_down, got_down, down_out, first_down))):
        cross(src, got, n).wait_send()
        pltpu.make_async_copy(own, out, x_local.at[n]).wait()
    hand.wait()
    for a in range(count):
        outs[a][:, weight_columns(fold.widths[a])[1]] = taken[:, packed[a]]


def closing(data, other, first, last, grad, final, count, cid):
    axes, n = torus_axes(count), 3
    vmem, anywhere = pl.BlockSpec(memory_space=pltpu.VMEM), pl.BlockSpec(memory_space=pl.ANY)
    dma, f32 = pltpu.SemaphoreType.DMA, jnp.float32
    rows = fold_shape(data).shape[0]
    half = pltpu.VMEM(fold_shape(data).shape, f32)
    experts = [pltpu.VMEM(w.shape, f32) for w in first]
    block = pltpu.VMEM(grad.shape, grad.dtype)
    return pl.pallas_call(
        functools.partial(closing_kernel, axes),
        out_shape=[jax.ShapeDtypeStruct((rows, 2 * w), f32) for w in fold_widths(data)] + [jax.ShapeDtypeStruct(w.shape, f32) for w in first]
        + [jax.ShapeDtypeStruct((2, *grad.shape), grad.dtype)],
        in_specs=fold_specs() + [vmem] + [anywhere] * 4 + [vmem] * 2,
        out_specs=[vmem] * n + [anywhere] * 2 + [vmem],
        scratch_shapes=fold_scratch(data) + [half] * 3 + experts * 2 + [block, block, dma((3,)), dma((3,)), dma((2,)), dma((1,)), dma((1,))],
        compiler_params=pltpu.CompilerParams(collective_id=cid, has_side_effects=True, vmem_limit_bytes=VMEM_BYTES),
        cost_estimate=pl.CostEstimate(flops=0, bytes_accessed=100_000_000, transcendentals=0),
        name="closing",
    )(*data, other, *first, *last, grad, final)


def mixture_kernel(mode, axes, count, layer, extra, folded, *refs):
    fore, back = "f" in mode, "b" in mode
    refs = list(refs)
    take = lambda n: [refs.pop(0) for _ in range(n)]
    mask_ref, router_ref, up_own, up_other, down_own, down_other, x_in = take(7)
    g_in = take(1)[0] if back else None
    next_in = take(1)[0] if extra else None
    data = take(folded)
    mixed_out = take(1)[0] if fore else None
    saved_out = take(1)[0] if mode == "f" else None
    if back:
        grad_out, chance_out, up_grad_out, down_grad_out = take(4)
    next_out = take(extra)
    raw_out = take(1)[0] if folded else None
    up, down, xg, gates_at, weight_at, local = take(6)
    ag_send, ag_recv, rs_send, rs_recv = take(4)
    gathers, folds = [], []
    if fore:
        share_f, got_f, act_at = take(3)
        gathers.append((x_in, xg))
        folds.append((share_f, got_f, mixed_out))
    if back:
        (gg, share_b, got_b, plain_at, ggu_at, actw_at, high_at, low_at, chance_row, chance_got, c_send, c_recv, out_sem) = take(13)
        gathers.append((g_in, gg))
        folds.append((share_b, got_b, grad_out))
    me, sec = lax.axis_index("dp"), lax.axis_index("section")
    n0, n1, n2 = [size for _, size in axes]
    plane = n1 * n2
    assert n0 == 4
    meet(axes, back, bool(extra or folded))
    spread_streams, fold_streams = [], []
    for own, full in gathers:
        for order, at, size in TOKEN_PARTS:
            rows = pl.ds(at, size)
            spread_streams.append((Route(axes, order), own.at[rows], lambda b, f=full, r=rows: f.at[b, r]))
    for share, got, out in folds:
        for order, at, size in TOKEN_PARTS:
            rows, route = pl.ds(at, size), Route(axes, order)
            fold_streams.append((route, lambda o, a=share, r=rows, w=route: a.at[w.block(o), r], lambda f, g=got, r=rows: g.at[f, r],
                                 out.at[rows], size))
    spread = Spread(spread_streams, ag_send, ag_recv)
    ranks = [3, 2, 1, 0]
    fold = Fold(fold_streams, rs_send, rs_recv, ranks)
    spread.step(0)
    if extra:
        other = WeightSpread(axes, next_in, take(1)[0], next_out, take(5))
    if folded:
        aside = WeightFold(axes, data, *take(4), raw_out, take(5), ranks)
        aside.begin()

    @pl.when(sec == layer)
    def _():
        pltpu.make_async_copy(up_own, up, local.at[0]).start()
        pltpu.make_async_copy(down_own, down, local.at[1]).start()

    @pl.when(sec != layer)
    def _():
        pltpu.make_async_copy(up_other, up, local.at[0]).start()
        pltpu.make_async_copy(down_other, down, local.at[1]).start()

    if not fore:
        bring = pltpu.make_async_copy(x_in, xg, local.at[2])
        bring.start()
    else:
        xg[me] = x_in[...]
    if back:
        gg[me] = g_in[...]
    pltpu.make_async_copy(up_own, up, local.at[0]).wait()
    pltpu.make_async_copy(down_own, down, local.at[1]).wait()
    if not fore:
        bring.wait()

    def span(n, size=SPAN):
        return pl.ds(pl.multiple_of(n * size, size), size)

    def tile(b0):
        blocks = pl.ds(b0, TILE // ROWS)
        here = pl.ds(pl.multiple_of(b0 * ROWS, TILE), TILE)
        x = xg[blocks].reshape(TILE, MODEL_WIDTH)
        lane = lax.broadcasted_iota(jnp.int32, (TILE, router_ref.shape[1]), 1)
        chance = jnp.where(lane < count, jnp.exp(dot(x, router_ref[...])), 0.0)
        total = jnp.sum(chance, axis=1, keepdims=True)
        ones = jnp.ones((8, 128), jnp.bfloat16)
        named = jnp.concatenate([contract(mask_ref[b0 + b], ones, (0, 0)) for b in range(TILE // ROWS)], axis=0)
        weight = jnp.sum(jnp.where(lane == me, chance, 0.0), axis=1, keepdims=True) / total
        weight_at[...] = jnp.where(lane[:, :128] == 0, weight * named, named)

        def gate_step(n, _):
            gates_at[:, span(n)] = dot(xg[blocks].reshape(TILE, MODEL_WIDTH), up[:, span(n)])
            return 0

        lax.fori_loop(0, 2 * FFE // SPAN, gate_step, 0)
        if back:
            def plain_step(n, _):
                plain_at[:, span(n)] = contract(gg[blocks].reshape(TILE, MODEL_WIDTH), down[span(n), :], (1, 1))
                return 0

            lax.fori_loop(0, FFE // SPAN, plain_step, 0)

        def strip(r, _):
            at = pl.ds(pl.multiple_of(r * STRIP, STRIP), STRIP)
            gate, raise_ = gates_at[at, :FFE], gates_at[at, FFE:]
            sigmoid = 1.0 / (1.0 + jnp.exp(-gate))
            silu = gate * sigmoid
            activated = silu * raise_
            if fore:
                act_at[at] = activated.astype(jnp.bfloat16)
            if back:
                row = pl.ds(pl.multiple_of(b0 * ROWS + r * STRIP, STRIP), STRIP)
                w, m = weight_at[at, 0:1], weight_at[at, 1:2]
                plain = plain_at[at]
                grad_act = plain * w
                ggu_at[row, :FFE] = (grad_act * raise_ * sigmoid * (1.0 + gate * (1.0 - sigmoid))).astype(jnp.bfloat16)
                ggu_at[row, FFE:] = (grad_act * silu).astype(jnp.bfloat16)
                actw_at[row] = (activated * w).astype(jnp.bfloat16)
                product = activated * plain * m
                high = product.astype(jnp.bfloat16)
                high_at[at] = high
                low_at[at] = (product - high.astype(jnp.float32)).astype(jnp.bfloat16)
            return 0

        lax.fori_loop(0, TILE // STRIP, strip, 0)
        if back:
            def back_step(n, _):
                part = contract(ggu_at[here], up[span(n), :], (1, 1))
                share_b[blocks, :, span(n)] = part.astype(jnp.bfloat16).reshape(TILE // ROWS, ROWS, SPAN)
                return 0

            lax.fori_loop(0, MODEL_WIDTH // SPAN, back_step, 0)
        if fore:
            def share_step(n, _):
                part = dot(act_at[...], down[:, span(n)]) * weight_at[:, 0:1]
                share_f[blocks, :, span(n)] = part.astype(jnp.bfloat16).reshape(TILE // ROWS, ROWS, SPAN)
                return 0

            lax.fori_loop(0, MODEL_WIDTH // SPAN, share_step, 0)
        if back:
            ones = jnp.ones((8, FFE), jnp.bfloat16)
            row = contract(ones, high_at[...], (1, 1)) + contract(ones, low_at[...], (1, 1))
            for b in range(TILE // ROWS):
                chance_row[b0 + b] = row[:, b * ROWS : (b + 1) * ROWS]

    for t in range(1, SPREAD_STEPS):
        spread.step(t)
        if folded:
            aside.step(t - 1)
    if extra:
        other.step(0)
    route = Route(axes, ORDERS[0])
    sources = [route.plane(k) for k in ranks]

    def chunk(c, _):
        source = sources[0]
        for v in range(1, n0):
            source = jnp.where(c == v, sources[v], source)

        def step(q, _):
            tile(source * plane + q * (TILE // ROWS))
            return 0

        lax.fori_loop(0, plane * ROWS // TILE, step, 0)

        for v in range(n0):
            @pl.when(c == v)
            def _(v=v):
                fold.step(v)
                if extra and v:
                    other.step(v)
                if folded:
                    aside.step(SPREAD_STEPS - 1 + v)
        return 0

    lax.fori_loop(0, n0, chunk, 0)
    if back:

        def chance_copy(offs, sender):
            block = route.block(offs)
            return remote(chance_row.at[block], chance_got.at[sender], c_send.at[route.flat(offs)], c_recv.at[sender], {"dp": block})

        for offs in route.others:
            chance_copy(offs, me).start()
        chance_got[me] = chance_row[me]

        up_held = gates_at.at[pl.ds(0, PIECE)]
        down_held = (gates_at.at[pl.ds(PIECE, PIECE)], plain_at.at[pl.ds(0, PIECE)])
        down_parts = ((0, 2 * FFE), (2 * FFE, MODEL_WIDTH - 2 * FFE))

        def put_up(n):
            return pltpu.make_async_copy(up_held, up_grad_out.at[span(n, PIECE)], out_sem.at[0, 0])

        def put_down(n, p):
            cols = pl.ds(*down_parts[p])
            return pltpu.make_async_copy(down_held[p], down_grad_out.at[span(n, PIECE), cols], out_sem.at[1, p])

        def up_gradient(n, _):
            @pl.when(n > 0)
            def _():
                put_up(n).wait()

            left = xg[:, :, span(n, PIECE)].reshape(count * ROWS, PIECE)
            up_held[...] = contract(left, ggu_at[...], (0, 0))
            put_up(n).start()
            return 0

        def down_gradient(n, _):
            @pl.when(n > 0)
            def _():
                put_down(n, 0).wait()
                put_down(n, 1).wait()

            for p, (at, width) in enumerate(down_parts):
                right = gg[:, :, at : at + width].reshape(count * ROWS, width)
                down_held[p][...] = contract(actw_at[:, span(n, PIECE)], right, (0, 0))
                put_down(n, p).start()
            return 0

    if saved_out is not None:
        save = pltpu.make_async_copy(xg, saved_out, local.at[2])
        save.start()
    last = fold.steps()
    assert last == 6
    for t in range(n0, last):
        if back and t == n0:
            lax.fori_loop(0, 4, up_gradient, 0)
        elif back:
            lax.fori_loop(4, MODEL_WIDTH // PIECE, up_gradient, 0)
            lax.fori_loop(0, FFE // PIECE, down_gradient, 0)
        fold.step(t)
        if extra:
            other.step(t)
    if folded:
        assert aside.steps() == 6
        aside.end()
    if extra:
        other.end()
    spread.end()
    fold.end()
    if back:
        put_up(0).wait()
        put_down(0, 0).wait()
        put_down(0, 1).wait()
        for offs in route.others:
            chance_copy(offs, route.block(offs)).wait()
        chance_out[...] = chance_got[...]
    if saved_out is not None:
        save.wait()


def mixture_call(mode, count, layer, cid, mask, router, expert, partner, x, g=None, following=None, widths=(), summed=()):
    axes = torus_axes(count)
    fore, back = "f" in mode, "b" in mode
    vmem, anywhere = pl.BlockSpec(memory_space=pltpu.VMEM), pl.BlockSpec(memory_space=pl.ANY)
    args = [mask, router, expert[0], partner[0], expert[1], partner[1], x]
    in_specs = [vmem, vmem] + [anywhere] * 4 + [vmem if fore else anywhere]
    if back:
        args.append(g)
        in_specs.append(vmem)
    args += ([following] if widths else []) + list(summed)
    in_specs += ([vmem] if widths else []) + (fold_specs() if summed else [])
    whole = (count, ROWS, MODEL_WIDTH)
    out_shape, out_specs = [], []
    block = jax.ShapeDtypeStruct((ROWS, MODEL_WIDTH), jnp.float32)
    if fore:
        out_shape.append(block)
        out_specs.append(vmem)
    if mode == "f":
        out_shape.append(jax.ShapeDtypeStruct(whole, jnp.bfloat16))
        out_specs.append(anywhere)
    if back:
        out_shape += [block, jax.ShapeDtypeStruct((count, 8, ROWS), jnp.float32)]
        out_shape += [jax.ShapeDtypeStruct(w.shape, jnp.float32) for w in expert]
        out_specs += [vmem, vmem, anywhere, anywhere]
    if widths:
        out_shape += weight_shapes(following, widths, count)
        out_specs += [anywhere] * len(widths)
    if summed:
        out_shape.append(fold_shape(summed))
        out_specs.append(vmem)
    dma = pltpu.SemaphoreType.DMA
    scratch = [pltpu.VMEM(expert[0].shape, jnp.bfloat16), pltpu.VMEM(expert[1].shape, jnp.bfloat16), pltpu.VMEM(whole, jnp.bfloat16),
               pltpu.VMEM((TILE, 2 * FFE), jnp.float32), pltpu.VMEM((TILE, 128), jnp.float32), dma((3,))]
    parts = len(TOKEN_PARTS)
    ag, rs = parts * (1 if mode == "b" else fore + back), parts * (fore + back)
    scratch += [dma((ag, count + 4)), dma((ag, count + 4)), dma((rs, count + 4)), dma((rs, count + 4))]
    blocks = pltpu.VMEM(whole, jnp.bfloat16)
    arrivals = pltpu.VMEM((count + 4, *whole[1:]), jnp.bfloat16)
    low = lambda rows, width: pltpu.VMEM((rows, width), jnp.bfloat16)
    if fore:
        scratch += [blocks, arrivals, low(TILE, FFE)]
    if back:
        scratch += [blocks, blocks, arrivals, pltpu.VMEM((TILE, FFE), jnp.float32),
                    low(count * ROWS, 2 * FFE), low(count * ROWS, FFE), low(TILE, FFE), low(TILE, FFE),
                    pltpu.VMEM((count, 8, ROWS), jnp.float32), pltpu.VMEM((count, 8, ROWS), jnp.float32), dma((count,)), dma((count,)),
                    dma((2, 2))]
    if widths:
        scratch += weight_scratch(following, widths, count)
    if summed:
        scratch += fold_scratch(summed)
    rows = count * ROWS
    flops = rows * 6 * MODEL_WIDTH * FFE * (fore + 2 * back + (mode == "b"))
    return pl.pallas_call(
        functools.partial(mixture_kernel, mode, axes, count, layer, len(widths), len(summed)),
        out_shape=out_shape,
        in_specs=in_specs,
        out_specs=out_specs,
        scratch_shapes=scratch,
        compiler_params=pltpu.CompilerParams(collective_id=cid, has_side_effects=True, vmem_limit_bytes=VMEM_BYTES),
        cost_estimate=pl.CostEstimate(flops=flops, bytes_accessed=4 * rows * MODEL_WIDTH, transcendentals=rows * FFE),
        name="mixture_" + mode,
    )(*args)

def swapped(value):
    return lax.ppermute(value, "section", [(0, 1), (1, 0)])


def layout(length_row):
    seq_ends = jnp.cumsum(length_row)
    seq_starts = seq_ends - length_row
    row_ids = jnp.arange(DEVICE_ROWS, dtype=jnp.int32)
    segment = jnp.sum((row_ids[:, None] >= seq_ends[None, :]).astype(jnp.int32), axis=-1)
    member = (segment[:, None] == jnp.arange(NSEQ, dtype=jnp.int32)[None, :]).astype(jnp.int32)
    token_position = row_ids - jnp.sum(member * seq_starts[None, :], axis=-1)
    return segment, token_position


def rotation(token_position):
    half_width = HEAD_SIZE // 2
    frequency = 10000.0 ** (-2.0 * jnp.arange(half_width, dtype=jnp.float32) / HEAD_SIZE)
    angles = token_position.astype(jnp.float32)[:, None] * frequency
    return jnp.cos(angles)[:, None, :], jnp.sin(angles)[:, None, :]


def rotary_embedding(values, cosine, sine):
    half_width = HEAD_SIZE // 2
    former, latter = values[..., :half_width], values[..., half_width:]
    return jnp.concatenate([former * cosine - latter * sine, latter * cosine + former * sine], axis=-1)


def dot(left, right):
    return jnp.dot(left, right, preferred_element_type=jnp.float32)


def dot_rows(left, right):
    return lax.dot_general(left, right, (((0,), (0,)), ((), ())), preferred_element_type=jnp.float32)


def dot_columns(left, right):
    return lax.dot_general(left, right, (((1,), (1,)), ((), ())), preferred_element_type=jnp.float32)


def router_chances(normed_two, router):
    chance = jnp.exp(dot(normed_two, router))
    return chance / jnp.sum(chance, axis=-1, keepdims=True)


def front(hidden, place, weights):
    joint, result_output, router, gain_attention, gain_mixture = weights
    allowed, cosine, sine = place
    rows = hidden.shape[0]
    inverse_one = lax.rsqrt(jnp.mean(hidden * hidden, axis=-1, keepdims=True) + norm_epsilon)
    scaled_one = hidden * inverse_one
    normed = (scaled_one * gain_attention).astype(jnp.bfloat16)
    projected = dot(normed, joint)
    query = rotary_embedding(projected[:, :QUERY_WIDTH].reshape(rows, QUERY_HEADS, HEAD_SIZE), cosine, sine)
    query = query.astype(jnp.bfloat16).reshape(rows, KEY_VALUE_HEADS, GROUP, HEAD_SIZE)
    key = rotary_embedding(projected[:, QUERY_WIDTH : QUERY_WIDTH + KEY_WIDTH].reshape(rows, KEY_VALUE_HEADS, HEAD_SIZE), cosine, sine)
    key = key.astype(jnp.bfloat16)
    value = projected[:, QUERY_WIDTH + KEY_WIDTH :].reshape(rows, KEY_VALUE_HEADS, HEAD_SIZE).astype(jnp.bfloat16)
    scores = jnp.einsum("qhgd,khd->hgqk", query, key, preferred_element_type=jnp.float32) * SCORE_SCALE
    exponent = jnp.where(allowed, jnp.exp(scores), 0.0)
    attention = exponent / jnp.sum(exponent, axis=-1, keepdims=True)
    context = jnp.einsum("hgqk,khd->qhgd", attention.astype(jnp.bfloat16), value, preferred_element_type=jnp.float32)
    context = context.reshape(rows, QUERY_WIDTH).astype(jnp.bfloat16)
    middle = hidden + dot(context, result_output)
    inverse_two = lax.rsqrt(jnp.mean(middle * middle, axis=-1, keepdims=True) + norm_epsilon)
    scaled_two = middle * inverse_two
    normed_two = (scaled_two * gain_mixture).astype(jnp.bfloat16)
    kept = (inverse_one, scaled_one, normed, query, key, value, attention, context, inverse_two, scaled_two, normed_two)
    return middle, normed_two, kept


def gates(everyone, up_weight):
    both = dot(everyone, up_weight)
    return both[:, :FFE], both[:, FFE:]


def expert_forward(everyone, mask, router, expert, count, me):
    up_weight, down_weight = expert
    chance = router_chances(everyone, router)
    own = jnp.arange(count, dtype=jnp.int32) == me
    weight = jnp.sum(jnp.where(own[None, :] & mask, chance, 0.0), axis=-1)
    gate, up = gates(everyone, up_weight)
    activated = (jax.nn.silu(gate) * up).astype(jnp.bfloat16)
    share = (dot(activated, down_weight) * weight[:, None]).astype(jnp.bfloat16)
    return share, weight, (gate, up)


def expert_backward(grads, everyone, weight, mask, held, expert):
    up_weight, down_weight = expert
    gate, up = held if held is not None else gates(everyone, up_weight)
    sigmoid = jax.nn.sigmoid(gate)
    silu = gate * sigmoid
    activated = silu * up
    grad_plain = dot_columns(grads, down_weight)
    grad_weight = jnp.where(mask[:, 0], jnp.sum(activated * grad_plain, axis=-1), 0.0)
    grad_act = grad_plain * weight[:, None]
    grad_gate = grad_act * up * sigmoid * (1.0 + gate * (1.0 - sigmoid))
    grad_gate_up = jnp.concatenate([grad_gate, grad_act * silu], axis=-1).astype(jnp.bfloat16)
    grad_down = dot_rows((activated * weight[:, None]).astype(jnp.bfloat16), grads)
    grad_up_weight = dot_rows(everyone, grad_gate_up)
    share = dot_columns(grad_gate_up, up_weight).astype(jnp.bfloat16)
    return share, grad_weight, grad_up_weight, grad_down


def pieces(value):
    return value.reshape(-1, CHUNK_ROWS, *value.shape[1:])


def mixture_forward(normed_two, router, mask, expert, count, me):
    (spread,) = gather_all([normed_two], count, 0)
    everyone = spread.reshape(-1, MODEL_WIDTH)
    if everyone.shape[0] <= CHUNK_ROWS:
        share, weight, held = expert_forward(everyone, mask, router, expert, count, me)
    else:
        share, weight = lax.map(
            lambda part: expert_forward(part[0], part[1], router, expert, count, me)[:2], (pieces(everyone), pieces(mask)))
        held = None
    (mixed,) = reduce_all([share.reshape(spread.shape)], count, 1)
    return mixed, (everyone, weight.reshape(-1), held)


def mixture_backward(grad_out, mask, kept, expert, count):
    everyone, weight, held = kept
    (spread,) = gather_all([grad_out], count, 0)
    grads = spread.reshape(-1, MODEL_WIDTH)
    if grads.shape[0] <= CHUNK_ROWS:
        share, grad_weight, grad_up, grad_down = expert_backward(grads, everyone, weight, mask, held, expert)
    else:
        def step(sums, part):
            share, grad_weight, grad_up, grad_down = expert_backward(*part, None, expert)
            return (sums[0] + grad_up, sums[1] + grad_down), (share, grad_weight)

        zero = tuple(jnp.zeros(w.shape, jnp.float32) for w in expert)
        (grad_up, grad_down), (share, grad_weight) = lax.scan(
            step, zero, (pieces(grads), pieces(everyone), pieces(weight), pieces(mask)))
    grad_chance = lax.all_to_all(grad_weight.reshape(count, DEVICE_ROWS), "dp", split_axis=0, concat_axis=0, tiled=True)
    (mixed,) = reduce_all([share.reshape(spread.shape)], count, 1)
    return mixed, grad_chance.T, grad_up, grad_down


def front_backward(grad_out, grad_mixed, grad_chance, kept, place, weights, fused):
    joint, result_output, router, gain_attention, gain_mixture = weights
    allowed, cosine, sine = place
    inverse_one, scaled_one, normed, query, key, value, attention, context, inverse_two, scaled_two, normed_two = kept
    rows = normed.shape[0]
    chance = router_chances(normed_two, router)
    grad_logit = (chance * (grad_chance - jnp.sum(grad_chance * chance, axis=-1, keepdims=True))).astype(jnp.bfloat16)
    grad_router = dot_rows(normed_two, grad_logit)
    grad_normed_two = grad_mixed + dot_columns(grad_logit, router)
    grad_gain_two = jnp.sum(grad_normed_two * scaled_two, axis=0)
    scaled_grad_two = grad_normed_two * gain_mixture
    grad_middle = grad_out + inverse_two * (scaled_grad_two - scaled_two * jnp.mean(scaled_grad_two * scaled_two, axis=-1, keepdims=True))
    branch = grad_middle.astype(jnp.bfloat16)
    grad_context = dot_columns(branch, result_output).astype(jnp.bfloat16).reshape(rows, KEY_VALUE_HEADS, GROUP, HEAD_SIZE)
    grad_attention = jnp.einsum("qhgd,khd->hgqk", grad_context, value, preferred_element_type=jnp.float32)
    grad_value = jnp.einsum("hgqk,qhgd->khd", attention.astype(jnp.bfloat16), grad_context, preferred_element_type=jnp.float32)
    grad_scores = (attention * (grad_attention - jnp.sum(grad_attention * attention, axis=-1, keepdims=True))).astype(jnp.bfloat16)
    grad_query = jnp.einsum("hgqk,khd->qhgd", grad_scores, key, preferred_element_type=jnp.float32).reshape(rows, QUERY_HEADS, HEAD_SIZE)
    grad_key = jnp.einsum("hgqk,qhgd->khd", grad_scores, query, preferred_element_type=jnp.float32)
    grad_query = rotary_embedding(grad_query * SCORE_SCALE, cosine, -sine)
    grad_key = rotary_embedding(grad_key * SCORE_SCALE, cosine, -sine)
    grad_projected = jnp.concatenate(
        [grad_query.reshape(rows, -1), grad_key.reshape(rows, -1), grad_value.reshape(rows, -1)], axis=-1).astype(jnp.bfloat16)
    pairs = (normed, context, grad_projected, branch)
    products = (pairs[0].T, pairs[1].T, *pairs[2:]) if fused else (dot_rows(normed, grad_projected), dot_rows(context, branch))
    grad_normed = dot_columns(grad_projected, joint)
    grad_gain_one = jnp.sum(grad_normed * scaled_one, axis=0)
    scaled_grad_one = grad_normed * gain_attention
    grad_hidden = grad_middle + inverse_one * (scaled_grad_one - scaled_one * jnp.mean(scaled_grad_one * scaled_one, axis=-1, keepdims=True))
    return grad_hidden, (products, None, grad_router, grad_gain_one, grad_gain_two)


def small_halves(rows, router, gains, codes):
    second = jnp.concatenate([gains, codes], axis=1)
    width = -(-max(router.shape[1], second.shape[1]) // 128) * 128
    pad = lambda v: jnp.pad(v, ((0, 0), (0, width - v.shape[1])))
    return pad(router), pad(second)


def body(tokens, cotangent, lengths, routes, combined_weight, output_weight, router_weight, attention_gain, mixture_gain,
         expert_gate_up, expert_down):
    count = lax.axis_size("dp")
    me, sec = lax.axis_index("dp"), lax.axis_index("section")
    layers = lax.axis_size("section")
    leading = sec == 0
    shard = combined_weight.shape[1]
    micro = lambda a, axis: lax.dynamic_index_in_dim(a, sec, axis, keepdims=False)

    gains = jnp.stack([attention_gain[0], mixture_gain[0]], axis=1)
    codes = routes[0].astype(jnp.bfloat16).reshape(-1)
    code_count = codes.shape[0]
    codes = jnp.pad(codes, (0, -code_count % shard)).reshape(shard, -1)
    fused = count * DEVICE_ROWS <= CHUNK_ROWS
    if fused:
        member = jnp.any(routes[0][:, None] == jnp.arange(count, dtype=jnp.int32)[None, :, None, None], axis=-1)
        member = member.astype(jnp.bfloat16).reshape(-1, DEVICE_ROWS)
        small = small_halves(shard, jnp.concatenate([router_weight[0], gains], axis=1), gains[:, :0], gains[:, :0])
        small = (small[0], jnp.pad(member, ((0, shard - member.shape[0]), (0, 0))))
    else:
        small = small_halves(shard, router_weight[0], gains, codes)
    small_width = small[0].shape[1]
    halves = [
        (combined_weight[0, :, : combined_weight.shape[2] // 2], combined_weight[0, :, combined_weight.shape[2] // 2 :]),
        (output_weight[0, :, : output_weight.shape[2] // 2], output_weight[0, :, output_weight.shape[2] // 2 :]),
        small,
    ]
    widths = [h[0].shape[1] for h in halves]
    mine = jnp.concatenate([jnp.where(leading, a, b) for a, b in halves], axis=1)
    given = swapped(jnp.concatenate([jnp.where(leading, b, a) for a, b in halves], axis=1))
    packs = [jnp.where(leading, mine, given), jnp.where(leading, given, mine)]
    partner_expert = tuple(swapped(w[0, 0]) for w in (expert_gate_up, expert_down))
    own_expert = (expert_gate_up[0, 0], expert_down[0, 0])
    experts, routers = [], []
    for layer in range(0 if fused else layers):
        keep = sec == layer
        experts.append((jnp.where(keep, expert_gate_up[0, 0], partner_expert[0]), jnp.where(keep, expert_down[0, 0], partner_expert[1])))

    def layer_parts(layer):
        at, parts = 0, []
        for w in widths:
            parts.append(packs[layer][:, at : at + w])
            at += w
        return parts

    def layer_weights(arrays):
        joint, output, tail = [a.reshape(MODEL_WIDTH, -1) for a in arrays]
        experts_wide = router_weight.shape[2]
        second = tail[:, small_width:] if not fused else tail[:, experts_wide:]
        weights = (joint, output, tail[:, :experts_wide], second[:, 0].astype(jnp.float32), second[:, 1].astype(jnp.float32))
        routers.append(tail[:, :small_width])
        if fused:
            rows = lax.dynamic_slice(arrays[2], (0, sec * count + me, small_width), (count, 1, DEVICE_ROWS))
            return weights, jnp.pad(rows, ((0, 0), (0, 7), (0, 0)))
        code = second[:, 2 : 2 + codes.shape[1]].reshape(count, -1)[:, :code_count].reshape(count, -1, DEVICE_ROWS, TOPK)
        named = lax.dynamic_index_in_dim(code, sec, 1, keepdims=False).reshape(count * DEVICE_ROWS, TOPK)
        mask = jnp.any(named == me.astype(jnp.bfloat16), axis=-1, keepdims=True)
        return weights, mask

    segment, token_position = layout(micro(lengths[:, 0], 0))
    row_ids = jnp.arange(DEVICE_ROWS, dtype=jnp.int32)
    allowed = (row_ids[:, None] >= row_ids[None, :]) & (segment[:, None] == segment[None, :])
    place = (allowed,) + rotation(token_position)

    weights, masks, stores = [], [], []
    hidden = micro(tokens, 0)
    for layer in range(layers):
        if not fused:
            arrays = gather_all(layer_parts(layer), count, 2, pair=True)
        elif layer == 0:
            arrays = weight_spread(packs[layer], widths, count, 2)
        got, mask = layer_weights(arrays)
        weights.append(got)
        masks.append(mask)
        middle, normed_two, kept = front(hidden.astype(jnp.float32), place, got)
        if not fused:
            mixed, kept_mixture = mixture_forward(normed_two, got[2], mask, experts[layer], count, me)
        else:
            named = mask
            call = lambda mode, cid, *data, **more: mixture_call(
                mode, count, layer, cid, named, routers[layer], own_expert, partner_expert, *data, **more)
            if layer < layers - 1:
                mixed, everyone, *arrays = call("f", 4, normed_two, following=packs[layer + 1], widths=tuple(widths))
                kept_mixture = (named, everyone)
            else:
                mixed, *kept_mixture = call("fb", 5, normed_two, micro(cotangent, 0))
        hidden = (middle + mixed).astype(jnp.bfloat16)
        stores.append((kept, kept_mixture))
    last = hidden
    grad = micro(cotangent, 0)
    shares, expert_grads = [None] * layers, [None] * layers
    for layer in reversed(range(layers)):
        kept, kept_mixture = stores[layer]
        if not fused:
            mixed, grad_chance, grad_up, grad_down = mixture_backward(grad, masks[layer], kept_mixture, experts[layer], count)
        else:
            if layer < layers - 1:
                named, everyone = kept_mixture
                kept_mixture = mixture_call("b", count, layer, 6, named, routers[layer], own_expert, partner_expert, everyone, grad,
                                            summed=packs[layer + 1])
            mixed, rows, grad_up, grad_down, *more = kept_mixture
            if more:
                shares[layer + 1] = more[0]
            grad_chance = rows[:, 0].T
        expert_grads[layer] = (grad_up, grad_down)
        grad_hidden, parts = front_backward(grad.astype(jnp.float32), mixed, grad_chance, kept, place, weights[layer], fused)
        grad = grad_hidden.astype(jnp.bfloat16)
        tail = small_halves(MODEL_WIDTH, parts[2], jnp.stack([parts[3], parts[4]], axis=1), parts[2][:, :0])
        small = jnp.concatenate(tail, axis=1).astype(jnp.bfloat16).reshape(count, shard, -1)
        if fused:
            packs[layer] = [*parts[0], small]
        else:
            packed = [a.astype(jnp.bfloat16).reshape(count, shard, -1) for a in parts[0]] + [small]
            shares[layer] = reduce_all(packed, count, 3, pair=True)
    if fused:
        *outs, grad_up, grad_down, boundary = closing(packs[0], shares[1], expert_grads[0], expert_grads[1], grad, last, count, 3)
        half = outs[2].shape[1] // 2
        return (
            boundary[None],
            outs[0][None],
            outs[1][None],
            outs[2][None, :, : router_weight.shape[2]],
            outs[2][None, :, half],
            outs[2][None, :, half + 1],
            grad_up[None, None],
            grad_down[None, None],
        )
    outs = []
    for a in range(3):
        kept_half = jnp.where(leading, shares[0][a], shares[1][a])
        got_half = swapped(jnp.where(leading, shares[1][a], shares[0][a]))
        outs.append(jnp.concatenate([jnp.where(leading, kept_half, got_half), jnp.where(leading, got_half, kept_half)], axis=1))
    expert_outs = []
    for a in range(2):
        kept_sum = jnp.where(leading, expert_grads[0][a], expert_grads[1][a])
        got_sum = swapped(jnp.where(leading, expert_grads[1][a], expert_grads[0][a]))
        expert_outs.append((kept_sum + got_sum)[None, None])
    partner = swapped(jnp.where(leading, last, grad))
    boundary = jnp.where(leading, jnp.stack([grad, partner]), jnp.stack([partner, last]))[None]
    half = outs[2].shape[1] // 2
    return (
        boundary,
        outs[0][None],
        outs[1][None],
        outs[2][None, :, : router_weight.shape[2]],
        outs[2][None, :, half],
        outs[2][None, :, half + 1],
        expert_outs[0],
        expert_outs[1],
    )


def solution(mesh):
    return jax.shard_map(
        body,
        mesh=mesh,
        in_specs=(
            P(None, "dp", None),
            P(None, "dp", None),
            P(None, "dp", None),
            P("section", None, "dp", None),
            P("section", "dp", None),
            P("section", "dp", None),
            P("section", "dp", None),
            P("section", "dp"),
            P("section", "dp"),
            P("section", "dp", None, None),
            P("section", "dp", None, None),
        ),
        out_specs=(
            P("section", None, "dp", None),
            P("section", "dp", None),
            P("section", "dp", None),
            P("section", "dp", None),
            P("section", "dp"),
            P("section", "dp"),
            P("section", "dp", None, None),
            P("section", "dp", None, None),
        ),
        check_vma=False,
    )
```
